32 devices in a mesh: dp: 8 (over z, x), tensor: 4 (over y, core).
Axes of the slice: x: 2, y: 2, z: 4, core: 2. Of those that a mesh axis runs over, the one named last changes fastest.
Arguments:
- hidden_in: bfloat16 [8, 256, 2048], P('dp'), may hold values from -6 to 6
- upstream_grad: bfloat16 [8, 256, 2048], P('dp'), may hold values from -6 to 6
- seq_lengths: int32 [8], replicated, may hold values from 1 to 256, 1536 in all
- position_order: int32 [8], replicated, may hold values from 0 to 7, each once
- query_weight: bfloat16 [2048, 2048], P(None, 'tensor'), may hold values from -0.125 to 0.125
- key_weight: bfloat16 [2048, 2048], P(None, 'tensor'), may hold values from -0.125 to 0.125
- value_weight: bfloat16 [2048, 2048], P(None, 'tensor'), may hold values from -0.125 to 0.125
- output_weight: bfloat16 [2048, 2048], P('tensor'), may hold values from -0.125 to 0.125
- query_gain: float32 [2048], P('tensor'), may hold values from 0.25 to 1.75
- key_gain: float32 [2048], P('tensor'), may hold values from 0.25 to 1.75
- attn_gain: float32 [2048], replicated, may hold values from 0.25 to 1.75
- gate_weight: bfloat16 [2048, 8192], P(None, 'tensor'), may hold values from -0.125 to 0.125
- up_weight: bfloat16 [2048, 8192], P(None, 'tensor'), may hold values from -0.125 to 0.125
- down_weight: bfloat16 [8192, 2048], P('tensor'), may hold values from -0.0625 to 0.0625
- mlp_gain: float32 [2048], replicated, may hold values from 0.25 to 1.75
Outputs:
- layer_out: bfloat16 [8, 256, 2048], P('dp')
- input_grad: bfloat16 [8, 256, 2048], P('dp')
- query_weight_grad: float32 [2048, 2048], P('dp', 'tensor')
- key_weight_grad: float32 [2048, 2048], P('dp', 'tensor')
- value_weight_grad: float32 [2048, 2048], P('dp', 'tensor')
- output_weight_grad: float32 [2048, 2048], P('tensor', 'dp')
- query_gain_grad: float32 [2048], P('tensor')
- key_gain_grad: float32 [2048], P('tensor')
- attn_gain_grad: float32 [2048], replicated
- gate_weight_grad: float32 [2048, 8192], P('dp', 'tensor')
- up_weight_grad: float32 [2048, 8192], P('dp', 'tensor')
- down_weight_grad: float32 [8192, 2048], P('tensor', 'dp')
- mlp_gain_grad: float32 [2048], replicated
- rms_values: float32 [3], replicated
The draws below stay inside these ranges and needn't reach their ends.
Inputs may be any that keep to these rules, and one draw needn't show every extreme that they name: `seq_lengths`: lengths of the 8 sequences in sequence order; one is exactly 256; they sum to 1536. `position_order`: a permutation: every sequence sits at exactly one data position.
All inputs are finite; a program needn't handle non-finite values.
Results may differ from the reference program's by a relative error of at most 0.019.
Values may be sent and summed in bfloat16 or wider, within the bound.
A program may use at most 192 MiB of HBM per device.

```python
import math
import jax
import jax.numpy as jnp
import numpy as np
from jax import lax

D = 2048
HEADS = 16
HEAD = 128
FF = 8192
SEQ_ROWS = 256
NSEQ = 8


def with_spikes(entries, rng, source, target, blocks, factor):
    owner, partner = [(jnp.arange(entries.shape[dim]) // (entries.shape[dim] // blocks)).reshape([-1 if axis == dim else 1 for axis in range(entries.ndim)]) for dim in (source, target)]
    chosen = jax.random.permutation(rng, blocks)[partner]
    strong = (owner == chosen) | (owner == (partner + blocks // 2) % blocks)
    return jnp.where(strong, factor * entries, entries)


def shard_levels(rng, extent, split, least, largest):
    loudness = 1.0
    for position, shards_of in split:
        steps = jax.random.uniform(jax.random.fold_in(jax.random.fold_in(rng, 6), position), (shards_of,), jnp.float32, least / len(split), largest / len(split))
        loudness = loudness * jnp.repeat(jnp.exp(steps), extent[position] // shards_of).reshape((-1,) + (1,) * (len(extent) - 1 - position))
    return loudness


def length_profile(number_of, total, bound, slope):
    portions = [(1 << 20) // math.isqrt(grade ** slope) + 1 for grade in range(2, number_of + 1)]
    spare, counts = total - bound - (number_of - 1), [1] * (number_of - 1)
    while spare > 0:
        free = [i for i in range(number_of - 1) if counts[i] < bound]
        mass, left = sum([portions[i] for i in free]), spare
        for i in free:
            more = min(bound - counts[i], max(1, left * portions[i] // mass), spare)
            counts[i] = counts[i] + more
            spare = spare - more
    return np.array([bound] + counts)


def uneven(key, count, total, reach, lean):
    if count == 2:
        one = jax.random.randint(key, (), max(1, total - reach), min(reach, total - 1) + 1)
        return jnp.stack([one, total - one])
    sizes = jnp.asarray(length_profile(count, total, reach, lean), jnp.int32)
    pairs = (count - 1) // 2
    giver, sink = sizes[1:1 + 2 * pairs:2], sizes[2:2 + 2 * pairs:2]
    margin = jnp.minimum(giver - 1, reach - sink)
    passed = jax.random.randint(jax.random.fold_in(key, 1), (pairs,), 0, 1 << 20) % (margin + 1)
    sizes = sizes.at[1:1 + 2 * pairs:2].set(giver - passed).at[2:2 + 2 * pairs:2].set(sink + passed)
    return sizes[jax.random.permutation(jax.random.fold_in(key, 2), count)]


def scatter_about(key, extent, scale, reach, split=(), held_as=jnp.bfloat16):
    result = scale * jax.random.normal(key, extent, jnp.float32)
    if split:
        result = result * shard_levels(key, extent, split, -0.22, 0.18)
    return jnp.clip(result, -reach, reach).astype(held_as)


def heavy_noise(own_key, extent, scale, reach, shards, heavy, kind=jnp.bfloat16):
    entries = scale * jax.random.normal(own_key, extent, jnp.float32)
    if shards:
        entries = entries * shard_levels(own_key, extent, shards, -0.22, 0.18)
    return jnp.clip(with_spikes(entries, jax.random.fold_in(own_key, 3), *heavy), -reach, reach).astype(kind)


def setup_inputs(seed: int = 0) -> dict:
    key_of = jax.random.split(jax.random.key(seed), 16)
    return {
        "hidden_in": heavy_noise(key_of[0], (NSEQ, SEQ_ROWS, D), 1.0, 6.0, ((0, 8),), (0, 2, 8, 2.0)),
        "upstream_grad": heavy_noise(key_of[1], (NSEQ, SEQ_ROWS, D), 1.0, 6.0, ((0, 8),), (0, 2, 8, 2.0)),
        "seq_lengths": uneven(key_of[2], NSEQ, NSEQ * SEQ_ROWS * 3 // 4, SEQ_ROWS, 1).astype(jnp.int32),
        "position_order": jax.random.permutation(key_of[3], NSEQ).astype(jnp.int32),
        "query_weight": scatter_about(key_of[4], (D, D), D ** -0.5, 0.125, ((1, 4),)),
        "key_weight": scatter_about(key_of[5], (D, D), D ** -0.5, 0.125, ((1, 4),)),
        "value_weight": scatter_about(key_of[6], (D, D), D ** -0.5, 0.125, ((1, 4),)),
        "output_weight": scatter_about(key_of[7], (D, D), D ** -0.5, 0.125, ((0, 4),)),
        "query_gain": jnp.clip(1.0 + 0.15 * jax.random.normal(key_of[8], (D,), jnp.float32), 0.25, 1.75),
        "key_gain": jnp.clip(1.0 + 0.15 * jax.random.normal(key_of[9], (D,), jnp.float32), 0.25, 1.75),
        "attn_gain": jnp.clip(1.0 + 0.15 * jax.random.normal(key_of[10], (D,), jnp.float32), 0.25, 1.75),
        "gate_weight": scatter_about(key_of[11], (D, FF), D ** -0.5, 0.125, ((1, 4),)),
        "up_weight": scatter_about(key_of[12], (D, FF), D ** -0.5, 0.125, ((1, 4),)),
        "down_weight": scatter_about(key_of[13], (FF, D), FF ** -0.5, 0.0625, ((0, 4),)),
        "mlp_gain": jnp.clip(1.0 + 0.15 * jax.random.normal(key_of[14], (D,), jnp.float32), 0.25, 1.75),
    }


@jax.custom_vjp
def low(v):
    return lax.optimization_barrier(v.astype(jnp.bfloat16)).astype(jnp.float32)

@jax.custom_vjp
def low_back(v):
    return v

def low_keep(v):
    return (low(v), None)

def low_pass(kept, grad):
    return (grad,)

def back_keep(v):
    return (v, None)

def back_low(kept, grad):
    return (low(grad),)
low.defvjp(low_keep, low_pass)
low_back.defvjp(back_keep, back_low)
EPS = 1e-06
HIGH = lax.Precision.HIGHEST

def matmul(left, right):
    return jnp.dot(left, right, precision=HIGH)

def rope_tables(rows, width):
    places = jnp.arange(rows, dtype=jnp.float32)
    freq = jnp.power(jnp.float32(500000.0), -jnp.arange(width // 2, dtype=jnp.float32) * (2.0 / width))
    angle = places[:, None] * freq[None, :]
    return (jnp.cos(angle), jnp.sin(angle))

def rotate(field, cosine, sine):
    half = field.shape[-1] // 2
    first = field[..., :half]
    second = field[..., half:]
    cosine = cosine[:, None, :]
    sine = sine[:, None, :]
    return jnp.concatenate([first * cosine - second * sine, second * cosine + first * sine], axis=-1)

def unit_rows(field):
    return field * lax.rsqrt(lax.optimization_barrier(jnp.mean(field * field, axis=-1, keepdims=True)) + EPS)

def sequence_layer(rows_in, length, weights):
    qweight, kweight, vweight, oweight, qgain, kgain, again, gweight, uweight, dweight, mgain = weights
    rows = rows_in.shape[0]
    q_raw = low_back(matmul(rows_in, qweight))
    k_raw = low_back(matmul(rows_in, kweight))
    values = low(low_back(matmul(rows_in, vweight))).reshape(rows, HEADS, HEAD)
    cosine, sine = rope_tables(rows, HEAD)
    queries = low(rotate((unit_rows(q_raw) * qgain).reshape(rows, HEADS, HEAD), cosine, sine))
    keys = low(rotate((unit_rows(k_raw) * kgain).reshape(rows, HEADS, HEAD), cosine, sine))
    scores = jnp.einsum('qhe,khe->hqk', queries, keys, precision=HIGH) / math.sqrt(HEAD)
    scores = low_back(scores)
    row_ids = jnp.arange(rows, dtype=jnp.int32)
    allowed = (row_ids[None, :] <= row_ids[:, None]) & (row_ids[None, :] < length)
    masked = jnp.where(allowed[None], scores, -1e+30)
    probs = low(jax.nn.softmax(masked, axis=-1))
    mix = jnp.einsum('hqk,khe->qhe', probs, values, precision=HIGH).reshape(rows, HEADS * HEAD)
    mix = low(low_back(mix))
    branch = low_back(matmul(mix, oweight))
    attn_out = again * unit_rows(branch)
    mid = rows_in + attn_out
    mid_low = low(mid)
    gate = low_back(matmul(mid_low, gweight))
    upper = low_back(matmul(mid_low, uweight))
    inner = low(jax.nn.silu(gate) * upper)
    mlp_branch = low_back(matmul(inner, dweight))
    mlp_out = mgain * unit_rows(mlp_branch)
    return (mid + mlp_out, (attn_out, mlp_out))

def reference(hidden_in, upstream_grad, seq_lengths, position_order, query_weight, key_weight, value_weight, output_weight, query_gain, key_gain, attn_gain, gate_weight, up_weight, down_weight, mlp_gain):
    count = seq_lengths.shape[0]
    rows = hidden_in.shape[1]
    index = jnp.arange(count, dtype=jnp.int32)
    pos_len = jnp.take(seq_lengths, position_order)
    inverse = lax.optimization_barrier(jnp.sum(index[None, :] * (position_order[None, :] == index[:, None]).astype(jnp.int32), axis=1)).astype(jnp.int32)
    live = (jnp.arange(rows, dtype=jnp.int32)[None, :] < pos_len[:, None]).astype(jnp.float32)[..., None]
    cot = jnp.take(upstream_grad.astype(jnp.float32), position_order, axis=0) * live
    rows_f = hidden_in.astype(jnp.float32)
    weights = tuple((w.astype(jnp.float32) for w in (query_weight, key_weight, value_weight, output_weight, query_gain, key_gain, attn_gain, gate_weight, up_weight, down_weight, mlp_gain)))
    step = jax.checkpoint(sequence_layer)

    def whole(xs, *ws):
        return lax.map(lambda item: step(item[0], item[1], ws), (xs, pos_len))
    out, pull, aux = jax.vjp(whole, rows_f, *weights, has_aux=True)
    grads = pull(cot)
    attn_out, mlp_out = aux
    layer_out = jnp.take(out * live, inverse, axis=0).astype(jnp.bfloat16)
    input_grad = jnp.take(grads[0] * live, inverse, axis=0).astype(jnp.bfloat16)
    total = jnp.sum(seq_lengths).astype(jnp.float32) * D
    squares = jnp.stack([jnp.sum(rows_f * rows_f * live), jnp.sum(attn_out * attn_out * live), jnp.sum(mlp_out * mlp_out * live)])
    rms_values = jnp.sqrt(squares / total)
    return (layer_out, input_grad, grads[1], grads[2], grads[3], grads[4], grads[5], grads[6], grads[7], grads[8], grads[9], grads[10], grads[11], rms_values)
```

```python
import math

import jax
import jax.numpy as jnp
from jax import lax
from jax.sharding import PartitionSpec as P

D = 2048
HEAD = 128
EPS = 1e-06
F32 = jnp.float32
BF16 = jnp.bfloat16


def matmul(left, right):
    return jnp.dot(left, right, preferred_element_type=F32)


def left_inner(left, right):
    return lax.dot_general(left, right, (((0,), (0,)), ((), ())), preferred_element_type=F32)


def right_inner(left, right):
    return lax.dot_general(left, right, (((1,), (1,)), ((), ())), preferred_element_type=F32)


def rope_tables(rows, width):
    places = jnp.arange(rows, dtype=F32)
    freq = jnp.power(F32(500000.0), -jnp.arange(width // 2, dtype=F32) * (2.0 / width))
    angle = places[:, None] * freq[None, :]
    return (jnp.cos(angle), jnp.sin(angle))


def rotate(field, cosine, sine, sign):
    half = field.shape[-1] // 2
    first = field[..., :half]
    second = field[..., half:]
    cosine = cosine[:, None, :]
    sine = sine[:, None, :] * sign
    return jnp.concatenate(
        [first * cosine - second * sine, second * cosine + first * sine], axis=-1
    )


class Grid:
    def __init__(self, count):
        self.count = count
        self.lanes = 2 ** ((count.bit_length() - 1) // 2)
        self.groups = count // self.lanes
        me = lax.axis_index("dp")
        self.group = me // self.lanes
        self.lane = me % self.lanes

    def shift_groups(self, field, step):
        pairs = [
            (g * self.lanes + a, ((g + step) % self.groups) * self.lanes + a)
            for g in range(self.groups)
            for a in range(self.lanes)
        ]
        return lax.ppermute(field, "dp", pairs)

    def shift_lanes(self, field, step):
        pairs = [
            (g * self.lanes + a, g * self.lanes + (a + step) % self.lanes)
            for g in range(self.groups)
            for a in range(self.lanes)
        ]
        return lax.ppermute(field, "dp", pairs)

    def ring(self, field):
        found = []
        for _ in range(self.groups - 1):
            field = self.shift_groups(field, 1)
            found.append(field)
        return found

    def total(self, field):
        step = 1
        while step < self.count:
            field = field + lax.ppermute(
                field, "dp", [(i, i ^ step) for i in range(self.count)]
            )
            step *= 2
        return field


def sibling(field):
    size = lax.axis_size("tensor")
    return lax.ppermute(field, "tensor", [(i, i ^ 1) for i in range(size)])


def across(field):
    size = lax.axis_size("tensor")
    return lax.ppermute(field, "tensor", [(i, (i + 2) % size) for i in range(size)])


def reduce_rows(partial):
    return lax.psum_scatter(partial, "tensor", scatter_dimension=0, tiled=True)


def gather_rows(shard):
    return lax.all_gather(shard, "tensor", axis=0, tiled=True)


def shared_ring(grid, rows_low):
    core = lax.axis_index("tensor") % 2
    half = rows_low.shape[0] // 2
    mine = lax.dynamic_slice_in_dim(rows_low, core * half, half, axis=0)
    pieces = []
    for piece in grid.ring(mine):
        pieces += [piece, sibling(piece)]
    return jnp.concatenate(pieces, axis=0)


def body(
    hidden_in,
    upstream_grad,
    seq_lengths,
    position_order,
    query_weight,
    key_weight,
    value_weight,
    output_weight,
    query_gain,
    key_gain,
    attn_gain,
    gate_weight,
    up_weight,
    down_weight,
    mlp_gain,
):
    count = lax.axis_size("dp")
    ways = lax.axis_size("tensor")
    myself = lax.axis_index("dp")
    part = lax.axis_index("tensor")
    grid = Grid(count)
    index = jnp.arange(count, dtype=jnp.int32)
    inverse = jnp.sum(
        index[None, :] * (position_order[None, :] == index[:, None]).astype(jnp.int32), axis=1
    )
    rows = hidden_in.shape[1]
    width = hidden_in.shape[2]
    shard = rows // ways
    piece = shard // count
    seq_here = jnp.sum(jnp.where(index == myself, position_order, 0))
    length = jnp.sum(jnp.where(index == seq_here, seq_lengths, 0))
    live = (part * shard + jnp.arange(shard, dtype=jnp.int32) < length)[:, None]

    def exchange(pieces):
        return lax.all_to_all(pieces, "dp", split_axis=0, concat_axis=0, tiled=True)

    def my_rows(field):
        return lax.dynamic_slice_in_dim(field, part * shard, shard, axis=0)

    first = exchange(my_rows(upstream_grad[0]).reshape(count, piece, width))
    second = exchange(jnp.take(first, position_order, axis=0))
    grad_in = jnp.where(live, second.reshape(shard, width).astype(F32), 0.0)

    rows_low = hidden_in[0]
    my_low = my_rows(rows_low)
    rows_f = my_low.astype(F32)
    local = query_weight.shape[1]
    heads_here = local // HEAD
    strip = width // grid.groups
    tile = width // count

    def strip_of(field, group):
        return lax.dynamic_slice_in_dim(field, group * strip, strip, axis=1)

    def strips(field):
        found = [strip_of(field, grid.group)]
        for step in range(1, grid.groups):
            found.append(
                grid.shift_groups(
                    strip_of(field, (grid.group + step) % grid.groups), step
                )
            )
        return jnp.concatenate(found, axis=0)

    def tile_of(field, lane):
        return lax.dynamic_slice_in_dim(field, lane * tile, tile, axis=1)

    def reduced(product, field):
        sent = []
        for step in range(1, grid.lanes):
            other = product(tile_of(field, (grid.lane + step) % grid.lanes)).astype(BF16)
            sent.append(grid.shift_lanes(other, step))
        mine = product(tile_of(field, grid.lane))
        for other in sent:
            mine = mine + other.astype(F32)
        return mine

    hidden_strips = strips(rows_low)

    q_raw = matmul(rows_low, query_weight)
    k_raw = matmul(rows_low, key_weight)
    values = matmul(rows_low, value_weight).astype(BF16).reshape(rows, heads_here, HEAD)
    q_total, k_total = lax.psum(
        (jnp.sum(q_raw * q_raw, axis=-1), jnp.sum(k_raw * k_raw, axis=-1)), "tensor"
    )
    q_scale = lax.rsqrt(q_total / D + EPS)[:, None]
    k_scale = lax.rsqrt(k_total / D + EPS)[:, None]
    q_unit = q_raw * q_scale
    k_unit = k_raw * k_scale
    cosine, sine = rope_tables(rows, HEAD)
    queries = rotate(
        (q_unit * query_gain).reshape(rows, heads_here, HEAD), cosine, sine, 1.0
    ).astype(BF16)
    keys = rotate((k_unit * key_gain).reshape(rows, heads_here, HEAD), cosine, sine, 1.0).astype(
        BF16
    )
    ids = jnp.arange(rows, dtype=jnp.int32)
    allowed = (ids[None, :] <= ids[:, None]) & (ids[None, :] < length)
    scores = jnp.einsum("qhe,khe->hqk", queries, keys, preferred_element_type=F32) / math.sqrt(HEAD)
    masked = jnp.where(allowed[None], scores, -1e30)
    top = jnp.max(masked, axis=-1, keepdims=True)
    expo = jnp.exp(masked - top)
    probs = expo / jnp.sum(expo, axis=-1, keepdims=True)
    probs_low = probs.astype(BF16)
    mix = jnp.einsum("hqk,khe->qhe", probs_low, values, preferred_element_type=F32)
    attn_mix = mix.reshape(rows, local).astype(BF16)
    mix_all = jnp.concatenate([attn_mix] + grid.ring(attn_mix), axis=0)

    branch = reduce_rows(matmul(attn_mix, output_weight))
    a_scale = lax.rsqrt(jnp.mean(branch * branch, axis=-1, keepdims=True) + EPS)
    a_unit = branch * a_scale
    attn_out = attn_gain * a_unit
    mid = rows_f + attn_out
    mid_low = gather_rows(mid.astype(BF16))
    mid_others = shared_ring(grid, mid_low)

    gate = matmul(mid_low, gate_weight)
    upper = matmul(mid_low, up_weight)
    sig = jax.nn.sigmoid(gate)
    inner = (gate * sig * upper).astype(BF16)
    m_branch = reduce_rows(matmul(inner, down_weight))
    m_scale = lax.rsqrt(jnp.mean(m_branch * m_branch, axis=-1, keepdims=True) + EPS)
    m_unit = m_branch * m_scale
    mlp_out = mlp_gain * m_unit
    layer_sum = mid + mlp_out
    mlp_gain_part = jnp.sum(grad_in * m_unit, axis=0)
    g_m = grad_in * mlp_gain
    d_mlp_mine = (
        m_scale * (g_m - m_unit * jnp.mean(g_m * m_unit, axis=-1, keepdims=True))
    ).astype(BF16)
    d_mlp = gather_rows(d_mlp_mine)
    d_mlp_others = shared_ring(grid, d_mlp)

    def inner_back(gate, upper, d_mlp):
        d_inner = right_inner(d_mlp, down_weight)
        sig = jax.nn.sigmoid(gate)
        d_gate = (d_inner * upper * sig * (1.0 + gate * (1.0 - sig))).astype(BF16)
        d_up = (d_inner * gate * sig).astype(BF16)
        return d_gate, d_up

    d_gate, d_up = inner_back(gate, upper, d_mlp)
    d_mid = grad_in + reduce_rows(
        right_inner(d_gate, gate_weight) + right_inner(d_up, up_weight)
    )
    attn_gain_part = jnp.sum(d_mid * a_unit, axis=0)
    g_a = d_mid * attn_gain
    d_branch = gather_rows(
        (a_scale * (g_a - a_unit * jnp.mean(g_a * a_unit, axis=-1, keepdims=True))).astype(BF16)
    )
    d_branch_strips = strips(d_branch)
    d_mix = right_inner(d_branch, output_weight).astype(BF16).reshape(rows, heads_here, HEAD)
    d_probs = jnp.einsum("qhe,khe->hqk", d_mix, values, preferred_element_type=F32)
    centre = jnp.sum(probs * d_probs, axis=-1, keepdims=True)
    d_scores = (probs * (d_probs - centre)).astype(BF16)
    d_queries = jnp.einsum("hqk,khe->qhe", d_scores, keys, preferred_element_type=F32) / math.sqrt(HEAD)
    d_keys = jnp.einsum("hqk,qhe->khe", d_scores, queries, preferred_element_type=F32) / math.sqrt(HEAD)
    d_values = jnp.einsum("hqk,qhe->khe", probs_low, d_mix, preferred_element_type=F32)
    d_q_hat = rotate(d_queries, cosine, sine, -1.0).reshape(rows, local)
    d_k_hat = rotate(d_keys, cosine, sine, -1.0).reshape(rows, local)
    query_gain_part = jnp.sum(d_q_hat * q_unit, axis=0)
    key_gain_part = jnp.sum(d_k_hat * k_unit, axis=0)
    q_scaled = d_q_hat * query_gain
    k_scaled = d_k_hat * key_gain
    q_inner, k_inner = lax.psum(
        (jnp.sum(q_scaled * q_unit, axis=-1), jnp.sum(k_scaled * k_unit, axis=-1)), "tensor"
    )
    d_q_raw = (q_scale * (q_scaled - q_unit * (q_inner / D)[:, None])).astype(BF16)
    d_k_raw = (k_scale * (k_scaled - k_unit * (k_inner / D)[:, None])).astype(BF16)
    d_v = d_values.reshape(rows, local).astype(BF16)
    d_heads = jnp.concatenate([d_q_raw, d_k_raw, d_v], axis=1)
    d_heads_all = jnp.concatenate([d_heads] + grid.ring(d_heads), axis=0)

    input_sum = d_mid + reduce_rows(
        right_inner(d_q_raw, query_weight)
        + right_inner(d_k_raw, key_weight)
        + right_inner(d_v, value_weight)
    )

    gate_o = matmul(mid_others, gate_weight)
    upper_o = matmul(mid_others, up_weight)
    inner_o = (jax.nn.silu(gate_o) * upper_o).astype(BF16)
    d_gate_o, d_up_o = inner_back(gate_o, upper_o, d_mlp_others)

    def strip_all(own, others):
        return jnp.concatenate([strip_of(own, grid.group), strip_of(others, grid.group)], axis=0)

    mid_strips = strip_all(mid_low, mid_others)
    d_mlp_strips = strip_all(d_mlp, d_mlp_others)
    d_gate_all = jnp.concatenate([d_gate, d_gate_o], axis=0)
    d_up_all = jnp.concatenate([d_up, d_up_o], axis=0)
    inner_all = jnp.concatenate([inner, inner_o], axis=0)
    gate_part = reduced(lambda tile: left_inner(tile, d_gate_all), mid_strips)
    up_part = reduced(lambda tile: left_inner(tile, d_up_all), mid_strips)
    down_part = reduced(lambda tile: left_inner(inner_all, tile), d_mlp_strips)
    output_part = reduced(lambda tile: left_inner(mix_all, tile), d_branch_strips)
    heads_part = reduced(lambda tile: left_inner(tile, d_heads_all), hidden_strips)
    query_part = heads_part[:, :local]
    key_part = heads_part[:, local : 2 * local]
    value_part = heads_part[:, 2 * local :]

    squares = jnp.stack(
        [
            jnp.sum(jnp.where(live, rows_f * rows_f, 0.0)),
            jnp.sum(jnp.where(live, attn_out * attn_out, 0.0)),
            jnp.sum(jnp.where(live, mlp_out * mlp_out, 0.0)),
        ]
    )
    shared = jnp.concatenate([attn_gain_part, mlp_gain_part, squares])
    shared = shared + sibling(shared)
    shared = shared + across(shared)
    sums = grid.total(jnp.concatenate([shared, query_gain_part, key_gain_part]))
    attn_gain_grad = sums[:width]
    mlp_gain_grad = sums[width : 2 * width]
    squares = sums[2 * width : 2 * width + 3]
    query_gain_grad = sums[2 * width + 3 : 2 * width + 3 + local]
    key_gain_grad = sums[2 * width + 3 + local :]
    rms_values = jnp.sqrt(squares / (jnp.sum(seq_lengths).astype(F32) * D))

    def give_back(field):
        pieces = exchange(jnp.where(live, field, 0.0).astype(BF16).reshape(count, piece, width))
        pieces = exchange(jnp.take(pieces, inverse, axis=0))
        return gather_rows(pieces.reshape(shard, width))[None]

    return (
        give_back(layer_sum),
        give_back(input_sum),
        query_part,
        key_part,
        value_part,
        output_part,
        query_gain_grad,
        key_gain_grad,
        attn_gain_grad,
        gate_part,
        up_part,
        down_part,
        mlp_gain_grad,
        rms_values,
    )


def solution(mesh):
    placed = (
        P("dp", None, None),
        P("dp", None, None),
        P(),
        P(),
        P(None, "tensor"),
        P(None, "tensor"),
        P(None, "tensor"),
        P("tensor", None),
        P("tensor"),
        P("tensor"),
        P(),
        P(None, "tensor"),
        P(None, "tensor"),
        P("tensor", None),
        P(),
    )
    return jax.shard_map(
        body,
        mesh=mesh,
        in_specs=placed,
        out_specs=(
            P("dp", None, None),
            P("dp", None, None),
            P("dp", "tensor"),
            P("dp", "tensor"),
            P("dp", "tensor"),
            P("tensor", "dp"),
            P("tensor"),
            P("tensor"),
            P(),
            P("dp", "tensor"),
            P("dp", "tensor"),
            P("tensor", "dp"),
            P(),
            P(),
        ),
        check_vma=False,
    )
```

```python
import math

import jax
import jax.numpy as jnp
from jax import lax
from jax.experimental import pallas as pl
from jax.experimental.pallas import tpu as pltpu
from jax.sharding import PartitionSpec as P

D = 2048
HEAD = 128
EPS = 1e-06
F32 = jnp.float32
BF16 = jnp.bfloat16


def matmul(left, right):
    return jnp.dot(left, right, preferred_element_type=F32)


def left_inner(left, right):
    return lax.dot_general(left, right, (((0,), (0,)), ((), ())), preferred_element_type=F32)


def right_inner(left, right):
    return lax.dot_general(left, right, (((1,), (1,)), ((), ())), preferred_element_type=F32)


def rope_tables(rows, width):
    places = jnp.arange(rows, dtype=F32)
    freq = jnp.power(F32(500000.0), -jnp.arange(width // 2, dtype=F32) * (2.0 / width))
    angle = places[:, None] * freq[None, :]
    return (jnp.cos(angle), jnp.sin(angle))


class Grid:
    def __init__(self, count):
        self.count = count
        self.lanes = 2 ** ((count.bit_length() - 1) // 2)
        self.groups = count // self.lanes
        me = lax.axis_index("dp")
        self.group = me // self.lanes
        self.lane = me % self.lanes

    def shift_groups(self, field, step):
        pairs = [
            (g * self.lanes + a, ((g + step) % self.groups) * self.lanes + a)
            for g in range(self.groups)
            for a in range(self.lanes)
        ]
        return lax.ppermute(field, "dp", pairs)

    def shift_lanes(self, field, step):
        pairs = [
            (g * self.lanes + a, g * self.lanes + (a + step) % self.lanes)
            for g in range(self.groups)
            for a in range(self.lanes)
        ]
        return lax.ppermute(field, "dp", pairs)

    def ring(self, field):
        found = []
        for _ in range(self.groups - 1):
            field = self.shift_groups(field, 1)
            found.append(field)
        return found

    def total(self, field):
        step = 1
        while step < self.count:
            field = field + lax.ppermute(
                field, "dp", [(i, i ^ step) for i in range(self.count)]
            )
            step *= 2
        return field


def sibling(field):
    size = lax.axis_size("tensor")
    return lax.ppermute(field, "tensor", [(i, i ^ 1) for i in range(size)])


def across(field):
    size = lax.axis_size("tensor")
    return lax.ppermute(field, "tensor", [(i, (i + 2) % size) for i in range(size)])


def shared_ring(grid, rows_low):
    core = lax.axis_index("tensor") % 2
    half = rows_low.shape[0] // 2
    mine = lax.dynamic_slice_in_dim(rows_low, core * half, half, axis=0)
    pieces = []
    for piece in grid.ring(mine):
        pieces += [piece, sibling(piece)]
    return jnp.concatenate(pieces, axis=0)


SLOTS = 4
TILES = 2
AT = pl.DeviceIdType.MESH
VMEM_CAP = 56 * 2**20


class Team:
    def __init__(self):
        self.row = lax.axis_index("dp")
        self.me = lax.axis_index("tensor")
        self.side = self.me // 2
        self.core = self.me % 2
        self.slot = self.core * 2 + self.side
        self.sibling = self.side * 2 + (1 - self.core)
        self.across = (1 - self.side) * 2 + self.core
        self.far = (1 - self.side) * 2 + (1 - self.core)

    def meet(self, *others):
        barrier = pltpu.get_barrier_semaphore()
        for other in others:
            pl.semaphore_signal(barrier, inc=1, device_id=(self.row, other), device_id_type=AT)
        pl.semaphore_wait(barrier, len(others))

    def copy(self, source, target, send, recv, other):
        return pltpu.make_async_remote_copy(
            src_ref=source,
            dst_ref=target,
            send_sem=send,
            recv_sem=recv,
            device_id=(self.row, other),
            device_id_type=AT,
        )


def at_rows(start, size):
    return pl.ds(pl.multiple_of(start, size), size)


class Reduce:
    def scratch(rows, width):
        shard = rows // SLOTS
        return [
            pltpu.VMEM((rows, width), BF16),
            pltpu.VMEM((3, shard, width), BF16),
            pltpu.VMEM((shard, width), BF16),
            pltpu.VMEM((shard, width), F32),
            pltpu.SemaphoreType.DMA((3, TILES)),
            pltpu.SemaphoreType.DMA((3, TILES)),
        ]

    def __init__(self, team, partial, came, gone, total, send, recv):
        self.team, self.partial, self.came, self.gone, self.total = team, partial, came, gone, total
        self.shard, width = total.shape
        self.tile = width // TILES
        self.send, self.recv = send, recv
        self.copies = {}

    def columns(self, tile):
        return pl.ds(tile * self.tile, self.tile)

    def block(self, core, side):
        return at_rows((core * 2 + side) * self.shard, self.shard)

    def launch(self, kind, tile, source, other):
        copy = self.team.copy(
            source,
            self.came.at[kind, :, self.columns(tile)],
            self.send.at[kind, tile],
            self.recv.at[kind, tile],
            other,
        )
        copy.start()
        self.copies[kind, tile] = copy

    def offer(self, tile):
        team, columns = self.team, self.columns(tile)
        for kind, side in ((0, 1 - team.side), (1, team.side)):
            self.launch(
                kind, tile, self.partial.at[self.block(1 - team.core, side), columns], team.sibling
            )

    def pass_on(self, tile):
        team, columns = self.team, self.columns(tile)
        self.copies[0, tile].wait_recv()
        mine = self.partial[self.block(team.core, 1 - team.side), columns].astype(F32)
        self.gone[:, columns] = (mine + self.came[0, :, columns].astype(F32)).astype(BF16)
        self.launch(2, tile, self.gone.at[:, columns], team.across)

    def finish(self, tile):
        team, columns = self.team, self.columns(tile)
        self.copies[1, tile].wait_recv()
        mine = self.partial[self.block(team.core, team.side), columns].astype(F32)
        mine = mine + self.came[1, :, columns].astype(F32)
        self.copies[2, tile].wait_recv()
        self.total[:, columns] = mine + self.came[2, :, columns].astype(F32)

    def settle(self):
        for copy in self.copies.values():
            copy.wait_send()

    def run(self, make):
        for tile in range(TILES):
            make(tile)
            self.offer(tile)
            if tile:
                self.pass_on(tile - 1)
        self.pass_on(TILES - 1)
        for tile in range(TILES):
            self.finish(tile)
        self.settle()


class Gather:
    scratch = [pltpu.SemaphoreType.DMA((3,)), pltpu.SemaphoreType.DMA((3,))]

    def __init__(self, team, whole, send, recv):
        self.team, self.whole = team, whole
        shard = whole.shape[0] // SLOTS
        mine = whole.at[at_rows(team.slot * shard, shard)]
        theirs = whole.at[at_rows((team.core * 2 + 1 - team.side) * shard, shard)]
        self.across = team.copy(mine, mine, send.at[0], recv.at[0], team.across)
        self.near = team.copy(mine, mine, send.at[1], recv.at[1], team.sibling)
        self.relay = team.copy(theirs, theirs, send.at[2], recv.at[2], team.sibling)

    def start(self):
        self.across.start()
        self.near.start()

    def finish(self):
        self.across.wait_recv()
        self.relay.start()
        self.across.wait_send()
        self.near.wait()
        self.relay.wait()


class RowSums:
    def scratch(rows):
        return [
            pltpu.VMEM((8, rows), F32),
            pltpu.VMEM((3, 8, rows), F32),
            pltpu.SemaphoreType.DMA((3,)),
            pltpu.SemaphoreType.DMA((3,)),
        ]

    def __init__(self, team, mine, came, send, recv):
        self.team, self.mine, self.came = team, mine, came
        self.copies = [
            team.copy(mine, came.at[i], send.at[i], recv.at[i], other)
            for i, other in enumerate((team.sibling, team.across, team.far))
        ]

    def start(self, first, second):
        rows = first.shape[0]
        lane = lax.broadcasted_iota(jnp.int32, (rows, 128), 1)
        both = jnp.where(lane == 0, first, jnp.where(lane == 1, second, 0.0))
        self.mine[...] = jnp.transpose(both)[:8]
        for copy in self.copies:
            copy.start()

    def finish(self):
        for copy in self.copies:
            copy.wait()
        total = self.mine[...] + self.came[0] + (self.came[1] + self.came[2])
        rows = total.shape[1]
        wide = jnp.transpose(jnp.concatenate([total] * 16, axis=0))
        return wide[:, 0:1], wide[:, 1:2]


def turn(field, cosine, sine):
    return field * cosine + pltpu.roll(field, HEAD // 2, 1) * sine


def head_probs(queries, keys, length):
    rows = queries.shape[0]
    scores = right_inner(queries, keys) * (1.0 / math.sqrt(HEAD))
    row = lax.broadcasted_iota(jnp.int32, (rows, rows), 0)
    column = lax.broadcasted_iota(jnp.int32, (rows, rows), 1)
    masked = jnp.where((column <= row) & (column < length), scores, -1e30)
    expo = jnp.exp(masked - jnp.max(masked, axis=-1, keepdims=True))
    return expo / jnp.sum(expo, axis=-1, keepdims=True)


def row_sum(field):
    return jnp.sum(field, axis=-1, keepdims=True)


def over_rows(count, step, work):
    def one(i, carry):
        work(pl.ds(pl.multiple_of(i * step, step), step))
        return carry

    lax.fori_loop(0, count // step, one, 0)


def attend_kernel(
    length_ref,
    hidden,
    mine_hidden,
    q_weight,
    k_weight,
    v_weight,
    o_weight,
    q_gain,
    k_gain,
    cosine,
    sine,
    a_gain,
    q_raw,
    k_raw,
    queries,
    keys,
    values,
    scales,
    mix,
    branch,
    mid_low,
    weights,
    out_weight,
    load,
    *scratch,
):
    team = Team()
    sums = RowSums(team, *scratch[0:4])
    reduce = Reduce(team, *scratch[4:10])
    gather = Gather(team, mid_low, *scratch[10:12])
    loads = [
        pltpu.make_async_copy(source, weights.at[i], load.at[i])
        for i, source in enumerate((q_weight, k_weight, v_weight))
    ] + [pltpu.make_async_copy(o_weight, out_weight, load.at[3])]
    for one in loads:
        one.start()
    team.meet(team.sibling, team.across, team.far)
    rows, local = mix.shape
    width = mid_low.shape[1]
    length = length_ref[0]

    def project(i):
        loads[i].wait()
        return matmul(hidden[...], weights[i])

    q = project(0)
    q_raw[...] = q
    k = project(1)
    k_raw[...] = k
    sums.start(row_sum(q * q), row_sum(k * k))
    values[...] = project(2).astype(BF16)
    q_total, k_total = sums.finish()
    q_scale = lax.rsqrt(q_total * (1.0 / D) + EPS)
    k_scale = lax.rsqrt(k_total * (1.0 / D) + EPS)
    lane = lax.broadcasted_iota(jnp.int32, (rows, 128), 1)
    scales[...] = jnp.where(lane == 0, q_scale, k_scale)
    for head in range(local // HEAD):
        at = pl.ds(head * HEAD, HEAD)
        q = turn(q_raw[:, at] * q_scale * q_gain[:, at], cosine[...], sine[...]).astype(BF16)
        k = turn(k_raw[:, at] * k_scale * k_gain[:, at], cosine[...], sine[...]).astype(BF16)
        queries[:, at] = q
        keys[:, at] = k
        probs = head_probs(q, k, length).astype(BF16)
        mix[:, at] = matmul(probs, values[:, at]).astype(BF16)
    loads[3].wait()

    def make(tile):
        at = reduce.columns(tile)
        reduce.partial[:, at] = matmul(mix[...], out_weight[:, at]).astype(BF16)

    reduce.run(make)
    shard = reduce.shard

    def norm(at):
        part = reduce.total[at, :]
        branch[at, :] = part
        unit = part * lax.rsqrt(row_sum(part * part) * (1.0 / D) + EPS)
        mid = mine_hidden[at, :].astype(F32) + a_gain[...] * unit
        whole_at = pl.ds(pl.multiple_of(team.slot * shard + at.start, at.size), at.size)
        mid_low[whole_at, :] = mid.astype(BF16)

    over_rows(shard, 16, norm)
    gather.start()
    gather.finish()


ANY = pl.BlockSpec(memory_space=pl.ANY)
ON_CHIP = pl.BlockSpec(memory_space=pltpu.VMEM)
SCALAR = pl.BlockSpec(memory_space=pltpu.SMEM)


def shaped(*pairs):
    return tuple(jax.ShapeDtypeStruct(shape, kind) for shape, kind in pairs)


def attend(length, hidden, mine_hidden, weights, gains, cosine, sine, a_gain):
    rows, width = hidden.shape
    local = weights[0].shape[1]
    shard = rows // SLOTS
    return pl.pallas_call(
        attend_kernel,
        out_shape=shaped(
            ((rows, local), F32),
            ((rows, local), F32),
            ((rows, local), BF16),
            ((rows, local), BF16),
            ((rows, local), BF16),
            ((rows, 128), F32),
            ((rows, local), BF16),
            ((shard, width), F32),
            ((rows, width), BF16),
        ),
        in_specs=[SCALAR, ON_CHIP, ON_CHIP] + [ANY] * 4 + [ON_CHIP] * 5,
        out_specs=(ON_CHIP,) * 9,
        scratch_shapes=[
            pltpu.VMEM((3, width, local), BF16),
            pltpu.VMEM((local, width), BF16),
            pltpu.SemaphoreType.DMA((4,)),
        ]
        + RowSums.scratch(rows)
        + Reduce.scratch(rows, width)
        + Gather.scratch,
        compiler_params=pltpu.CompilerParams(
            collective_id=0, has_side_effects=True, vmem_limit_bytes=VMEM_CAP
        ),
        name="attend",
    )(length, hidden, mine_hidden, *weights, *gains, cosine, sine, a_gain)


def settle_kernel(
    length_ref,
    partial_in,
    mine_hidden,
    branch,
    grad_in,
    a_gain,
    m_gain,
    layer,
    d_mlp,
    m_gain_part,
    squares,
    *scratch,
):
    team = Team()
    reduce = Reduce(team, *scratch[0:6])
    gather = Gather(team, d_mlp, *scratch[6:8])
    team.meet(team.sibling, team.across)

    def make(tile):
        at = reduce.columns(tile)
        reduce.partial[:, at] = partial_in[:, at]

    reduce.run(make)
    shard = reduce.shard
    length = length_ref[0]
    m_gain_part[...] = jnp.zeros_like(m_gain_part)
    squares[...] = jnp.zeros_like(squares)

    def folded(field):
        return sum([field[8 * i : 8 * i + 8] for i in range(field.shape[0] // 8)])

    def norm(at):
        part = reduce.total[at, :]
        scale = lax.rsqrt(row_sum(part * part) * (1.0 / D) + EPS)
        unit = part * scale
        base = branch[at, :]
        a_unit = base * lax.rsqrt(row_sum(base * base) * (1.0 / D) + EPS)
        attn_out = a_gain[...] * a_unit
        mlp_out = m_gain[...] * unit
        rows_f = mine_hidden[at, :].astype(F32)
        row = team.slot * shard + at.start + lax.broadcasted_iota(jnp.int32, (at.size, 1), 0)
        live = row < length
        layer[at, :] = jnp.where(live, rows_f + attn_out + mlp_out, 0.0).astype(BF16)
        grad = jnp.where(live, grad_in[at, :].astype(F32), 0.0)
        m_gain_part[...] += folded(grad * unit)
        for i, field in enumerate((rows_f, attn_out, mlp_out)):
            squares[i] += folded(jnp.where(live, field * field, 0.0))
        scaled = grad * m_gain[...]
        back = scale * (scaled - unit * (row_sum(scaled * unit) * (1.0 / D)))
        whole_at = pl.ds(pl.multiple_of(team.slot * shard + at.start, at.size), at.size)
        d_mlp[whole_at, :] = back.astype(BF16)

    over_rows(shard, 16, norm)
    gather.start()
    gather.finish()


def settle(length, partial, mine_hidden, branch, grad_in, a_gain, m_gain):
    rows, width = partial.shape
    shard = rows // SLOTS
    return pl.pallas_call(
        settle_kernel,
        out_shape=shaped(
            ((shard, width), BF16),
            ((rows, width), BF16),
            ((8, width), F32),
            ((3, 8, width), F32),
        ),
        in_specs=[SCALAR] + [ON_CHIP] * 6,
        out_specs=(ON_CHIP,) * 4,
        scratch_shapes=Reduce.scratch(rows, width) + Gather.scratch,
        compiler_params=pltpu.CompilerParams(
            collective_id=1, has_side_effects=True, vmem_limit_bytes=VMEM_CAP
        ),
        name="settle",
    )(length, partial, mine_hidden, branch, grad_in, a_gain, m_gain)


def unattend_kernel(
    length_ref,
    partial_in,
    branch,
    grad_in,
    a_gain,
    o_weight,
    q_raw,
    k_raw,
    queries,
    keys,
    values,
    scales,
    q_gain,
    k_gain,
    cosine,
    sine,
    d_mid,
    a_gain_part,
    d_branch,
    d_heads,
    q_gain_part,
    k_gain_part,
    out_weight,
    d_mix,
    d_q,
    d_k,
    load,
    *scratch,
):
    team = Team()
    sums = RowSums(team, *scratch[0:4])
    reduce = Reduce(team, *scratch[4:10])
    gather = Gather(team, d_branch, *scratch[10:12])
    fetch = pltpu.make_async_copy(o_weight, out_weight, load.at[0])
    fetch.start()
    team.meet(team.sibling, team.across, team.far)
    rows, local = queries.shape

    def make(tile):
        at = reduce.columns(tile)
        reduce.partial[:, at] = partial_in[:, at]

    reduce.run(make)
    shard = reduce.shard
    length = length_ref[0]
    a_gain_part[...] = jnp.zeros_like(a_gain_part)

    def norm(at):
        row = team.slot * shard + at.start + lax.broadcasted_iota(jnp.int32, (at.size, 1), 0)
        grad = jnp.where(row < length, grad_in[at, :].astype(F32), 0.0) + reduce.total[at, :]
        d_mid[at, :] = grad
        base = branch[at, :]
        scale = lax.rsqrt(row_sum(base * base) * (1.0 / D) + EPS)
        unit = base * scale
        product = grad * unit
        a_gain_part[...] += sum([product[8 * i : 8 * i + 8] for i in range(at.size // 8)])
        scaled = grad * a_gain[...]
        back = scale * (scaled - unit * (row_sum(scaled * unit) * (1.0 / D)))
        whole_at = pl.ds(pl.multiple_of(team.slot * shard + at.start, at.size), at.size)
        d_branch[whole_at, :] = back.astype(BF16)

    over_rows(shard, 16, norm)
    gather.start()
    gather.finish()
    fetch.wait()
    d_mix[...] = right_inner(d_branch[...], out_weight[...]).astype(BF16)
    q_scale = scales[:, 0:1]
    k_scale = scales[:, 1:2]
    q_inner = jnp.zeros((rows, 1), F32)
    k_inner = jnp.zeros((rows, 1), F32)
    shrink = 1.0 / math.sqrt(HEAD)
    for head in range(local // HEAD):
        at = pl.ds(head * HEAD, HEAD)
        q, k, v, back = queries[:, at], keys[:, at], values[:, at], d_mix[:, at]
        probs = head_probs(q, k, length)
        d_probs = right_inner(back, v)
        d_scores = (probs * (d_probs - row_sum(probs * d_probs))).astype(BF16)
        d_heads[:, pl.ds(2 * local + head * HEAD, HEAD)] = left_inner(
            probs.astype(BF16), back
        ).astype(BF16)
        d_q_hat = turn(matmul(d_scores, k) * shrink, cosine[...], -sine[...])
        d_k_hat = turn(left_inner(d_scores, q) * shrink, cosine[...], -sine[...])
        q_unit = q_raw[:, at] * q_scale
        k_unit = k_raw[:, at] * k_scale
        q_gain_part[:, at] = jnp.sum(d_q_hat * q_unit, axis=0, keepdims=True)
        k_gain_part[:, at] = jnp.sum(d_k_hat * k_unit, axis=0, keepdims=True)
        q_scaled = d_q_hat * q_gain[:, at]
        k_scaled = d_k_hat * k_gain[:, at]
        d_q[:, at] = q_scaled
        d_k[:, at] = k_scaled
        q_inner += row_sum(q_scaled * q_unit)
        k_inner += row_sum(k_scaled * k_unit)
    sums.start(q_inner, k_inner)
    q_inner, k_inner = sums.finish()
    for i, (grad, raw, scale, inner) in enumerate(
        ((d_q, q_raw, q_scale, q_inner), (d_k, k_raw, k_scale, k_inner))
    ):
        factor = scale * scale * inner * (1.0 / D)
        d_heads[:, pl.ds(i * local, local)] = (scale * grad[...] - raw[...] * factor).astype(BF16)


def unattend(
    length, partial, branch, grad_in, a_gain, o_weight, kept, gains, cosine, sine
):
    rows, width = partial.shape
    local = o_weight.shape[0]
    shard = rows // SLOTS
    return pl.pallas_call(
        unattend_kernel,
        out_shape=shaped(
            ((shard, width), F32),
            ((8, width), F32),
            ((rows, width), BF16),
            ((rows, 3 * local), BF16),
            ((1, local), F32),
            ((1, local), F32),
        ),
        in_specs=[SCALAR] + [ON_CHIP] * 4 + [ANY] + [ON_CHIP] * 10,
        out_specs=(ON_CHIP,) * 6,
        scratch_shapes=[
            pltpu.VMEM((local, width), BF16),
            pltpu.VMEM((rows, local), BF16),
            pltpu.VMEM((rows, local), F32),
            pltpu.VMEM((rows, local), F32),
            pltpu.SemaphoreType.DMA((1,)),
        ]
        + RowSums.scratch(rows)
        + Reduce.scratch(rows, width)
        + Gather.scratch,
        compiler_params=pltpu.CompilerParams(
            collective_id=2, has_side_effects=True, vmem_limit_bytes=VMEM_CAP
        ),
        name="unattend",
    )(length, partial, branch, grad_in, a_gain, o_weight, *kept, *gains, cosine, sine)


class Deal:
    def __init__(self, count, shard, width):
        self.count = count
        self.columns = max(128, width // count)
        self.across = width // self.columns
        self.rows = shard * self.across // count

    def at(self, chunk, base=0):
        return (
            at_rows(base + (chunk // self.across) * self.rows, self.rows),
            at_rows((chunk % self.across) * self.columns, self.columns),
        )


def finish_kernel(
    length_ref,
    inverse,
    partial_in,
    d_mid,
    layer,
    layer_out,
    input_grad,
    closed,
    parked,
    leaving,
    deal_send,
    deal_recv,
    *scratch,
):
    team = Team()
    reduce = Reduce(team, *scratch[0:6])
    gathers = [
        Gather(team, whole, *scratch[6 + 2 * i : 8 + 2 * i])
        for i, whole in enumerate((layer_out, input_grad))
    ]
    count = lax.axis_size("dp")
    shard, width = d_mid.shape
    deal = Deal(count, shard, width)
    barrier = pltpu.get_barrier_semaphore()
    for step in range(1, count):
        pl.semaphore_signal(
            barrier, inc=1, device_id=(lax.rem(team.row + step, count), team.me), device_id_type=AT
        )
    for other in (team.sibling, team.across):
        pl.semaphore_signal(barrier, inc=1, device_id=(team.row, other), device_id_type=AT)
    pl.semaphore_wait(barrier, count + 1)

    def make(tile):
        at = reduce.columns(tile)
        reduce.partial[:, at] = partial_in[:, at]

    reduce.run(make)
    length = length_ref[0]

    def close(at):
        row = team.slot * shard + at.start + lax.broadcasted_iota(jnp.int32, (at.size, 1), 0)
        closed[at, :] = jnp.where(row < length, reduce.total[at, :] + d_mid[at, :], 0.0).astype(BF16)

    over_rows(shard, 16, close)

    def send(phase, step, i, source, target):
        return pltpu.make_async_remote_copy(
            src_ref=source,
            dst_ref=target,
            send_sem=deal_send.at[phase, step, i],
            recv_sem=deal_recv.at[phase, step, i],
            device_id=(lax.rem(team.row + step, count), team.me),
            device_id_type=AT,
        )

    first = []
    for i, source in enumerate((layer, closed)):
        for step in range(1, count):
            other = lax.rem(team.row + step, count)
            copy = send(0, step, i, source.at[deal.at(other)], parked.at[team.row, i])
            copy.start()
            first.append(copy)
        parked[team.row, i] = source[deal.at(team.row)]
    for copy in first:
        copy.wait()
    mine = team.slot * shard
    second = []
    for i, target in enumerate((layer_out, input_grad)):
        for step in range(1, count):
            other = lax.rem(team.row + step, count)
            leaving[other, i] = parked[inverse[other], i]
            copy = send(1, step, i, leaving.at[other, i], target.at[deal.at(team.row, mine)])
            copy.start()
            second.append(copy)
        target[deal.at(team.row, mine)] = parked[inverse[team.row], i]
    for copy in second:
        copy.wait()
    for gather in gathers:
        gather.start()
    for gather in gathers:
        gather.finish()


def close_layer(length, inverse, partial, d_mid, layer):
    rows, width = partial.shape
    shard = rows // SLOTS
    count = lax.axis_size("dp")
    deal = Deal(count, shard, width)
    chunk = (count, 2, deal.rows, deal.columns)
    return pl.pallas_call(
        finish_kernel,
        out_shape=shaped(((rows, width), BF16), ((rows, width), BF16)),
        in_specs=[SCALAR, SCALAR] + [ON_CHIP] * 3,
        out_specs=(ON_CHIP,) * 2,
        scratch_shapes=[
            pltpu.VMEM((shard, width), BF16),
            pltpu.VMEM(chunk, BF16),
            pltpu.VMEM(chunk, BF16),
            pltpu.SemaphoreType.DMA((2, count, 2)),
            pltpu.SemaphoreType.DMA((2, count, 2)),
        ]
        + Reduce.scratch(rows, width)
        + Gather.scratch * 2,
        compiler_params=pltpu.CompilerParams(
            collective_id=3, has_side_effects=True, vmem_limit_bytes=VMEM_CAP
        ),
        name="close_layer",
    )(length, inverse, partial, d_mid, layer)


def body(
    hidden_in,
    upstream_grad,
    seq_lengths,
    position_order,
    query_weight,
    key_weight,
    value_weight,
    output_weight,
    query_gain,
    key_gain,
    attn_gain,
    gate_weight,
    up_weight,
    down_weight,
    mlp_gain,
):
    count = lax.axis_size("dp")
    ways = lax.axis_size("tensor")
    myself = lax.axis_index("dp")
    part = lax.axis_index("tensor")
    grid = Grid(count)
    index = jnp.arange(count, dtype=jnp.int32)
    inverse = jnp.sum(
        index[None, :] * (position_order[None, :] == index[:, None]).astype(jnp.int32), axis=1
    )
    rows = hidden_in.shape[1]
    width = hidden_in.shape[2]
    shard = rows // ways
    piece = shard // count
    seq_here = jnp.sum(jnp.where(index == myself, position_order, 0))
    length = jnp.sum(jnp.where(index == seq_here, seq_lengths, 0))[None]
    slot = part % 2 * 2 + part // 2

    def exchange(pieces):
        return lax.all_to_all(pieces, "dp", split_axis=0, concat_axis=0, tiled=True)

    def my_rows(field):
        return lax.dynamic_slice_in_dim(field, slot * shard, shard, axis=0)

    first = exchange(my_rows(upstream_grad[0]).reshape(count, piece, width))
    second = exchange(jnp.take(first, position_order, axis=0))
    grad_in = second.reshape(shard, width)

    rows_low = hidden_in[0]
    my_low = my_rows(rows_low)
    local = query_weight.shape[1]
    strip = width // grid.groups
    tile = width // count

    def strip_of(field, group):
        return lax.dynamic_slice_in_dim(field, group * strip, strip, axis=1)

    def strips(field):
        found = [strip_of(field, grid.group)]
        for step in range(1, grid.groups):
            found.append(
                grid.shift_groups(
                    strip_of(field, (grid.group + step) % grid.groups), step
                )
            )
        return jnp.concatenate(found, axis=0)

    def tile_of(field, lane):
        return lax.dynamic_slice_in_dim(field, lane * tile, tile, axis=1)

    def reduced(product, field):
        sent = []
        for step in range(1, grid.lanes):
            other = product(tile_of(field, (grid.lane + step) % grid.lanes)).astype(BF16)
            sent.append(grid.shift_lanes(other, step))
        mine = product(tile_of(field, grid.lane))
        for other in sent:
            mine = mine + other.astype(F32)
        return mine

    hidden_strips = strips(rows_low)

    cosine, sine = rope_tables(rows, HEAD)
    cosine = jnp.concatenate([cosine, cosine], axis=1)
    sine = jnp.concatenate([-sine, sine], axis=1)
    gains = (query_gain[None], key_gain[None])
    q_raw, k_raw, queries, keys, values, scales, attn_mix, branch, mid_low = attend(
        length,
        rows_low,
        my_low,
        (query_weight, key_weight, value_weight, output_weight),
        gains,
        cosine,
        sine,
        attn_gain[None],
    )
    mix_all = jnp.concatenate([attn_mix] + grid.ring(attn_mix), axis=0)
    mid_others = shared_ring(grid, mid_low)

    gate = matmul(mid_low, gate_weight)
    upper = matmul(mid_low, up_weight)
    sig = jax.nn.sigmoid(gate)
    inner = (gate * sig * upper).astype(BF16)
    layer, d_mlp, mlp_gain_part, squares = settle(
        length,
        matmul(inner, down_weight).astype(BF16),
        my_low,
        branch,
        grad_in,
        attn_gain[None],
        mlp_gain[None],
    )
    d_mlp_others = shared_ring(grid, d_mlp)

    def inner_back(gate, upper, d_mlp):
        d_inner = right_inner(d_mlp, down_weight)
        sig = jax.nn.sigmoid(gate)
        d_gate = (d_inner * upper * sig * (1.0 + gate * (1.0 - sig))).astype(BF16)
        d_up = (d_inner * gate * sig).astype(BF16)
        return d_gate, d_up

    d_gate, d_up = inner_back(gate, upper, d_mlp)
    d_mid, attn_gain_part, d_branch, d_heads, query_gain_part, key_gain_part = unattend(
        length,
        (right_inner(d_gate, gate_weight) + right_inner(d_up, up_weight)).astype(BF16),
        branch,
        grad_in,
        attn_gain[None],
        output_weight,
        (q_raw, k_raw, queries, keys, values, scales),
        gains,
        cosine,
        sine,
    )
    d_branch_strips = strips(d_branch)
    d_heads_all = jnp.concatenate([d_heads] + grid.ring(d_heads), axis=0)
    layer_out, input_grad = close_layer(
        length,
        inverse,
        (
            right_inner(d_heads[:, :local], query_weight)
            + right_inner(d_heads[:, local : 2 * local], key_weight)
            + right_inner(d_heads[:, 2 * local :], value_weight)
        ).astype(BF16),
        d_mid,
        layer,
    )

    gate_o = matmul(mid_others, gate_weight)
    upper_o = matmul(mid_others, up_weight)
    inner_o = (jax.nn.silu(gate_o) * upper_o).astype(BF16)
    d_gate_o, d_up_o = inner_back(gate_o, upper_o, d_mlp_others)

    def strip_all(own, others):
        return jnp.concatenate([strip_of(own, grid.group), strip_of(others, grid.group)], axis=0)

    mid_strips = strip_all(mid_low, mid_others)
    d_mlp_strips = strip_all(d_mlp, d_mlp_others)
    d_gate_all = jnp.concatenate([d_gate, d_gate_o], axis=0)
    d_up_all = jnp.concatenate([d_up, d_up_o], axis=0)
    inner_all = jnp.concatenate([inner, inner_o], axis=0)
    gate_part = reduced(lambda tile: left_inner(tile, d_gate_all), mid_strips)
    up_part = reduced(lambda tile: left_inner(tile, d_up_all), mid_strips)
    down_part = reduced(lambda tile: left_inner(inner_all, tile), d_mlp_strips)
    output_part = reduced(lambda tile: left_inner(mix_all, tile), d_branch_strips)
    heads_part = reduced(lambda tile: left_inner(tile, d_heads_all), hidden_strips)
    query_part = heads_part[:, :local]
    key_part = heads_part[:, local : 2 * local]
    value_part = heads_part[:, 2 * local :]

    shared = jnp.concatenate(
        [jnp.sum(attn_gain_part, axis=0), jnp.sum(mlp_gain_part, axis=0), jnp.sum(squares, axis=(1, 2))]
    )
    shared = shared + sibling(shared)
    shared = shared + across(shared)
    sums = grid.total(jnp.concatenate([shared, query_gain_part[0], key_gain_part[0]]))
    attn_gain_grad = sums[:width]
    mlp_gain_grad = sums[width : 2 * width]
    squares = sums[2 * width : 2 * width + 3]
    query_gain_grad = sums[2 * width + 3 : 2 * width + 3 + local]
    key_gain_grad = sums[2 * width + 3 + local :]
    rms_values = jnp.sqrt(squares / (jnp.sum(seq_lengths).astype(F32) * D))

    return (
        layer_out[None],
        input_grad[None],
        query_part,
        key_part,
        value_part,
        output_part,
        query_gain_grad,
        key_gain_grad,
        attn_gain_grad,
        gate_part,
        up_part,
        down_part,
        mlp_gain_grad,
        rms_values,
    )


def solution(mesh):
    placed = (
        P("dp", None, None),
        P("dp", None, None),
        P(),
        P(),
        P(None, "tensor"),
        P(None, "tensor"),
        P(None, "tensor"),
        P("tensor", None),
        P("tensor"),
        P("tensor"),
        P(),
        P(None, "tensor"),
        P(None, "tensor"),
        P("tensor", None),
        P(),
    )
    return jax.shard_map(
        body,
        mesh=mesh,
        in_specs=placed,
        out_specs=(
            P("dp", None, None),
            P("dp", None, None),
            P("dp", "tensor"),
            P("dp", "tensor"),
            P("dp", "tensor"),
            P("tensor", "dp"),
            P("tensor"),
            P("tensor"),
            P(),
            P("dp", "tensor"),
            P("dp", "tensor"),
            P("tensor", "dp"),
            P(),
            P(),
        ),
        check_vma=False,
    )
```

```python
import functools
import math
import types

import jax
import jax.numpy as jnp
import numpy as np
from jax import lax
from jax.experimental import pallas as pl
from jax.experimental.pallas import tpu as pltpu
from jax.sharding import PartitionSpec as P

D = 2048
HEAD = 128
EPS = 1e-06
F32 = jnp.float32
BF16 = jnp.bfloat16


def matmul(left, right):
    return jnp.dot(left, right, preferred_element_type=F32)


def left_inner(left, right):
    return lax.dot_general(left, right, (((0,), (0,)), ((), ())), preferred_element_type=F32)


def right_inner(left, right):
    return lax.dot_general(left, right, (((1,), (1,)), ((), ())), preferred_element_type=F32)


def rope_tables(rows, width):
    places = jnp.arange(rows, dtype=F32)
    freq = jnp.power(F32(500000.0), -jnp.arange(width // 2, dtype=F32) * (2.0 / width))
    angle = places[:, None] * freq[None, :]
    return (jnp.cos(angle), jnp.sin(angle))


def rope_constants(rows, width):
    half = width // 2
    exponent = -np.arange(half, dtype=np.float32) * np.float32(2.0 / width)
    freq = np.power(np.float32(500000.0), exponent, dtype=np.float32)
    angle = (np.arange(rows, dtype=np.float32)[:, None] * freq[None, :]).astype(np.float64)
    cosine, sine = np.cos(angle), np.sin(angle)
    return (
        jnp.asarray(np.concatenate([cosine, cosine], axis=1), F32),
        jnp.asarray(np.concatenate([-sine, sine], axis=1), F32),
    )


class Grid:
    def __init__(self, count):
        self.count = count
        self.lanes = 2 ** ((count.bit_length() - 1) // 2)
        self.groups = count // self.lanes
        me = lax.axis_index("dp")
        self.group = me // self.lanes
        self.lane = me % self.lanes

    def shift_groups(self, field, step):
        pairs = [
            (g * self.lanes + a, ((g + step) % self.groups) * self.lanes + a)
            for g in range(self.groups)
            for a in range(self.lanes)
        ]
        return lax.ppermute(field, "dp", pairs)

    def shift_lanes(self, field, step):
        pairs = [
            (g * self.lanes + a, g * self.lanes + (a + step) % self.lanes)
            for g in range(self.groups)
            for a in range(self.lanes)
        ]
        return lax.ppermute(field, "dp", pairs)

    def ring(self, field):
        found = []
        for _ in range(self.groups - 1):
            field = self.shift_groups(field, 1)
            found.append(field)
        return found

    def total(self, field):
        step = 1
        while step < self.count:
            field = field + lax.ppermute(
                field, "dp", [(i, i ^ step) for i in range(self.count)]
            )
            step *= 2
        return field


def sibling(field):
    size = lax.axis_size("tensor")
    return lax.ppermute(field, "tensor", [(i, i ^ 1) for i in range(size)])


def across(field):
    size = lax.axis_size("tensor")
    return lax.ppermute(field, "tensor", [(i, (i + 2) % size) for i in range(size)])


def shared_ring(grid, rows_low):
    core = lax.axis_index("tensor") % 2
    half = rows_low.shape[0] // 2
    mine = lax.dynamic_slice_in_dim(rows_low, core * half, half, axis=0)
    pieces = []
    for piece in grid.ring(mine):
        pieces += [piece, sibling(piece)]
    return jnp.concatenate(pieces, axis=0)


SLOTS = 4
TILES = 4
AT = pl.DeviceIdType.MESH
VMEM_CAP = 56 * 2**20


class Team:
    def __init__(self):
        self.row = lax.axis_index("dp")
        self.me = lax.axis_index("tensor")
        self.side = self.me // 2
        self.core = self.me % 2
        self.slot = self.core * 2 + self.side
        self.sibling = self.side * 2 + (1 - self.core)
        self.across = (1 - self.side) * 2 + self.core
        self.far = (1 - self.side) * 2 + (1 - self.core)

    def meet(self, *others):
        barrier = pltpu.get_barrier_semaphore()
        for other in others:
            pl.semaphore_signal(barrier, inc=1, device_id=(self.row, other), device_id_type=AT)
        pl.semaphore_wait(barrier, len(others))

    def copy(self, source, target, send, recv, other):
        return pltpu.make_async_remote_copy(
            src_ref=source,
            dst_ref=target,
            send_sem=send,
            recv_sem=recv,
            device_id=(self.row, other),
            device_id_type=AT,
        )


def at_rows(start, size):
    return pl.ds(pl.multiple_of(start, size), size)


class Reduce:
    def scratch(rows, width):
        shard = rows // SLOTS
        return [
            pltpu.VMEM((rows, width), BF16),
            pltpu.VMEM((3, shard, width), BF16),
            pltpu.VMEM((shard, width), BF16),
            pltpu.VMEM((shard, width), F32),
            pltpu.SemaphoreType.DMA((3, TILES)),
            pltpu.SemaphoreType.DMA((3, TILES)),
        ]

    def __init__(self, team, partial, came, gone, total, send, recv):
        self.team, self.partial, self.came, self.gone, self.total = team, partial, came, gone, total
        self.shard, width = total.shape
        self.tiles = send.shape[1]
        self.tile = width // self.tiles
        self.send, self.recv = send, recv
        self.copies = {}

    def columns(self, tile):
        return pl.ds(tile * self.tile, self.tile)

    def block(self, core, side):
        return at_rows((core * 2 + side) * self.shard, self.shard)

    def launch(self, kind, tile, source, other):
        copy = self.team.copy(
            source,
            self.came.at[kind, :, self.columns(tile)],
            self.send.at[kind, tile],
            self.recv.at[kind, tile],
            other,
        )
        copy.start()
        self.copies[kind, tile] = copy

    def offer(self, tile):
        team, columns = self.team, self.columns(tile)
        for kind, side in ((0, 1 - team.side), (1, team.side)):
            self.launch(
                kind, tile, self.partial.at[self.block(1 - team.core, side), columns], team.sibling
            )

    def pass_on(self, tile):
        team, columns = self.team, self.columns(tile)
        self.copies[0, tile].wait_recv()
        mine = self.partial[self.block(team.core, 1 - team.side), columns].astype(F32)
        self.gone[:, columns] = (mine + self.came[0, :, columns].astype(F32)).astype(BF16)
        self.launch(2, tile, self.gone.at[:, columns], team.across)

    def finish(self, tile):
        team, columns = self.team, self.columns(tile)
        self.copies[1, tile].wait_recv()
        mine = self.partial[self.block(team.core, team.side), columns].astype(F32)
        mine = mine + self.came[1, :, columns].astype(F32)
        self.copies[2, tile].wait_recv()
        self.total[:, columns] = mine + self.came[2, :, columns].astype(F32)

    def settle(self):
        for copy in self.copies.values():
            copy.wait_send()

    def run(self, make, meanwhile=None):
        self.copies = {}
        for tile in range(self.tiles):
            make(self.columns(tile))
            self.offer(tile)
            if tile:
                self.pass_on(tile - 1)
        self.pass_on(self.tiles - 1)
        if meanwhile is not None:
            meanwhile()
        for tile in range(self.tiles):
            self.finish(tile)
        self.settle()


class Gather:
    scratch = [pltpu.SemaphoreType.DMA((3,)), pltpu.SemaphoreType.DMA((3,))]

    def __init__(self, team, whole, send, recv):
        self.team, self.whole = team, whole
        shard = whole.shape[0] // SLOTS
        mine = whole.at[at_rows(team.slot * shard, shard)]
        theirs = whole.at[at_rows((team.core * 2 + 1 - team.side) * shard, shard)]
        self.across = team.copy(mine, mine, send.at[0], recv.at[0], team.across)
        self.near = team.copy(mine, mine, send.at[1], recv.at[1], team.sibling)
        self.relay = team.copy(theirs, theirs, send.at[2], recv.at[2], team.sibling)

    def start(self):
        self.across.start()
        self.near.start()

    def half(self):
        self.across.wait_recv()
        self.relay.start()

    def finish(self):
        self.across.wait_send()
        self.near.wait()
        self.relay.wait()


class RowSums:
    def scratch(rows):
        return [
            pltpu.VMEM((8, rows), F32),
            pltpu.VMEM((3, 8, rows), F32),
            pltpu.SemaphoreType.DMA((3,)),
            pltpu.SemaphoreType.DMA((3,)),
        ]

    def __init__(self, team, mine, came, send, recv):
        self.team, self.mine, self.came = team, mine, came
        self.copies = [
            team.copy(mine, came.at[i], send.at[i], recv.at[i], other)
            for i, other in enumerate((team.sibling, team.across, team.far))
        ]

    def start(self, first, second):
        rows = first.shape[0]
        lane = lax.broadcasted_iota(jnp.int32, (rows, 128), 1)
        both = jnp.where(lane == 0, first, jnp.where(lane == 1, second, 0.0))
        self.mine[...] = jnp.transpose(both)[:8]
        for copy in self.copies:
            copy.start()

    def finish(self):
        for copy in self.copies:
            copy.wait()
        total = self.mine[...] + self.came[0] + (self.came[1] + self.came[2])
        rows = total.shape[1]
        wide = jnp.transpose(jnp.concatenate([total] * 16, axis=0))
        return wide[:, 0:1], wide[:, 1:2]


def turn(field, cosine, sine):
    return field * cosine + pltpu.roll(field, HEAD // 2, 1) * sine


def head_probs(queries, keys, length):
    rows = queries.shape[0]
    scores = right_inner(queries, keys) * (1.0 / math.sqrt(HEAD))
    row = lax.broadcasted_iota(jnp.int32, (rows, rows), 0)
    column = lax.broadcasted_iota(jnp.int32, (rows, rows), 1)
    masked = jnp.where((column <= row) & (column < length), scores, -1e30)
    expo = jnp.exp(masked - jnp.max(masked, axis=-1, keepdims=True))
    return expo / jnp.sum(expo, axis=-1, keepdims=True)


def row_sum(field):
    return jnp.sum(field, axis=-1, keepdims=True)


def over_rows(count, step, work):
    def one(i, carry):
        work(pl.ds(pl.multiple_of(i * step, step), step))
        return carry

    lax.fori_loop(0, count // step, one, 0)


def attend_kernel(
    length_ref,
    hidden,
    mine_hidden,
    q_weight,
    k_weight,
    v_weight,
    o_weight,
    q_gain,
    k_gain,
    cosine,
    sine,
    a_gain,
    q_raw,
    k_raw,
    queries,
    keys,
    values,
    scales,
    mix,
    branch,
    mid_low,
    weights,
    out_weight,
    load,
    *scratch,
):
    team = Team()
    sums = RowSums(team, *scratch[0:4])
    reduce = Reduce(team, *scratch[4:10])
    gather = Gather(team, mid_low, *scratch[10:12])
    loads = [
        pltpu.make_async_copy(source, weights.at[i], load.at[i])
        for i, source in enumerate((q_weight, k_weight, v_weight))
    ] + [pltpu.make_async_copy(o_weight, out_weight, load.at[3])]
    for one in loads:
        one.start()
    team.meet(team.sibling, team.across, team.far)
    rows, local = mix.shape
    width = mid_low.shape[1]
    length = length_ref[0]

    def project(i):
        loads[i].wait()
        return matmul(hidden[...], weights[i])

    q = project(0)
    q_raw[...] = q
    k = project(1)
    k_raw[...] = k
    sums.start(row_sum(q * q), row_sum(k * k))
    values[...] = project(2).astype(BF16)
    q_total, k_total = sums.finish()
    q_scale = lax.rsqrt(q_total * (1.0 / D) + EPS)
    k_scale = lax.rsqrt(k_total * (1.0 / D) + EPS)
    lane = lax.broadcasted_iota(jnp.int32, (rows, 128), 1)
    scales[...] = jnp.where(lane == 0, q_scale, k_scale)
    for head in range(local // HEAD):
        at = pl.ds(head * HEAD, HEAD)
        q = turn(q_raw[:, at] * q_scale * q_gain[:, at], cosine[...], sine[...]).astype(BF16)
        k = turn(k_raw[:, at] * k_scale * k_gain[:, at], cosine[...], sine[...]).astype(BF16)
        queries[:, at] = q
        keys[:, at] = k
        probs = head_probs(q, k, length).astype(BF16)
        mix[:, at] = matmul(probs, values[:, at]).astype(BF16)
    loads[3].wait()

    def make(at):
        reduce.partial[:, at] = matmul(mix[...], out_weight[:, at]).astype(BF16)

    reduce.run(make)
    shard = reduce.shard

    def norm(at):
        part = reduce.total[at, :]
        branch[at, :] = part
        unit = part * lax.rsqrt(row_sum(part * part) * (1.0 / D) + EPS)
        mid = mine_hidden[at, :].astype(F32) + a_gain[...] * unit
        whole_at = pl.ds(pl.multiple_of(team.slot * shard + at.start, at.size), at.size)
        mid_low[whole_at, :] = mid.astype(BF16)

    over_rows(shard, 16, norm)
    gather.start()
    gather.half()
    gather.finish()


ANY = pl.BlockSpec(memory_space=pl.ANY)
ON_CHIP = pl.BlockSpec(memory_space=pltpu.VMEM)
SCALAR = pl.BlockSpec(memory_space=pltpu.SMEM)


def shaped(*pairs):
    return tuple(jax.ShapeDtypeStruct(shape, kind) for shape, kind in pairs)


def attend(length, hidden, mine_hidden, weights, gains, cosine, sine, a_gain):
    rows, width = hidden.shape
    local = weights[0].shape[1]
    shard = rows // SLOTS
    return pl.pallas_call(
        attend_kernel,
        out_shape=shaped(
            ((rows, local), F32),
            ((rows, local), F32),
            ((rows, local), BF16),
            ((rows, local), BF16),
            ((rows, local), BF16),
            ((rows, 128), F32),
            ((rows, local), BF16),
            ((shard, width), F32),
            ((rows, width), BF16),
        ),
        in_specs=[SCALAR, ON_CHIP, ON_CHIP] + [ANY] * 4 + [ON_CHIP] * 5,
        out_specs=(ON_CHIP,) * 9,
        scratch_shapes=[
            pltpu.VMEM((3, width, local), BF16),
            pltpu.VMEM((local, width), BF16),
            pltpu.SemaphoreType.DMA((4,)),
        ]
        + RowSums.scratch(rows)
        + Reduce.scratch(rows, width)
        + Gather.scratch,
        compiler_params=pltpu.CompilerParams(
            collective_id=0, has_side_effects=True, vmem_limit_bytes=VMEM_CAP
        ),
        name="attend",
    )(length, hidden, mine_hidden, *weights, *gains, cosine, sine, a_gain)


def settle_kernel(
    length_ref,
    partial_in,
    mine_hidden,
    branch,
    grad_in,
    a_gain,
    m_gain,
    layer,
    d_mlp,
    m_gain_part,
    squares,
    *scratch,
):
    team = Team()
    reduce = Reduce(team, *scratch[0:6])
    gather = Gather(team, d_mlp, *scratch[6:8])
    team.meet(team.sibling, team.across)

    def make(at):
        reduce.partial[:, at] = partial_in[:, at]

    reduce.run(make)
    shard = reduce.shard
    length = length_ref[0]
    m_gain_part[...] = jnp.zeros_like(m_gain_part)
    squares[...] = jnp.zeros_like(squares)

    def folded(field):
        return sum([field[8 * i : 8 * i + 8] for i in range(field.shape[0] // 8)])

    def norm(at):
        part = reduce.total[at, :]
        scale = lax.rsqrt(row_sum(part * part) * (1.0 / D) + EPS)
        unit = part * scale
        base = branch[at, :]
        a_unit = base * lax.rsqrt(row_sum(base * base) * (1.0 / D) + EPS)
        attn_out = a_gain[...] * a_unit
        mlp_out = m_gain[...] * unit
        rows_f = mine_hidden[at, :].astype(F32)
        row = team.slot * shard + at.start + lax.broadcasted_iota(jnp.int32, (at.size, 1), 0)
        live = row < length
        layer[at, :] = jnp.where(live, rows_f + attn_out + mlp_out, 0.0).astype(BF16)
        grad = jnp.where(live, grad_in[at, :].astype(F32), 0.0)
        m_gain_part[...] += folded(grad * unit)
        for i, field in enumerate((rows_f, attn_out, mlp_out)):
            squares[i] += folded(jnp.where(live, field * field, 0.0))
        scaled = grad * m_gain[...]
        back = scale * (scaled - unit * (row_sum(scaled * unit) * (1.0 / D)))
        whole_at = pl.ds(pl.multiple_of(team.slot * shard + at.start, at.size), at.size)
        d_mlp[whole_at, :] = back.astype(BF16)

    over_rows(shard, 16, norm)
    gather.start()
    gather.half()
    gather.finish()


def settle(length, partial, mine_hidden, branch, grad_in, a_gain, m_gain):
    rows, width = partial.shape
    shard = rows // SLOTS
    return pl.pallas_call(
        settle_kernel,
        out_shape=shaped(
            ((shard, width), BF16),
            ((rows, width), BF16),
            ((8, width), F32),
            ((3, 8, width), F32),
        ),
        in_specs=[SCALAR] + [ON_CHIP] * 6,
        out_specs=(ON_CHIP,) * 4,
        scratch_shapes=Reduce.scratch(rows, width) + Gather.scratch,
        compiler_params=pltpu.CompilerParams(
            collective_id=1, has_side_effects=True, vmem_limit_bytes=VMEM_CAP
        ),
        name="settle",
    )(length, partial, mine_hidden, branch, grad_in, a_gain, m_gain)


def unattend_kernel(
    length_ref,
    partial_in,
    branch,
    grad_in,
    a_gain,
    o_weight,
    q_raw,
    k_raw,
    queries,
    keys,
    values,
    scales,
    q_gain,
    k_gain,
    cosine,
    sine,
    d_mid,
    a_gain_part,
    d_branch,
    d_heads,
    q_gain_part,
    k_gain_part,
    out_weight,
    d_mix,
    d_q,
    d_k,
    load,
    *scratch,
):
    team = Team()
    sums = RowSums(team, *scratch[0:4])
    reduce = Reduce(team, *scratch[4:10])
    gather = Gather(team, d_branch, *scratch[10:12])
    fetch = pltpu.make_async_copy(o_weight, out_weight, load.at[0])
    fetch.start()
    team.meet(team.sibling, team.across, team.far)
    rows, local = queries.shape

    def make(at):
        reduce.partial[:, at] = partial_in[:, at]

    reduce.run(make)
    shard = reduce.shard
    length = length_ref[0]
    a_gain_part[...] = jnp.zeros_like(a_gain_part)

    def norm(at):
        row = team.slot * shard + at.start + lax.broadcasted_iota(jnp.int32, (at.size, 1), 0)
        grad = jnp.where(row < length, grad_in[at, :].astype(F32), 0.0) + reduce.total[at, :]
        d_mid[at, :] = grad
        base = branch[at, :]
        scale = lax.rsqrt(row_sum(base * base) * (1.0 / D) + EPS)
        unit = base * scale
        product = grad * unit
        a_gain_part[...] += sum([product[8 * i : 8 * i + 8] for i in range(at.size // 8)])
        scaled = grad * a_gain[...]
        back = scale * (scaled - unit * (row_sum(scaled * unit) * (1.0 / D)))
        whole_at = pl.ds(pl.multiple_of(team.slot * shard + at.start, at.size), at.size)
        d_branch[whole_at, :] = back.astype(BF16)

    over_rows(shard, 16, norm)
    gather.start()
    gather.half()
    gather.finish()
    fetch.wait()
    d_mix[...] = right_inner(d_branch[...], out_weight[...]).astype(BF16)
    q_scale = scales[:, 0:1]
    k_scale = scales[:, 1:2]
    q_inner = jnp.zeros((rows, 1), F32)
    k_inner = jnp.zeros((rows, 1), F32)
    shrink = 1.0 / math.sqrt(HEAD)
    for head in range(local // HEAD):
        at = pl.ds(head * HEAD, HEAD)
        q, k, v, back = queries[:, at], keys[:, at], values[:, at], d_mix[:, at]
        probs = head_probs(q, k, length)
        d_probs = right_inner(back, v)
        d_scores = (probs * (d_probs - row_sum(probs * d_probs))).astype(BF16)
        d_heads[:, pl.ds(2 * local + head * HEAD, HEAD)] = left_inner(
            probs.astype(BF16), back
        ).astype(BF16)
        d_q_hat = turn(matmul(d_scores, k) * shrink, cosine[...], -sine[...])
        d_k_hat = turn(left_inner(d_scores, q) * shrink, cosine[...], -sine[...])
        q_unit = q_raw[:, at] * q_scale
        k_unit = k_raw[:, at] * k_scale
        q_gain_part[:, at] = jnp.sum(d_q_hat * q_unit, axis=0, keepdims=True)
        k_gain_part[:, at] = jnp.sum(d_k_hat * k_unit, axis=0, keepdims=True)
        q_scaled = d_q_hat * q_gain[:, at]
        k_scaled = d_k_hat * k_gain[:, at]
        d_q[:, at] = q_scaled
        d_k[:, at] = k_scaled
        q_inner += row_sum(q_scaled * q_unit)
        k_inner += row_sum(k_scaled * k_unit)
    sums.start(q_inner, k_inner)
    q_inner, k_inner = sums.finish()
    for i, (grad, raw, scale, inner) in enumerate(
        ((d_q, q_raw, q_scale, q_inner), (d_k, k_raw, k_scale, k_inner))
    ):
        factor = scale * scale * inner * (1.0 / D)
        d_heads[:, pl.ds(i * local, local)] = (scale * grad[...] - raw[...] * factor).astype(BF16)


def unattend(
    length, partial, branch, grad_in, a_gain, o_weight, kept, gains, cosine, sine
):
    rows, width = partial.shape
    local = o_weight.shape[0]
    shard = rows // SLOTS
    return pl.pallas_call(
        unattend_kernel,
        out_shape=shaped(
            ((shard, width), F32),
            ((8, width), F32),
            ((rows, width), BF16),
            ((rows, 3 * local), BF16),
            ((1, local), F32),
            ((1, local), F32),
        ),
        in_specs=[SCALAR] + [ON_CHIP] * 4 + [ANY] + [ON_CHIP] * 10,
        out_specs=(ON_CHIP,) * 6,
        scratch_shapes=[
            pltpu.VMEM((local, width), BF16),
            pltpu.VMEM((rows, local), BF16),
            pltpu.VMEM((rows, local), F32),
            pltpu.VMEM((rows, local), F32),
            pltpu.SemaphoreType.DMA((1,)),
        ]
        + RowSums.scratch(rows)
        + Reduce.scratch(rows, width)
        + Gather.scratch,
        compiler_params=pltpu.CompilerParams(
            collective_id=2, has_side_effects=True, vmem_limit_bytes=VMEM_CAP
        ),
        name="unattend",
    )(length, partial, branch, grad_in, a_gain, o_weight, *kept, *gains, cosine, sine)


class Deal:
    def __init__(self, count, shard, width):
        self.count = count
        self.columns = max(128, width // count)
        self.across = width // self.columns
        self.rows = shard * self.across // count

    def at(self, chunk, base=0):
        return (
            at_rows(base + (chunk // self.across) * self.rows, self.rows),
            at_rows((chunk % self.across) * self.columns, self.columns),
        )


def finish_kernel(
    length_ref,
    inverse,
    partial_in,
    d_mid,
    layer,
    layer_out,
    input_grad,
    closed,
    parked,
    leaving,
    deal_send,
    deal_recv,
    *scratch,
):
    team = Team()
    reduce = Reduce(team, *scratch[0:6])
    gathers = [
        Gather(team, whole, *scratch[6 + 2 * i : 8 + 2 * i])
        for i, whole in enumerate((layer_out, input_grad))
    ]
    count = lax.axis_size("dp")
    shard, width = d_mid.shape
    deal = Deal(count, shard, width)
    barrier = pltpu.get_barrier_semaphore()
    for step in range(1, count):
        pl.semaphore_signal(
            barrier, inc=1, device_id=(lax.rem(team.row + step, count), team.me), device_id_type=AT
        )
    for other in (team.sibling, team.across):
        pl.semaphore_signal(barrier, inc=1, device_id=(team.row, other), device_id_type=AT)
    pl.semaphore_wait(barrier, count + 1)

    def make(at):
        reduce.partial[:, at] = partial_in[:, at]

    reduce.run(make)
    length = length_ref[0]

    def close(at):
        row = team.slot * shard + at.start + lax.broadcasted_iota(jnp.int32, (at.size, 1), 0)
        closed[at, :] = jnp.where(row < length, reduce.total[at, :] + d_mid[at, :], 0.0).astype(BF16)

    over_rows(shard, 16, close)

    def send(phase, step, i, source, target):
        return pltpu.make_async_remote_copy(
            src_ref=source,
            dst_ref=target,
            send_sem=deal_send.at[phase, step, i],
            recv_sem=deal_recv.at[phase, step, i],
            device_id=(lax.rem(team.row + step, count), team.me),
            device_id_type=AT,
        )

    first = []
    for i, source in enumerate((layer, closed)):
        for step in range(1, count):
            other = lax.rem(team.row + step, count)
            copy = send(0, step, i, source.at[deal.at(other)], parked.at[team.row, i])
            copy.start()
            first.append(copy)
        parked[team.row, i] = source[deal.at(team.row)]
    for copy in first:
        copy.wait()
    mine = team.slot * shard
    second = []
    for i, target in enumerate((layer_out, input_grad)):
        for step in range(1, count):
            other = lax.rem(team.row + step, count)
            leaving[other, i] = parked[inverse[other], i]
            copy = send(1, step, i, leaving.at[other, i], target.at[deal.at(team.row, mine)])
            copy.start()
            second.append(copy)
        target[deal.at(team.row, mine)] = parked[inverse[team.row], i]
    for copy in second:
        copy.wait()
    for gather in gathers:
        gather.start()
    for gather in gathers:
        gather.half()
    for gather in gathers:
        gather.finish()


def close_layer(length, inverse, partial, d_mid, layer):
    rows, width = partial.shape
    shard = rows // SLOTS
    count = lax.axis_size("dp")
    deal = Deal(count, shard, width)
    chunk = (count, 2, deal.rows, deal.columns)
    return pl.pallas_call(
        finish_kernel,
        out_shape=shaped(((rows, width), BF16), ((rows, width), BF16)),
        in_specs=[SCALAR, SCALAR] + [ON_CHIP] * 3,
        out_specs=(ON_CHIP,) * 2,
        scratch_shapes=[
            pltpu.VMEM((shard, width), BF16),
            pltpu.VMEM(chunk, BF16),
            pltpu.VMEM(chunk, BF16),
            pltpu.SemaphoreType.DMA((2, count, 2)),
            pltpu.SemaphoreType.DMA((2, count, 2)),
        ]
        + Reduce.scratch(rows, width)
        + Gather.scratch * 2,
        compiler_params=pltpu.CompilerParams(
            collective_id=3, has_side_effects=True, vmem_limit_bytes=VMEM_CAP
        ),
        name="close_layer",
    )(length, inverse, partial, d_mid, layer)


SPLIT = 4
STEP = 256


class Wires:
    def __init__(self, send, recv):
        self.send, self.recv, self.used = send, recv, 0

    def book(self, number=1):
        self.used += number
        assert self.used <= self.send.shape[0]
        return self.used - number

    def copy(self, source, target, device, index):
        return pltpu.make_async_remote_copy(
            src_ref=source,
            dst_ref=target,
            send_sem=self.send.at[index],
            recv_sem=self.recv.at[index],
            device_id=device,
            device_id_type=AT,
        )


class Circle:
    def __init__(self, wires, blocks, following, sibling=None):
        steps = range(1, len(blocks))
        self.hops = [
            wires.copy(blocks[k - 1], blocks[k], following, wires.book()) for k in steps
        ]
        self.relays = []
        if sibling is not None:
            self.relays = [wires.copy(blocks[k], blocks[k], sibling, wires.book()) for k in steps]
        self.done = 0

    def start(self):
        self.hops[0].start()

    def pump(self):
        k = self.done
        if k == len(self.hops):
            return
        self.hops[k].wait_recv()
        if k + 1 < len(self.hops):
            self.hops[k + 1].start()
        if self.relays:
            self.relays[k].start()
        self.done += 1

    def drain(self):
        while self.done < len(self.hops):
            self.pump()
        for hop in self.hops:
            hop.wait_send()
        for relay in self.relays:
            relay.wait()


class Strips:
    def __init__(self, wires, grid, team, source, target, strip):
        rows = source.shape[0]
        half = at_rows(team.core * (rows // 2), rows // 2)
        self.sends, self.relays = [], []
        for step in range(1, grid.groups):
            group = lax.rem(grid.group + step, grid.groups)
            self.sends.append(
                wires.copy(
                    source.at[half, at_rows(group * strip, strip)],
                    target.at[step, half],
                    (group * grid.lanes + grid.lane, team.me),
                    wires.book(),
                )
            )
            self.relays.append(
                wires.copy(
                    target.at[step, half],
                    target.at[step, half],
                    (team.row, team.sibling),
                    wires.book(),
                )
            )

    def start(self):
        for send in self.sends:
            send.start()

    def relay(self):
        for send, relay in zip(self.sends, self.relays, strict=True):
            send.wait_recv()
            relay.start()

    def drain(self):
        for send, relay in zip(self.sends, self.relays, strict=True):
            send.wait_send()
            relay.wait()


def silu_parts(gate, upper):
    sig = jax.nn.sigmoid(gate)
    return sig, (gate * sig * upper).astype(BF16)


def silu_back(gate, upper, sig, d_inner):
    d_gate = (d_inner * upper * sig * (1.0 + gate * (1.0 - sig))).astype(BF16)
    return d_gate, (d_inner * gate * sig).astype(BF16)


def folded(field):
    return sum([field[8 * i : 8 * i + 8] for i in range(field.shape[0] // 8)])


def layer_kernel(names, *refs):
    m = types.SimpleNamespace(**dict(zip(names, refs, strict=True)))
    team, grid = Team(), Grid(lax.axis_size("dp"))
    wires = Wires(m.wire_send, m.wire_recv)
    count, groups, lanes = grid.count, grid.groups, grid.lanes
    rows, width = m.hid.shape
    local, hidden = m.mix.shape[1], m.gate.shape[1]
    shard, strip, tile = rows // SLOTS, width // groups, width // count
    every = groups * rows
    me = team.row

    loads = {}

    def load(name, source, target):
        loads[name] = pltpu.make_async_copy(source, target, m.load.at[len(loads)])
        loads[name].start()

    load("hid", m.hidden_in, m.hid)
    load("q", m.q_weight, m.qkv.at[0])
    load("k", m.k_weight, m.qkv.at[1])
    load("v", m.v_weight, m.qkv.at[2])
    load("grad", m.upstream.at[at_rows(team.slot * shard, shard)], m.closed)
    load("o", m.o_weight, m.wo)
    load("g", m.g_weight, m.wg)
    load("u", m.u_weight, m.wu)
    load("d", m.d_weight, m.wd)

    def peer(step):
        return lax.rem(me + step, count)

    barrier = pltpu.get_barrier_semaphore()
    for step in range(1, count):
        pl.semaphore_signal(barrier, inc=1, device_id=(peer(step), team.me), device_id_type=AT)
    for other in (team.sibling, team.across, team.far):
        pl.semaphore_signal(barrier, inc=1, device_id=(me, other), device_id_type=AT)
    pl.semaphore_wait(barrier, count + 2)

    length = m.lengths[m.order[me]]

    def holder(sequence):
        found = jnp.int32(0)
        for place in range(count):
            found = jnp.where(m.order[place] == sequence, place, found)
        return found

    following = (lax.rem(grid.group + 1, groups) * lanes + grid.lane, team.me)
    sums = RowSums(team, m.sum_mine, m.sum_came, m.sum_send, m.sum_recv)
    deal = Deal(count, shard, width)

    loads["grad"].wait()
    dealt = wires.book(2 * count)
    first = []
    for step in range(1, count):
        copy = wires.copy(
            m.closed.at[deal.at(peer(step))],
            m.back_parked.at[me, 0],
            (peer(step), team.me),
            dealt + step,
        )
        copy.start()
        first.append(copy)
    m.back_parked[me, 0] = m.closed[deal.at(me)]

    loads["hid"].wait()
    hidden_strips = Strips(wires, grid, team, m.hid, m.hid_strips, strip)
    hidden_strips.start()

    loads["q"].wait()
    q = matmul(m.hid[...], m.qkv[0])
    m.q_raw[...] = q
    loads["k"].wait()
    k = matmul(m.hid[...], m.qkv[1])
    m.k_raw[...] = k
    sums.start(row_sum(q * q), row_sum(k * k))
    loads["v"].wait()
    m.values[...] = matmul(m.hid[...], m.qkv[2]).astype(BF16)
    q_total, k_total = sums.finish()
    q_scale = lax.rsqrt(q_total * (1.0 / D) + EPS)
    k_scale = lax.rsqrt(k_total * (1.0 / D) + EPS)
    lane = lax.broadcasted_iota(jnp.int32, (rows, 128), 1)
    m.scales[...] = jnp.where(lane == 0, q_scale, k_scale)
    for head in range(local // HEAD):
        at = pl.ds(head * HEAD, HEAD)
        q = turn(m.q_raw[:, at] * q_scale * m.q_gain[:, at], m.cosine[...], m.sine[...]).astype(BF16)
        k = turn(m.k_raw[:, at] * k_scale * m.k_gain[:, at], m.cosine[...], m.sine[...]).astype(BF16)
        m.queries[:, at] = q
        m.keys[:, at] = k
        probs = head_probs(q, k, length).astype(BF16)
        m.mix[:, at] = matmul(probs, m.values[:, at]).astype(BF16)

    mix_circle = Circle(wires, [m.mix] + [m.mix_got.at[k] for k in range(1, groups)], following)
    mix_circle.start()

    for copy in first:
        copy.wait()
    for step in range(1, count):
        m.back_leaving[peer(step), 0] = m.back_parked[m.order[peer(step)], 0]
    m.grad_in[deal.at(me)] = m.back_parked[m.order[me], 0]
    second = []
    for step in range(1, count):
        copy = wires.copy(
            m.back_leaving.at[peer(step), 0],
            m.grad_in.at[deal.at(me)],
            (peer(step), team.me),
            dealt + count + step,
        )
        copy.start()
        second.append(copy)

    reduce = Reduce(
        team, m.partial, m.came, m.gone, m.total, m.reduce_send, m.reduce_recv
    )

    def gather(whole, number):
        return Gather(team, whole, m.gather_send.at[number], m.gather_recv.at[number])

    loads["o"].wait()

    def make_branch(at):
        m.partial[:, at] = matmul(m.mix[...], m.wo[:, at]).astype(BF16)

    reduce.run(make_branch)
    mix_circle.pump()
    hidden_strips.relay()
    own = m.mid_all.at[pl.ds(0, rows)]

    def whole_at(at):
        return pl.ds(pl.multiple_of(team.slot * shard + at.start, at.size), at.size)

    def norm_mid(at):
        part = m.total[at, :]
        m.branch[at, :] = part
        unit = part * lax.rsqrt(row_sum(part * part) * (1.0 / D) + EPS)
        mid = m.hid[whole_at(at), :].astype(F32) + m.a_gain[...] * unit
        m.mid_all[whole_at(at), :] = mid.astype(BF16)

    over_rows(shard, 16, norm_mid)
    mid_gather = gather(own, 0)
    mid_gather.start()

    def half_blocks(field):
        return [field.at[at_rows(k * rows + team.core * (rows // 2), rows // 2)] for k in range(groups)]

    mid_circle = Circle(wires, half_blocks(m.mid_all), following, (me, team.sibling))
    mid_gather.half()
    mid_circle.start()
    mid_gather.finish()
    mix_circle.pump()

    loads["g"].wait()
    loads["u"].wait()

    def widen(i, carry):
        at = at_rows(i * STEP, STEP)
        gate = matmul(m.mid_all[0:rows], m.wg[:, at])
        upper = matmul(m.mid_all[0:rows], m.wu[:, at])
        m.gate[:, at] = gate.astype(BF16)
        m.upper[:, at] = upper.astype(BF16)
        m.inner[:, at] = silu_parts(gate, upper)[1]
        return carry

    lax.fori_loop(0, hidden // STEP, widen, 0)
    loads["d"].wait()

    def make_mlp(at):
        m.partial[:, at] = matmul(m.inner[...], m.wd[:, at]).astype(BF16)

    for copy in second:
        copy.wait()
    reduce.run(make_mlp, mid_circle.pump)
    m.stats[...] = jnp.zeros_like(m.stats)
    m.fold[...] = jnp.zeros_like(m.fold)

    def norm_mlp(at):
        part = m.total[at, :]
        scale = lax.rsqrt(row_sum(part * part) * (1.0 / D) + EPS)
        unit = part * scale
        base = m.branch[at, :]
        a_unit = base * lax.rsqrt(row_sum(base * base) * (1.0 / D) + EPS)
        attn_out = m.a_gain[...] * a_unit
        mlp_out = m.m_gain[...] * unit
        rows_f = m.hid[whole_at(at), :].astype(F32)
        row = team.slot * shard + at.start + lax.broadcasted_iota(jnp.int32, (at.size, 1), 0)
        live = row < length
        m.layer[at, :] = jnp.where(live, rows_f + attn_out + mlp_out, 0.0).astype(BF16)
        grad = jnp.where(live, m.grad_in[at, :].astype(F32), 0.0)
        m.fold[0] += folded(grad * unit)
        for i, field in enumerate((rows_f, attn_out, mlp_out)):
            m.fold[i + 1] += folded(jnp.where(live, field * field, 0.0))
        scaled = grad * m.m_gain[...]
        back = scale * (scaled - unit * (row_sum(scaled * unit) * (1.0 / D)))
        m.dm_all[whole_at(at), :] = back.astype(BF16)

    over_rows(shard, 16, norm_mlp)
    dm_gather = gather(m.dm_all.at[pl.ds(0, rows)], 1)
    dm_gather.start()
    dm_circle = Circle(wires, half_blocks(m.dm_all), following, (me, team.sibling))
    dm_gather.half()
    dm_circle.start()
    m.stats[0:1, :] = jnp.sum(m.fold[0], axis=0, keepdims=True)
    for i in range(3):
        m.stats[3 + i : 4 + i, :] = jnp.sum(m.fold[i + 1], axis=0, keepdims=True)
    dm_gather.finish()
    mid_circle.pump()

    def narrow(i, carry):
        at = at_rows(i * STEP, STEP)
        d_inner = right_inner(m.dm_all[0:rows], m.wd[at, :])
        gate = m.gate[:, at].astype(F32)
        upper = m.upper[:, at].astype(F32)
        m.gate[:, at], m.upper[:, at] = silu_back(gate, upper, jax.nn.sigmoid(gate), d_inner)
        return carry

    lax.fori_loop(0, hidden // STEP, narrow, 0)

    def make_d_mid(at):
        m.partial[:, at] = (
            right_inner(m.gate[...], m.wg[at, :]) + right_inner(m.upper[...], m.wu[at, :])
        ).astype(BF16)

    reduce.run(make_d_mid, dm_circle.pump)
    m.fold[0] = jnp.zeros_like(m.fold[0])

    def norm_d_mid(at):
        row = team.slot * shard + at.start + lax.broadcasted_iota(jnp.int32, (at.size, 1), 0)
        grad = jnp.where(row < length, m.grad_in[at, :].astype(F32), 0.0) + m.total[at, :]
        m.d_mid[at, :] = grad
        base = m.branch[at, :]
        scale = lax.rsqrt(row_sum(base * base) * (1.0 / D) + EPS)
        unit = base * scale
        m.fold[0] += folded(grad * unit)
        scaled = grad * m.a_gain[...]
        back = scale * (scaled - unit * (row_sum(scaled * unit) * (1.0 / D)))
        m.d_branch[whole_at(at), :] = back.astype(BF16)

    over_rows(shard, 16, norm_d_mid)
    d_gather = gather(m.d_branch, 2)
    d_gather.start()
    m.stats[1:2, :] = jnp.sum(m.fold[0], axis=0, keepdims=True)
    mix_circle.pump()
    mid_circle.pump()
    d_gather.half()
    d_gather.finish()
    branch_strips = Strips(wires, grid, team, m.d_branch, m.branch_strips, strip)
    branch_strips.start()

    d_mix = m.partial.at[:, pl.ds(0, local)]
    d_mix[...] = right_inner(m.d_branch[...], m.wo[...]).astype(BF16)
    q_scale = m.scales[:, 0:1]
    k_scale = m.scales[:, 1:2]
    q_inner = jnp.zeros((rows, 1), F32)
    k_inner = jnp.zeros((rows, 1), F32)
    shrink = 1.0 / math.sqrt(HEAD)
    for head in range(local // HEAD):
        at = pl.ds(head * HEAD, HEAD)
        q, k, v, back = m.queries[:, at], m.keys[:, at], m.values[:, at], d_mix[:, at]
        probs = head_probs(q, k, length)
        d_probs = right_inner(back, v)
        d_scores = (probs * (d_probs - row_sum(probs * d_probs))).astype(BF16)
        m.d_heads[:, pl.ds(2 * local + head * HEAD, HEAD)] = left_inner(
            probs.astype(BF16), back
        ).astype(BF16)
        d_q_hat = turn(matmul(d_scores, k) * shrink, m.cosine[...], -m.sine[...])
        d_k_hat = turn(left_inner(d_scores, q) * shrink, m.cosine[...], -m.sine[...])
        q_unit = m.q_raw[:, at] * q_scale
        k_unit = m.k_raw[:, at] * k_scale
        m.stats[2:3, at] = jnp.sum(d_q_hat * q_unit, axis=0, keepdims=True)
        m.stats[2:3, pl.ds(local + head * HEAD, HEAD)] = jnp.sum(d_k_hat * k_unit, axis=0, keepdims=True)
        q_scaled = d_q_hat * m.q_gain[:, at]
        k_scaled = d_k_hat * m.k_gain[:, at]
        m.stage[0, :, at] = q_scaled
        m.stage[1, :, at] = k_scaled
        q_inner += row_sum(q_scaled * q_unit)
        k_inner += row_sum(k_scaled * k_unit)
    sums.start(q_inner, k_inner)
    dm_circle.pump()
    q_inner, k_inner = sums.finish()
    for i, (raw, scale, inner) in enumerate(
        ((m.q_raw, q_scale, q_inner), (m.k_raw, k_scale, k_inner))
    ):
        factor = scale * scale * inner * (1.0 / D)
        m.d_heads[:, pl.ds(i * local, local)] = (
            scale * m.stage[i] - raw[...] * factor
        ).astype(BF16)
    heads_circle = Circle(
        wires, [m.d_heads] + [m.heads_got.at[k] for k in range(1, groups)], following
    )
    heads_circle.start()

    m.stat_team[team.me] = m.stats[...]
    stat_at = wires.book(3 + count)
    stat_team = [
        wires.copy(m.stats, m.stat_team.at[team.me], (me, other), stat_at + i)
        for i, other in enumerate((team.sibling, team.across, team.far))
    ]
    for copy in stat_team:
        copy.start()

    def make_input(at):
        m.partial[:, at] = (
            right_inner(m.d_heads[:, 0:local], m.qkv[0, at, :])
            + right_inner(m.d_heads[:, local : 2 * local], m.qkv[1, at, :])
            + right_inner(m.d_heads[:, 2 * local : 3 * local], m.qkv[2, at, :])
        ).astype(BF16)

    mid_circle.drain()
    dm_circle.drain()
    for k in range(groups):
        m.mid_turned[:, pl.ds(k * rows, rows)] = jnp.transpose(
            m.mid_all[pl.ds(k * rows, rows), at_rows(grid.group * strip, strip)]
        )
    crossed = wires.book(3 * (hidden // STEP))
    crossing = (grid.group * lanes + (1 - grid.lane), team.me)

    def tile_of(lane):
        return at_rows((grid.group * lanes + lane) * tile, tile)

    def crossings(n):
        at = at_rows(n * STEP, STEP)
        spare = pl.ds(every, tile)
        return [
            wires.copy(m.wg.at[spare, at], m.x_gate.at[:, at], crossing, crossed + 3 * n),
            wires.copy(m.wu.at[spare, at], m.x_up.at[:, at], crossing, crossed + 3 * n + 1),
            wires.copy(m.wd.at[at, spare], m.x_down.at[at, :], crossing, crossed + 3 * n + 2),
        ]

    def again(n, carry):
        at = at_rows(n * STEP, STEP)
        results = []
        for k in range(1, groups):
            block = pl.ds(k * rows, rows)
            gate = matmul(m.mid_all[block, :], m.wg[:, at])
            upper = matmul(m.mid_all[block, :], m.wu[:, at])
            d_inner = right_inner(m.dm_all[block, :], m.wd[at, :])
            sig, inner = silu_parts(gate, upper)
            kept = pl.ds((k - 1) * rows, rows)
            m.keep[0, kept, :] = inner
            m.keep[1, kept, :], m.keep[2, kept, :] = silu_back(gate, upper, sig, d_inner)
        whole = pl.ds(rows, every - rows)
        m.wg[0:rows, at] = m.gate[:, at]
        m.wu[0:rows, at] = m.upper[:, at]
        m.wd[at, 0:rows] = jnp.transpose(m.inner[:, at])
        m.wg[whole, at] = m.keep[1]
        m.wu[whole, at] = m.keep[2]
        for k in range(1, groups):
            kept = pl.ds((k - 1) * rows, rows)
            m.wd[at, pl.ds(k * rows, rows)] = jnp.transpose(m.keep[0, kept, :])
        turned = m.mid_turned[at_rows((1 - grid.lane) * tile, tile), :]
        spare = pl.ds(every, tile)
        m.wg[spare, at] = matmul(turned, m.wg[0:every, at]).astype(BF16)
        m.wu[spare, at] = matmul(turned, m.wu[0:every, at]).astype(BF16)
        m.wd[at, spare] = matmul(m.wd[at, 0:every], m.dm_all[:, tile_of(1 - grid.lane)]).astype(BF16)
        for copy in crossings(n):
            copy.start()
        return carry

    def redo(start, stop):
        lax.fori_loop(start, stop, again, 0)

    tiles = hidden // STEP
    reduce.run(make_input, lambda: redo(0, tiles // 4))
    for copy in stat_team:
        copy.wait()
    total = (m.stat_team[0] + m.stat_team[1]) + (m.stat_team[2] + m.stat_team[3])
    line = lax.broadcasted_iota(jnp.int32, total.shape, 0)
    m.stats[...] = jnp.where(line == 2, m.stats[...], total)
    m.stat_dp[me] = m.stats[...]
    stat_dp = [
        wires.copy(m.stats, m.stat_dp.at[me], (peer(step), team.me), stat_at + 2 + step)
        for step in range(1, count)
    ]
    for copy in stat_dp:
        copy.start()

    def close(at):
        row = team.slot * shard + at.start + lax.broadcasted_iota(jnp.int32, (at.size, 1), 0)
        m.closed[at, :] = jnp.where(row < length, m.total[at, :] + m.d_mid[at, :], 0.0).astype(BF16)

    over_rows(shard, 16, close)
    heads_circle.pump()
    branch_strips.relay()

    returned = wires.book(4 * count)
    first = []
    for i, source in enumerate((m.layer, m.closed)):
        for step in range(1, count):
            copy = wires.copy(
                source.at[deal.at(peer(step))],
                m.back_parked.at[me, i],
                (peer(step), team.me),
                returned + i * count + step,
            )
            copy.start()
            first.append(copy)
        m.back_parked[me, i] = source[deal.at(me)]
    redo(tiles // 4, tiles // 2)
    for copy in first:
        copy.wait()
    second = []
    for step in range(count):
        place = holder(peer(step))
        for i, target in enumerate((m.layer_out, m.input_grad)):
            m.back_leaving[peer(step), i] = m.back_parked[place, i]
            if step:
                copy = wires.copy(
                    m.back_leaving.at[peer(step), i],
                    target.at[deal.at(me, team.slot * shard)],
                    (peer(step), team.me),
                    returned + (2 + i) * count + step,
                )
            else:
                copy = pltpu.make_async_copy(
                    m.back_leaving.at[me, i],
                    target.at[deal.at(me, team.slot * shard)],
                    m.put.at[i],
                )
            copy.start()
            second.append(copy)
    redo(tiles // 2, 3 * tiles // 4)
    heads_circle.pump()
    for copy in second:
        copy.wait()
    out_gathers = [gather(m.layer_out, 3), gather(m.input_grad, 4)]
    for one in out_gathers:
        one.start()
    redo(3 * tiles // 4, tiles)
    for one in out_gathers:
        one.half()
    for one in out_gathers:
        one.finish()
    for copy in stat_dp:
        copy.wait()
    m.stat_out[...] = sum([m.stat_dp[i] for i in range(1, count)], m.stat_dp[0])

    def put(source, target, index):
        return pltpu.make_async_copy(source, target, m.put.at[index])

    puts = []

    def store(value, target, tall=False):
        index = len(puts)
        slot = sum(kind == tall for kind, _ in puts) % 2
        stage = m.tall if tall else m.stage
        older = [copy for kind, copy in puts if kind == tall]
        if len(older) >= 2:
            older[-2].wait()
        stage[slot] = value
        copy = put(stage.at[slot], target, 2 + 2 * tall + slot)
        copy.start()
        puts.append((tall, copy))

    turned_own = m.mid_turned.at[at_rows(grid.lane * tile, tile)]
    wide = m.stage.shape[2]
    for weight, target in ((m.wg, m.g_own), (m.wu, m.u_own)):
        for i in range(hidden // wide):
            at = pl.ds(i * wide, wide)
            store(matmul(turned_own[...], weight[0:every, at]), target.at[:, at])
    high = m.tall.shape[1]
    for i in range(hidden // high):
        at = pl.ds(i * high, high)
        store(matmul(m.wd[at, 0:every], m.dm_all[:, tile_of(grid.lane)]), m.d_own.at[at, :], True)

    heads_circle.pump()
    heads_circle.drain()
    mix_circle.drain()
    hidden_strips.drain()
    branch_strips.drain()
    late = []

    def bring(source, target):
        copy = pltpu.make_async_copy(source, target, m.late.at[len(late)])
        copy.start()
        late.append(copy)

    mine = at_rows(grid.group * strip, strip)
    heads_at, strips_at = pl.ds(0, 3 * local), pl.ds(3 * local, strip)
    for k in range(groups):
        block = pl.ds(k * rows, rows)
        bring(m.heads_got.at[k] if k else m.d_heads, m.mid_all.at[block, heads_at])
        bring(m.hid_strips.at[k] if k else m.hid.at[:, mine], m.mid_all.at[block, strips_at])
        bring(m.mix_got.at[k] if k else m.mix, m.qkv.at[0, block, :])
        bring(m.branch_strips.at[k] if k else m.d_branch.at[:, mine], m.qkv.at[1, block, pl.ds(0, strip)])
    for copy in late:
        copy.wait()

    def lane_of(lane):
        return at_rows(lane * tile, tile)

    other, this = 1 - grid.lane, grid.lane
    last = wires.book(4)
    finals = []
    strips_ref = m.mid_all.at[:, strips_at]
    for i, target in enumerate((m.x_q, m.x_k, m.x_v)):
        spare = m.qkv.at[2, pl.ds(i * tile, tile)]
        spare[...] = left_inner(
            strips_ref[:, lane_of(other)], m.mid_all[:, i * local : (i + 1) * local]
        ).astype(BF16)
        finals.append(wires.copy(spare, target, crossing, last + i))
        finals[-1].start()
    spare = m.qkv.at[2, pl.ds(3 * tile, local), pl.ds(0, tile)]
    spare[...] = left_inner(m.qkv[0, 0:every, :], m.qkv[1, 0:every, lane_of(other)]).astype(BF16)
    finals.append(wires.copy(spare, m.x_o, crossing, last + 3))
    finals[-1].start()
    for i, target in enumerate((m.q_own, m.k_own, m.v_own)):
        store(
            left_inner(strips_ref[:, lane_of(this)], m.mid_all[:, i * local : (i + 1) * local]), target
        )
    output = left_inner(m.qkv[0, 0:every, :], m.qkv[1, 0:every, lane_of(this)])
    for i in range(local // high):
        store(output[i * high : (i + 1) * high], m.o_own.at[pl.ds(i * high, high), :], True)
    for kind in (False, True):
        for copy in [copy for tall, copy in puts if tall == kind][-2:]:
            copy.wait()

    def arrived(n, carry):
        for copy in crossings(n):
            copy.wait()
        return carry

    lax.fori_loop(0, tiles, arrived, 0)
    for copy in finals:
        copy.wait()


def whole_layer(grid, args):
    (hidden_in, upstream, lengths, order, q_weight, k_weight, v_weight, o_weight) = args[:8]
    (q_gain, k_gain, a_gain, g_weight, u_weight, d_weight, m_gain, cosine, sine) = args[8:]
    rows, width = hidden_in.shape
    local, hidden = q_weight.shape[1], g_weight.shape[1]
    count, groups = grid.count, grid.groups
    shard, strip, tile = rows // SLOTS, width // groups, width // count
    every = groups * rows
    deal = Deal(count, shard, width)
    chunk = (deal.rows, deal.columns)
    inputs = [
        ("lengths", SCALAR, lengths),
        ("order", SCALAR, order),
        ("hidden_in", ANY, hidden_in),
        ("upstream", ANY, upstream),
        ("q_weight", ANY, q_weight),
        ("k_weight", ANY, k_weight),
        ("v_weight", ANY, v_weight),
        ("o_weight", ANY, o_weight),
        ("g_weight", ANY, g_weight),
        ("u_weight", ANY, u_weight),
        ("d_weight", ANY, d_weight),
        ("q_gain", ON_CHIP, q_gain),
        ("k_gain", ON_CHIP, k_gain),
        ("a_gain", ON_CHIP, a_gain),
        ("m_gain", ON_CHIP, m_gain),
        ("cosine", ON_CHIP, cosine),
        ("sine", ON_CHIP, sine),
    ]
    outputs = [
        ("layer_out", (rows, width), BF16),
        ("input_grad", (rows, width), BF16),
        ("g_own", (tile, hidden), F32),
        ("u_own", (tile, hidden), F32),
        ("d_own", (hidden, tile), F32),
        ("q_own", (tile, local), F32),
        ("k_own", (tile, local), F32),
        ("v_own", (tile, local), F32),
        ("o_own", (local, tile), F32),
        ("x_gate", (tile, hidden), BF16),
        ("x_up", (tile, hidden), BF16),
        ("x_down", (hidden, tile), BF16),
        ("x_q", (tile, local), BF16),
        ("x_k", (tile, local), BF16),
        ("x_v", (tile, local), BF16),
        ("x_o", (local, tile), BF16),
        ("hid_strips", (groups, rows, strip), BF16),
        ("branch_strips", (groups, rows, strip), BF16),
        ("mix_got", (groups, rows, local), BF16),
        ("heads_got", (groups, rows, 3 * local), BF16),
        ("stat_out", (8, width), F32),
    ]
    wires = 160
    scratch = [
        ("qkv", pltpu.VMEM((3, width, local), BF16)),
        ("wo", pltpu.VMEM((local, width), BF16)),
        ("wg", pltpu.VMEM((width, hidden), BF16)),
        ("wu", pltpu.VMEM((width, hidden), BF16)),
        ("wd", pltpu.VMEM((hidden, width), BF16)),
        ("hid", pltpu.VMEM((rows, width), BF16)),
        ("mid_all", pltpu.VMEM((every, width), BF16)),
        ("dm_all", pltpu.VMEM((every, width), BF16)),
        ("gate", pltpu.VMEM((rows, hidden), BF16)),
        ("upper", pltpu.VMEM((rows, hidden), BF16)),
        ("inner", pltpu.VMEM((rows, hidden), BF16)),
        ("q_raw", pltpu.VMEM((rows, local), F32)),
        ("k_raw", pltpu.VMEM((rows, local), F32)),
        ("queries", pltpu.VMEM((rows, local), BF16)),
        ("keys", pltpu.VMEM((rows, local), BF16)),
        ("values", pltpu.VMEM((rows, local), BF16)),
        ("scales", pltpu.VMEM((rows, 128), F32)),
        ("mix", pltpu.VMEM((rows, local), BF16)),
        ("d_branch", pltpu.VMEM((rows, width), BF16)),
        ("d_heads", pltpu.VMEM((rows, 3 * local), BF16)),
        ("mid_turned", pltpu.VMEM((strip, every), BF16)),
        ("keep", pltpu.VMEM((3, every - rows, STEP), BF16)),
        ("stage", pltpu.VMEM((2, rows, local), F32)),
        ("tall", pltpu.VMEM((2, 256, tile), F32)),
        ("branch", pltpu.VMEM((shard, width), F32)),
        ("d_mid", pltpu.VMEM((shard, width), F32)),
        ("layer", pltpu.VMEM((shard, width), BF16)),
        ("closed", pltpu.VMEM((shard, width), BF16)),
        ("grad_in", pltpu.VMEM((shard, width), BF16)),
        ("back_parked", pltpu.VMEM((count, 2) + chunk, BF16)),
        ("back_leaving", pltpu.VMEM((count, 2) + chunk, BF16)),
        ("fold", pltpu.VMEM((4, 8, width), F32)),
        ("stats", pltpu.VMEM((8, width), F32)),
        ("stat_team", pltpu.VMEM((SLOTS, 8, width), F32)),
        ("stat_dp", pltpu.VMEM((count, 8, width), F32)),
        ("partial", pltpu.VMEM((rows, width), BF16)),
        ("came", pltpu.VMEM((3, shard, width), BF16)),
        ("gone", pltpu.VMEM((shard, width), BF16)),
        ("total", pltpu.VMEM((shard, width), F32)),
        ("sum_mine", pltpu.VMEM((8, rows), F32)),
        ("sum_came", pltpu.VMEM((3, 8, rows), F32)),
        ("sum_send", pltpu.SemaphoreType.DMA((3,))),
        ("sum_recv", pltpu.SemaphoreType.DMA((3,))),
        ("reduce_send", pltpu.SemaphoreType.DMA((3, SPLIT))),
        ("reduce_recv", pltpu.SemaphoreType.DMA((3, SPLIT))),
        ("gather_send", pltpu.SemaphoreType.DMA((5, 3))),
        ("gather_recv", pltpu.SemaphoreType.DMA((5, 3))),
        ("wire_send", pltpu.SemaphoreType.DMA((wires,))),
        ("wire_recv", pltpu.SemaphoreType.DMA((wires,))),
        ("load", pltpu.SemaphoreType.DMA((9,))),
        ("put", pltpu.SemaphoreType.DMA((6,))),
        ("late", pltpu.SemaphoreType.DMA((4 * groups,))),
    ]
    names = [entry[0] for entry in inputs + outputs + scratch]
    results = pl.pallas_call(
        functools.partial(layer_kernel, names),
        out_shape=shaped(*[entry[1:] for entry in outputs]),
        in_specs=[entry[1] for entry in inputs],
        out_specs=(ANY,) * (len(outputs) - 1) + (ON_CHIP,),
        scratch_shapes=[entry[1] for entry in scratch],
        compiler_params=pltpu.CompilerParams(
            collective_id=4, has_side_effects=True, vmem_limit_bytes=62 * 2**20
        ),
        name="whole_layer",
    )(*[entry[2] for entry in inputs])
    return dict(zip([entry[0] for entry in outputs], results, strict=True))


def body(
    hidden_in,
    upstream_grad,
    seq_lengths,
    position_order,
    query_weight,
    key_weight,
    value_weight,
    output_weight,
    query_gain,
    key_gain,
    attn_gain,
    gate_weight,
    up_weight,
    down_weight,
    mlp_gain,
):
    count = lax.axis_size("dp")
    ways = lax.axis_size("tensor")
    myself = lax.axis_index("dp")
    part = lax.axis_index("tensor")
    grid = Grid(count)
    index = jnp.arange(count, dtype=jnp.int32)
    inverse = jnp.sum(
        index[None, :] * (position_order[None, :] == index[:, None]).astype(jnp.int32), axis=1
    )
    rows = hidden_in.shape[1]
    width = hidden_in.shape[2]
    shard = rows // ways
    if grid.lanes == 2 and grid.groups * rows + width // count <= width:
        cosine, sine = rope_constants(rows, HEAD)
        found = whole_layer(
            grid,
            (
                hidden_in[0],
                upstream_grad[0],
                seq_lengths,
                position_order,
                query_weight,
                key_weight,
                value_weight,
                output_weight,
                query_gain[None],
                key_gain[None],
                attn_gain[None],
                gate_weight,
                up_weight,
                down_weight,
                mlp_gain[None],
                cosine,
                sine,
            ),
        )
        local = query_weight.shape[1]

        def joined(own, other):
            return found[own] + found[other].astype(F32)

        stats = found["stat_out"]
        squares = jnp.sum(stats[3:6], axis=1)
        return (
            found["layer_out"][None],
            found["input_grad"][None],
            joined("q_own", "x_q"),
            joined("k_own", "x_k"),
            joined("v_own", "x_v"),
            joined("o_own", "x_o"),
            stats[2, :local],
            stats[2, local : 2 * local],
            stats[1],
            joined("g_own", "x_gate"),
            joined("u_own", "x_up"),
            joined("d_own", "x_down"),
            stats[0],
            jnp.sqrt(squares / (jnp.sum(seq_lengths).astype(F32) * D)),
        )

    piece = shard // count
    seq_here = jnp.sum(jnp.where(index == myself, position_order, 0))
    length = jnp.sum(jnp.where(index == seq_here, seq_lengths, 0))[None]
    slot = part % 2 * 2 + part // 2

    def exchange(pieces):
        return lax.all_to_all(pieces, "dp", split_axis=0, concat_axis=0, tiled=True)

    def my_rows(field):
        return lax.dynamic_slice_in_dim(field, slot * shard, shard, axis=0)

    first = exchange(my_rows(upstream_grad[0]).reshape(count, piece, width))
    second = exchange(jnp.take(first, position_order, axis=0))
    grad_in = second.reshape(shard, width)

    rows_low = hidden_in[0]
    my_low = my_rows(rows_low)
    local = query_weight.shape[1]
    strip = width // grid.groups
    tile = width // count

    def strip_of(field, group):
        return lax.dynamic_slice_in_dim(field, group * strip, strip, axis=1)

    def strips(field):
        found = [strip_of(field, grid.group)]
        for step in range(1, grid.groups):
            found.append(
                grid.shift_groups(
                    strip_of(field, (grid.group + step) % grid.groups), step
                )
            )
        return jnp.concatenate(found, axis=0)

    def tile_of(field, lane):
        return lax.dynamic_slice_in_dim(field, lane * tile, tile, axis=1)

    def reduced(product, field):
        sent = []
        for step in range(1, grid.lanes):
            other = product(tile_of(field, (grid.lane + step) % grid.lanes)).astype(BF16)
            sent.append(grid.shift_lanes(other, step))
        mine = product(tile_of(field, grid.lane))
        for other in sent:
            mine = mine + other.astype(F32)
        return mine

    hidden_strips = strips(rows_low)

    cosine, sine = rope_tables(rows, HEAD)
    cosine = jnp.concatenate([cosine, cosine], axis=1)
    sine = jnp.concatenate([-sine, sine], axis=1)
    gains = (query_gain[None], key_gain[None])
    q_raw, k_raw, queries, keys, values, scales, attn_mix, branch, mid_low = attend(
        length,
        rows_low,
        my_low,
        (query_weight, key_weight, value_weight, output_weight),
        gains,
        cosine,
        sine,
        attn_gain[None],
    )
    mix_all = jnp.concatenate([attn_mix] + grid.ring(attn_mix), axis=0)
    mid_others = shared_ring(grid, mid_low)

    gate = matmul(mid_low, gate_weight)
    upper = matmul(mid_low, up_weight)
    sig = jax.nn.sigmoid(gate)
    inner = (gate * sig * upper).astype(BF16)
    layer, d_mlp, mlp_gain_part, squares = settle(
        length,
        matmul(inner, down_weight).astype(BF16),
        my_low,
        branch,
        grad_in,
        attn_gain[None],
        mlp_gain[None],
    )
    d_mlp_others = shared_ring(grid, d_mlp)

    def inner_back(gate, upper, d_mlp):
        d_inner = right_inner(d_mlp, down_weight)
        sig = jax.nn.sigmoid(gate)
        d_gate = (d_inner * upper * sig * (1.0 + gate * (1.0 - sig))).astype(BF16)
        d_up = (d_inner * gate * sig).astype(BF16)
        return d_gate, d_up

    d_gate, d_up = inner_back(gate, upper, d_mlp)
    d_mid, attn_gain_part, d_branch, d_heads, query_gain_part, key_gain_part = unattend(
        length,
        (right_inner(d_gate, gate_weight) + right_inner(d_up, up_weight)).astype(BF16),
        branch,
        grad_in,
        attn_gain[None],
        output_weight,
        (q_raw, k_raw, queries, keys, values, scales),
        gains,
        cosine,
        sine,
    )
    d_branch_strips = strips(d_branch)
    d_heads_all = jnp.concatenate([d_heads] + grid.ring(d_heads), axis=0)
    layer_out, input_grad = close_layer(
        length,
        inverse,
        (
            right_inner(d_heads[:, :local], query_weight)
            + right_inner(d_heads[:, local : 2 * local], key_weight)
            + right_inner(d_heads[:, 2 * local :], value_weight)
        ).astype(BF16),
        d_mid,
        layer,
    )

    gate_o = matmul(mid_others, gate_weight)
    upper_o = matmul(mid_others, up_weight)
    inner_o = (jax.nn.silu(gate_o) * upper_o).astype(BF16)
    d_gate_o, d_up_o = inner_back(gate_o, upper_o, d_mlp_others)

    def strip_all(own, others):
        return jnp.concatenate([strip_of(own, grid.group), strip_of(others, grid.group)], axis=0)

    mid_strips = strip_all(mid_low, mid_others)
    d_mlp_strips = strip_all(d_mlp, d_mlp_others)
    d_gate_all = jnp.concatenate([d_gate, d_gate_o], axis=0)
    d_up_all = jnp.concatenate([d_up, d_up_o], axis=0)
    inner_all = jnp.concatenate([inner, inner_o], axis=0)
    gate_part = reduced(lambda tile: left_inner(tile, d_gate_all), mid_strips)
    up_part = reduced(lambda tile: left_inner(tile, d_up_all), mid_strips)
    down_part = reduced(lambda tile: left_inner(inner_all, tile), d_mlp_strips)
    output_part = reduced(lambda tile: left_inner(mix_all, tile), d_branch_strips)
    heads_part = reduced(lambda tile: left_inner(tile, d_heads_all), hidden_strips)
    query_part = heads_part[:, :local]
    key_part = heads_part[:, local : 2 * local]
    value_part = heads_part[:, 2 * local :]

    shared = jnp.concatenate(
        [jnp.sum(attn_gain_part, axis=0), jnp.sum(mlp_gain_part, axis=0), jnp.sum(squares, axis=(1, 2))]
    )
    shared = shared + sibling(shared)
    shared = shared + across(shared)
    sums = grid.total(jnp.concatenate([shared, query_gain_part[0], key_gain_part[0]]))
    attn_gain_grad = sums[:width]
    mlp_gain_grad = sums[width : 2 * width]
    squares = sums[2 * width : 2 * width + 3]
    query_gain_grad = sums[2 * width + 3 : 2 * width + 3 + local]
    key_gain_grad = sums[2 * width + 3 + local :]
    rms_values = jnp.sqrt(squares / (jnp.sum(seq_lengths).astype(F32) * D))

    return (
        layer_out[None],
        input_grad[None],
        query_part,
        key_part,
        value_part,
        output_part,
        query_gain_grad,
        key_gain_grad,
        attn_gain_grad,
        gate_part,
        up_part,
        down_part,
        mlp_gain_grad,
        rms_values,
    )


def solution(mesh):
    placed = (
        P("dp", None, None),
        P("dp", None, None),
        P(),
        P(),
        P(None, "tensor"),
        P(None, "tensor"),
        P(None, "tensor"),
        P("tensor", None),
        P("tensor"),
        P("tensor"),
        P(),
        P(None, "tensor"),
        P(None, "tensor"),
        P("tensor", None),
        P(),
    )
    return jax.shard_map(
        body,
        mesh=mesh,
        in_specs=placed,
        out_specs=(
            P("dp", None, None),
            P("dp", None, None),
            P("dp", "tensor"),
            P("dp", "tensor"),
            P("dp", "tensor"),
            P("tensor", "dp"),
            P("tensor"),
            P("tensor"),
            P(),
            P("dp", "tensor"),
            P("dp", "tensor"),
            P("tensor", "dp"),
            P(),
            P(),
        ),
        check_vma=False,
    )
```

```python
import functools
import math
import types

import jax
import jax.numpy as jnp
import numpy as np
from jax import lax
from jax.experimental import pallas as pl
from jax.experimental.pallas import tpu as pltpu
from jax.sharding import PartitionSpec as P

D = 2048
HEAD = 128
EPS = 1e-06
F32 = jnp.float32
BF16 = jnp.bfloat16


def matmul(left, right):
    return jnp.dot(left, right, preferred_element_type=F32)


def left_inner(left, right):
    return lax.dot_general(left, right, (((0,), (0,)), ((), ())), preferred_element_type=F32)


def right_inner(left, right):
    return lax.dot_general(left, right, (((1,), (1,)), ((), ())), preferred_element_type=F32)


def rope_tables(rows, width):
    places = jnp.arange(rows, dtype=F32)
    freq = jnp.power(F32(500000.0), -jnp.arange(width // 2, dtype=F32) * (2.0 / width))
    angle = places[:, None] * freq[None, :]
    return (jnp.cos(angle), jnp.sin(angle))


def rope_constants(rows, width):
    half = width // 2
    exponent = -np.arange(half, dtype=np.float32) * np.float32(2.0 / width)
    freq = np.power(np.float32(500000.0), exponent, dtype=np.float32)
    angle = (np.arange(rows, dtype=np.float32)[:, None] * freq[None, :]).astype(np.float64)
    cosine, sine = np.cos(angle), np.sin(angle)
    return (
        jnp.asarray(np.concatenate([cosine, cosine], axis=1), F32),
        jnp.asarray(np.concatenate([-sine, sine], axis=1), F32),
    )


class Grid:
    def __init__(self, count):
        self.count = count
        self.lanes = 2 ** ((count.bit_length() - 1) // 2)
        self.groups = count // self.lanes
        me = lax.axis_index("dp")
        self.group = me // self.lanes
        self.lane = me % self.lanes

    def shift_groups(self, field, step):
        pairs = [
            (g * self.lanes + a, ((g + step) % self.groups) * self.lanes + a)
            for g in range(self.groups)
            for a in range(self.lanes)
        ]
        return lax.ppermute(field, "dp", pairs)

    def shift_lanes(self, field, step):
        pairs = [
            (g * self.lanes + a, g * self.lanes + (a + step) % self.lanes)
            for g in range(self.groups)
            for a in range(self.lanes)
        ]
        return lax.ppermute(field, "dp", pairs)

    def ring(self, field):
        found = []
        for _ in range(self.groups - 1):
            field = self.shift_groups(field, 1)
            found.append(field)
        return found

    def total(self, field):
        step = 1
        while step < self.count:
            field = field + lax.ppermute(
                field, "dp", [(i, i ^ step) for i in range(self.count)]
            )
            step *= 2
        return field


def sibling(field):
    size = lax.axis_size("tensor")
    return lax.ppermute(field, "tensor", [(i, i ^ 1) for i in range(size)])


def across(field):
    size = lax.axis_size("tensor")
    return lax.ppermute(field, "tensor", [(i, (i + 2) % size) for i in range(size)])


def shared_ring(grid, rows_low):
    core = lax.axis_index("tensor") % 2
    half = rows_low.shape[0] // 2
    mine = lax.dynamic_slice_in_dim(rows_low, core * half, half, axis=0)
    pieces = []
    for piece in grid.ring(mine):
        pieces += [piece, sibling(piece)]
    return jnp.concatenate(pieces, axis=0)


SLOTS = 4
TILES = 4
AT = pl.DeviceIdType.MESH
VMEM_CAP = 56 * 2**20


class Team:
    def __init__(self):
        self.row = lax.axis_index("dp")
        self.me = lax.axis_index("tensor")
        self.side = self.me // 2
        self.core = self.me % 2
        self.slot = self.core * 2 + self.side
        self.sibling = self.side * 2 + (1 - self.core)
        self.across = (1 - self.side) * 2 + self.core
        self.far = (1 - self.side) * 2 + (1 - self.core)

    def meet(self, *others):
        barrier = pltpu.get_barrier_semaphore()
        for other in others:
            pl.semaphore_signal(barrier, inc=1, device_id=(self.row, other), device_id_type=AT)
        pl.semaphore_wait(barrier, len(others))

    def copy(self, source, target, send, recv, other):
        return pltpu.make_async_remote_copy(
            src_ref=source,
            dst_ref=target,
            send_sem=send,
            recv_sem=recv,
            device_id=(self.row, other),
            device_id_type=AT,
        )


def at_rows(start, size):
    return pl.ds(pl.multiple_of(start, size), size)


class Reduce:
    def scratch(rows, width):
        shard = rows // SLOTS
        return [
            pltpu.VMEM((rows, width), BF16),
            pltpu.VMEM((3, shard, width), BF16),
            pltpu.VMEM((shard, width), BF16),
            pltpu.VMEM((shard, width), F32),
            pltpu.SemaphoreType.DMA((3, TILES)),
            pltpu.SemaphoreType.DMA((3, TILES)),
        ]

    def __init__(self, team, partial, came, gone, total, send, recv):
        self.team, self.partial, self.came, self.gone, self.total = team, partial, came, gone, total
        self.shard, width = total.shape
        self.tiles = send.shape[1]
        self.tile = width // self.tiles
        self.send, self.recv = send, recv
        self.copies = {}

    def columns(self, tile):
        return pl.ds(tile * self.tile, self.tile)

    def block(self, core, side):
        return at_rows((core * 2 + side) * self.shard, self.shard)

    def launch(self, kind, tile, source, other):
        copy = self.team.copy(
            source,
            self.came.at[kind, :, self.columns(tile)],
            self.send.at[kind, tile],
            self.recv.at[kind, tile],
            other,
        )
        copy.start()
        self.copies[kind, tile] = copy

    def offer(self, tile):
        team, columns = self.team, self.columns(tile)
        for kind, side in ((0, 1 - team.side), (1, team.side)):
            self.launch(
                kind, tile, self.partial.at[self.block(1 - team.core, side), columns], team.sibling
            )

    def pass_on(self, tile):
        team, columns = self.team, self.columns(tile)
        self.copies[0, tile].wait_recv()
        mine = self.partial[self.block(team.core, 1 - team.side), columns].astype(F32)
        self.gone[:, columns] = (mine + self.came[0, :, columns].astype(F32)).astype(BF16)
        self.launch(2, tile, self.gone.at[:, columns], team.across)

    def finish(self, tile):
        team, columns = self.team, self.columns(tile)
        self.copies[1, tile].wait_recv()
        mine = self.partial[self.block(team.core, team.side), columns].astype(F32)
        mine = mine + self.came[1, :, columns].astype(F32)
        self.copies[2, tile].wait_recv()
        self.total[:, columns] = mine + self.came[2, :, columns].astype(F32)

    def settle(self):
        for copy in self.copies.values():
            copy.wait_send()

    def begin(self, make):
        self.copies = {}
        for tile in range(self.tiles):
            make(self.columns(tile))
            self.offer(tile)
            if tile:
                self.pass_on(tile - 1)
        self.pass_on(self.tiles - 1)

    def end(self):
        for tile in range(self.tiles):
            self.finish(tile)
        self.settle()

    def run(self, make):
        self.begin(make)
        self.end()


class Gather:
    scratch = [pltpu.SemaphoreType.DMA((3,)), pltpu.SemaphoreType.DMA((3,))]

    def __init__(self, team, whole, send, recv):
        self.team, self.whole = team, whole
        shard = whole.shape[0] // SLOTS
        mine = whole.at[at_rows(team.slot * shard, shard)]
        theirs = whole.at[at_rows((team.core * 2 + 1 - team.side) * shard, shard)]
        self.across = team.copy(mine, mine, send.at[0], recv.at[0], team.across)
        self.near = team.copy(mine, mine, send.at[1], recv.at[1], team.sibling)
        self.relay = team.copy(theirs, theirs, send.at[2], recv.at[2], team.sibling)

    def start(self):
        self.across.start()
        self.near.start()

    def half(self):
        self.across.wait_recv()
        self.relay.start()

    def finish(self):
        self.across.wait_send()
        self.near.wait()
        self.relay.wait()


class RowSums:
    def scratch(rows):
        return [
            pltpu.VMEM((8, rows), F32),
            pltpu.VMEM((3, 8, rows), F32),
            pltpu.SemaphoreType.DMA((3,)),
            pltpu.SemaphoreType.DMA((3,)),
        ]

    def __init__(self, team, mine, came, send, recv):
        self.team, self.mine, self.came = team, mine, came
        self.copies = [
            team.copy(mine, came.at[i], send.at[i], recv.at[i], other)
            for i, other in enumerate((team.sibling, team.across, team.far))
        ]

    def start(self, first, second):
        rows = first.shape[0]
        lane = lax.broadcasted_iota(jnp.int32, (rows, 128), 1)
        both = jnp.where(lane == 0, first, jnp.where(lane == 1, second, 0.0))
        self.mine[...] = jnp.transpose(both)[:8]
        for copy in self.copies:
            copy.start()

    def finish(self):
        for copy in self.copies:
            copy.wait()
        total = self.mine[...] + self.came[0] + (self.came[1] + self.came[2])
        rows = total.shape[1]
        wide = jnp.transpose(jnp.concatenate([total] * 16, axis=0))
        return wide[:, 0:1], wide[:, 1:2]


def turn(field, cosine, sine):
    return field * cosine + pltpu.roll(field, HEAD // 2, 1) * sine


def head_probs(queries, keys, length):
    rows = queries.shape[0]
    scores = right_inner(queries, keys) * (1.0 / math.sqrt(HEAD))
    row = lax.broadcasted_iota(jnp.int32, (rows, rows), 0)
    column = lax.broadcasted_iota(jnp.int32, (rows, rows), 1)
    masked = jnp.where((column <= row) & (column < length), scores, -1e30)
    expo = jnp.exp(masked - jnp.max(masked, axis=-1, keepdims=True))
    return expo / jnp.sum(expo, axis=-1, keepdims=True)


def row_sum(field):
    return jnp.sum(field, axis=-1, keepdims=True)


def over_rows(count, step, work):
    def one(i, carry):
        work(pl.ds(pl.multiple_of(i * step, step), step))
        return carry

    lax.fori_loop(0, count // step, one, 0)


def attend_kernel(
    length_ref,
    hidden,
    mine_hidden,
    q_weight,
    k_weight,
    v_weight,
    o_weight,
    q_gain,
    k_gain,
    cosine,
    sine,
    a_gain,
    q_raw,
    k_raw,
    queries,
    keys,
    values,
    scales,
    mix,
    branch,
    mid_low,
    weights,
    out_weight,
    load,
    *scratch,
):
    team = Team()
    sums = RowSums(team, *scratch[0:4])
    reduce = Reduce(team, *scratch[4:10])
    gather = Gather(team, mid_low, *scratch[10:12])
    loads = [
        pltpu.make_async_copy(source, weights.at[i], load.at[i])
        for i, source in enumerate((q_weight, k_weight, v_weight))
    ] + [pltpu.make_async_copy(o_weight, out_weight, load.at[3])]
    for one in loads:
        one.start()
    team.meet(team.sibling, team.across, team.far)
    rows, local = mix.shape
    width = mid_low.shape[1]
    length = length_ref[0]

    def project(i):
        loads[i].wait()
        return matmul(hidden[...], weights[i])

    q = project(0)
    q_raw[...] = q
    k = project(1)
    k_raw[...] = k
    sums.start(row_sum(q * q), row_sum(k * k))
    values[...] = project(2).astype(BF16)
    q_total, k_total = sums.finish()
    q_scale = lax.rsqrt(q_total * (1.0 / D) + EPS)
    k_scale = lax.rsqrt(k_total * (1.0 / D) + EPS)
    lane = lax.broadcasted_iota(jnp.int32, (rows, 128), 1)
    scales[...] = jnp.where(lane == 0, q_scale, k_scale)
    for head in range(local // HEAD):
        at = pl.ds(head * HEAD, HEAD)
        q = turn(q_raw[:, at] * q_scale * q_gain[:, at], cosine[...], sine[...]).astype(BF16)
        k = turn(k_raw[:, at] * k_scale * k_gain[:, at], cosine[...], sine[...]).astype(BF16)
        queries[:, at] = q
        keys[:, at] = k
        probs = head_probs(q, k, length).astype(BF16)
        mix[:, at] = matmul(probs, values[:, at]).astype(BF16)
    loads[3].wait()

    def make(at):
        reduce.partial[:, at] = matmul(mix[...], out_weight[:, at]).astype(BF16)

    reduce.run(make)
    shard = reduce.shard

    def norm(at):
        part = reduce.total[at, :]
        branch[at, :] = part
        unit = part * lax.rsqrt(row_sum(part * part) * (1.0 / D) + EPS)
        mid = mine_hidden[at, :].astype(F32) + a_gain[...] * unit
        whole_at = pl.ds(pl.multiple_of(team.slot * shard + at.start, at.size), at.size)
        mid_low[whole_at, :] = mid.astype(BF16)

    over_rows(shard, 16, norm)
    gather.start()
    gather.half()
    gather.finish()


ANY = pl.BlockSpec(memory_space=pl.ANY)
ON_CHIP = pl.BlockSpec(memory_space=pltpu.VMEM)
SCALAR = pl.BlockSpec(memory_space=pltpu.SMEM)


def shaped(*pairs):
    return tuple(jax.ShapeDtypeStruct(shape, kind) for shape, kind in pairs)


def attend(length, hidden, mine_hidden, weights, gains, cosine, sine, a_gain):
    rows, width = hidden.shape
    local = weights[0].shape[1]
    shard = rows // SLOTS
    return pl.pallas_call(
        attend_kernel,
        out_shape=shaped(
            ((rows, local), F32),
            ((rows, local), F32),
            ((rows, local), BF16),
            ((rows, local), BF16),
            ((rows, local), BF16),
            ((rows, 128), F32),
            ((rows, local), BF16),
            ((shard, width), F32),
            ((rows, width), BF16),
        ),
        in_specs=[SCALAR, ON_CHIP, ON_CHIP] + [ANY] * 4 + [ON_CHIP] * 5,
        out_specs=(ON_CHIP,) * 9,
        scratch_shapes=[
            pltpu.VMEM((3, width, local), BF16),
            pltpu.VMEM((local, width), BF16),
            pltpu.SemaphoreType.DMA((4,)),
        ]
        + RowSums.scratch(rows)
        + Reduce.scratch(rows, width)
        + Gather.scratch,
        compiler_params=pltpu.CompilerParams(
            collective_id=0, has_side_effects=True, vmem_limit_bytes=VMEM_CAP
        ),
        name="attend",
    )(length, hidden, mine_hidden, *weights, *gains, cosine, sine, a_gain)


def settle_kernel(
    length_ref,
    partial_in,
    mine_hidden,
    branch,
    grad_in,
    a_gain,
    m_gain,
    layer,
    d_mlp,
    m_gain_part,
    squares,
    *scratch,
):
    team = Team()
    reduce = Reduce(team, *scratch[0:6])
    gather = Gather(team, d_mlp, *scratch[6:8])
    team.meet(team.sibling, team.across)

    def make(at):
        reduce.partial[:, at] = partial_in[:, at]

    reduce.run(make)
    shard = reduce.shard
    length = length_ref[0]
    m_gain_part[...] = jnp.zeros_like(m_gain_part)
    squares[...] = jnp.zeros_like(squares)

    def folded(field):
        return sum([field[8 * i : 8 * i + 8] for i in range(field.shape[0] // 8)])

    def norm(at):
        part = reduce.total[at, :]
        scale = lax.rsqrt(row_sum(part * part) * (1.0 / D) + EPS)
        unit = part * scale
        base = branch[at, :]
        a_unit = base * lax.rsqrt(row_sum(base * base) * (1.0 / D) + EPS)
        attn_out = a_gain[...] * a_unit
        mlp_out = m_gain[...] * unit
        rows_f = mine_hidden[at, :].astype(F32)
        row = team.slot * shard + at.start + lax.broadcasted_iota(jnp.int32, (at.size, 1), 0)
        live = row < length
        layer[at, :] = jnp.where(live, rows_f + attn_out + mlp_out, 0.0).astype(BF16)
        grad = jnp.where(live, grad_in[at, :].astype(F32), 0.0)
        m_gain_part[...] += folded(grad * unit)
        for i, field in enumerate((rows_f, attn_out, mlp_out)):
            squares[i] += folded(jnp.where(live, field * field, 0.0))
        scaled = grad * m_gain[...]
        back = scale * (scaled - unit * (row_sum(scaled * unit) * (1.0 / D)))
        whole_at = pl.ds(pl.multiple_of(team.slot * shard + at.start, at.size), at.size)
        d_mlp[whole_at, :] = back.astype(BF16)

    over_rows(shard, 16, norm)
    gather.start()
    gather.half()
    gather.finish()


def settle(length, partial, mine_hidden, branch, grad_in, a_gain, m_gain):
    rows, width = partial.shape
    shard = rows // SLOTS
    return pl.pallas_call(
        settle_kernel,
        out_shape=shaped(
            ((shard, width), BF16),
            ((rows, width), BF16),
            ((8, width), F32),
            ((3, 8, width), F32),
        ),
        in_specs=[SCALAR] + [ON_CHIP] * 6,
        out_specs=(ON_CHIP,) * 4,
        scratch_shapes=Reduce.scratch(rows, width) + Gather.scratch,
        compiler_params=pltpu.CompilerParams(
            collective_id=1, has_side_effects=True, vmem_limit_bytes=VMEM_CAP
        ),
        name="settle",
    )(length, partial, mine_hidden, branch, grad_in, a_gain, m_gain)


def unattend_kernel(
    length_ref,
    partial_in,
    branch,
    grad_in,
    a_gain,
    o_weight,
    q_raw,
    k_raw,
    queries,
    keys,
    values,
    scales,
    q_gain,
    k_gain,
    cosine,
    sine,
    d_mid,
    a_gain_part,
    d_branch,
    d_heads,
    q_gain_part,
    k_gain_part,
    out_weight,
    d_mix,
    d_q,
    d_k,
    load,
    *scratch,
):
    team = Team()
    sums = RowSums(team, *scratch[0:4])
    reduce = Reduce(team, *scratch[4:10])
    gather = Gather(team, d_branch, *scratch[10:12])
    fetch = pltpu.make_async_copy(o_weight, out_weight, load.at[0])
    fetch.start()
    team.meet(team.sibling, team.across, team.far)
    rows, local = queries.shape

    def make(at):
        reduce.partial[:, at] = partial_in[:, at]

    reduce.run(make)
    shard = reduce.shard
    length = length_ref[0]
    a_gain_part[...] = jnp.zeros_like(a_gain_part)

    def norm(at):
        row = team.slot * shard + at.start + lax.broadcasted_iota(jnp.int32, (at.size, 1), 0)
        grad = jnp.where(row < length, grad_in[at, :].astype(F32), 0.0) + reduce.total[at, :]
        d_mid[at, :] = grad
        base = branch[at, :]
        scale = lax.rsqrt(row_sum(base * base) * (1.0 / D) + EPS)
        unit = base * scale
        product = grad * unit
        a_gain_part[...] += sum([product[8 * i : 8 * i + 8] for i in range(at.size // 8)])
        scaled = grad * a_gain[...]
        back = scale * (scaled - unit * (row_sum(scaled * unit) * (1.0 / D)))
        whole_at = pl.ds(pl.multiple_of(team.slot * shard + at.start, at.size), at.size)
        d_branch[whole_at, :] = back.astype(BF16)

    over_rows(shard, 16, norm)
    gather.start()
    gather.half()
    gather.finish()
    fetch.wait()
    d_mix[...] = right_inner(d_branch[...], out_weight[...]).astype(BF16)
    q_scale = scales[:, 0:1]
    k_scale = scales[:, 1:2]
    q_inner = jnp.zeros((rows, 1), F32)
    k_inner = jnp.zeros((rows, 1), F32)
    shrink = 1.0 / math.sqrt(HEAD)
    for head in range(local // HEAD):
        at = pl.ds(head * HEAD, HEAD)
        q, k, v, back = queries[:, at], keys[:, at], values[:, at], d_mix[:, at]
        probs = head_probs(q, k, length)
        d_probs = right_inner(back, v)
        d_scores = (probs * (d_probs - row_sum(probs * d_probs))).astype(BF16)
        d_heads[:, pl.ds(2 * local + head * HEAD, HEAD)] = left_inner(
            probs.astype(BF16), back
        ).astype(BF16)
        d_q_hat = turn(matmul(d_scores, k) * shrink, cosine[...], -sine[...])
        d_k_hat = turn(left_inner(d_scores, q) * shrink, cosine[...], -sine[...])
        q_unit = q_raw[:, at] * q_scale
        k_unit = k_raw[:, at] * k_scale
        q_gain_part[:, at] = jnp.sum(d_q_hat * q_unit, axis=0, keepdims=True)
        k_gain_part[:, at] = jnp.sum(d_k_hat * k_unit, axis=0, keepdims=True)
        q_scaled = d_q_hat * q_gain[:, at]
        k_scaled = d_k_hat * k_gain[:, at]
        d_q[:, at] = q_scaled
        d_k[:, at] = k_scaled
        q_inner += row_sum(q_scaled * q_unit)
        k_inner += row_sum(k_scaled * k_unit)
    sums.start(q_inner, k_inner)
    q_inner, k_inner = sums.finish()
    for i, (grad, raw, scale, inner) in enumerate(
        ((d_q, q_raw, q_scale, q_inner), (d_k, k_raw, k_scale, k_inner))
    ):
        factor = scale * scale * inner * (1.0 / D)
        d_heads[:, pl.ds(i * local, local)] = (scale * grad[...] - raw[...] * factor).astype(BF16)


def unattend(
    length, partial, branch, grad_in, a_gain, o_weight, kept, gains, cosine, sine
):
    rows, width = partial.shape
    local = o_weight.shape[0]
    shard = rows // SLOTS
    return pl.pallas_call(
        unattend_kernel,
        out_shape=shaped(
            ((shard, width), F32),
            ((8, width), F32),
            ((rows, width), BF16),
            ((rows, 3 * local), BF16),
            ((1, local), F32),
            ((1, local), F32),
        ),
        in_specs=[SCALAR] + [ON_CHIP] * 4 + [ANY] + [ON_CHIP] * 10,
        out_specs=(ON_CHIP,) * 6,
        scratch_shapes=[
            pltpu.VMEM((local, width), BF16),
            pltpu.VMEM((rows, local), BF16),
            pltpu.VMEM((rows, local), F32),
            pltpu.VMEM((rows, local), F32),
            pltpu.SemaphoreType.DMA((1,)),
        ]
        + RowSums.scratch(rows)
        + Reduce.scratch(rows, width)
        + Gather.scratch,
        compiler_params=pltpu.CompilerParams(
            collective_id=2, has_side_effects=True, vmem_limit_bytes=VMEM_CAP
        ),
        name="unattend",
    )(length, partial, branch, grad_in, a_gain, o_weight, *kept, *gains, cosine, sine)


class Deal:
    def __init__(self, count, shard, width):
        self.count = count
        self.columns = max(128, width // count)
        self.across = width // self.columns
        self.rows = shard * self.across // count

    def at(self, chunk, base=0):
        return (
            at_rows(base + (chunk // self.across) * self.rows, self.rows),
            at_rows((chunk % self.across) * self.columns, self.columns),
        )


def finish_kernel(
    length_ref,
    inverse,
    partial_in,
    d_mid,
    layer,
    layer_out,
    input_grad,
    closed,
    parked,
    leaving,
    deal_send,
    deal_recv,
    *scratch,
):
    team = Team()
    reduce = Reduce(team, *scratch[0:6])
    gathers = [
        Gather(team, whole, *scratch[6 + 2 * i : 8 + 2 * i])
        for i, whole in enumerate((layer_out, input_grad))
    ]
    count = lax.axis_size("dp")
    shard, width = d_mid.shape
    deal = Deal(count, shard, width)
    barrier = pltpu.get_barrier_semaphore()
    for step in range(1, count):
        pl.semaphore_signal(
            barrier, inc=1, device_id=(lax.rem(team.row + step, count), team.me), device_id_type=AT
        )
    for other in (team.sibling, team.across):
        pl.semaphore_signal(barrier, inc=1, device_id=(team.row, other), device_id_type=AT)
    pl.semaphore_wait(barrier, count + 1)

    def make(at):
        reduce.partial[:, at] = partial_in[:, at]

    reduce.run(make)
    length = length_ref[0]

    def close(at):
        row = team.slot * shard + at.start + lax.broadcasted_iota(jnp.int32, (at.size, 1), 0)
        closed[at, :] = jnp.where(row < length, reduce.total[at, :] + d_mid[at, :], 0.0).astype(BF16)

    over_rows(shard, 16, close)

    def send(phase, step, i, source, target):
        return pltpu.make_async_remote_copy(
            src_ref=source,
            dst_ref=target,
            send_sem=deal_send.at[phase, step, i],
            recv_sem=deal_recv.at[phase, step, i],
            device_id=(lax.rem(team.row + step, count), team.me),
            device_id_type=AT,
        )

    first = []
    for i, source in enumerate((layer, closed)):
        for step in range(1, count):
            other = lax.rem(team.row + step, count)
            copy = send(0, step, i, source.at[deal.at(other)], parked.at[team.row, i])
            copy.start()
            first.append(copy)
        parked[team.row, i] = source[deal.at(team.row)]
    for copy in first:
        copy.wait()
    mine = team.slot * shard
    second = []
    for i, target in enumerate((layer_out, input_grad)):
        for step in range(1, count):
            other = lax.rem(team.row + step, count)
            leaving[other, i] = parked[inverse[other], i]
            copy = send(1, step, i, leaving.at[other, i], target.at[deal.at(team.row, mine)])
            copy.start()
            second.append(copy)
        target[deal.at(team.row, mine)] = parked[inverse[team.row], i]
    for copy in second:
        copy.wait()
    for gather in gathers:
        gather.start()
    for gather in gathers:
        gather.half()
    for gather in gathers:
        gather.finish()


def close_layer(length, inverse, partial, d_mid, layer):
    rows, width = partial.shape
    shard = rows // SLOTS
    count = lax.axis_size("dp")
    deal = Deal(count, shard, width)
    chunk = (count, 2, deal.rows, deal.columns)
    return pl.pallas_call(
        finish_kernel,
        out_shape=shaped(((rows, width), BF16), ((rows, width), BF16)),
        in_specs=[SCALAR, SCALAR] + [ON_CHIP] * 3,
        out_specs=(ON_CHIP,) * 2,
        scratch_shapes=[
            pltpu.VMEM((shard, width), BF16),
            pltpu.VMEM(chunk, BF16),
            pltpu.VMEM(chunk, BF16),
            pltpu.SemaphoreType.DMA((2, count, 2)),
            pltpu.SemaphoreType.DMA((2, count, 2)),
        ]
        + Reduce.scratch(rows, width)
        + Gather.scratch * 2,
        compiler_params=pltpu.CompilerParams(
            collective_id=3, has_side_effects=True, vmem_limit_bytes=VMEM_CAP
        ),
        name="close_layer",
    )(length, inverse, partial, d_mid, layer)


SPLIT = 4
STEP = 256


class Wires:
    def __init__(self, send, recv):
        self.send, self.recv, self.used = send, recv, 0

    def book(self, number=1):
        self.used += number
        assert self.used <= self.send.shape[0]
        return self.used - number

    def copy(self, source, target, device, index):
        return pltpu.make_async_remote_copy(
            src_ref=source,
            dst_ref=target,
            send_sem=self.send.at[index],
            recv_sem=self.recv.at[index],
            device_id=device,
            device_id_type=AT,
        )


class Spread:
    def __init__(self, wires, grid, team, source, field):
        shard = source.shape[0] // SLOTS
        mine = at_rows(team.slot * shard, shard)
        half = at_rows(team.core * 2 * shard, 2 * shard)
        self.hops, self.sides, self.pairs = {}, {}, {}
        for step in range(1, grid.groups):
            group = lax.rem(grid.group + step, grid.groups)
            block = field.at[step]
            self.hops[step] = wires.copy(
                source.at[mine],
                block.at[mine],
                (group * grid.lanes + grid.lane, team.me),
                wires.book(),
            )
            self.sides[step] = wires.copy(
                block.at[mine], block.at[mine], (team.row, team.across), wires.book()
            )
            self.pairs[step] = wires.copy(
                block.at[half], block.at[half], (team.row, team.sibling), wires.book()
            )
        near = sorted(self.hops, key=lambda step: min(step, grid.groups - step))
        self.plan = {"hop": list(near), "side": list(near), "pair": list(near)}

    def start(self):
        for step in self.plan["hop"]:
            self.hops[step].start()

    def side(self, number=1):
        for step in self.plan["side"][:number]:
            self.hops[step].wait_recv()
            self.sides[step].start()
        del self.plan["side"][:number]

    def pair(self, number=1):
        for step in self.plan["pair"][:number]:
            self.sides[step].wait_recv()
            self.pairs[step].start()
        del self.plan["pair"][:number]

    def drain(self):
        self.side(len(self.hops))
        self.pair(len(self.hops))
        for step in self.hops:
            self.hops[step].wait_send()
            self.sides[step].wait_send()
            self.pairs[step].wait()


def silu_parts(gate, upper):
    sig = jax.nn.sigmoid(gate)
    return sig, (gate * sig * upper).astype(BF16)


def silu_back(gate, upper, sig, d_inner):
    d_gate = (d_inner * upper * sig * (1.0 + gate * (1.0 - sig))).astype(BF16)
    return d_gate, (d_inner * gate * sig).astype(BF16)


def head_back(q, k, v, back, cosine, sine, length):
    probs = head_probs(q, k, length)
    low = probs.astype(BF16)
    mix = matmul(low, v).astype(BF16)
    d_probs = right_inner(back, v)
    d_scores = (probs * (d_probs - row_sum(probs * d_probs))).astype(BF16)
    shrink = 1.0 / math.sqrt(HEAD)
    return (
        mix,
        left_inner(low, back).astype(BF16),
        turn(matmul(d_scores, k) * shrink, cosine, -sine),
        turn(left_inner(d_scores, q) * shrink, cosine, -sine),
    )


def folded(field):
    return sum([field[8 * i : 8 * i + 8] for i in range(field.shape[0] // 8)])


def layer_kernel(names, *refs):
    m = types.SimpleNamespace(**dict(zip(names, refs, strict=True)))
    team, grid = Team(), Grid(lax.axis_size("dp"))
    wires = Wires(m.wire_send, m.wire_recv)
    count, groups, lanes = grid.count, grid.groups, grid.lanes
    rows, width = m.hid.shape
    local, hidden = m.mix.shape[1], m.gate.shape[1]
    shard, strip, tile = rows // SLOTS, width // groups, width // count
    every = groups * rows
    me = team.row

    loads = {}

    def load(name, source, target):
        loads[name] = pltpu.make_async_copy(source, target, m.load.at[len(loads)])
        loads[name].start()

    load("hid", m.hidden_in, m.hid)
    load("q", m.q_weight, m.qkv.at[0])
    load("k", m.k_weight, m.qkv.at[1])
    load("v", m.v_weight, m.qkv.at[2])
    load("grad", m.upstream.at[at_rows(team.slot * shard, shard)], m.closed)
    load("o", m.o_weight, m.wo)
    load("g", m.g_weight, m.wg)
    load("u", m.u_weight, m.wu)
    load("d", m.d_weight, m.wd)

    def peer(step):
        return lax.rem(me + step, count)

    barrier = pltpu.get_barrier_semaphore()
    for step in range(1, count):
        pl.semaphore_signal(barrier, inc=1, device_id=(peer(step), team.me), device_id_type=AT)
    for other in (team.sibling, team.across, team.far):
        pl.semaphore_signal(barrier, inc=1, device_id=(me, other), device_id_type=AT)
    pl.semaphore_wait(barrier, count + 2)

    length = m.lengths[m.order[me]]

    def holder(sequence):
        found = jnp.int32(0)
        for place in range(count):
            found = jnp.where(m.order[place] == sequence, place, found)
        return found

    following = (lax.rem(grid.group + 1, groups) * lanes + grid.lane, team.me)
    sums = RowSums(team, m.sum_mine, m.sum_came, m.sum_send, m.sum_recv)
    deal = Deal(count, shard, width)

    loads["grad"].wait()
    dealt = wires.book(2 * count)
    first = []
    for step in range(1, count):
        copy = wires.copy(
            m.closed.at[deal.at(peer(step))],
            m.back_parked.at[me, 0],
            (peer(step), team.me),
            dealt + step,
        )
        copy.start()
        first.append(copy)
    m.back_parked[me, 0] = m.closed[deal.at(me)]

    loads["hid"].wait()
    hid_spread = Spread(wires, grid, team, m.hid, m.hid_all)
    hid_spread.start()

    loads["q"].wait()
    q = matmul(m.hid[...], m.qkv[0])
    m.q_raw[...] = q
    loads["k"].wait()
    k = matmul(m.hid[...], m.qkv[1])
    m.k_raw[...] = k
    sums.start(row_sum(q * q), row_sum(k * k))
    loads["v"].wait()
    m.values[...] = matmul(m.hid[...], m.qkv[2]).astype(BF16)
    q_total, k_total = sums.finish()
    q_scale = lax.rsqrt(q_total * (1.0 / D) + EPS)
    k_scale = lax.rsqrt(k_total * (1.0 / D) + EPS)
    lane = lax.broadcasted_iota(jnp.int32, (rows, 128), 1)
    m.scales[...] = jnp.where(lane == 0, q_scale, k_scale)

    def attend_head(head, carry):
        at = at_rows(head * HEAD, HEAD)
        q = turn(m.q_raw[:, at] * q_scale * m.q_gain[:, at], m.cosine[...], m.sine[...]).astype(BF16)
        k = turn(m.k_raw[:, at] * k_scale * m.k_gain[:, at], m.cosine[...], m.sine[...]).astype(BF16)
        m.queries[:, at] = q
        m.keys[:, at] = k
        probs = head_probs(q, k, length).astype(BF16)
        m.mix[:, at] = matmul(probs, m.values[:, at]).astype(BF16)
        return carry

    lax.fori_loop(0, local // HEAD, attend_head, 0)

    for copy in first:
        copy.wait()
    for step in range(1, count):
        m.back_leaving[peer(step), 0] = m.back_parked[m.order[peer(step)], 0]
    m.grad_in[deal.at(me)] = m.back_parked[m.order[me], 0]
    second = []
    for step in range(1, count):
        copy = wires.copy(
            m.back_leaving.at[peer(step), 0],
            m.grad_in.at[deal.at(me)],
            (peer(step), team.me),
            dealt + count + step,
        )
        copy.start()
        second.append(copy)

    reduce = Reduce(
        team, m.partial, m.came, m.gone, m.total, m.reduce_send, m.reduce_recv
    )

    def gather(whole, number):
        return Gather(team, whole, m.gather_send.at[number], m.gather_recv.at[number])

    loads["o"].wait()

    def make_branch(at):
        m.partial[:, at] = matmul(m.mix[...], m.wo[:, at]).astype(BF16)

    reduce.run(make_branch)
    own = m.mid_all.at[0]

    def whole_at(at):
        return pl.ds(pl.multiple_of(team.slot * shard + at.start, at.size), at.size)

    def norm_mid(at):
        part = m.total[at, :]
        m.branch[at, :] = part
        unit = part * lax.rsqrt(row_sum(part * part) * (1.0 / D) + EPS)
        mid = m.hid[whole_at(at), :].astype(F32) + m.a_gain[...] * unit
        m.mid_all[0, whole_at(at), :] = mid.astype(BF16)

    over_rows(shard, 16, norm_mid)
    mid_gather = gather(own, 0)
    mid_gather.start()
    mid_spread = Spread(wires, grid, team, own, m.mid_all)
    mid_spread.start()
    mid_gather.half()
    mid_gather.finish()
    hid_spread.side(groups)

    loads["g"].wait()
    loads["u"].wait()

    def widen(i, carry):
        at = at_rows(i * STEP, STEP)
        gate = matmul(m.mid_all[0], m.wg[:, at])
        upper = matmul(m.mid_all[0], m.wu[:, at])
        m.gate[:, at] = gate.astype(BF16)
        m.upper[:, at] = upper.astype(BF16)
        m.inner[:, at] = silu_parts(gate, upper)[1]
        return carry

    lax.fori_loop(0, hidden // STEP, widen, 0)
    loads["d"].wait()

    def make_mlp(at):
        m.partial[:, at] = matmul(m.inner[...], m.wd[:, at]).astype(BF16)

    for copy in second:
        copy.wait()
    reduce.run(make_mlp)
    m.stats[...] = jnp.zeros_like(m.stats)
    m.fold[...] = jnp.zeros_like(m.fold)

    def norm_mlp(at):
        part = m.total[at, :]
        scale = lax.rsqrt(row_sum(part * part) * (1.0 / D) + EPS)
        unit = part * scale
        base = m.branch[at, :]
        a_unit = base * lax.rsqrt(row_sum(base * base) * (1.0 / D) + EPS)
        attn_out = m.a_gain[...] * a_unit
        mlp_out = m.m_gain[...] * unit
        rows_f = m.hid[whole_at(at), :].astype(F32)
        row = team.slot * shard + at.start + lax.broadcasted_iota(jnp.int32, (at.size, 1), 0)
        live = row < length
        m.layer[at, :] = jnp.where(live, rows_f + attn_out + mlp_out, 0.0).astype(BF16)
        grad = jnp.where(live, m.grad_in[at, :].astype(F32), 0.0)
        m.fold[0] += folded(grad * unit)
        for i, field in enumerate((rows_f, attn_out, mlp_out)):
            m.fold[i + 1] += folded(jnp.where(live, field * field, 0.0))
        scaled = grad * m.m_gain[...]
        back = scale * (scaled - unit * (row_sum(scaled * unit) * (1.0 / D)))
        m.dm_all[0, whole_at(at), :] = back.astype(BF16)

    over_rows(shard, 16, norm_mlp)
    own_back = m.dm_all.at[0]
    dm_gather = gather(own_back, 1)
    dm_gather.start()
    dm_spread = Spread(wires, grid, team, own_back, m.dm_all)
    dm_spread.start()
    dm_gather.half()
    m.stats[0:1, :] = jnp.sum(m.fold[0], axis=0, keepdims=True)
    for i in range(3):
        m.stats[3 + i : 4 + i, :] = jnp.sum(m.fold[i + 1], axis=0, keepdims=True)
    dm_gather.finish()
    hid_spread.pair(groups)
    mid_spread.side(groups)

    def narrow(i, carry):
        at = at_rows(i * STEP, STEP)
        d_inner = right_inner(m.dm_all[0], m.wd[at, :])
        gate = m.gate[:, at].astype(F32)
        upper = m.upper[:, at].astype(F32)
        m.gate[:, at], m.upper[:, at] = silu_back(gate, upper, jax.nn.sigmoid(gate), d_inner)
        return carry

    lax.fori_loop(0, hidden // STEP, narrow, 0)

    def make_d_mid(at):
        m.partial[:, at] = (
            right_inner(m.gate[...], m.wg[at, :]) + right_inner(m.upper[...], m.wu[at, :])
        ).astype(BF16)

    reduce.run(make_d_mid)
    m.fold[0] = jnp.zeros_like(m.fold[0])

    def norm_d_mid(at):
        row = team.slot * shard + at.start + lax.broadcasted_iota(jnp.int32, (at.size, 1), 0)
        grad = jnp.where(row < length, m.grad_in[at, :].astype(F32), 0.0) + m.total[at, :]
        m.d_mid[at, :] = grad
        base = m.branch[at, :]
        scale = lax.rsqrt(row_sum(base * base) * (1.0 / D) + EPS)
        unit = base * scale
        m.fold[0] += folded(grad * unit)
        scaled = grad * m.a_gain[...]
        back = scale * (scaled - unit * (row_sum(scaled * unit) * (1.0 / D)))
        m.d_branch[whole_at(at), :] = back.astype(BF16)

    over_rows(shard, 16, norm_d_mid)
    d_gather = gather(m.d_branch, 2)
    d_gather.start()
    m.stats[1:2, :] = jnp.sum(m.fold[0], axis=0, keepdims=True)
    d_gather.half()
    d_gather.finish()
    dm_spread.side(2)
    mid_spread.pair(groups)
    branch_spread = Spread(wires, grid, team, m.d_branch, m.branch_all)
    branch_spread.start()

    d_mix = m.partial.at[:, pl.ds(0, local)]
    d_mix[...] = right_inner(m.d_branch[...], m.wo[...]).astype(BF16)
    q_inner = jnp.zeros((rows, 1), F32)
    k_inner = jnp.zeros((rows, 1), F32)
    q_scale = m.scales[:, 0:1]
    k_scale = m.scales[:, 1:2]

    def unattend_head(head, carry):
        at = at_rows(head * HEAD, HEAD)
        _, d_v, d_q_hat, d_k_hat = head_back(
            m.queries[:, at],
            m.keys[:, at],
            m.values[:, at],
            d_mix[:, at],
            m.cosine[...],
            m.sine[...],
            length,
        )
        m.d_heads[:, at_rows(2 * local + head * HEAD, HEAD)] = d_v
        q_unit = m.q_raw[:, at] * q_scale
        k_unit = m.k_raw[:, at] * k_scale
        m.stats[2:3, at] = jnp.sum(d_q_hat * q_unit, axis=0, keepdims=True)
        m.stats[2:3, at_rows(local + head * HEAD, HEAD)] = jnp.sum(
            d_k_hat * k_unit, axis=0, keepdims=True
        )
        q_scaled = d_q_hat * m.q_gain[:, at]
        k_scaled = d_k_hat * m.k_gain[:, at]
        m.stage[0, :, at] = q_scaled
        m.stage[1, :, at] = k_scaled
        return carry[0] + row_sum(q_scaled * q_unit), carry[1] + row_sum(k_scaled * k_unit)

    q_inner, k_inner = lax.fori_loop(0, local // HEAD, unattend_head, (q_inner, k_inner))
    sums.start(q_inner, k_inner)
    dm_spread.side()
    q_inner, k_inner = sums.finish()
    for i, (raw, scale, inner) in enumerate(
        ((m.q_raw, q_scale, q_inner), (m.k_raw, k_scale, k_inner))
    ):
        factor = scale * scale * inner * (1.0 / D)
        m.d_heads[:, pl.ds(i * local, local)] = (
            scale * m.stage[i] - raw[...] * factor
        ).astype(BF16)
    m.stat_team[team.me] = m.stats[...]
    stat_at = wires.book(3 + count)
    stat_team = [
        wires.copy(m.stats, m.stat_team.at[team.me], (me, other), stat_at + i)
        for i, other in enumerate((team.sibling, team.across, team.far))
    ]
    for copy in stat_team:
        copy.start()

    def make_input(at):
        m.partial[:, at] = (
            right_inner(m.d_heads[:, 0:local], m.qkv[0, at, :])
            + right_inner(m.d_heads[:, local : 2 * local], m.qkv[1, at, :])
            + right_inner(m.d_heads[:, 2 * local : 3 * local], m.qkv[2, at, :])
        ).astype(BF16)

    reduce.begin(make_input)

    hid_spread.drain()
    mid_spread.drain()
    dm_spread.drain()
    for k in range(groups):
        m.mid_turned[:, pl.ds(k * rows, rows)] = jnp.transpose(
            m.mid_all[k, :, at_rows(grid.group * strip, strip)]
        )
    crossed = wires.book(3 * (hidden // STEP))
    crossing = (grid.group * lanes + (1 - grid.lane), team.me)

    def tile_of(lane):
        return at_rows((grid.group * lanes + lane) * tile, tile)

    def all_rows(field, columns):
        block = field[:, :, columns]
        return block.reshape(every, block.shape[2])

    def crossings(n):
        at = at_rows(n * STEP, STEP)
        spare = pl.ds(every, tile)
        return [
            wires.copy(m.wg.at[spare, at], m.x_gate.at[:, at], crossing, crossed + 3 * n),
            wires.copy(m.wu.at[spare, at], m.x_up.at[:, at], crossing, crossed + 3 * n + 1),
            wires.copy(m.wd.at[at, spare], m.x_down.at[at, :], crossing, crossed + 3 * n + 2),
        ]

    def again(n, carry):
        at = at_rows(n * STEP, STEP)

        def block_again(k, carry):
            gate = matmul(m.mid_all[k], m.wg[:, at])
            upper = matmul(m.mid_all[k], m.wu[:, at])
            d_inner = right_inner(m.dm_all[k], m.wd[at, :])
            sig, inner = silu_parts(gate, upper)
            kept = at_rows((k - 1) * rows, rows)
            m.keep[0, kept, :] = inner
            m.keep[1, kept, :], m.keep[2, kept, :] = silu_back(gate, upper, sig, d_inner)
            return carry

        lax.fori_loop(1, groups, block_again, 0)
        whole = pl.ds(rows, every - rows)
        m.wg[0:rows, at] = m.gate[:, at]
        m.wu[0:rows, at] = m.upper[:, at]
        m.wd[at, 0:rows] = jnp.transpose(m.inner[:, at])
        m.wg[whole, at] = m.keep[1]
        m.wu[whole, at] = m.keep[2]
        for k in range(1, groups):
            kept = pl.ds((k - 1) * rows, rows)
            m.wd[at, pl.ds(k * rows, rows)] = jnp.transpose(m.keep[0, kept, :])
        turned = m.mid_turned[at_rows((1 - grid.lane) * tile, tile), :]
        spare = pl.ds(every, tile)
        m.wg[spare, at] = matmul(turned, m.wg[0:every, at]).astype(BF16)
        m.wu[spare, at] = matmul(turned, m.wu[0:every, at]).astype(BF16)
        m.wd[at, spare] = matmul(m.wd[at, 0:every], all_rows(m.dm_all, tile_of(1 - grid.lane))).astype(BF16)
        for copy in crossings(n):
            copy.start()
        for place, event in events.items():
            pl.when(n == place)(event)
        return carry

    tiles = hidden // STEP
    stat_dp = [
        wires.copy(m.stats, m.stat_dp.at[me], (peer(step), team.me), stat_at + 2 + step)
        for step in range(1, count)
    ]
    returned = wires.book(4 * count)
    parked = [
        wires.copy(
            source.at[deal.at(peer(step))],
            m.back_parked.at[me, i],
            (peer(step), team.me),
            returned + i * count + step,
        )
        for step in range(1, count)
        for i, source in enumerate((m.layer, m.closed))
    ]
    placed = [
        wires.copy(
            m.back_leaving.at[peer(step), i],
            target.at[deal.at(me, team.slot * shard)],
            (peer(step), team.me),
            returned + (2 + i) * count + step,
        )
        if step
        else pltpu.make_async_copy(
            m.back_leaving.at[me, i],
            target.at[deal.at(me, team.slot * shard)],
            m.put.at[i],
        )
        for step in range(count)
        for i, target in enumerate((m.layer_out, m.input_grad))
    ]
    holders = [holder(peer(step)) for step in range(count)]
    out_gathers = [gather(m.layer_out, 3), gather(m.input_grad, 4)]

    def add_stats():
        for copy in stat_team:
            copy.wait()
        total = (m.stat_team[0] + m.stat_team[1]) + (m.stat_team[2] + m.stat_team[3])
        line = lax.broadcasted_iota(jnp.int32, total.shape, 0)
        m.stats[...] = jnp.where(line == 2, m.stats[...], total)
        m.stat_dp[me] = m.stats[...]
        for copy in stat_dp:
            copy.start()

    def close(at):
        row = team.slot * shard + at.start + lax.broadcasted_iota(jnp.int32, (at.size, 1), 0)
        m.closed[at, :] = jnp.where(row < length, m.total[at, :] + m.d_mid[at, :], 0.0).astype(BF16)

    def park():
        reduce.end()
        over_rows(shard, 16, close)
        for copy in parked:
            copy.start()
        for i, source in enumerate((m.layer, m.closed)):
            m.back_parked[me, i] = source[deal.at(me)]
        branch_spread.side(groups)

    def place():
        for copy in parked:
            copy.wait()
        for step in range(count):
            for i in range(2):
                m.back_leaving[peer(step), i] = m.back_parked[holders[step], i]
        for copy in placed:
            copy.start()

    def share():
        for copy in placed:
            copy.wait()
        for one in out_gathers:
            one.start()

    events = {
        0: add_stats,
        1: park,
        3: place,
        4: lambda: branch_spread.pair(groups),
        tiles - 2: share,
    }
    lax.fori_loop(0, tiles, again, 0)
    for one in out_gathers:
        one.half()
    def put(source, target, index):
        return pltpu.make_async_copy(source, target, m.put.at[index])

    puts = []

    def store(value, target):
        slot = len(puts) % 2
        if len(puts) >= 2:
            puts[-2].wait()
        stage = m.stage.at[slot, pl.ds(0, value.shape[0]), pl.ds(0, value.shape[1])]
        stage[...] = value
        puts.append(put(stage, target, 2 + slot))
        puts[-1].start()

    late = []

    def bring(source, target):
        copy = pltpu.make_async_copy(source, target, m.late.at[len(late)])
        copy.start()
        late.append(copy)

    for k in range(1, groups):
        bring(m.hid_all.at[k], m.mid_all.at[k])
    turned_own = m.mid_turned.at[at_rows(grid.lane * tile, tile)]
    wide = m.stage.shape[2]
    high = rows

    def narrow_stage(slot):
        return m.stage.at[slot, :, pl.ds(0, tile)]

    def flush(copies, last, i, values):
        @pl.when(i > 0)
        def _():
            for copy in copies(i - 1):
                copy.wait()

        for copy, slot, value in zip(copies(i), last, values, strict=True):
            slot[...] = value
            copy.start()

    def wide_copies(i):
        at = at_rows(i * wide, wide)
        return [put(m.stage.at[0], m.g_own.at[:, at], 2), put(m.stage.at[1], m.u_own.at[:, at], 3)]

    def wide_part(i, carry):
        at = at_rows(i * wide, wide)
        flush(
            wide_copies,
            (m.stage.at[0], m.stage.at[1]),
            i,
            [matmul(turned_own[...], weight[0:every, at]) for weight in (m.wg, m.wu)],
        )
        return carry

    lax.fori_loop(0, hidden // wide, wide_part, 0)
    for copy in wide_copies(hidden // wide - 1):
        copy.wait()

    def high_at(i, slot):
        return at_rows((2 * i + slot) * high, high)

    def high_copies(i):
        return [put(narrow_stage(slot), m.d_own.at[high_at(i, slot), :], 2 + slot) for slot in range(2)]

    def high_part(i, carry):
        right = all_rows(m.dm_all, tile_of(grid.lane))
        flush(
            high_copies,
            (narrow_stage(0), narrow_stage(1)),
            i,
            [matmul(m.wd[high_at(i, slot), 0:every], right) for slot in range(2)],
        )
        return carry

    lax.fori_loop(0, hidden // high // 2, high_part, 0)
    for copy in high_copies(hidden // high // 2 - 1):
        copy.wait()
    for one in out_gathers:
        one.finish()

    branch_spread.drain()
    for k in range(1, groups):
        bring(m.branch_all.at[k], m.dm_all.at[k])
    for copy in late[: groups - 1]:
        copy.wait()
    for k in range(groups):
        source = m.mid_all.at[k] if k else m.hid
        m.mid_turned[:, pl.ds(k * rows, rows)] = jnp.transpose(
            source[:, at_rows(grid.group * strip, strip)]
        )
    wide_sums = RowSums(
        team, m.wide_mine, m.wide_came.at[0], m.wide_send.at[0], m.wide_recv.at[0]
    )
    spare_rows = every + tile

    def project_again(k, carry):
        block = at_rows(spare_rows + (k - 1) * rows, rows)
        lane = lax.broadcasted_iota(jnp.int32, (rows, 128), 1)
        found = jnp.zeros((rows, 128), F32)
        for i in range(2):
            raw = matmul(m.mid_all[k], m.qkv[i])
            m.wu[block, pl.ds(2 * local + i * local, local)] = raw.astype(BF16)
            found = jnp.where(lane == i, row_sum(raw * raw), found)
        m.wide_inner[at_rows((k - 1) * rows, rows), :] = found
        m.wu[block, pl.ds(local, local)] = matmul(m.mid_all[k], m.qkv[2]).astype(BF16)
        return carry

    lax.fori_loop(1, groups, project_again, 0)
    wide_sums.start(m.wide_inner[:, 0:1], m.wide_inner[:, 1:2])
    for copy in late[groups - 1 :]:
        copy.wait()
    q_total, k_total = wide_sums.finish()
    lane = lax.broadcasted_iota(jnp.int32, (every - rows, 128), 1)
    m.wide_scales[...] = lax.rsqrt(jnp.where(lane == 0, q_total, k_total) * (1.0 / D) + EPS)
    m.wide_inner[...] = jnp.zeros_like(m.wide_inner)

    def attention_again(k, carry):
        back_length = m.lengths[
            m.order[lax.rem(grid.group - k + groups, groups) * lanes + grid.lane]
        ]
        block = at_rows(spare_rows + (k - 1) * rows, rows)
        inside = at_rows((k - 1) * rows, rows)
        q_scale = m.wide_scales[inside, 0:1]
        k_scale = m.wide_scales[inside, 1:2]
        d_mix[...] = right_inner(m.dm_all[k], m.wo[...]).astype(BF16)
        q_inner = jnp.zeros((rows, 1), F32)
        k_inner = jnp.zeros((rows, 1), F32)

        def head_again(head, carry):
            at = at_rows(head * HEAD, HEAD)
            q_unit = m.wu[block, at_rows(2 * local + head * HEAD, HEAD)].astype(F32) * q_scale
            k_unit = m.wu[block, at_rows(3 * local + head * HEAD, HEAD)].astype(F32) * k_scale
            mix, d_v, d_q_hat, d_k_hat = head_back(
                turn(q_unit * m.q_gain[:, at], m.cosine[...], m.sine[...]).astype(BF16),
                turn(k_unit * m.k_gain[:, at], m.cosine[...], m.sine[...]).astype(BF16),
                m.wu[block, at_rows(local + head * HEAD, HEAD)],
                d_mix[:, at],
                m.cosine[...],
                m.sine[...],
                back_length,
            )
            m.wu[block, at] = mix
            m.wg[block, at_rows(2 * local + head * HEAD, HEAD)] = d_v
            q_scaled = d_q_hat * m.q_gain[:, at]
            k_scaled = d_k_hat * m.k_gain[:, at]
            m.wg[block, at] = q_scaled.astype(BF16)
            m.wg[block, at_rows(local + head * HEAD, HEAD)] = k_scaled.astype(BF16)
            return carry[0] + row_sum(q_scaled * q_unit), carry[1] + row_sum(k_scaled * k_unit)

        q_inner, k_inner = lax.fori_loop(0, local // HEAD, head_again, (q_inner, k_inner))
        lane = lax.broadcasted_iota(jnp.int32, (rows, 128), 1)
        m.wide_inner[inside, :] = jnp.where(lane == 0, q_inner, jnp.where(lane == 1, k_inner, 0.0))
        return carry

    lax.fori_loop(1, groups, attention_again, 0)
    wide_sums = RowSums(
        team, m.wide_mine, m.wide_came.at[1], m.wide_send.at[1], m.wide_recv.at[1]
    )
    wide_sums.start(m.wide_inner[:, 0:1], m.wide_inner[:, 1:2])
    other, this = 1 - grid.lane, grid.lane
    others = pl.ds(spare_rows, every - rows)

    def lane_of(lane):
        return at_rows(grid.group * strip + lane * tile, tile)

    def o_part(lane):
        return left_inner(m.mix[...], m.d_branch[:, lane_of(lane)]) + left_inner(
            m.wu[others, 0:local],
            m.dm_all[1:groups, :, lane_of(lane)].reshape(every - rows, tile),
        )

    def heads_part(lane, at):
        turned = m.mid_turned.at[at_rows(lane * tile, tile)]
        return matmul(turned[:, 0:rows], m.d_heads[:, at]) + matmul(
            turned[:, rows:every], m.wg[others, at]
        )

    last = wires.book(4)
    finals = []
    spare = m.qkv.at[2, pl.ds(3 * tile, local), pl.ds(0, tile)]
    spare[...] = o_part(other).astype(BF16)
    finals.append(wires.copy(spare, m.x_o, crossing, last + 3))
    finals[-1].start()
    q_inner, k_inner = wide_sums.finish()
    lane = lax.broadcasted_iota(jnp.int32, (every - rows, 128), 1)
    m.wide_inner[...] = jnp.where(lane == 0, q_inner, k_inner)

    def close_heads(k, carry):
        block = at_rows(spare_rows + (k - 1) * rows, rows)
        inside = at_rows((k - 1) * rows, rows)
        for i in range(2):
            at = pl.ds(i * local, local)
            scale = m.wide_scales[inside, i : i + 1]
            factor = scale * scale * m.wide_inner[inside, i : i + 1] * (1.0 / D)
            raw = m.wu[block, pl.ds(2 * local + i * local, local)].astype(F32)
            m.wg[block, at] = (scale * m.wg[block, at].astype(F32) - raw * factor).astype(BF16)
        return carry

    lax.fori_loop(1, groups, close_heads, 0)
    for i, target in ((2, m.x_v), (0, m.x_q), (1, m.x_k)):
        spare = m.qkv.at[2, pl.ds(i * tile, tile)]
        spare[...] = heads_part(other, pl.ds(i * local, local)).astype(BF16)
        finals.append(wires.copy(spare, target, crossing, last + i))
        finals[-1].start()
    for i, target in enumerate((m.q_own, m.k_own, m.v_own)):
        store(heads_part(this, pl.ds(i * local, local)), target)
    output = o_part(this)
    for i in range(local // high):
        store(output[i * high : (i + 1) * high], m.o_own.at[pl.ds(i * high, high), :])
    for copy in puts[-2:]:
        copy.wait()

    def arrived(n, carry):
        for copy in crossings(n):
            copy.wait()
        return carry

    for copy in stat_dp:
        copy.wait()
    m.stat_out[...] = sum([m.stat_dp[i] for i in range(1, count)], m.stat_dp[0])
    lax.fori_loop(0, tiles, arrived, 0)
    for copy in finals:
        copy.wait()


def whole_layer(grid, args):
    (hidden_in, upstream, lengths, order, q_weight, k_weight, v_weight, o_weight) = args[:8]
    (q_gain, k_gain, a_gain, g_weight, u_weight, d_weight, m_gain, cosine, sine) = args[8:]
    rows, width = hidden_in.shape
    local, hidden = q_weight.shape[1], g_weight.shape[1]
    count, groups = grid.count, grid.groups
    shard, strip, tile = rows // SLOTS, width // groups, width // count
    every = groups * rows
    deal = Deal(count, shard, width)
    chunk = (deal.rows, deal.columns)
    inputs = [
        ("lengths", SCALAR, lengths),
        ("order", SCALAR, order),
        ("hidden_in", ANY, hidden_in),
        ("upstream", ANY, upstream),
        ("q_weight", ANY, q_weight),
        ("k_weight", ANY, k_weight),
        ("v_weight", ANY, v_weight),
        ("o_weight", ANY, o_weight),
        ("g_weight", ANY, g_weight),
        ("u_weight", ANY, u_weight),
        ("d_weight", ANY, d_weight),
        ("q_gain", ON_CHIP, q_gain),
        ("k_gain", ON_CHIP, k_gain),
        ("a_gain", ON_CHIP, a_gain),
        ("m_gain", ON_CHIP, m_gain),
        ("cosine", ON_CHIP, cosine),
        ("sine", ON_CHIP, sine),
    ]
    outputs = [
        ("layer_out", (rows, width), BF16),
        ("input_grad", (rows, width), BF16),
        ("g_own", (tile, hidden), F32),
        ("u_own", (tile, hidden), F32),
        ("d_own", (hidden, tile), F32),
        ("q_own", (tile, local), F32),
        ("k_own", (tile, local), F32),
        ("v_own", (tile, local), F32),
        ("o_own", (local, tile), F32),
        ("x_gate", (tile, hidden), BF16),
        ("x_up", (tile, hidden), BF16),
        ("x_down", (hidden, tile), BF16),
        ("x_q", (tile, local), BF16),
        ("x_k", (tile, local), BF16),
        ("x_v", (tile, local), BF16),
        ("x_o", (local, tile), BF16),
        ("hid_all", (groups, rows, width), BF16),
        ("branch_all", (groups, rows, width), BF16),
        ("stat_out", (8, width), F32),
    ]
    wires = 160
    scratch = [
        ("qkv", pltpu.VMEM((3, width, local), BF16)),
        ("wo", pltpu.VMEM((local, width), BF16)),
        ("wg", pltpu.VMEM((width, hidden), BF16)),
        ("wu", pltpu.VMEM((width, hidden), BF16)),
        ("wd", pltpu.VMEM((hidden, width), BF16)),
        ("hid", pltpu.VMEM((rows, width), BF16)),
        ("mid_all", pltpu.VMEM((groups, rows, width), BF16)),
        ("dm_all", pltpu.VMEM((groups, rows, width), BF16)),
        ("gate", pltpu.VMEM((rows, hidden), BF16)),
        ("upper", pltpu.VMEM((rows, hidden), BF16)),
        ("inner", pltpu.VMEM((rows, hidden), BF16)),
        ("q_raw", pltpu.VMEM((rows, local), F32)),
        ("k_raw", pltpu.VMEM((rows, local), F32)),
        ("queries", pltpu.VMEM((rows, local), BF16)),
        ("keys", pltpu.VMEM((rows, local), BF16)),
        ("values", pltpu.VMEM((rows, local), BF16)),
        ("scales", pltpu.VMEM((rows, 128), F32)),
        ("mix", pltpu.VMEM((rows, local), BF16)),
        ("d_branch", pltpu.VMEM((rows, width), BF16)),
        ("d_heads", pltpu.VMEM((rows, 3 * local), BF16)),
        ("mid_turned", pltpu.VMEM((strip, every), BF16)),
        ("keep", pltpu.VMEM((3, every - rows, STEP), BF16)),
        ("stage", pltpu.VMEM((2, rows, local), F32)),
        ("branch", pltpu.VMEM((shard, width), F32)),
        ("d_mid", pltpu.VMEM((shard, width), F32)),
        ("layer", pltpu.VMEM((shard, width), BF16)),
        ("closed", pltpu.VMEM((shard, width), BF16)),
        ("grad_in", pltpu.VMEM((shard, width), BF16)),
        ("back_parked", pltpu.VMEM((count, 2) + chunk, BF16)),
        ("back_leaving", pltpu.VMEM((count, 2) + chunk, BF16)),
        ("fold", pltpu.VMEM((4, 8, width), F32)),
        ("stats", pltpu.VMEM((8, width), F32)),
        ("stat_team", pltpu.VMEM((SLOTS, 8, width), F32)),
        ("stat_dp", pltpu.VMEM((count, 8, width), F32)),
        ("partial", pltpu.VMEM((rows, width), BF16)),
        ("came", pltpu.VMEM((3, shard, width), BF16)),
        ("gone", pltpu.VMEM((shard, width), BF16)),
        ("total", pltpu.VMEM((shard, width), F32)),
        ("sum_mine", pltpu.VMEM((8, rows), F32)),
        ("sum_came", pltpu.VMEM((3, 8, rows), F32)),
        ("wide_mine", pltpu.VMEM((8, every - rows), F32)),
        ("wide_came", pltpu.VMEM((2, 3, 8, every - rows), F32)),
        ("wide_scales", pltpu.VMEM((every - rows, 128), F32)),
        ("wide_inner", pltpu.VMEM((every - rows, 128), F32)),
        ("wide_send", pltpu.SemaphoreType.DMA((2, 3))),
        ("wide_recv", pltpu.SemaphoreType.DMA((2, 3))),
        ("sum_send", pltpu.SemaphoreType.DMA((3,))),
        ("sum_recv", pltpu.SemaphoreType.DMA((3,))),
        ("reduce_send", pltpu.SemaphoreType.DMA((3, SPLIT))),
        ("reduce_recv", pltpu.SemaphoreType.DMA((3, SPLIT))),
        ("gather_send", pltpu.SemaphoreType.DMA((5, 3))),
        ("gather_recv", pltpu.SemaphoreType.DMA((5, 3))),
        ("wire_send", pltpu.SemaphoreType.DMA((wires,))),
        ("wire_recv", pltpu.SemaphoreType.DMA((wires,))),
        ("load", pltpu.SemaphoreType.DMA((9,))),
        ("put", pltpu.SemaphoreType.DMA((4,))),
        ("late", pltpu.SemaphoreType.DMA((2 * groups,))),
    ]
    names = [entry[0] for entry in inputs + outputs + scratch]
    results = pl.pallas_call(
        functools.partial(layer_kernel, names),
        out_shape=shaped(*[entry[1:] for entry in outputs]),
        in_specs=[entry[1] for entry in inputs],
        out_specs=(ANY,) * (len(outputs) - 1) + (ON_CHIP,),
        scratch_shapes=[entry[1] for entry in scratch],
        compiler_params=pltpu.CompilerParams(
            collective_id=4, has_side_effects=True, vmem_limit_bytes=63 * 2**20
        ),
        name="whole_layer",
    )(*[entry[2] for entry in inputs])
    return dict(zip([entry[0] for entry in outputs], results, strict=True))


def body(
    hidden_in,
    upstream_grad,
    seq_lengths,
    position_order,
    query_weight,
    key_weight,
    value_weight,
    output_weight,
    query_gain,
    key_gain,
    attn_gain,
    gate_weight,
    up_weight,
    down_weight,
    mlp_gain,
):
    count = lax.axis_size("dp")
    ways = lax.axis_size("tensor")
    myself = lax.axis_index("dp")
    part = lax.axis_index("tensor")
    grid = Grid(count)
    index = jnp.arange(count, dtype=jnp.int32)
    inverse = jnp.sum(
        index[None, :] * (position_order[None, :] == index[:, None]).astype(jnp.int32), axis=1
    )
    rows = hidden_in.shape[1]
    width = hidden_in.shape[2]
    shard = rows // ways
    if grid.lanes == 2 and grid.groups * rows + width // count <= width:
        cosine, sine = rope_constants(rows, HEAD)
        found = whole_layer(
            grid,
            (
                hidden_in[0],
                upstream_grad[0],
                seq_lengths,
                position_order,
                query_weight,
                key_weight,
                value_weight,
                output_weight,
                query_gain[None],
                key_gain[None],
                attn_gain[None],
                gate_weight,
                up_weight,
                down_weight,
                mlp_gain[None],
                cosine,
                sine,
            ),
        )
        local = query_weight.shape[1]

        def joined(own, other):
            return found[own] + found[other].astype(F32)

        stats = found["stat_out"]
        squares = jnp.sum(stats[3:6], axis=1)
        return (
            found["layer_out"][None],
            found["input_grad"][None],
            joined("q_own", "x_q"),
            joined("k_own", "x_k"),
            joined("v_own", "x_v"),
            joined("o_own", "x_o"),
            stats[2, :local],
            stats[2, local : 2 * local],
            stats[1],
            joined("g_own", "x_gate"),
            joined("u_own", "x_up"),
            joined("d_own", "x_down"),
            stats[0],
            jnp.sqrt(squares / (jnp.sum(seq_lengths).astype(F32) * D)),
        )

    piece = shard // count
    seq_here = jnp.sum(jnp.where(index == myself, position_order, 0))
    length = jnp.sum(jnp.where(index == seq_here, seq_lengths, 0))[None]
    slot = part % 2 * 2 + part // 2

    def exchange(pieces):
        return lax.all_to_all(pieces, "dp", split_axis=0, concat_axis=0, tiled=True)

    def my_rows(field):
        return lax.dynamic_slice_in_dim(field, slot * shard, shard, axis=0)

    first = exchange(my_rows(upstream_grad[0]).reshape(count, piece, width))
    second = exchange(jnp.take(first, position_order, axis=0))
    grad_in = second.reshape(shard, width)

    rows_low = hidden_in[0]
    my_low = my_rows(rows_low)
    local = query_weight.shape[1]
    strip = width // grid.groups
    tile = width // count

    def strip_of(field, group):
        return lax.dynamic_slice_in_dim(field, group * strip, strip, axis=1)

    def strips(field):
        found = [strip_of(field, grid.group)]
        for step in range(1, grid.groups):
            found.append(
                grid.shift_groups(
                    strip_of(field, (grid.group + step) % grid.groups), step
                )
            )
        return jnp.concatenate(found, axis=0)

    def tile_of(field, lane):
        return lax.dynamic_slice_in_dim(field, lane * tile, tile, axis=1)

    def reduced(product, field):
        sent = []
        for step in range(1, grid.lanes):
            other = product(tile_of(field, (grid.lane + step) % grid.lanes)).astype(BF16)
            sent.append(grid.shift_lanes(other, step))
        mine = product(tile_of(field, grid.lane))
        for other in sent:
            mine = mine + other.astype(F32)
        return mine

    hidden_strips = strips(rows_low)

    cosine, sine = rope_tables(rows, HEAD)
    cosine = jnp.concatenate([cosine, cosine], axis=1)
    sine = jnp.concatenate([-sine, sine], axis=1)
    gains = (query_gain[None], key_gain[None])
    q_raw, k_raw, queries, keys, values, scales, attn_mix, branch, mid_low = attend(
        length,
        rows_low,
        my_low,
        (query_weight, key_weight, value_weight, output_weight),
        gains,
        cosine,
        sine,
        attn_gain[None],
    )
    mix_all = jnp.concatenate([attn_mix] + grid.ring(attn_mix), axis=0)
    mid_others = shared_ring(grid, mid_low)

    gate = matmul(mid_low, gate_weight)
    upper = matmul(mid_low, up_weight)
    sig = jax.nn.sigmoid(gate)
    inner = (gate * sig * upper).astype(BF16)
    layer, d_mlp, mlp_gain_part, squares = settle(
        length,
        matmul(inner, down_weight).astype(BF16),
        my_low,
        branch,
        grad_in,
        attn_gain[None],
        mlp_gain[None],
    )
    d_mlp_others = shared_ring(grid, d_mlp)

    def inner_back(gate, upper, d_mlp):
        d_inner = right_inner(d_mlp, down_weight)
        sig = jax.nn.sigmoid(gate)
        d_gate = (d_inner * upper * sig * (1.0 + gate * (1.0 - sig))).astype(BF16)
        d_up = (d_inner * gate * sig).astype(BF16)
        return d_gate, d_up

    d_gate, d_up = inner_back(gate, upper, d_mlp)
    d_mid, attn_gain_part, d_branch, d_heads, query_gain_part, key_gain_part = unattend(
        length,
        (right_inner(d_gate, gate_weight) + right_inner(d_up, up_weight)).astype(BF16),
        branch,
        grad_in,
        attn_gain[None],
        output_weight,
        (q_raw, k_raw, queries, keys, values, scales),
        gains,
        cosine,
        sine,
    )
    d_branch_strips = strips(d_branch)
    d_heads_all = jnp.concatenate([d_heads] + grid.ring(d_heads), axis=0)
    layer_out, input_grad = close_layer(
        length,
        inverse,
        (
            right_inner(d_heads[:, :local], query_weight)
            + right_inner(d_heads[:, local : 2 * local], key_weight)
            + right_inner(d_heads[:, 2 * local :], value_weight)
        ).astype(BF16),
        d_mid,
        layer,
    )

    gate_o = matmul(mid_others, gate_weight)
    upper_o = matmul(mid_others, up_weight)
    inner_o = (jax.nn.silu(gate_o) * upper_o).astype(BF16)
    d_gate_o, d_up_o = inner_back(gate_o, upper_o, d_mlp_others)

    def strip_all(own, others):
        return jnp.concatenate([strip_of(own, grid.group), strip_of(others, grid.group)], axis=0)

    mid_strips = strip_all(mid_low, mid_others)
    d_mlp_strips = strip_all(d_mlp, d_mlp_others)
    d_gate_all = jnp.concatenate([d_gate, d_gate_o], axis=0)
    d_up_all = jnp.concatenate([d_up, d_up_o], axis=0)
    inner_all = jnp.concatenate([inner, inner_o], axis=0)
    gate_part = reduced(lambda tile: left_inner(tile, d_gate_all), mid_strips)
    up_part = reduced(lambda tile: left_inner(tile, d_up_all), mid_strips)
    down_part = reduced(lambda tile: left_inner(inner_all, tile), d_mlp_strips)
    output_part = reduced(lambda tile: left_inner(mix_all, tile), d_branch_strips)
    heads_part = reduced(lambda tile: left_inner(tile, d_heads_all), hidden_strips)
    query_part = heads_part[:, :local]
    key_part = heads_part[:, local : 2 * local]
    value_part = heads_part[:, 2 * local :]

    shared = jnp.concatenate(
        [jnp.sum(attn_gain_part, axis=0), jnp.sum(mlp_gain_part, axis=0), jnp.sum(squares, axis=(1, 2))]
    )
    shared = shared + sibling(shared)
    shared = shared + across(shared)
    sums = grid.total(jnp.concatenate([shared, query_gain_part[0], key_gain_part[0]]))
    attn_gain_grad = sums[:width]
    mlp_gain_grad = sums[width : 2 * width]
    squares = sums[2 * width : 2 * width + 3]
    query_gain_grad = sums[2 * width + 3 : 2 * width + 3 + local]
    key_gain_grad = sums[2 * width + 3 + local :]
    rms_values = jnp.sqrt(squares / (jnp.sum(seq_lengths).astype(F32) * D))

    return (
        layer_out[None],
        input_grad[None],
        query_part,
        key_part,
        value_part,
        output_part,
        query_gain_grad,
        key_gain_grad,
        attn_gain_grad,
        gate_part,
        up_part,
        down_part,
        mlp_gain_grad,
        rms_values,
    )


def solution(mesh):
    placed = (
        P("dp", None, None),
        P("dp", None, None),
        P(),
        P(),
        P(None, "tensor"),
        P(None, "tensor"),
        P(None, "tensor"),
        P("tensor", None),
        P("tensor"),
        P("tensor"),
        P(),
        P(None, "tensor"),
        P(None, "tensor"),
        P("tensor", None),
        P(),
    )
    return jax.shard_map(
        body,
        mesh=mesh,
        in_specs=placed,
        out_specs=(
            P("dp", None, None),
            P("dp", None, None),
            P("dp", "tensor"),
            P("dp", "tensor"),
            P("dp", "tensor"),
            P("tensor", "dp"),
            P("tensor"),
            P("tensor"),
            P(),
            P("dp", "tensor"),
            P("dp", "tensor"),
            P("tensor", "dp"),
            P(),
            P(),
        ),
        check_vma=False,
    )
```

```python
import functools
import math
import types

import jax
import jax.numpy as jnp
import numpy as np
from jax import lax
from jax.experimental import pallas as pl
from jax.experimental.pallas import tpu as pltpu
from jax.sharding import PartitionSpec as P

D = 2048
HEAD = 128
EPS = 1e-06
F32 = jnp.float32
BF16 = jnp.bfloat16


def matmul(left, right):
    return jnp.dot(left, right, preferred_element_type=F32)


def left_inner(left, right):
    return lax.dot_general(left, right, (((0,), (0,)), ((), ())), preferred_element_type=F32)


def right_inner(left, right):
    return lax.dot_general(left, right, (((1,), (1,)), ((), ())), preferred_element_type=F32)


def rope_tables(rows, width):
    places = jnp.arange(rows, dtype=F32)
    freq = jnp.power(F32(500000.0), -jnp.arange(width // 2, dtype=F32) * (2.0 / width))
    angle = places[:, None] * freq[None, :]
    return (jnp.cos(angle), jnp.sin(angle))


def rope_constants(rows, width):
    half = width // 2
    exponent = -np.arange(half, dtype=np.float32) * np.float32(2.0 / width)
    freq = np.power(np.float32(500000.0), exponent, dtype=np.float32)
    angle = (np.arange(rows, dtype=np.float32)[:, None] * freq[None, :]).astype(np.float64)
    cosine, sine = np.cos(angle), np.sin(angle)
    return (
        jnp.asarray(np.concatenate([cosine, cosine], axis=1), F32),
        jnp.asarray(np.concatenate([-sine, sine], axis=1), F32),
    )


class Grid:
    def __init__(self, count):
        self.count = count
        self.lanes = 2 ** ((count.bit_length() - 1) // 2)
        self.groups = count // self.lanes
        me = lax.axis_index("dp")
        self.group = me // self.lanes
        self.lane = me % self.lanes

    def shift_groups(self, field, step):
        pairs = [
            (g * self.lanes + a, ((g + step) % self.groups) * self.lanes + a)
            for g in range(self.groups)
            for a in range(self.lanes)
        ]
        return lax.ppermute(field, "dp", pairs)

    def shift_lanes(self, field, step):
        pairs = [
            (g * self.lanes + a, g * self.lanes + (a + step) % self.lanes)
            for g in range(self.groups)
            for a in range(self.lanes)
        ]
        return lax.ppermute(field, "dp", pairs)

    def ring(self, field):
        found = []
        for _ in range(self.groups - 1):
            field = self.shift_groups(field, 1)
            found.append(field)
        return found

    def total(self, field):
        step = 1
        while step < self.count:
            field = field + lax.ppermute(
                field, "dp", [(i, i ^ step) for i in range(self.count)]
            )
            step *= 2
        return field


def sibling(field):
    size = lax.axis_size("tensor")
    return lax.ppermute(field, "tensor", [(i, i ^ 1) for i in range(size)])


def across(field):
    size = lax.axis_size("tensor")
    return lax.ppermute(field, "tensor", [(i, (i + 2) % size) for i in range(size)])


def shared_ring(grid, rows_low):
    core = lax.axis_index("tensor") % 2
    half = rows_low.shape[0] // 2
    mine = lax.dynamic_slice_in_dim(rows_low, core * half, half, axis=0)
    pieces = []
    for piece in grid.ring(mine):
        pieces += [piece, sibling(piece)]
    return jnp.concatenate(pieces, axis=0)


SLOTS = 4
TILES = 4
AT = pl.DeviceIdType.MESH
VMEM_CAP = 56 * 2**20


class Team:
    def __init__(self):
        self.row = lax.axis_index("dp")
        self.me = lax.axis_index("tensor")
        self.side = self.me // 2
        self.core = self.me % 2
        self.slot = self.core * 2 + self.side
        self.sibling = self.side * 2 + (1 - self.core)
        self.across = (1 - self.side) * 2 + self.core
        self.far = (1 - self.side) * 2 + (1 - self.core)

    def meet(self, *others):
        barrier = pltpu.get_barrier_semaphore()
        for other in others:
            pl.semaphore_signal(barrier, inc=1, device_id=(self.row, other), device_id_type=AT)
        pl.semaphore_wait(barrier, len(others))

    def copy(self, source, target, send, recv, other):
        return pltpu.make_async_remote_copy(
            src_ref=source,
            dst_ref=target,
            send_sem=send,
            recv_sem=recv,
            device_id=(self.row, other),
            device_id_type=AT,
        )


def at_rows(start, size):
    return pl.ds(pl.multiple_of(start, size), size)


class Reduce:
    def scratch(rows, width):
        shard = rows // SLOTS
        return [
            pltpu.VMEM((rows, width), BF16),
            pltpu.VMEM((3, shard, width), BF16),
            pltpu.VMEM((shard, width), BF16),
            pltpu.VMEM((shard, width), F32),
            pltpu.SemaphoreType.DMA((3, TILES)),
            pltpu.SemaphoreType.DMA((3, TILES)),
        ]

    def __init__(self, team, partial, came, gone, total, send, recv):
        self.team, self.partial, self.came, self.gone, self.total = team, partial, came, gone, total
        self.shard, width = total.shape
        self.tiles = send.shape[1]
        self.tile = width // self.tiles
        self.send, self.recv = send, recv
        self.copies = {}

    def columns(self, tile):
        return pl.ds(tile * self.tile, self.tile)

    def block(self, core, side):
        return at_rows((core * 2 + side) * self.shard, self.shard)

    def launch(self, kind, tile, source, other):
        copy = self.team.copy(
            source,
            self.came.at[kind, :, self.columns(tile)],
            self.send.at[kind, tile],
            self.recv.at[kind, tile],
            other,
        )
        copy.start()
        self.copies[kind, tile] = copy

    def offer(self, tile):
        team, columns = self.team, self.columns(tile)
        for kind, side in ((0, 1 - team.side), (1, team.side)):
            self.launch(
                kind, tile, self.partial.at[self.block(1 - team.core, side), columns], team.sibling
            )

    def pass_on(self, tile):
        team, columns = self.team, self.columns(tile)
        self.copies[0, tile].wait_recv()
        mine = self.partial[self.block(team.core, 1 - team.side), columns].astype(F32)
        self.gone[:, columns] = (mine + self.came[0, :, columns].astype(F32)).astype(BF16)
        self.launch(2, tile, self.gone.at[:, columns], team.across)

    def finish(self, tile):
        team, columns = self.team, self.columns(tile)
        self.copies[1, tile].wait_recv()
        mine = self.partial[self.block(team.core, team.side), columns].astype(F32)
        mine = mine + self.came[1, :, columns].astype(F32)
        self.copies[2, tile].wait_recv()
        self.total[:, columns] = mine + self.came[2, :, columns].astype(F32)

    def settle(self):
        for copy in self.copies.values():
            copy.wait_send()

    def begin(self, make):
        self.copies = {}
        for tile in range(self.tiles):
            make(self.columns(tile))
            self.offer(tile)
            if tile:
                self.pass_on(tile - 1)
        self.pass_on(self.tiles - 1)

    def end(self):
        for tile in range(self.tiles):
            self.finish(tile)
        self.settle()

    def run(self, make):
        self.begin(make)
        self.end()


class Gather:
    scratch = [pltpu.SemaphoreType.DMA((3,)), pltpu.SemaphoreType.DMA((3,))]

    def __init__(self, team, whole, send, recv):
        self.team, self.whole = team, whole
        shard = whole.shape[0] // SLOTS
        mine = whole.at[at_rows(team.slot * shard, shard)]
        theirs = whole.at[at_rows((team.core * 2 + 1 - team.side) * shard, shard)]
        self.across = team.copy(mine, mine, send.at[0], recv.at[0], team.across)
        self.near = team.copy(mine, mine, send.at[1], recv.at[1], team.sibling)
        self.relay = team.copy(theirs, theirs, send.at[2], recv.at[2], team.sibling)

    def start(self):
        self.across.start()
        self.near.start()

    def half(self):
        self.across.wait_recv()
        self.relay.start()

    def finish(self):
        self.across.wait_send()
        self.near.wait()
        self.relay.wait()


class RowSums:
    def scratch(rows):
        return [
            pltpu.VMEM((8, rows), F32),
            pltpu.VMEM((3, 8, rows), F32),
            pltpu.SemaphoreType.DMA((3,)),
            pltpu.SemaphoreType.DMA((3,)),
        ]

    def __init__(self, team, mine, came, send, recv):
        self.team, self.mine, self.came = team, mine, came
        self.copies = [
            team.copy(mine, came.at[i], send.at[i], recv.at[i], other)
            for i, other in enumerate((team.sibling, team.across, team.far))
        ]

    def start(self, first, second):
        rows = first.shape[0]
        lane = lax.broadcasted_iota(jnp.int32, (rows, 128), 1)
        both = jnp.where(lane == 0, first, jnp.where(lane == 1, second, 0.0))
        self.mine[...] = jnp.transpose(both)[:8]
        for copy in self.copies:
            copy.start()

    def finish(self):
        for copy in self.copies:
            copy.wait()
        total = self.mine[...] + self.came[0] + (self.came[1] + self.came[2])
        rows = total.shape[1]
        wide = jnp.transpose(jnp.concatenate([total] * 16, axis=0))
        return wide[:, 0:1], wide[:, 1:2]


def turn(field, cosine, sine):
    return field * cosine + pltpu.roll(field, HEAD // 2, 1) * sine


def head_probs(queries, keys, length):
    rows = queries.shape[0]
    scores = right_inner(queries, keys) * (1.0 / math.sqrt(HEAD))
    row = lax.broadcasted_iota(jnp.int32, (rows, rows), 0)
    column = lax.broadcasted_iota(jnp.int32, (rows, rows), 1)
    masked = jnp.where((column <= row) & (column < length), scores, -1e30)
    expo = jnp.exp(masked - jnp.max(masked, axis=-1, keepdims=True))
    return expo / jnp.sum(expo, axis=-1, keepdims=True)


def row_sum(field):
    return jnp.sum(field, axis=-1, keepdims=True)


def over_rows(count, step, work):
    def one(i, carry):
        work(pl.ds(pl.multiple_of(i * step, step), step))
        return carry

    lax.fori_loop(0, count // step, one, 0)


def attend_kernel(
    length_ref,
    hidden,
    mine_hidden,
    q_weight,
    k_weight,
    v_weight,
    o_weight,
    q_gain,
    k_gain,
    cosine,
    sine,
    a_gain,
    q_raw,
    k_raw,
    queries,
    keys,
    values,
    scales,
    mix,
    branch,
    mid_low,
    weights,
    out_weight,
    load,
    *scratch,
):
    team = Team()
    sums = RowSums(team, *scratch[0:4])
    reduce = Reduce(team, *scratch[4:10])
    gather = Gather(team, mid_low, *scratch[10:12])
    loads = [
        pltpu.make_async_copy(source, weights.at[i], load.at[i])
        for i, source in enumerate((q_weight, k_weight, v_weight))
    ] + [pltpu.make_async_copy(o_weight, out_weight, load.at[3])]
    for one in loads:
        one.start()
    team.meet(team.sibling, team.across, team.far)
    rows, local = mix.shape
    width = mid_low.shape[1]
    length = length_ref[0]

    def project(i):
        loads[i].wait()
        return matmul(hidden[...], weights[i])

    q = project(0)
    q_raw[...] = q
    k = project(1)
    k_raw[...] = k
    sums.start(row_sum(q * q), row_sum(k * k))
    values[...] = project(2).astype(BF16)
    q_total, k_total = sums.finish()
    q_scale = lax.rsqrt(q_total * (1.0 / D) + EPS)
    k_scale = lax.rsqrt(k_total * (1.0 / D) + EPS)
    lane = lax.broadcasted_iota(jnp.int32, (rows, 128), 1)
    scales[...] = jnp.where(lane == 0, q_scale, k_scale)
    for head in range(local // HEAD):
        at = pl.ds(head * HEAD, HEAD)
        q = turn(q_raw[:, at] * q_scale * q_gain[:, at], cosine[...], sine[...]).astype(BF16)
        k = turn(k_raw[:, at] * k_scale * k_gain[:, at], cosine[...], sine[...]).astype(BF16)
        queries[:, at] = q
        keys[:, at] = k
        probs = head_probs(q, k, length).astype(BF16)
        mix[:, at] = matmul(probs, values[:, at]).astype(BF16)
    loads[3].wait()

    def make(at):
        reduce.partial[:, at] = matmul(mix[...], out_weight[:, at]).astype(BF16)

    reduce.run(make)
    shard = reduce.shard

    def norm(at):
        part = reduce.total[at, :]
        branch[at, :] = part
        unit = part * lax.rsqrt(row_sum(part * part) * (1.0 / D) + EPS)
        mid = mine_hidden[at, :].astype(F32) + a_gain[...] * unit
        whole_at = pl.ds(pl.multiple_of(team.slot * shard + at.start, at.size), at.size)
        mid_low[whole_at, :] = mid.astype(BF16)

    over_rows(shard, 16, norm)
    gather.start()
    gather.half()
    gather.finish()


ANY = pl.BlockSpec(memory_space=pl.ANY)
ON_CHIP = pl.BlockSpec(memory_space=pltpu.VMEM)
SCALAR = pl.BlockSpec(memory_space=pltpu.SMEM)


def shaped(*pairs):
    return tuple(jax.ShapeDtypeStruct(shape, kind) for shape, kind in pairs)


def attend(length, hidden, mine_hidden, weights, gains, cosine, sine, a_gain):
    rows, width = hidden.shape
    local = weights[0].shape[1]
    shard = rows // SLOTS
    return pl.pallas_call(
        attend_kernel,
        out_shape=shaped(
            ((rows, local), F32),
            ((rows, local), F32),
            ((rows, local), BF16),
            ((rows, local), BF16),
            ((rows, local), BF16),
            ((rows, 128), F32),
            ((rows, local), BF16),
            ((shard, width), F32),
            ((rows, width), BF16),
        ),
        in_specs=[SCALAR, ON_CHIP, ON_CHIP] + [ANY] * 4 + [ON_CHIP] * 5,
        out_specs=(ON_CHIP,) * 9,
        scratch_shapes=[
            pltpu.VMEM((3, width, local), BF16),
            pltpu.VMEM((local, width), BF16),
            pltpu.SemaphoreType.DMA((4,)),
        ]
        + RowSums.scratch(rows)
        + Reduce.scratch(rows, width)
        + Gather.scratch,
        compiler_params=pltpu.CompilerParams(
            collective_id=0, has_side_effects=True, vmem_limit_bytes=VMEM_CAP
        ),
        name="attend",
    )(length, hidden, mine_hidden, *weights, *gains, cosine, sine, a_gain)


def settle_kernel(
    length_ref,
    partial_in,
    mine_hidden,
    branch,
    grad_in,
    a_gain,
    m_gain,
    layer,
    d_mlp,
    m_gain_part,
    squares,
    *scratch,
):
    team = Team()
    reduce = Reduce(team, *scratch[0:6])
    gather = Gather(team, d_mlp, *scratch[6:8])
    team.meet(team.sibling, team.across)

    def make(at):
        reduce.partial[:, at] = partial_in[:, at]

    reduce.run(make)
    shard = reduce.shard
    length = length_ref[0]
    m_gain_part[...] = jnp.zeros_like(m_gain_part)
    squares[...] = jnp.zeros_like(squares)

    def folded(field):
        return sum([field[8 * i : 8 * i + 8] for i in range(field.shape[0] // 8)])

    def norm(at):
        part = reduce.total[at, :]
        scale = lax.rsqrt(row_sum(part * part) * (1.0 / D) + EPS)
        unit = part * scale
        base = branch[at, :]
        a_unit = base * lax.rsqrt(row_sum(base * base) * (1.0 / D) + EPS)
        attn_out = a_gain[...] * a_unit
        mlp_out = m_gain[...] * unit
        rows_f = mine_hidden[at, :].astype(F32)
        row = team.slot * shard + at.start + lax.broadcasted_iota(jnp.int32, (at.size, 1), 0)
        live = row < length
        layer[at, :] = jnp.where(live, rows_f + attn_out + mlp_out, 0.0).astype(BF16)
        grad = jnp.where(live, grad_in[at, :].astype(F32), 0.0)
        m_gain_part[...] += folded(grad * unit)
        for i, field in enumerate((rows_f, attn_out, mlp_out)):
            squares[i] += folded(jnp.where(live, field * field, 0.0))
        scaled = grad * m_gain[...]
        back = scale * (scaled - unit * (row_sum(scaled * unit) * (1.0 / D)))
        whole_at = pl.ds(pl.multiple_of(team.slot * shard + at.start, at.size), at.size)
        d_mlp[whole_at, :] = back.astype(BF16)

    over_rows(shard, 16, norm)
    gather.start()
    gather.half()
    gather.finish()


def settle(length, partial, mine_hidden, branch, grad_in, a_gain, m_gain):
    rows, width = partial.shape
    shard = rows // SLOTS
    return pl.pallas_call(
        settle_kernel,
        out_shape=shaped(
            ((shard, width), BF16),
            ((rows, width), BF16),
            ((8, width), F32),
            ((3, 8, width), F32),
        ),
        in_specs=[SCALAR] + [ON_CHIP] * 6,
        out_specs=(ON_CHIP,) * 4,
        scratch_shapes=Reduce.scratch(rows, width) + Gather.scratch,
        compiler_params=pltpu.CompilerParams(
            collective_id=1, has_side_effects=True, vmem_limit_bytes=VMEM_CAP
        ),
        name="settle",
    )(length, partial, mine_hidden, branch, grad_in, a_gain, m_gain)


def unattend_kernel(
    length_ref,
    partial_in,
    branch,
    grad_in,
    a_gain,
    o_weight,
    q_raw,
    k_raw,
    queries,
    keys,
    values,
    scales,
    q_gain,
    k_gain,
    cosine,
    sine,
    d_mid,
    a_gain_part,
    d_branch,
    d_heads,
    q_gain_part,
    k_gain_part,
    out_weight,
    d_mix,
    d_q,
    d_k,
    load,
    *scratch,
):
    team = Team()
    sums = RowSums(team, *scratch[0:4])
    reduce = Reduce(team, *scratch[4:10])
    gather = Gather(team, d_branch, *scratch[10:12])
    fetch = pltpu.make_async_copy(o_weight, out_weight, load.at[0])
    fetch.start()
    team.meet(team.sibling, team.across, team.far)
    rows, local = queries.shape

    def make(at):
        reduce.partial[:, at] = partial_in[:, at]

    reduce.run(make)
    shard = reduce.shard
    length = length_ref[0]
    a_gain_part[...] = jnp.zeros_like(a_gain_part)

    def norm(at):
        row = team.slot * shard + at.start + lax.broadcasted_iota(jnp.int32, (at.size, 1), 0)
        grad = jnp.where(row < length, grad_in[at, :].astype(F32), 0.0) + reduce.total[at, :]
        d_mid[at, :] = grad
        base = branch[at, :]
        scale = lax.rsqrt(row_sum(base * base) * (1.0 / D) + EPS)
        unit = base * scale
        product = grad * unit
        a_gain_part[...] += sum([product[8 * i : 8 * i + 8] for i in range(at.size // 8)])
        scaled = grad * a_gain[...]
        back = scale * (scaled - unit * (row_sum(scaled * unit) * (1.0 / D)))
        whole_at = pl.ds(pl.multiple_of(team.slot * shard + at.start, at.size), at.size)
        d_branch[whole_at, :] = back.astype(BF16)

    over_rows(shard, 16, norm)
    gather.start()
    gather.half()
    gather.finish()
    fetch.wait()
    d_mix[...] = right_inner(d_branch[...], out_weight[...]).astype(BF16)
    q_scale = scales[:, 0:1]
    k_scale = scales[:, 1:2]
    q_inner = jnp.zeros((rows, 1), F32)
    k_inner = jnp.zeros((rows, 1), F32)
    shrink = 1.0 / math.sqrt(HEAD)
    for head in range(local // HEAD):
        at = pl.ds(head * HEAD, HEAD)
        q, k, v, back = queries[:, at], keys[:, at], values[:, at], d_mix[:, at]
        probs = head_probs(q, k, length)
        d_probs = right_inner(back, v)
        d_scores = (probs * (d_probs - row_sum(probs * d_probs))).astype(BF16)
        d_heads[:, pl.ds(2 * local + head * HEAD, HEAD)] = left_inner(
            probs.astype(BF16), back
        ).astype(BF16)
        d_q_hat = turn(matmul(d_scores, k) * shrink, cosine[...], -sine[...])
        d_k_hat = turn(left_inner(d_scores, q) * shrink, cosine[...], -sine[...])
        q_unit = q_raw[:, at] * q_scale
        k_unit = k_raw[:, at] * k_scale
        q_gain_part[:, at] = jnp.sum(d_q_hat * q_unit, axis=0, keepdims=True)
        k_gain_part[:, at] = jnp.sum(d_k_hat * k_unit, axis=0, keepdims=True)
        q_scaled = d_q_hat * q_gain[:, at]
        k_scaled = d_k_hat * k_gain[:, at]
        d_q[:, at] = q_scaled
        d_k[:, at] = k_scaled
        q_inner += row_sum(q_scaled * q_unit)
        k_inner += row_sum(k_scaled * k_unit)
    sums.start(q_inner, k_inner)
    q_inner, k_inner = sums.finish()
    for i, (grad, raw, scale, inner) in enumerate(
        ((d_q, q_raw, q_scale, q_inner), (d_k, k_raw, k_scale, k_inner))
    ):
        factor = scale * scale * inner * (1.0 / D)
        d_heads[:, pl.ds(i * local, local)] = (scale * grad[...] - raw[...] * factor).astype(BF16)


def unattend(
    length, partial, branch, grad_in, a_gain, o_weight, kept, gains, cosine, sine
):
    rows, width = partial.shape
    local = o_weight.shape[0]
    shard = rows // SLOTS
    return pl.pallas_call(
        unattend_kernel,
        out_shape=shaped(
            ((shard, width), F32),
            ((8, width), F32),
            ((rows, width), BF16),
            ((rows, 3 * local), BF16),
            ((1, local), F32),
            ((1, local), F32),
        ),
        in_specs=[SCALAR] + [ON_CHIP] * 4 + [ANY] + [ON_CHIP] * 10,
        out_specs=(ON_CHIP,) * 6,
        scratch_shapes=[
            pltpu.VMEM((local, width), BF16),
            pltpu.VMEM((rows, local), BF16),
            pltpu.VMEM((rows, local), F32),
            pltpu.VMEM((rows, local), F32),
            pltpu.SemaphoreType.DMA((1,)),
        ]
        + RowSums.scratch(rows)
        + Reduce.scratch(rows, width)
        + Gather.scratch,
        compiler_params=pltpu.CompilerParams(
            collective_id=2, has_side_effects=True, vmem_limit_bytes=VMEM_CAP
        ),
        name="unattend",
    )(length, partial, branch, grad_in, a_gain, o_weight, *kept, *gains, cosine, sine)


class Deal:
    def __init__(self, count, shard, width):
        self.count = count
        self.columns = max(128, width // count)
        self.across = width // self.columns
        self.rows = shard * self.across // count

    def at(self, chunk, base=0):
        return (
            at_rows(base + (chunk // self.across) * self.rows, self.rows),
            at_rows((chunk % self.across) * self.columns, self.columns),
        )


def finish_kernel(
    length_ref,
    inverse,
    partial_in,
    d_mid,
    layer,
    layer_out,
    input_grad,
    closed,
    parked,
    leaving,
    deal_send,
    deal_recv,
    *scratch,
):
    team = Team()
    reduce = Reduce(team, *scratch[0:6])
    gathers = [
        Gather(team, whole, *scratch[6 + 2 * i : 8 + 2 * i])
        for i, whole in enumerate((layer_out, input_grad))
    ]
    count = lax.axis_size("dp")
    shard, width = d_mid.shape
    deal = Deal(count, shard, width)
    barrier = pltpu.get_barrier_semaphore()
    for step in range(1, count):
        pl.semaphore_signal(
            barrier, inc=1, device_id=(lax.rem(team.row + step, count), team.me), device_id_type=AT
        )
    for other in (team.sibling, team.across):
        pl.semaphore_signal(barrier, inc=1, device_id=(team.row, other), device_id_type=AT)
    pl.semaphore_wait(barrier, count + 1)

    def make(at):
        reduce.partial[:, at] = partial_in[:, at]

    reduce.run(make)
    length = length_ref[0]

    def close(at):
        row = team.slot * shard + at.start + lax.broadcasted_iota(jnp.int32, (at.size, 1), 0)
        closed[at, :] = jnp.where(row < length, reduce.total[at, :] + d_mid[at, :], 0.0).astype(BF16)

    over_rows(shard, 16, close)

    def send(phase, step, i, source, target):
        return pltpu.make_async_remote_copy(
            src_ref=source,
            dst_ref=target,
            send_sem=deal_send.at[phase, step, i],
            recv_sem=deal_recv.at[phase, step, i],
            device_id=(lax.rem(team.row + step, count), team.me),
            device_id_type=AT,
        )

    first = []
    for i, source in enumerate((layer, closed)):
        for step in range(1, count):
            other = lax.rem(team.row + step, count)
            copy = send(0, step, i, source.at[deal.at(other)], parked.at[team.row, i])
            copy.start()
            first.append(copy)
        parked[team.row, i] = source[deal.at(team.row)]
    for copy in first:
        copy.wait()
    mine = team.slot * shard
    second = []
    for i, target in enumerate((layer_out, input_grad)):
        for step in range(1, count):
            other = lax.rem(team.row + step, count)
            leaving[other, i] = parked[inverse[other], i]
            copy = send(1, step, i, leaving.at[other, i], target.at[deal.at(team.row, mine)])
            copy.start()
            second.append(copy)
        target[deal.at(team.row, mine)] = parked[inverse[team.row], i]
    for copy in second:
        copy.wait()
    for gather in gathers:
        gather.start()
    for gather in gathers:
        gather.half()
    for gather in gathers:
        gather.finish()


def close_layer(length, inverse, partial, d_mid, layer):
    rows, width = partial.shape
    shard = rows // SLOTS
    count = lax.axis_size("dp")
    deal = Deal(count, shard, width)
    chunk = (count, 2, deal.rows, deal.columns)
    return pl.pallas_call(
        finish_kernel,
        out_shape=shaped(((rows, width), BF16), ((rows, width), BF16)),
        in_specs=[SCALAR, SCALAR] + [ON_CHIP] * 3,
        out_specs=(ON_CHIP,) * 2,
        scratch_shapes=[
            pltpu.VMEM((shard, width), BF16),
            pltpu.VMEM(chunk, BF16),
            pltpu.VMEM(chunk, BF16),
            pltpu.SemaphoreType.DMA((2, count, 2)),
            pltpu.SemaphoreType.DMA((2, count, 2)),
        ]
        + Reduce.scratch(rows, width)
        + Gather.scratch * 2,
        compiler_params=pltpu.CompilerParams(
            collective_id=3, has_side_effects=True, vmem_limit_bytes=VMEM_CAP
        ),
        name="close_layer",
    )(length, inverse, partial, d_mid, layer)


SPLIT = 4
STEP = 256


class Wires:
    def __init__(self, send, recv):
        self.send, self.recv, self.used = send, recv, 0

    def book(self, number=1):
        self.used += number
        assert self.used <= self.send.shape[0]
        return self.used - number

    def copy(self, source, target, device, index):
        return pltpu.make_async_remote_copy(
            src_ref=source,
            dst_ref=target,
            send_sem=self.send.at[index],
            recv_sem=self.recv.at[index],
            device_id=device,
            device_id_type=AT,
        )


class Spread:
    def __init__(self, wires, grid, team, source, field):
        shard = source.shape[0] // SLOTS
        mine = at_rows(team.slot * shard, shard)
        half = at_rows(team.core * 2 * shard, 2 * shard)
        self.hops, self.sides, self.pairs = {}, {}, {}
        for step in range(1, grid.groups):
            group = lax.rem(grid.group + step, grid.groups)
            block = field.at[step]
            self.hops[step] = wires.copy(
                source.at[mine],
                block.at[mine],
                (group * grid.lanes + grid.lane, team.me),
                wires.book(),
            )
            self.sides[step] = wires.copy(
                block.at[mine], block.at[mine], (team.row, team.across), wires.book()
            )
            self.pairs[step] = wires.copy(
                block.at[half], block.at[half], (team.row, team.sibling), wires.book()
            )
        near = sorted(self.hops, key=lambda step: min(step, grid.groups - step))
        self.plan = {"hop": list(near), "side": list(near), "pair": list(near)}

    def start(self):
        for step in self.plan["hop"]:
            self.hops[step].start()

    def side(self, number=1):
        for step in self.plan["side"][:number]:
            self.hops[step].wait_recv()
            self.sides[step].start()
        del self.plan["side"][:number]

    def pair(self, number=1):
        for step in self.plan["pair"][:number]:
            self.sides[step].wait_recv()
            self.pairs[step].start()
        del self.plan["pair"][:number]

    def drain(self):
        self.side(len(self.hops))
        self.pair(len(self.hops))
        for step in self.hops:
            self.hops[step].wait_send()
            self.sides[step].wait_send()
            self.pairs[step].wait()


def silu_parts(gate, upper):
    sig = jax.nn.sigmoid(gate)
    return sig, (gate * sig * upper).astype(BF16)


def silu_back(gate, upper, sig, d_inner):
    d_gate = (d_inner * upper * sig * (1.0 + gate * (1.0 - sig))).astype(BF16)
    return d_gate, (d_inner * gate * sig).astype(BF16)


def head_back(q, k, v, back, cosine, sine, length):
    probs = head_probs(q, k, length)
    low = probs.astype(BF16)
    mix = matmul(low, v).astype(BF16)
    d_probs = right_inner(back, v)
    d_scores = (probs * (d_probs - row_sum(probs * d_probs))).astype(BF16)
    shrink = 1.0 / math.sqrt(HEAD)
    return (
        mix,
        left_inner(low, back).astype(BF16),
        turn(matmul(d_scores, k) * shrink, cosine, -sine),
        turn(left_inner(d_scores, q) * shrink, cosine, -sine),
    )


def folded(field):
    return sum([field[8 * i : 8 * i + 8] for i in range(field.shape[0] // 8)])


def layer_kernel(names, *refs):
    m = types.SimpleNamespace(**dict(zip(names, refs, strict=True)))
    team, grid = Team(), Grid(lax.axis_size("dp"))
    wires = Wires(m.wire_send, m.wire_recv)
    count, groups, lanes = grid.count, grid.groups, grid.lanes
    rows, width = m.hid.shape
    local, hidden = m.mix.shape[1], m.gate.shape[1]
    shard, strip, tile = rows // SLOTS, width // groups, width // count
    every = groups * rows
    me = team.row

    loads = {}

    def load(name, source, target):
        loads[name] = pltpu.make_async_copy(source, target, m.load.at[len(loads)])
        loads[name].start()

    load("hid", m.hidden_in, m.hid)
    load("q", m.q_weight, m.qkv.at[0])
    load("k", m.k_weight, m.qkv.at[1])
    load("v", m.v_weight, m.qkv.at[2])
    load("grad", m.upstream.at[at_rows(team.slot * shard, shard)], m.closed)
    load("o", m.o_weight, m.wo)
    load("g", m.g_weight, m.wg)
    load("u", m.u_weight, m.wu)
    load("d", m.d_weight, m.wd)

    def peer(step):
        return lax.rem(me + step, count)

    barrier = pltpu.get_barrier_semaphore()
    for step in range(1, count):
        pl.semaphore_signal(barrier, inc=1, device_id=(peer(step), team.me), device_id_type=AT)
    for other in (team.sibling, team.across, team.far):
        pl.semaphore_signal(barrier, inc=1, device_id=(me, other), device_id_type=AT)
    pl.semaphore_wait(barrier, count + 2)

    length = m.lengths[m.order[me]]

    def holder(sequence):
        found = jnp.int32(0)
        for place in range(count):
            found = jnp.where(m.order[place] == sequence, place, found)
        return found

    following = (lax.rem(grid.group + 1, groups) * lanes + grid.lane, team.me)
    sums = RowSums(team, m.sum_mine, m.sum_came, m.sum_send, m.sum_recv)
    deal = Deal(count, shard, width)

    loads["grad"].wait()
    dealt = wires.book(2 * count)
    first = []
    for step in range(1, count):
        copy = wires.copy(
            m.closed.at[deal.at(peer(step))],
            m.back_parked.at[me, 0],
            (peer(step), team.me),
            dealt + step,
        )
        copy.start()
        first.append(copy)
    m.back_parked[me, 0] = m.closed[deal.at(me)]

    loads["hid"].wait()

    loads["q"].wait()
    q = matmul(m.hid[...], m.qkv[0])
    m.q_raw[...] = q
    loads["k"].wait()
    k = matmul(m.hid[...], m.qkv[1])
    m.k_raw[...] = k
    sums.start(row_sum(q * q), row_sum(k * k))
    loads["v"].wait()
    m.values[...] = matmul(m.hid[...], m.qkv[2]).astype(BF16)
    q_total, k_total = sums.finish()
    q_scale = lax.rsqrt(q_total * (1.0 / D) + EPS)
    k_scale = lax.rsqrt(k_total * (1.0 / D) + EPS)
    lane = lax.broadcasted_iota(jnp.int32, (rows, 128), 1)
    m.scales[...] = jnp.where(lane == 0, q_scale, k_scale)

    def attend_head(head, carry):
        at = at_rows(head * HEAD, HEAD)
        q = turn(m.q_raw[:, at] * q_scale * m.q_gain[:, at], m.cosine[...], m.sine[...]).astype(BF16)
        k = turn(m.k_raw[:, at] * k_scale * m.k_gain[:, at], m.cosine[...], m.sine[...]).astype(BF16)
        m.queries[:, at] = q
        m.keys[:, at] = k
        probs = head_probs(q, k, length).astype(BF16)
        m.mix[:, at] = matmul(probs, m.values[:, at]).astype(BF16)
        return carry

    lax.fori_loop(0, local // HEAD, attend_head, 0)

    for copy in first:
        copy.wait()
    for step in range(1, count):
        m.back_leaving[peer(step), 0] = m.back_parked[m.order[peer(step)], 0]
    m.grad_in[deal.at(me)] = m.back_parked[m.order[me], 0]
    second = []
    for step in range(1, count):
        copy = wires.copy(
            m.back_leaving.at[peer(step), 0],
            m.grad_in.at[deal.at(me)],
            (peer(step), team.me),
            dealt + count + step,
        )
        copy.start()
        second.append(copy)

    reduce = Reduce(
        team, m.partial, m.came, m.gone, m.total, m.reduce_send, m.reduce_recv
    )

    def gather(whole, number):
        return Gather(team, whole, m.gather_send.at[number], m.gather_recv.at[number])

    loads["o"].wait()

    def make_branch(at):
        m.partial[:, at] = matmul(m.mix[...], m.wo[:, at]).astype(BF16)

    reduce.run(make_branch)
    own = m.mid_all.at[0]

    def whole_at(at):
        return pl.ds(pl.multiple_of(team.slot * shard + at.start, at.size), at.size)

    def norm_mid(at):
        part = m.total[at, :]
        m.branch[at, :] = part
        unit = part * lax.rsqrt(row_sum(part * part) * (1.0 / D) + EPS)
        mid = m.hid[whole_at(at), :].astype(F32) + m.a_gain[...] * unit
        m.mid_all[0, whole_at(at), :] = mid.astype(BF16)

    over_rows(shard, 16, norm_mid)
    mid_gather = gather(own, 0)
    mid_gather.start()
    mid_spread = Spread(wires, grid, team, own, m.mid_all)
    mid_spread.start()
    mid_gather.half()
    mid_gather.finish()
    loads["g"].wait()
    loads["u"].wait()

    def widen(i, carry):
        at = at_rows(i * STEP, STEP)
        gate = matmul(m.mid_all[0], m.wg[:, at])
        upper = matmul(m.mid_all[0], m.wu[:, at])
        m.gate[:, at] = gate.astype(BF16)
        m.upper[:, at] = upper.astype(BF16)
        m.inner[:, at] = silu_parts(gate, upper)[1]
        return carry

    lax.fori_loop(0, hidden // STEP, widen, 0)
    loads["d"].wait()

    def make_mlp(at):
        m.partial[:, at] = matmul(m.inner[...], m.wd[:, at]).astype(BF16)

    for copy in second:
        copy.wait()
    reduce.run(make_mlp)
    m.stats[...] = jnp.zeros_like(m.stats)
    m.fold[...] = jnp.zeros_like(m.fold)

    def norm_mlp(at):
        part = m.total[at, :]
        scale = lax.rsqrt(row_sum(part * part) * (1.0 / D) + EPS)
        unit = part * scale
        base = m.branch[at, :]
        a_unit = base * lax.rsqrt(row_sum(base * base) * (1.0 / D) + EPS)
        attn_out = m.a_gain[...] * a_unit
        mlp_out = m.m_gain[...] * unit
        rows_f = m.hid[whole_at(at), :].astype(F32)
        row = team.slot * shard + at.start + lax.broadcasted_iota(jnp.int32, (at.size, 1), 0)
        live = row < length
        m.layer[at, :] = jnp.where(live, rows_f + attn_out + mlp_out, 0.0).astype(BF16)
        grad = jnp.where(live, m.grad_in[at, :].astype(F32), 0.0)
        m.fold[0] += folded(grad * unit)
        for i, field in enumerate((rows_f, attn_out, mlp_out)):
            m.fold[i + 1] += folded(jnp.where(live, field * field, 0.0))
        scaled = grad * m.m_gain[...]
        back = scale * (scaled - unit * (row_sum(scaled * unit) * (1.0 / D)))
        m.dm_all[0, whole_at(at), :] = back.astype(BF16)

    over_rows(shard, 16, norm_mlp)
    own_back = m.dm_all.at[0]
    dm_gather = gather(own_back, 1)
    dm_gather.start()
    dm_spread = Spread(wires, grid, team, own_back, m.dm_all)
    dm_spread.start()
    dm_gather.half()
    m.stats[0:1, :] = jnp.sum(m.fold[0], axis=0, keepdims=True)
    for i in range(3):
        m.stats[3 + i : 4 + i, :] = jnp.sum(m.fold[i + 1], axis=0, keepdims=True)
    dm_gather.finish()
    mid_spread.side(groups)
    hid_spread = Spread(wires, grid, team, m.hid, m.hid_all)
    hid_spread.start()

    def narrow(i, carry):
        at = at_rows(i * STEP, STEP)
        d_inner = right_inner(m.dm_all[0], m.wd[at, :])
        gate = m.gate[:, at].astype(F32)
        upper = m.upper[:, at].astype(F32)
        m.gate[:, at], m.upper[:, at] = silu_back(gate, upper, jax.nn.sigmoid(gate), d_inner)
        return carry

    lax.fori_loop(0, hidden // STEP, narrow, 0)

    def make_d_mid(at):
        m.partial[:, at] = (
            right_inner(m.gate[...], m.wg[at, :]) + right_inner(m.upper[...], m.wu[at, :])
        ).astype(BF16)

    reduce.run(make_d_mid)
    m.fold[0] = jnp.zeros_like(m.fold[0])

    def norm_d_mid(at):
        row = team.slot * shard + at.start + lax.broadcasted_iota(jnp.int32, (at.size, 1), 0)
        grad = jnp.where(row < length, m.grad_in[at, :].astype(F32), 0.0) + m.total[at, :]
        m.d_mid[at, :] = grad
        base = m.branch[at, :]
        scale = lax.rsqrt(row_sum(base * base) * (1.0 / D) + EPS)
        unit = base * scale
        m.fold[0] += folded(grad * unit)
        scaled = grad * m.a_gain[...]
        back = scale * (scaled - unit * (row_sum(scaled * unit) * (1.0 / D)))
        m.d_branch[whole_at(at), :] = back.astype(BF16)

    over_rows(shard, 16, norm_d_mid)
    d_gather = gather(m.d_branch, 2)
    d_gather.start()
    m.stats[1:2, :] = jnp.sum(m.fold[0], axis=0, keepdims=True)
    d_gather.half()
    d_gather.finish()
    dm_spread.side(groups)
    mid_spread.pair(groups)
    branch_spread = Spread(wires, grid, team, m.d_branch, m.branch_all)
    branch_spread.start()

    d_mix = m.partial.at[:, pl.ds(0, local)]
    d_mix[...] = right_inner(m.d_branch[...], m.wo[...]).astype(BF16)
    q_inner = jnp.zeros((rows, 1), F32)
    k_inner = jnp.zeros((rows, 1), F32)
    q_scale = m.scales[:, 0:1]
    k_scale = m.scales[:, 1:2]

    def unattend_head(head, carry):
        at = at_rows(head * HEAD, HEAD)
        _, d_v, d_q_hat, d_k_hat = head_back(
            m.queries[:, at],
            m.keys[:, at],
            m.values[:, at],
            d_mix[:, at],
            m.cosine[...],
            m.sine[...],
            length,
        )
        m.d_heads[:, at_rows(2 * local + head * HEAD, HEAD)] = d_v
        q_unit = m.q_raw[:, at] * q_scale
        k_unit = m.k_raw[:, at] * k_scale
        m.stats[2:3, at] = jnp.sum(d_q_hat * q_unit, axis=0, keepdims=True)
        m.stats[2:3, at_rows(local + head * HEAD, HEAD)] = jnp.sum(
            d_k_hat * k_unit, axis=0, keepdims=True
        )
        q_scaled = d_q_hat * m.q_gain[:, at]
        k_scaled = d_k_hat * m.k_gain[:, at]
        m.stage[0, :, at] = q_scaled
        m.stage[1, :, at] = k_scaled
        return carry[0] + row_sum(q_scaled * q_unit), carry[1] + row_sum(k_scaled * k_unit)

    q_inner, k_inner = lax.fori_loop(0, local // HEAD, unattend_head, (q_inner, k_inner))
    sums.start(q_inner, k_inner)
    q_inner, k_inner = sums.finish()
    for i, (raw, scale, inner) in enumerate(
        ((m.q_raw, q_scale, q_inner), (m.k_raw, k_scale, k_inner))
    ):
        factor = scale * scale * inner * (1.0 / D)
        m.d_heads[:, pl.ds(i * local, local)] = (
            scale * m.stage[i] - raw[...] * factor
        ).astype(BF16)
    m.stat_team[team.me] = m.stats[...]
    stat_at = wires.book(3 + count)
    stat_team = [
        wires.copy(m.stats, m.stat_team.at[team.me], (me, other), stat_at + i)
        for i, other in enumerate((team.sibling, team.across, team.far))
    ]
    for copy in stat_team:
        copy.start()

    def make_input(at):
        m.partial[:, at] = (
            right_inner(m.d_heads[:, 0:local], m.qkv[0, at, :])
            + right_inner(m.d_heads[:, local : 2 * local], m.qkv[1, at, :])
            + right_inner(m.d_heads[:, 2 * local : 3 * local], m.qkv[2, at, :])
        ).astype(BF16)

    reduce.begin(make_input)

    mid_spread.drain()
    dm_spread.drain()
    for k in range(groups):
        m.mid_turned[:, pl.ds(k * rows, rows)] = jnp.transpose(
            m.mid_all[k, :, at_rows(grid.group * strip, strip)]
        )
    crossed = wires.book(3 * (hidden // STEP))
    crossing = (grid.group * lanes + (1 - grid.lane), team.me)

    def tile_of(lane):
        return at_rows((grid.group * lanes + lane) * tile, tile)

    def all_rows(field, columns):
        block = field[:, :, columns]
        return block.reshape(every, block.shape[2])

    def crossings(n):
        at = at_rows(n * STEP, STEP)
        spare = pl.ds(every, tile)
        return [
            wires.copy(m.wg.at[spare, at], m.x_gate.at[:, at], crossing, crossed + 3 * n),
            wires.copy(m.wu.at[spare, at], m.x_up.at[:, at], crossing, crossed + 3 * n + 1),
            wires.copy(m.wd.at[at, spare], m.x_down.at[at, :], crossing, crossed + 3 * n + 2),
        ]

    def again(n, carry):
        at = at_rows(n * STEP, STEP)

        def block_again(k, carry):
            gate = matmul(m.mid_all[k], m.wg[:, at])
            upper = matmul(m.mid_all[k], m.wu[:, at])
            d_inner = right_inner(m.dm_all[k], m.wd[at, :])
            sig, inner = silu_parts(gate, upper)
            kept = at_rows((k - 1) * rows, rows)
            m.keep[0, kept, :] = inner
            m.keep[1, kept, :], m.keep[2, kept, :] = silu_back(gate, upper, sig, d_inner)
            return carry

        lax.fori_loop(1, groups, block_again, 0)
        whole = pl.ds(rows, every - rows)
        m.wg[0:rows, at] = m.gate[:, at]
        m.wu[0:rows, at] = m.upper[:, at]
        m.wd[at, 0:rows] = jnp.transpose(m.inner[:, at])
        m.wg[whole, at] = m.keep[1]
        m.wu[whole, at] = m.keep[2]
        for k in range(1, groups):
            kept = pl.ds((k - 1) * rows, rows)
            m.wd[at, pl.ds(k * rows, rows)] = jnp.transpose(m.keep[0, kept, :])
        turned = m.mid_turned[at_rows((1 - grid.lane) * tile, tile), :]
        spare = pl.ds(every, tile)
        m.wg[spare, at] = matmul(turned, m.wg[0:every, at]).astype(BF16)
        m.wu[spare, at] = matmul(turned, m.wu[0:every, at]).astype(BF16)
        m.wd[at, spare] = matmul(m.wd[at, 0:every], all_rows(m.dm_all, tile_of(1 - grid.lane))).astype(BF16)
        for copy in crossings(n):
            copy.start()
        for place, event in events.items():
            pl.when(n == place)(event)
        return carry

    tiles = hidden // STEP
    stat_dp = [
        wires.copy(m.stats, m.stat_dp.at[me], (peer(step), team.me), stat_at + 2 + step)
        for step in range(1, count)
    ]
    returned = wires.book(4 * count)
    parked = [
        wires.copy(
            source.at[deal.at(peer(step))],
            m.back_parked.at[me, i],
            (peer(step), team.me),
            returned + i * count + step,
        )
        for step in range(1, count)
        for i, source in enumerate((m.layer, m.closed))
    ]
    placed = [
        wires.copy(
            m.back_leaving.at[peer(step), i],
            target.at[deal.at(me, team.slot * shard)],
            (peer(step), team.me),
            returned + (2 + i) * count + step,
        )
        if step
        else pltpu.make_async_copy(
            m.back_leaving.at[me, i],
            target.at[deal.at(me, team.slot * shard)],
            m.put.at[i],
        )
        for step in range(count)
        for i, target in enumerate((m.layer_out, m.input_grad))
    ]
    holders = [holder(peer(step)) for step in range(count)]
    out_gathers = [gather(m.layer_out, 3), gather(m.input_grad, 4)]

    def add_stats():
        for copy in stat_team:
            copy.wait()
        total = (m.stat_team[0] + m.stat_team[1]) + (m.stat_team[2] + m.stat_team[3])
        line = lax.broadcasted_iota(jnp.int32, total.shape, 0)
        m.stats[...] = jnp.where(line == 2, m.stats[...], total)
        m.stat_dp[me] = m.stats[...]
        for copy in stat_dp:
            copy.start()

    def close(at):
        row = team.slot * shard + at.start + lax.broadcasted_iota(jnp.int32, (at.size, 1), 0)
        m.closed[at, :] = jnp.where(row < length, m.total[at, :] + m.d_mid[at, :], 0.0).astype(BF16)

    def park():
        reduce.end()
        over_rows(shard, 16, close)
        for copy in parked:
            copy.start()
        for i, source in enumerate((m.layer, m.closed)):
            m.back_parked[me, i] = source[deal.at(me)]
        hid_spread.side(groups)

    def place():
        for copy in parked:
            copy.wait()
        for step in range(count):
            for i in range(2):
                m.back_leaving[peer(step), i] = m.back_parked[holders[step], i]
        for copy in placed:
            copy.start()

    def share():
        for copy in placed:
            copy.wait()
        for one in out_gathers:
            one.start()

    events = {
        0: add_stats,
        1: park,
        tiles - 3: lambda: hid_spread.pair(groups),
        tiles - 2: lambda: branch_spread.side(groups),
    }
    lax.fori_loop(0, tiles, again, 0)
    hid_spread.drain()
    def put(source, target, index):
        return pltpu.make_async_copy(source, target, m.put.at[index])

    puts = []

    def store(value, target):
        slot = len(puts) % 2
        if len(puts) >= 2:
            puts[-2].wait()
        stage = m.stage.at[slot, pl.ds(0, value.shape[0]), pl.ds(0, value.shape[1])]
        stage[...] = value
        puts.append(put(stage, target, 2 + slot))
        puts[-1].start()

    late = []

    def bring(source, target):
        copy = pltpu.make_async_copy(source, target, m.late.at[len(late)])
        copy.start()
        late.append(copy)

    for k in range(1, groups):
        bring(m.hid_all.at[k], m.mid_all.at[k])
    turned_own = m.mid_turned.at[at_rows(grid.lane * tile, tile)]
    wide = m.stage.shape[2]
    high = rows

    def narrow_stage(slot):
        return m.stage.at[slot, :, pl.ds(0, tile)]

    def flush(copies, last, i, values):
        @pl.when(i > 0)
        def _():
            for copy in copies(i - 1):
                copy.wait()

        for copy, slot, value in zip(copies(i), last, values, strict=True):
            slot[...] = value
            copy.start()

    def wide_copies(i):
        at = at_rows(i * wide, wide)
        return [put(m.stage.at[0], m.g_own.at[:, at], 2), put(m.stage.at[1], m.u_own.at[:, at], 3)]

    def wide_part(i, carry):
        at = at_rows(i * wide, wide)
        flush(
            wide_copies,
            (m.stage.at[0], m.stage.at[1]),
            i,
            [matmul(turned_own[...], weight[0:every, at]) for weight in (m.wg, m.wu)],
        )
        return carry

    lax.fori_loop(0, hidden // wide, wide_part, 0)
    for copy in wide_copies(hidden // wide - 1):
        copy.wait()

    def high_at(i, slot):
        return at_rows((2 * i + slot) * high, high)

    def high_copies(i):
        return [put(narrow_stage(slot), m.d_own.at[high_at(i, slot), :], 2 + slot) for slot in range(2)]

    def high_part(i, carry):
        right = all_rows(m.dm_all, tile_of(grid.lane))
        flush(
            high_copies,
            (narrow_stage(0), narrow_stage(1)),
            i,
            [matmul(m.wd[high_at(i, slot), 0:every], right) for slot in range(2)],
        )
        return carry

    lax.fori_loop(0, hidden // high // 2, high_part, 0)
    for copy in high_copies(hidden // high // 2 - 1):
        copy.wait()

    for copy in late:
        copy.wait()
    for k in range(groups):
        source = m.mid_all.at[k] if k else m.hid
        m.mid_turned[:, pl.ds(k * rows, rows)] = jnp.transpose(
            source[:, at_rows(grid.group * strip, strip)]
        )
    wide_sums = RowSums(
        team, m.wide_mine, m.wide_came.at[0], m.wide_send.at[0], m.wide_recv.at[0]
    )
    spare_rows = every + tile

    def project_again(k, carry):
        block = at_rows(spare_rows + (k - 1) * rows, rows)
        lane = lax.broadcasted_iota(jnp.int32, (rows, 128), 1)
        found = jnp.zeros((rows, 128), F32)
        for i in range(2):
            raw = matmul(m.mid_all[k], m.qkv[i])
            m.wu[block, pl.ds(2 * local + i * local, local)] = raw.astype(BF16)
            found = jnp.where(lane == i, row_sum(raw * raw), found)
        m.wide_inner[at_rows((k - 1) * rows, rows), :] = found
        m.wu[block, pl.ds(local, local)] = matmul(m.mid_all[k], m.qkv[2]).astype(BF16)
        return carry

    lax.fori_loop(1, groups, project_again, 0)
    wide_sums.start(m.wide_inner[:, 0:1], m.wide_inner[:, 1:2])
    branch_spread.pair(groups)
    place()
    branch_spread.drain()
    for k in range(1, groups):
        bring(m.branch_all.at[k], m.dm_all.at[k])
    for copy in late[groups - 1 :]:
        copy.wait()
    q_total, k_total = wide_sums.finish()
    lane = lax.broadcasted_iota(jnp.int32, (every - rows, 128), 1)
    m.wide_scales[...] = lax.rsqrt(jnp.where(lane == 0, q_total, k_total) * (1.0 / D) + EPS)
    m.wide_inner[...] = jnp.zeros_like(m.wide_inner)

    def attention_again(k, carry):
        back_length = m.lengths[
            m.order[lax.rem(grid.group - k + groups, groups) * lanes + grid.lane]
        ]
        block = at_rows(spare_rows + (k - 1) * rows, rows)
        inside = at_rows((k - 1) * rows, rows)
        q_scale = m.wide_scales[inside, 0:1]
        k_scale = m.wide_scales[inside, 1:2]
        d_mix[...] = right_inner(m.dm_all[k], m.wo[...]).astype(BF16)
        q_inner = jnp.zeros((rows, 1), F32)
        k_inner = jnp.zeros((rows, 1), F32)

        def head_again(head, carry):
            at = at_rows(head * HEAD, HEAD)
            q_unit = m.wu[block, at_rows(2 * local + head * HEAD, HEAD)].astype(F32) * q_scale
            k_unit = m.wu[block, at_rows(3 * local + head * HEAD, HEAD)].astype(F32) * k_scale
            mix, d_v, d_q_hat, d_k_hat = head_back(
                turn(q_unit * m.q_gain[:, at], m.cosine[...], m.sine[...]).astype(BF16),
                turn(k_unit * m.k_gain[:, at], m.cosine[...], m.sine[...]).astype(BF16),
                m.wu[block, at_rows(local + head * HEAD, HEAD)],
                d_mix[:, at],
                m.cosine[...],
                m.sine[...],
                back_length,
            )
            m.wu[block, at] = mix
            m.wg[block, at_rows(2 * local + head * HEAD, HEAD)] = d_v
            q_scaled = d_q_hat * m.q_gain[:, at]
            k_scaled = d_k_hat * m.k_gain[:, at]
            m.wg[block, at] = q_scaled.astype(BF16)
            m.wg[block, at_rows(local + head * HEAD, HEAD)] = k_scaled.astype(BF16)
            return carry[0] + row_sum(q_scaled * q_unit), carry[1] + row_sum(k_scaled * k_unit)

        q_inner, k_inner = lax.fori_loop(0, local // HEAD, head_again, (q_inner, k_inner))
        lane = lax.broadcasted_iota(jnp.int32, (rows, 128), 1)
        m.wide_inner[inside, :] = jnp.where(lane == 0, q_inner, jnp.where(lane == 1, k_inner, 0.0))
        return carry

    lax.fori_loop(1, groups, attention_again, 0)
    wide_sums = RowSums(
        team, m.wide_mine, m.wide_came.at[1], m.wide_send.at[1], m.wide_recv.at[1]
    )
    wide_sums.start(m.wide_inner[:, 0:1], m.wide_inner[:, 1:2])
    other, this = 1 - grid.lane, grid.lane
    others = pl.ds(spare_rows, every - rows)

    def lane_of(lane):
        return at_rows(grid.group * strip + lane * tile, tile)

    def o_part(lane):
        return left_inner(m.mix[...], m.d_branch[:, lane_of(lane)]) + left_inner(
            m.wu[others, 0:local],
            m.dm_all[1:groups, :, lane_of(lane)].reshape(every - rows, tile),
        )

    def heads_part(lane, at):
        turned = m.mid_turned.at[at_rows(lane * tile, tile)]
        return matmul(turned[:, 0:rows], m.d_heads[:, at]) + matmul(
            turned[:, rows:every], m.wg[others, at]
        )

    last = wires.book(4)
    finals = []
    spare = m.qkv.at[2, pl.ds(3 * tile, local), pl.ds(0, tile)]
    spare[...] = o_part(other).astype(BF16)
    finals.append(wires.copy(spare, m.x_o, crossing, last + 3))
    finals[-1].start()
    q_inner, k_inner = wide_sums.finish()
    lane = lax.broadcasted_iota(jnp.int32, (every - rows, 128), 1)
    m.wide_inner[...] = jnp.where(lane == 0, q_inner, k_inner)

    def close_heads(k, carry):
        block = at_rows(spare_rows + (k - 1) * rows, rows)
        inside = at_rows((k - 1) * rows, rows)
        for i in range(2):
            at = pl.ds(i * local, local)
            scale = m.wide_scales[inside, i : i + 1]
            factor = scale * scale * m.wide_inner[inside, i : i + 1] * (1.0 / D)
            raw = m.wu[block, pl.ds(2 * local + i * local, local)].astype(F32)
            m.wg[block, at] = (scale * m.wg[block, at].astype(F32) - raw * factor).astype(BF16)
        return carry

    lax.fori_loop(1, groups, close_heads, 0)
    for i, target in ((2, m.x_v), (0, m.x_q), (1, m.x_k)):
        spare = m.qkv.at[2, pl.ds(i * tile, tile)]
        spare[...] = heads_part(other, pl.ds(i * local, local)).astype(BF16)
        finals.append(wires.copy(spare, target, crossing, last + i))
        finals[-1].start()
    share()
    for i, target in enumerate((m.q_own, m.k_own, m.v_own)):
        store(heads_part(this, pl.ds(i * local, local)), target)
    output = o_part(this)
    for i in range(local // high):
        store(output[i * high : (i + 1) * high], m.o_own.at[pl.ds(i * high, high), :])
    for copy in puts[-2:]:
        copy.wait()

    def arrived(n, carry):
        for copy in crossings(n):
            copy.wait()
        return carry

    for one in out_gathers:
        one.half()
    for one in out_gathers:
        one.finish()
    for copy in stat_dp:
        copy.wait()
    m.stat_out[...] = sum([m.stat_dp[i] for i in range(1, count)], m.stat_dp[0])
    lax.fori_loop(0, tiles, arrived, 0)
    for copy in finals:
        copy.wait()


def whole_layer(grid, args):
    (hidden_in, upstream, lengths, order, q_weight, k_weight, v_weight, o_weight) = args[:8]
    (q_gain, k_gain, a_gain, g_weight, u_weight, d_weight, m_gain, cosine, sine) = args[8:]
    rows, width = hidden_in.shape
    local, hidden = q_weight.shape[1], g_weight.shape[1]
    count, groups = grid.count, grid.groups
    shard, strip, tile = rows // SLOTS, width // groups, width // count
    every = groups * rows
    deal = Deal(count, shard, width)
    chunk = (deal.rows, deal.columns)
    inputs = [
        ("lengths", SCALAR, lengths),
        ("order", SCALAR, order),
        ("hidden_in", ANY, hidden_in),
        ("upstream", ANY, upstream),
        ("q_weight", ANY, q_weight),
        ("k_weight", ANY, k_weight),
        ("v_weight", ANY, v_weight),
        ("o_weight", ANY, o_weight),
        ("g_weight", ANY, g_weight),
        ("u_weight", ANY, u_weight),
        ("d_weight", ANY, d_weight),
        ("q_gain", ON_CHIP, q_gain),
        ("k_gain", ON_CHIP, k_gain),
        ("a_gain", ON_CHIP, a_gain),
        ("m_gain", ON_CHIP, m_gain),
        ("cosine", ON_CHIP, cosine),
        ("sine", ON_CHIP, sine),
    ]
    outputs = [
        ("layer_out", (rows, width), BF16),
        ("input_grad", (rows, width), BF16),
        ("g_own", (tile, hidden), F32),
        ("u_own", (tile, hidden), F32),
        ("d_own", (hidden, tile), F32),
        ("q_own", (tile, local), F32),
        ("k_own", (tile, local), F32),
        ("v_own", (tile, local), F32),
        ("o_own", (local, tile), F32),
        ("x_gate", (tile, hidden), BF16),
        ("x_up", (tile, hidden), BF16),
        ("x_down", (hidden, tile), BF16),
        ("x_q", (tile, local), BF16),
        ("x_k", (tile, local), BF16),
        ("x_v", (tile, local), BF16),
        ("x_o", (local, tile), BF16),
        ("hid_all", (groups, rows, width), BF16),
        ("branch_all", (groups, rows, width), BF16),
        ("stat_out", (8, width), F32),
    ]
    wires = 160
    scratch = [
        ("qkv", pltpu.VMEM((3, width, local), BF16)),
        ("wo", pltpu.VMEM((local, width), BF16)),
        ("wg", pltpu.VMEM((width, hidden), BF16)),
        ("wu", pltpu.VMEM((width, hidden), BF16)),
        ("wd", pltpu.VMEM((hidden, width), BF16)),
        ("hid", pltpu.VMEM((rows, width), BF16)),
        ("mid_all", pltpu.VMEM((groups, rows, width), BF16)),
        ("dm_all", pltpu.VMEM((groups, rows, width), BF16)),
        ("gate", pltpu.VMEM((rows, hidden), BF16)),
        ("upper", pltpu.VMEM((rows, hidden), BF16)),
        ("inner", pltpu.VMEM((rows, hidden), BF16)),
        ("q_raw", pltpu.VMEM((rows, local), F32)),
        ("k_raw", pltpu.VMEM((rows, local), F32)),
        ("queries", pltpu.VMEM((rows, local), BF16)),
        ("keys", pltpu.VMEM((rows, local), BF16)),
        ("values", pltpu.VMEM((rows, local), BF16)),
        ("scales", pltpu.VMEM((rows, 128), F32)),
        ("mix", pltpu.VMEM((rows, local), BF16)),
        ("d_branch", pltpu.VMEM((rows, width), BF16)),
        ("d_heads", pltpu.VMEM((rows, 3 * local), BF16)),
        ("mid_turned", pltpu.VMEM((strip, every), BF16)),
        ("keep", pltpu.VMEM((3, every - rows, STEP), BF16)),
        ("stage", pltpu.VMEM((2, rows, local), F32)),
        ("branch", pltpu.VMEM((shard, width), F32)),
        ("d_mid", pltpu.VMEM((shard, width), F32)),
        ("layer", pltpu.VMEM((shard, width), BF16)),
        ("closed", pltpu.VMEM((shard, width), BF16)),
        ("grad_in", pltpu.VMEM((shard, width), BF16)),
        ("back_parked", pltpu.VMEM((count, 2) + chunk, BF16)),
        ("back_leaving", pltpu.VMEM((count, 2) + chunk, BF16)),
        ("fold", pltpu.VMEM((4, 8, width), F32)),
        ("stats", pltpu.VMEM((8, width), F32)),
        ("stat_team", pltpu.VMEM((SLOTS, 8, width), F32)),
        ("stat_dp", pltpu.VMEM((count, 8, width), F32)),
        ("partial", pltpu.VMEM((rows, width), BF16)),
        ("came", pltpu.VMEM((3, shard, width), BF16)),
        ("gone", pltpu.VMEM((shard, width), BF16)),
        ("total", pltpu.VMEM((shard, width), F32)),
        ("sum_mine", pltpu.VMEM((8, rows), F32)),
        ("sum_came", pltpu.VMEM((3, 8, rows), F32)),
        ("wide_mine", pltpu.VMEM((8, every - rows), F32)),
        ("wide_came", pltpu.VMEM((2, 3, 8, every - rows), F32)),
        ("wide_scales", pltpu.VMEM((every - rows, 128), F32)),
        ("wide_inner", pltpu.VMEM((every - rows, 128), F32)),
        ("wide_send", pltpu.SemaphoreType.DMA((2, 3))),
        ("wide_recv", pltpu.SemaphoreType.DMA((2, 3))),
        ("sum_send", pltpu.SemaphoreType.DMA((3,))),
        ("sum_recv", pltpu.SemaphoreType.DMA((3,))),
        ("reduce_send", pltpu.SemaphoreType.DMA((3, SPLIT))),
        ("reduce_recv", pltpu.SemaphoreType.DMA((3, SPLIT))),
        ("gather_send", pltpu.SemaphoreType.DMA((5, 3))),
        ("gather_recv", pltpu.SemaphoreType.DMA((5, 3))),
        ("wire_send", pltpu.SemaphoreType.DMA((wires,))),
        ("wire_recv", pltpu.SemaphoreType.DMA((wires,))),
        ("load", pltpu.SemaphoreType.DMA((9,))),
        ("put", pltpu.SemaphoreType.DMA((4,))),
        ("late", pltpu.SemaphoreType.DMA((2 * groups,))),
    ]
    names = [entry[0] for entry in inputs + outputs + scratch]
    results = pl.pallas_call(
        functools.partial(layer_kernel, names),
        out_shape=shaped(*[entry[1:] for entry in outputs]),
        in_specs=[entry[1] for entry in inputs],
        out_specs=(ANY,) * (len(outputs) - 1) + (ON_CHIP,),
        scratch_shapes=[entry[1] for entry in scratch],
        compiler_params=pltpu.CompilerParams(
            collective_id=4, has_side_effects=True, vmem_limit_bytes=63 * 2**20
        ),
        name="whole_layer",
    )(*[entry[2] for entry in inputs])
    return dict(zip([entry[0] for entry in outputs], results, strict=True))


def body(
    hidden_in,
    upstream_grad,
    seq_lengths,
    position_order,
    query_weight,
    key_weight,
    value_weight,
    output_weight,
    query_gain,
    key_gain,
    attn_gain,
    gate_weight,
    up_weight,
    down_weight,
    mlp_gain,
):
    count = lax.axis_size("dp")
    ways = lax.axis_size("tensor")
    myself = lax.axis_index("dp")
    part = lax.axis_index("tensor")
    grid = Grid(count)
    index = jnp.arange(count, dtype=jnp.int32)
    inverse = jnp.sum(
        index[None, :] * (position_order[None, :] == index[:, None]).astype(jnp.int32), axis=1
    )
    rows = hidden_in.shape[1]
    width = hidden_in.shape[2]
    shard = rows // ways
    if grid.lanes == 2 and grid.groups * rows + width // count <= width:
        cosine, sine = rope_constants(rows, HEAD)
        found = whole_layer(
            grid,
            (
                hidden_in[0],
                upstream_grad[0],
                seq_lengths,
                position_order,
                query_weight,
                key_weight,
                value_weight,
                output_weight,
                query_gain[None],
                key_gain[None],
                attn_gain[None],
                gate_weight,
                up_weight,
                down_weight,
                mlp_gain[None],
                cosine,
                sine,
            ),
        )
        local = query_weight.shape[1]

        def joined(own, other):
            return found[own] + found[other].astype(F32)

        stats = found["stat_out"]
        squares = jnp.sum(stats[3:6], axis=1)
        return (
            found["layer_out"][None],
            found["input_grad"][None],
            joined("q_own", "x_q"),
            joined("k_own", "x_k"),
            joined("v_own", "x_v"),
            joined("o_own", "x_o"),
            stats[2, :local],
            stats[2, local : 2 * local],
            stats[1],
            joined("g_own", "x_gate"),
            joined("u_own", "x_up"),
            joined("d_own", "x_down"),
            stats[0],
            jnp.sqrt(squares / (jnp.sum(seq_lengths).astype(F32) * D)),
        )

    piece = shard // count
    seq_here = jnp.sum(jnp.where(index == myself, position_order, 0))
    length = jnp.sum(jnp.where(index == seq_here, seq_lengths, 0))[None]
    slot = part % 2 * 2 + part // 2

    def exchange(pieces):
        return lax.all_to_all(pieces, "dp", split_axis=0, concat_axis=0, tiled=True)

    def my_rows(field):
        return lax.dynamic_slice_in_dim(field, slot * shard, shard, axis=0)

    first = exchange(my_rows(upstream_grad[0]).reshape(count, piece, width))
    second = exchange(jnp.take(first, position_order, axis=0))
    grad_in = second.reshape(shard, width)

    rows_low = hidden_in[0]
    my_low = my_rows(rows_low)
    local = query_weight.shape[1]
    strip = width // grid.groups
    tile = width // count

    def strip_of(field, group):
        return lax.dynamic_slice_in_dim(field, group * strip, strip, axis=1)

    def strips(field):
        found = [strip_of(field, grid.group)]
        for step in range(1, grid.groups):
            found.append(
                grid.shift_groups(
                    strip_of(field, (grid.group + step) % grid.groups), step
                )
            )
        return jnp.concatenate(found, axis=0)

    def tile_of(field, lane):
        return lax.dynamic_slice_in_dim(field, lane * tile, tile, axis=1)

    def reduced(product, field):
        sent = []
        for step in range(1, grid.lanes):
            other = product(tile_of(field, (grid.lane + step) % grid.lanes)).astype(BF16)
            sent.append(grid.shift_lanes(other, step))
        mine = product(tile_of(field, grid.lane))
        for other in sent:
            mine = mine + other.astype(F32)
        return mine

    hidden_strips = strips(rows_low)

    cosine, sine = rope_tables(rows, HEAD)
    cosine = jnp.concatenate([cosine, cosine], axis=1)
    sine = jnp.concatenate([-sine, sine], axis=1)
    gains = (query_gain[None], key_gain[None])
    q_raw, k_raw, queries, keys, values, scales, attn_mix, branch, mid_low = attend(
        length,
        rows_low,
        my_low,
        (query_weight, key_weight, value_weight, output_weight),
        gains,
        cosine,
        sine,
        attn_gain[None],
    )
    mix_all = jnp.concatenate([attn_mix] + grid.ring(attn_mix), axis=0)
    mid_others = shared_ring(grid, mid_low)

    gate = matmul(mid_low, gate_weight)
    upper = matmul(mid_low, up_weight)
    sig = jax.nn.sigmoid(gate)
    inner = (gate * sig * upper).astype(BF16)
    layer, d_mlp, mlp_gain_part, squares = settle(
        length,
        matmul(inner, down_weight).astype(BF16),
        my_low,
        branch,
        grad_in,
        attn_gain[None],
        mlp_gain[None],
    )
    d_mlp_others = shared_ring(grid, d_mlp)

    def inner_back(gate, upper, d_mlp):
        d_inner = right_inner(d_mlp, down_weight)
        sig = jax.nn.sigmoid(gate)
        d_gate = (d_inner * upper * sig * (1.0 + gate * (1.0 - sig))).astype(BF16)
        d_up = (d_inner * gate * sig).astype(BF16)
        return d_gate, d_up

    d_gate, d_up = inner_back(gate, upper, d_mlp)
    d_mid, attn_gain_part, d_branch, d_heads, query_gain_part, key_gain_part = unattend(
        length,
        (right_inner(d_gate, gate_weight) + right_inner(d_up, up_weight)).astype(BF16),
        branch,
        grad_in,
        attn_gain[None],
        output_weight,
        (q_raw, k_raw, queries, keys, values, scales),
        gains,
        cosine,
        sine,
    )
    d_branch_strips = strips(d_branch)
    d_heads_all = jnp.concatenate([d_heads] + grid.ring(d_heads), axis=0)
    layer_out, input_grad = close_layer(
        length,
        inverse,
        (
            right_inner(d_heads[:, :local], query_weight)
            + right_inner(d_heads[:, local : 2 * local], key_weight)
            + right_inner(d_heads[:, 2 * local :], value_weight)
        ).astype(BF16),
        d_mid,
        layer,
    )

    gate_o = matmul(mid_others, gate_weight)
    upper_o = matmul(mid_others, up_weight)
    inner_o = (jax.nn.silu(gate_o) * upper_o).astype(BF16)
    d_gate_o, d_up_o = inner_back(gate_o, upper_o, d_mlp_others)

    def strip_all(own, others):
        return jnp.concatenate([strip_of(own, grid.group), strip_of(others, grid.group)], axis=0)

    mid_strips = strip_all(mid_low, mid_others)
    d_mlp_strips = strip_all(d_mlp, d_mlp_others)
    d_gate_all = jnp.concatenate([d_gate, d_gate_o], axis=0)
    d_up_all = jnp.concatenate([d_up, d_up_o], axis=0)
    inner_all = jnp.concatenate([inner, inner_o], axis=0)
    gate_part = reduced(lambda tile: left_inner(tile, d_gate_all), mid_strips)
    up_part = reduced(lambda tile: left_inner(tile, d_up_all), mid_strips)
    down_part = reduced(lambda tile: left_inner(inner_all, tile), d_mlp_strips)
    output_part = reduced(lambda tile: left_inner(mix_all, tile), d_branch_strips)
    heads_part = reduced(lambda tile: left_inner(tile, d_heads_all), hidden_strips)
    query_part = heads_part[:, :local]
    key_part = heads_part[:, local : 2 * local]
    value_part = heads_part[:, 2 * local :]

    shared = jnp.concatenate(
        [jnp.sum(attn_gain_part, axis=0), jnp.sum(mlp_gain_part, axis=0), jnp.sum(squares, axis=(1, 2))]
    )
    shared = shared + sibling(shared)
    shared = shared + across(shared)
    sums = grid.total(jnp.concatenate([shared, query_gain_part[0], key_gain_part[0]]))
    attn_gain_grad = sums[:width]
    mlp_gain_grad = sums[width : 2 * width]
    squares = sums[2 * width : 2 * width + 3]
    query_gain_grad = sums[2 * width + 3 : 2 * width + 3 + local]
    key_gain_grad = sums[2 * width + 3 + local :]
    rms_values = jnp.sqrt(squares / (jnp.sum(seq_lengths).astype(F32) * D))

    return (
        layer_out[None],
        input_grad[None],
        query_part,
        key_part,
        value_part,
        output_part,
        query_gain_grad,
        key_gain_grad,
        attn_gain_grad,
        gate_part,
        up_part,
        down_part,
        mlp_gain_grad,
        rms_values,
    )


def solution(mesh):
    placed = (
        P("dp", None, None),
        P("dp", None, None),
        P(),
        P(),
        P(None, "tensor"),
        P(None, "tensor"),
        P(None, "tensor"),
        P("tensor", None),
        P("tensor"),
        P("tensor"),
        P(),
        P(None, "tensor"),
        P(None, "tensor"),
        P("tensor", None),
        P(),
    )
    return jax.shard_map(
        body,
        mesh=mesh,
        in_specs=placed,
        out_specs=(
            P("dp", None, None),
            P("dp", None, None),
            P("dp", "tensor"),
            P("dp", "tensor"),
            P("dp", "tensor"),
            P("tensor", "dp"),
            P("tensor"),
            P("tensor"),
            P(),
            P("dp", "tensor"),
            P("dp", "tensor"),
            P("tensor", "dp"),
            P(),
            P(),
        ),
        check_vma=False,
    )
```

```python
import functools
import math
import types

import jax
import jax.numpy as jnp
import numpy as np
from jax import lax
from jax.experimental import pallas as pl
from jax.experimental.pallas import tpu as pltpu
from jax.sharding import PartitionSpec as P

D = 2048
HEAD = 128
EPS = 1e-06
F32 = jnp.float32
BF16 = jnp.bfloat16


def matmul(left, right):
    return jnp.dot(left, right, preferred_element_type=F32)


def left_inner(left, right):
    return lax.dot_general(left, right, (((0,), (0,)), ((), ())), preferred_element_type=F32)


def right_inner(left, right):
    return lax.dot_general(left, right, (((1,), (1,)), ((), ())), preferred_element_type=F32)


def rope_tables(rows, width):
    places = jnp.arange(rows, dtype=F32)
    freq = jnp.power(F32(500000.0), -jnp.arange(width // 2, dtype=F32) * (2.0 / width))
    angle = places[:, None] * freq[None, :]
    return (jnp.cos(angle), jnp.sin(angle))


def rope_constants(rows, width):
    half = width // 2
    exponent = -np.arange(half, dtype=np.float32) * np.float32(2.0 / width)
    freq = np.power(np.float32(500000.0), exponent, dtype=np.float32)
    angle = (np.arange(rows, dtype=np.float32)[:, None] * freq[None, :]).astype(np.float64)
    cosine, sine = np.cos(angle), np.sin(angle)
    return (
        jnp.asarray(np.concatenate([cosine, cosine], axis=1), F32),
        jnp.asarray(np.concatenate([-sine, sine], axis=1), F32),
    )


class Grid:
    def __init__(self, count):
        self.count = count
        self.lanes = 2 ** ((count.bit_length() - 1) // 2)
        self.groups = count // self.lanes
        me = lax.axis_index("dp")
        self.group = me // self.lanes
        self.lane = me % self.lanes

    def shift_groups(self, field, step):
        pairs = [
            (g * self.lanes + a, ((g + step) % self.groups) * self.lanes + a)
            for g in range(self.groups)
            for a in range(self.lanes)
        ]
        return lax.ppermute(field, "dp", pairs)

    def shift_lanes(self, field, step):
        pairs = [
            (g * self.lanes + a, g * self.lanes + (a + step) % self.lanes)
            for g in range(self.groups)
            for a in range(self.lanes)
        ]
        return lax.ppermute(field, "dp", pairs)

    def ring(self, field):
        found = []
        for _ in range(self.groups - 1):
            field = self.shift_groups(field, 1)
            found.append(field)
        return found

    def total(self, field):
        step = 1
        while step < self.count:
            field = field + lax.ppermute(
                field, "dp", [(i, i ^ step) for i in range(self.count)]
            )
            step *= 2
        return field


def sibling(field):
    size = lax.axis_size("tensor")
    return lax.ppermute(field, "tensor", [(i, i ^ 1) for i in range(size)])


def across(field):
    size = lax.axis_size("tensor")
    return lax.ppermute(field, "tensor", [(i, (i + 2) % size) for i in range(size)])


def shared_ring(grid, rows_low):
    core = lax.axis_index("tensor") % 2
    half = rows_low.shape[0] // 2
    mine = lax.dynamic_slice_in_dim(rows_low, core * half, half, axis=0)
    pieces = []
    for piece in grid.ring(mine):
        pieces += [piece, sibling(piece)]
    return jnp.concatenate(pieces, axis=0)


SLOTS = 4
TILES = 4
AT = pl.DeviceIdType.MESH
VMEM_CAP = 56 * 2**20


class Team:
    def __init__(self):
        self.row = lax.axis_index("dp")
        self.me = lax.axis_index("tensor")
        self.side = self.me // 2
        self.core = self.me % 2
        self.slot = self.core * 2 + self.side
        self.sibling = self.side * 2 + (1 - self.core)
        self.across = (1 - self.side) * 2 + self.core
        self.far = (1 - self.side) * 2 + (1 - self.core)

    def meet(self, *others):
        barrier = pltpu.get_barrier_semaphore()
        for other in others:
            pl.semaphore_signal(barrier, inc=1, device_id=(self.row, other), device_id_type=AT)
        pl.semaphore_wait(barrier, len(others))

    def copy(self, source, target, send, recv, other):
        return pltpu.make_async_remote_copy(
            src_ref=source,
            dst_ref=target,
            send_sem=send,
            recv_sem=recv,
            device_id=(self.row, other),
            device_id_type=AT,
        )


def at_rows(start, size):
    return pl.ds(pl.multiple_of(start, size), size)


class Reduce:
    def scratch(rows, width):
        shard = rows // SLOTS
        return [
            pltpu.VMEM((rows, width), BF16),
            pltpu.VMEM((3, shard, width), BF16),
            pltpu.VMEM((shard, width), BF16),
            pltpu.VMEM((shard, width), F32),
            pltpu.SemaphoreType.DMA((3, TILES)),
            pltpu.SemaphoreType.DMA((3, TILES)),
        ]

    def __init__(self, team, partial, came, gone, total, send, recv):
        self.team, self.partial, self.came, self.gone, self.total = team, partial, came, gone, total
        self.shard, width = total.shape
        self.tiles = send.shape[1]
        self.tile = width // self.tiles
        self.send, self.recv = send, recv
        self.copies = {}

    def columns(self, tile):
        return pl.ds(tile * self.tile, self.tile)

    def block(self, core, side):
        return at_rows((core * 2 + side) * self.shard, self.shard)

    def launch(self, kind, tile, source, other):
        copy = self.team.copy(
            source,
            self.came.at[kind, :, self.columns(tile)],
            self.send.at[kind, tile],
            self.recv.at[kind, tile],
            other,
        )
        copy.start()
        self.copies[kind, tile] = copy

    def offer(self, tile):
        team, columns = self.team, self.columns(tile)
        for kind, side in ((0, 1 - team.side), (1, team.side)):
            self.launch(
                kind, tile, self.partial.at[self.block(1 - team.core, side), columns], team.sibling
            )

    def pass_on(self, tile):
        team, columns = self.team, self.columns(tile)
        self.copies[0, tile].wait_recv()
        mine = self.partial[self.block(team.core, 1 - team.side), columns].astype(F32)
        self.gone[:, columns] = (mine + self.came[0, :, columns].astype(F32)).astype(BF16)
        self.launch(2, tile, self.gone.at[:, columns], team.across)

    def finish(self, tile):
        team, columns = self.team, self.columns(tile)
        self.copies[1, tile].wait_recv()
        mine = self.partial[self.block(team.core, team.side), columns].astype(F32)
        mine = mine + self.came[1, :, columns].astype(F32)
        self.copies[2, tile].wait_recv()
        self.total[:, columns] = mine + self.came[2, :, columns].astype(F32)

    def settle(self):
        for copy in self.copies.values():
            copy.wait_send()

    def begin(self, make):
        self.copies = {}
        for tile in range(self.tiles):
            make(self.columns(tile))
            self.offer(tile)
            if tile:
                self.pass_on(tile - 1)
        self.pass_on(self.tiles - 1)

    def end(self):
        for tile in range(self.tiles):
            self.finish(tile)
        self.settle()

    def run(self, make):
        self.begin(make)
        self.end()


class Gather:
    scratch = [pltpu.SemaphoreType.DMA((3,)), pltpu.SemaphoreType.DMA((3,))]

    def __init__(self, team, whole, send, recv):
        self.team, self.whole = team, whole
        shard = whole.shape[0] // SLOTS
        mine = whole.at[at_rows(team.slot * shard, shard)]
        theirs = whole.at[at_rows((team.core * 2 + 1 - team.side) * shard, shard)]
        self.across = team.copy(mine, mine, send.at[0], recv.at[0], team.across)
        self.near = team.copy(mine, mine, send.at[1], recv.at[1], team.sibling)
        self.relay = team.copy(theirs, theirs, send.at[2], recv.at[2], team.sibling)

    def start(self):
        self.across.start()
        self.near.start()

    def half(self):
        self.across.wait_recv()
        self.relay.start()

    def finish(self):
        self.across.wait_send()
        self.near.wait()
        self.relay.wait()


class RowSums:
    def scratch(rows):
        return [
            pltpu.VMEM((8, rows), F32),
            pltpu.VMEM((3, 8, rows), F32),
            pltpu.SemaphoreType.DMA((3,)),
            pltpu.SemaphoreType.DMA((3,)),
        ]

    def __init__(self, team, mine, came, send, recv):
        self.team, self.mine, self.came = team, mine, came
        self.copies = [
            team.copy(mine, came.at[i], send.at[i], recv.at[i], other)
            for i, other in enumerate((team.sibling, team.across, team.far))
        ]

    def start(self, first, second):
        rows = first.shape[0]
        lane = lax.broadcasted_iota(jnp.int32, (rows, 128), 1)
        both = jnp.where(lane == 0, first, jnp.where(lane == 1, second, 0.0))
        self.mine[...] = jnp.transpose(both)[:8]
        for copy in self.copies:
            copy.start()

    def finish(self):
        for copy in self.copies:
            copy.wait()
        total = self.mine[...] + self.came[0] + (self.came[1] + self.came[2])
        rows = total.shape[1]
        wide = jnp.transpose(jnp.concatenate([total] * 16, axis=0))
        return wide[:, 0:1], wide[:, 1:2]


def turn(field, cosine, sine):
    return field * cosine + pltpu.roll(field, HEAD // 2, 1) * sine


def head_probs(queries, keys, length):
    rows = queries.shape[0]
    scores = right_inner(queries, keys) * (1.0 / math.sqrt(HEAD))
    row = lax.broadcasted_iota(jnp.int32, (rows, rows), 0)
    column = lax.broadcasted_iota(jnp.int32, (rows, rows), 1)
    masked = jnp.where((column <= row) & (column < length), scores, -1e30)
    expo = jnp.exp(masked - jnp.max(masked, axis=-1, keepdims=True))
    return expo / jnp.sum(expo, axis=-1, keepdims=True)


def row_sum(field):
    return jnp.sum(field, axis=-1, keepdims=True)


def over_rows(count, step, work):
    def one(i, carry):
        work(pl.ds(pl.multiple_of(i * step, step), step))
        return carry

    lax.fori_loop(0, count // step, one, 0)


def attend_kernel(
    length_ref,
    hidden,
    mine_hidden,
    q_weight,
    k_weight,
    v_weight,
    o_weight,
    q_gain,
    k_gain,
    cosine,
    sine,
    a_gain,
    q_raw,
    k_raw,
    queries,
    keys,
    values,
    scales,
    mix,
    branch,
    mid_low,
    weights,
    out_weight,
    load,
    *scratch,
):
    team = Team()
    sums = RowSums(team, *scratch[0:4])
    reduce = Reduce(team, *scratch[4:10])
    gather = Gather(team, mid_low, *scratch[10:12])
    loads = [
        pltpu.make_async_copy(source, weights.at[i], load.at[i])
        for i, source in enumerate((q_weight, k_weight, v_weight))
    ] + [pltpu.make_async_copy(o_weight, out_weight, load.at[3])]
    for one in loads:
        one.start()
    team.meet(team.sibling, team.across, team.far)
    rows, local = mix.shape
    width = mid_low.shape[1]
    length = length_ref[0]

    def project(i):
        loads[i].wait()
        return matmul(hidden[...], weights[i])

    q = project(0)
    q_raw[...] = q
    k = project(1)
    k_raw[...] = k
    sums.start(row_sum(q * q), row_sum(k * k))
    values[...] = project(2).astype(BF16)
    q_total, k_total = sums.finish()
    q_scale = lax.rsqrt(q_total * (1.0 / D) + EPS)
    k_scale = lax.rsqrt(k_total * (1.0 / D) + EPS)
    lane = lax.broadcasted_iota(jnp.int32, (rows, 128), 1)
    scales[...] = jnp.where(lane == 0, q_scale, k_scale)
    for head in range(local // HEAD):
        at = pl.ds(head * HEAD, HEAD)
        q = turn(q_raw[:, at] * q_scale * q_gain[:, at], cosine[...], sine[...]).astype(BF16)
        k = turn(k_raw[:, at] * k_scale * k_gain[:, at], cosine[...], sine[...]).astype(BF16)
        queries[:, at] = q
        keys[:, at] = k
        probs = head_probs(q, k, length).astype(BF16)
        mix[:, at] = matmul(probs, values[:, at]).astype(BF16)
    loads[3].wait()

    def make(at):
        reduce.partial[:, at] = matmul(mix[...], out_weight[:, at]).astype(BF16)

    reduce.run(make)
    shard = reduce.shard

    def norm(at):
        part = reduce.total[at, :]
        branch[at, :] = part
        unit = part * lax.rsqrt(row_sum(part * part) * (1.0 / D) + EPS)
        mid = mine_hidden[at, :].astype(F32) + a_gain[...] * unit
        whole_at = pl.ds(pl.multiple_of(team.slot * shard + at.start, at.size), at.size)
        mid_low[whole_at, :] = mid.astype(BF16)

    over_rows(shard, 16, norm)
    gather.start()
    gather.half()
    gather.finish()


ANY = pl.BlockSpec(memory_space=pl.ANY)
ON_CHIP = pl.BlockSpec(memory_space=pltpu.VMEM)
SCALAR = pl.BlockSpec(memory_space=pltpu.SMEM)


def shaped(*pairs):
    return tuple(jax.ShapeDtypeStruct(shape, kind) for shape, kind in pairs)


def attend(length, hidden, mine_hidden, weights, gains, cosine, sine, a_gain):
    rows, width = hidden.shape
    local = weights[0].shape[1]
    shard = rows // SLOTS
    return pl.pallas_call(
        attend_kernel,
        out_shape=shaped(
            ((rows, local), F32),
            ((rows, local), F32),
            ((rows, local), BF16),
            ((rows, local), BF16),
            ((rows, local), BF16),
            ((rows, 128), F32),
            ((rows, local), BF16),
            ((shard, width), F32),
            ((rows, width), BF16),
        ),
        in_specs=[SCALAR, ON_CHIP, ON_CHIP] + [ANY] * 4 + [ON_CHIP] * 5,
        out_specs=(ON_CHIP,) * 9,
        scratch_shapes=[
            pltpu.VMEM((3, width, local), BF16),
            pltpu.VMEM((local, width), BF16),
            pltpu.SemaphoreType.DMA((4,)),
        ]
        + RowSums.scratch(rows)
        + Reduce.scratch(rows, width)
        + Gather.scratch,
        compiler_params=pltpu.CompilerParams(
            collective_id=0, has_side_effects=True, vmem_limit_bytes=VMEM_CAP
        ),
        name="attend",
    )(length, hidden, mine_hidden, *weights, *gains, cosine, sine, a_gain)


def settle_kernel(
    length_ref,
    partial_in,
    mine_hidden,
    branch,
    grad_in,
    a_gain,
    m_gain,
    layer,
    d_mlp,
    m_gain_part,
    squares,
    *scratch,
):
    team = Team()
    reduce = Reduce(team, *scratch[0:6])
    gather = Gather(team, d_mlp, *scratch[6:8])
    team.meet(team.sibling, team.across)

    def make(at):
        reduce.partial[:, at] = partial_in[:, at]

    reduce.run(make)
    shard = reduce.shard
    length = length_ref[0]
    m_gain_part[...] = jnp.zeros_like(m_gain_part)
    squares[...] = jnp.zeros_like(squares)

    def folded(field):
        return sum([field[8 * i : 8 * i + 8] for i in range(field.shape[0] // 8)])

    def norm(at):
        part = reduce.total[at, :]
        scale = lax.rsqrt(row_sum(part * part) * (1.0 / D) + EPS)
        unit = part * scale
        base = branch[at, :]
        a_unit = base * lax.rsqrt(row_sum(base * base) * (1.0 / D) + EPS)
        attn_out = a_gain[...] * a_unit
        mlp_out = m_gain[...] * unit
        rows_f = mine_hidden[at, :].astype(F32)
        row = team.slot * shard + at.start + lax.broadcasted_iota(jnp.int32, (at.size, 1), 0)
        live = row < length
        layer[at, :] = jnp.where(live, rows_f + attn_out + mlp_out, 0.0).astype(BF16)
        grad = jnp.where(live, grad_in[at, :].astype(F32), 0.0)
        m_gain_part[...] += folded(grad * unit)
        for i, field in enumerate((rows_f, attn_out, mlp_out)):
            squares[i] += folded(jnp.where(live, field * field, 0.0))
        scaled = grad * m_gain[...]
        back = scale * (scaled - unit * (row_sum(scaled * unit) * (1.0 / D)))
        whole_at = pl.ds(pl.multiple_of(team.slot * shard + at.start, at.size), at.size)
        d_mlp[whole_at, :] = back.astype(BF16)

    over_rows(shard, 16, norm)
    gather.start()
    gather.half()
    gather.finish()


def settle(length, partial, mine_hidden, branch, grad_in, a_gain, m_gain):
    rows, width = partial.shape
    shard = rows // SLOTS
    return pl.pallas_call(
        settle_kernel,
        out_shape=shaped(
            ((shard, width), BF16),
            ((rows, width), BF16),
            ((8, width), F32),
            ((3, 8, width), F32),
        ),
        in_specs=[SCALAR] + [ON_CHIP] * 6,
        out_specs=(ON_CHIP,) * 4,
        scratch_shapes=Reduce.scratch(rows, width) + Gather.scratch,
        compiler_params=pltpu.CompilerParams(
            collective_id=1, has_side_effects=True, vmem_limit_bytes=VMEM_CAP
        ),
        name="settle",
    )(length, partial, mine_hidden, branch, grad_in, a_gain, m_gain)


def unattend_kernel(
    length_ref,
    partial_in,
    branch,
    grad_in,
    a_gain,
    o_weight,
    q_raw,
    k_raw,
    queries,
    keys,
    values,
    scales,
    q_gain,
    k_gain,
    cosine,
    sine,
    d_mid,
    a_gain_part,
    d_branch,
    d_heads,
    q_gain_part,
    k_gain_part,
    out_weight,
    d_mix,
    d_q,
    d_k,
    load,
    *scratch,
):
    team = Team()
    sums = RowSums(team, *scratch[0:4])
    reduce = Reduce(team, *scratch[4:10])
    gather = Gather(team, d_branch, *scratch[10:12])
    fetch = pltpu.make_async_copy(o_weight, out_weight, load.at[0])
    fetch.start()
    team.meet(team.sibling, team.across, team.far)
    rows, local = queries.shape

    def make(at):
        reduce.partial[:, at] = partial_in[:, at]

    reduce.run(make)
    shard = reduce.shard
    length = length_ref[0]
    a_gain_part[...] = jnp.zeros_like(a_gain_part)

    def norm(at):
        row = team.slot * shard + at.start + lax.broadcasted_iota(jnp.int32, (at.size, 1), 0)
        grad = jnp.where(row < length, grad_in[at, :].astype(F32), 0.0) + reduce.total[at, :]
        d_mid[at, :] = grad
        base = branch[at, :]
        scale = lax.rsqrt(row_sum(base * base) * (1.0 / D) + EPS)
        unit = base * scale
        product = grad * unit
        a_gain_part[...] += sum([product[8 * i : 8 * i + 8] for i in range(at.size // 8)])
        scaled = grad * a_gain[...]
        back = scale * (scaled - unit * (row_sum(scaled * unit) * (1.0 / D)))
        whole_at = pl.ds(pl.multiple_of(team.slot * shard + at.start, at.size), at.size)
        d_branch[whole_at, :] = back.astype(BF16)

    over_rows(shard, 16, norm)
    gather.start()
    gather.half()
    gather.finish()
    fetch.wait()
    d_mix[...] = right_inner(d_branch[...], out_weight[...]).astype(BF16)
    q_scale = scales[:, 0:1]
    k_scale = scales[:, 1:2]
    q_inner = jnp.zeros((rows, 1), F32)
    k_inner = jnp.zeros((rows, 1), F32)
    shrink = 1.0 / math.sqrt(HEAD)
    for head in range(local // HEAD):
        at = pl.ds(head * HEAD, HEAD)
        q, k, v, back = queries[:, at], keys[:, at], values[:, at], d_mix[:, at]
        probs = head_probs(q, k, length)
        d_probs = right_inner(back, v)
        d_scores = (probs * (d_probs - row_sum(probs * d_probs))).astype(BF16)
        d_heads[:, pl.ds(2 * local + head * HEAD, HEAD)] = left_inner(
            probs.astype(BF16), back
        ).astype(BF16)
        d_q_hat = turn(matmul(d_scores, k) * shrink, cosine[...], -sine[...])
        d_k_hat = turn(left_inner(d_scores, q) * shrink, cosine[...], -sine[...])
        q_unit = q_raw[:, at] * q_scale
        k_unit = k_raw[:, at] * k_scale
        q_gain_part[:, at] = jnp.sum(d_q_hat * q_unit, axis=0, keepdims=True)
        k_gain_part[:, at] = jnp.sum(d_k_hat * k_unit, axis=0, keepdims=True)
        q_scaled = d_q_hat * q_gain[:, at]
        k_scaled = d_k_hat * k_gain[:, at]
        d_q[:, at] = q_scaled
        d_k[:, at] = k_scaled
        q_inner += row_sum(q_scaled * q_unit)
        k_inner += row_sum(k_scaled * k_unit)
    sums.start(q_inner, k_inner)
    q_inner, k_inner = sums.finish()
    for i, (grad, raw, scale, inner) in enumerate(
        ((d_q, q_raw, q_scale, q_inner), (d_k, k_raw, k_scale, k_inner))
    ):
        factor = scale * scale * inner * (1.0 / D)
        d_heads[:, pl.ds(i * local, local)] = (scale * grad[...] - raw[...] * factor).astype(BF16)


def unattend(
    length, partial, branch, grad_in, a_gain, o_weight, kept, gains, cosine, sine
):
    rows, width = partial.shape
    local = o_weight.shape[0]
    shard = rows // SLOTS
    return pl.pallas_call(
        unattend_kernel,
        out_shape=shaped(
            ((shard, width), F32),
            ((8, width), F32),
            ((rows, width), BF16),
            ((rows, 3 * local), BF16),
            ((1, local), F32),
            ((1, local), F32),
        ),
        in_specs=[SCALAR] + [ON_CHIP] * 4 + [ANY] + [ON_CHIP] * 10,
        out_specs=(ON_CHIP,) * 6,
        scratch_shapes=[
            pltpu.VMEM((local, width), BF16),
            pltpu.VMEM((rows, local), BF16),
            pltpu.VMEM((rows, local), F32),
            pltpu.VMEM((rows, local), F32),
            pltpu.SemaphoreType.DMA((1,)),
        ]
        + RowSums.scratch(rows)
        + Reduce.scratch(rows, width)
        + Gather.scratch,
        compiler_params=pltpu.CompilerParams(
            collective_id=2, has_side_effects=True, vmem_limit_bytes=VMEM_CAP
        ),
        name="unattend",
    )(length, partial, branch, grad_in, a_gain, o_weight, *kept, *gains, cosine, sine)


class Deal:
    def __init__(self, count, shard, width):
        self.count = count
        self.columns = max(128, width // count)
        self.across = width // self.columns
        self.rows = shard * self.across // count

    def at(self, chunk, base=0):
        return (
            at_rows(base + (chunk // self.across) * self.rows, self.rows),
            at_rows((chunk % self.across) * self.columns, self.columns),
        )


def finish_kernel(
    length_ref,
    inverse,
    partial_in,
    d_mid,
    layer,
    layer_out,
    input_grad,
    closed,
    parked,
    leaving,
    deal_send,
    deal_recv,
    *scratch,
):
    team = Team()
    reduce = Reduce(team, *scratch[0:6])
    gathers = [
        Gather(team, whole, *scratch[6 + 2 * i : 8 + 2 * i])
        for i, whole in enumerate((layer_out, input_grad))
    ]
    count = lax.axis_size("dp")
    shard, width = d_mid.shape
    deal = Deal(count, shard, width)
    barrier = pltpu.get_barrier_semaphore()
    for step in range(1, count):
        pl.semaphore_signal(
            barrier, inc=1, device_id=(lax.rem(team.row + step, count), team.me), device_id_type=AT
        )
    for other in (team.sibling, team.across):
        pl.semaphore_signal(barrier, inc=1, device_id=(team.row, other), device_id_type=AT)
    pl.semaphore_wait(barrier, count + 1)

    def make(at):
        reduce.partial[:, at] = partial_in[:, at]

    reduce.run(make)
    length = length_ref[0]

    def close(at):
        row = team.slot * shard + at.start + lax.broadcasted_iota(jnp.int32, (at.size, 1), 0)
        closed[at, :] = jnp.where(row < length, reduce.total[at, :] + d_mid[at, :], 0.0).astype(BF16)

    over_rows(shard, 16, close)

    def send(phase, step, i, source, target):
        return pltpu.make_async_remote_copy(
            src_ref=source,
            dst_ref=target,
            send_sem=deal_send.at[phase, step, i],
            recv_sem=deal_recv.at[phase, step, i],
            device_id=(lax.rem(team.row + step, count), team.me),
            device_id_type=AT,
        )

    first = []
    for i, source in enumerate((layer, closed)):
        for step in range(1, count):
            other = lax.rem(team.row + step, count)
            copy = send(0, step, i, source.at[deal.at(other)], parked.at[team.row, i])
            copy.start()
            first.append(copy)
        parked[team.row, i] = source[deal.at(team.row)]
    for copy in first:
        copy.wait()
    mine = team.slot * shard
    second = []
    for i, target in enumerate((layer_out, input_grad)):
        for step in range(1, count):
            other = lax.rem(team.row + step, count)
            leaving[other, i] = parked[inverse[other], i]
            copy = send(1, step, i, leaving.at[other, i], target.at[deal.at(team.row, mine)])
            copy.start()
            second.append(copy)
        target[deal.at(team.row, mine)] = parked[inverse[team.row], i]
    for copy in second:
        copy.wait()
    for gather in gathers:
        gather.start()
    for gather in gathers:
        gather.half()
    for gather in gathers:
        gather.finish()


def close_layer(length, inverse, partial, d_mid, layer):
    rows, width = partial.shape
    shard = rows // SLOTS
    count = lax.axis_size("dp")
    deal = Deal(count, shard, width)
    chunk = (count, 2, deal.rows, deal.columns)
    return pl.pallas_call(
        finish_kernel,
        out_shape=shaped(((rows, width), BF16), ((rows, width), BF16)),
        in_specs=[SCALAR, SCALAR] + [ON_CHIP] * 3,
        out_specs=(ON_CHIP,) * 2,
        scratch_shapes=[
            pltpu.VMEM((shard, width), BF16),
            pltpu.VMEM(chunk, BF16),
            pltpu.VMEM(chunk, BF16),
            pltpu.SemaphoreType.DMA((2, count, 2)),
            pltpu.SemaphoreType.DMA((2, count, 2)),
        ]
        + Reduce.scratch(rows, width)
        + Gather.scratch * 2,
        compiler_params=pltpu.CompilerParams(
            collective_id=3, has_side_effects=True, vmem_limit_bytes=VMEM_CAP
        ),
        name="close_layer",
    )(length, inverse, partial, d_mid, layer)


SPLIT = 4
PACKED = 768
STEP = 256


class Wires:
    def __init__(self, send, recv):
        self.send, self.recv, self.used = send, recv, 0

    def book(self, number=1):
        self.used += number
        assert self.used <= self.send.shape[0]
        return self.used - number

    def copy(self, source, target, device, index):
        return pltpu.make_async_remote_copy(
            src_ref=source,
            dst_ref=target,
            send_sem=self.send.at[index],
            recv_sem=self.recv.at[index],
            device_id=device,
            device_id_type=AT,
        )


class Spread:
    def __init__(self, wires, grid, team, source, field):
        shard = source.shape[0] // SLOTS
        mine = at_rows(team.slot * shard, shard)
        half = at_rows(team.core * 2 * shard, 2 * shard)
        self.hops, self.sides, self.pairs = {}, {}, {}
        for step in range(1, grid.groups):
            group = lax.rem(grid.group + step, grid.groups)
            block = field.at[step]
            self.hops[step] = wires.copy(
                source.at[mine],
                block.at[mine],
                (group * grid.lanes + grid.lane, team.me),
                wires.book(),
            )
            self.sides[step] = wires.copy(
                block.at[mine], block.at[mine], (team.row, team.across), wires.book()
            )
            self.pairs[step] = wires.copy(
                block.at[half], block.at[half], (team.row, team.sibling), wires.book()
            )
        near = sorted(self.hops, key=lambda step: min(step, grid.groups - step))
        self.plan = {"hop": list(near), "side": list(near), "pair": list(near)}

    def start(self):
        for step in self.plan["hop"]:
            self.hops[step].start()

    def side(self, number=1):
        for step in self.plan["side"][:number]:
            self.hops[step].wait_recv()
            self.sides[step].start()
        del self.plan["side"][:number]

    def pair(self, number=1):
        for step in self.plan["pair"][:number]:
            self.sides[step].wait_recv()
            self.pairs[step].start()
        del self.plan["pair"][:number]

    def drain(self):
        self.side(len(self.hops))
        self.pair(len(self.hops))
        for step in self.hops:
            self.hops[step].wait_send()
            self.sides[step].wait_send()
            self.pairs[step].wait()


def silu_parts(gate, upper):
    sig = jax.nn.sigmoid(gate)
    return sig, (gate * sig * upper).astype(BF16)


def silu_back(gate, upper, sig, d_inner):
    d_gate = (d_inner * upper * sig * (1.0 + gate * (1.0 - sig))).astype(BF16)
    return d_gate, (d_inner * gate * sig).astype(BF16)


def head_back(q, k, v, back, cosine, sine, length):
    probs = head_probs(q, k, length)
    low = probs.astype(BF16)
    mix = matmul(low, v).astype(BF16)
    d_probs = right_inner(back, v)
    d_scores = (probs * (d_probs - row_sum(probs * d_probs))).astype(BF16)
    shrink = 1.0 / math.sqrt(HEAD)
    return (
        mix,
        left_inner(low, back).astype(BF16),
        turn(matmul(d_scores, k) * shrink, cosine, -sine),
        turn(left_inner(d_scores, q) * shrink, cosine, -sine),
    )


def folded(field):
    return sum([field[8 * i : 8 * i + 8] for i in range(field.shape[0] // 8)])


def layer_kernel(names, *refs):
    m = types.SimpleNamespace(**dict(zip(names, refs, strict=True)))
    team, grid = Team(), Grid(lax.axis_size("dp"))
    wires = Wires(m.wire_send, m.wire_recv)
    count, groups, lanes = grid.count, grid.groups, grid.lanes
    rows, width = m.hid.shape
    local, hidden = m.mix.shape[1], m.gate.shape[1]
    shard, strip, tile = rows // SLOTS, width // groups, width // count
    every = groups * rows
    me = team.row

    loads = {}

    def load(name, source, target):
        loads[name] = pltpu.make_async_copy(source, target, m.load.at[len(loads)])
        loads[name].start()

    load("hid", m.hidden_in, m.hid)
    load("q", m.q_weight, m.qkv.at[0])
    load("k", m.k_weight, m.qkv.at[1])
    load("v", m.v_weight, m.qkv.at[2])
    load("grad", m.upstream.at[at_rows(team.slot * shard, shard)], m.closed)
    load("o", m.o_weight, m.wo)
    load("g", m.g_weight, m.wg)
    load("u", m.u_weight, m.wu)
    load("d", m.d_weight, m.wd)

    def peer(step):
        return lax.rem(me + step, count)

    barrier = pltpu.get_barrier_semaphore()
    for step in range(1, count):
        pl.semaphore_signal(barrier, inc=1, device_id=(peer(step), team.me), device_id_type=AT)
    for other in (team.sibling, team.across, team.far):
        pl.semaphore_signal(barrier, inc=1, device_id=(me, other), device_id_type=AT)
    pl.semaphore_wait(barrier, count + 2)

    length = m.lengths[m.order[me]]

    def holder(sequence):
        found = jnp.int32(0)
        for place in range(count):
            found = jnp.where(m.order[place] == sequence, place, found)
        return found

    following = (lax.rem(grid.group + 1, groups) * lanes + grid.lane, team.me)
    sums = RowSums(team, m.sum_mine, m.sum_came, m.sum_send, m.sum_recv)
    deal = Deal(count, shard, width)

    class Return:
        def __init__(self, lot, source, target):
            self.lot, self.source = lot, source
            self.room = (m.parked, m.parked_too)[lot]
            start = wires.book(2 * count)
            self.parked = [
                wires.copy(
                    source.at[deal.at(peer(step))],
                    self.room.at[me],
                    (peer(step), team.me),
                    start + step,
                )
                for step in range(1, count)
            ]
            goal = target.at[deal.at(me, team.slot * shard)]
            self.placed = [
                wires.copy(
                    m.back_leaving.at[peer(step), lot],
                    goal,
                    (peer(step), team.me),
                    start + count + step,
                )
                for step in range(1, count)
            ]
            self.placed.append(
                pltpu.make_async_copy(m.back_leaving.at[me, lot], goal, m.put.at[lot])
            )
            self.holders = [holder(peer(step)) for step in range(count)]

        def park(self):
            for copy in self.parked:
                copy.start()
            self.room[me] = self.source[deal.at(me)]

        def place(self):
            for copy in self.parked:
                copy.wait()
            for step in range(count):
                m.back_leaving[peer(step), self.lot] = self.room[self.holders[step]]
            for copy in self.placed:
                copy.start()

        def wait(self):
            for copy in self.placed:
                copy.wait()

    loads["grad"].wait()
    dealt = wires.book(2 * count)
    first = []
    for step in range(1, count):
        copy = wires.copy(
            m.closed.at[deal.at(peer(step))],
            m.parked.at[me],
            (peer(step), team.me),
            dealt + step,
        )
        copy.start()
        first.append(copy)
    m.parked[me] = m.closed[deal.at(me)]

    loads["hid"].wait()

    loads["q"].wait()
    q = matmul(m.hid[...], m.qkv[0])
    m.q_raw[...] = q
    loads["k"].wait()
    k = matmul(m.hid[...], m.qkv[1])
    m.k_raw[...] = k
    sums.start(row_sum(q * q), row_sum(k * k))
    loads["v"].wait()
    m.values[...] = matmul(m.hid[...], m.qkv[2]).astype(BF16)
    q_total, k_total = sums.finish()
    q_scale = lax.rsqrt(q_total * (1.0 / D) + EPS)
    k_scale = lax.rsqrt(k_total * (1.0 / D) + EPS)
    lane = lax.broadcasted_iota(jnp.int32, (rows, 128), 1)
    m.scales[...] = jnp.where(lane == 0, q_scale, k_scale)

    def attend_head(head, carry):
        at = at_rows(head * HEAD, HEAD)
        q = turn(m.q_raw[:, at] * q_scale * m.q_gain[:, at], m.cosine[...], m.sine[...]).astype(BF16)
        k = turn(m.k_raw[:, at] * k_scale * m.k_gain[:, at], m.cosine[...], m.sine[...]).astype(BF16)
        m.queries[:, at] = q
        m.keys[:, at] = k
        probs = head_probs(q, k, length).astype(BF16)
        m.mix[:, at] = matmul(probs, m.values[:, at]).astype(BF16)
        return carry

    lax.fori_loop(0, local // HEAD, attend_head, 0)

    for copy in first:
        copy.wait()
    for step in range(1, count):
        m.back_leaving[peer(step), 0] = m.parked[m.order[peer(step)]]
    m.grad_in[deal.at(me)] = m.parked[m.order[me]]
    second = []
    for step in range(1, count):
        copy = wires.copy(
            m.back_leaving.at[peer(step), 0],
            m.grad_in.at[deal.at(me)],
            (peer(step), team.me),
            dealt + count + step,
        )
        copy.start()
        second.append(copy)

    reduce = Reduce(
        team, m.partial, m.came, m.gone, m.total, m.reduce_send, m.reduce_recv
    )

    def gather(whole, number):
        return Gather(team, whole, m.gather_send.at[number], m.gather_recv.at[number])

    loads["o"].wait()

    def make_branch(at):
        m.partial[:, at] = matmul(m.mix[...], m.wo[:, at]).astype(BF16)

    reduce.run(make_branch)
    own = m.mid_all.at[0]

    def whole_at(at):
        return pl.ds(pl.multiple_of(team.slot * shard + at.start, at.size), at.size)

    def norm_mid(at):
        part = m.total[at, :]
        m.branch[at, :] = part
        unit = part * lax.rsqrt(row_sum(part * part) * (1.0 / D) + EPS)
        mid = m.hid[whole_at(at), :].astype(F32) + m.a_gain[...] * unit
        m.mid_all[0, whole_at(at), :] = mid.astype(BF16)

    over_rows(shard, 16, norm_mid)
    mid_gather = gather(own, 0)
    mid_gather.start()
    mid_spread = Spread(wires, grid, team, own, m.mid_all)
    mid_spread.start()
    mid_gather.half()
    mid_gather.finish()
    loads["g"].wait()
    loads["u"].wait()

    def widen(i, carry):
        at = at_rows(i * STEP, STEP)
        gate = matmul(m.mid_all[0], m.wg[:, at])
        upper = matmul(m.mid_all[0], m.wu[:, at])
        m.gate[:, at] = gate.astype(BF16)
        m.upper[:, at] = upper.astype(BF16)
        m.inner[:, at] = silu_parts(gate, upper)[1]
        return carry

    lax.fori_loop(0, hidden // STEP, widen, 0)
    loads["d"].wait()

    def make_mlp(at):
        m.partial[:, at] = matmul(m.inner[...], m.wd[:, at]).astype(BF16)

    for copy in second:
        copy.wait()
    reduce.run(make_mlp)
    m.stats[...] = jnp.zeros_like(m.stats)
    m.fold[...] = jnp.zeros_like(m.fold)

    def norm_mlp(at):
        part = m.total[at, :]
        scale = lax.rsqrt(row_sum(part * part) * (1.0 / D) + EPS)
        unit = part * scale
        base = m.branch[at, :]
        a_unit = base * lax.rsqrt(row_sum(base * base) * (1.0 / D) + EPS)
        attn_out = m.a_gain[...] * a_unit
        mlp_out = m.m_gain[...] * unit
        rows_f = m.hid[whole_at(at), :].astype(F32)
        row = team.slot * shard + at.start + lax.broadcasted_iota(jnp.int32, (at.size, 1), 0)
        live = row < length
        m.layer[at, :] = jnp.where(live, rows_f + attn_out + mlp_out, 0.0).astype(BF16)
        grad = jnp.where(live, m.grad_in[at, :].astype(F32), 0.0)
        m.fold[0] += folded(grad * unit)
        for i, field in enumerate((rows_f, attn_out, mlp_out)):
            m.fold[i + 1] += folded(jnp.where(live, field * field, 0.0))
        scaled = grad * m.m_gain[...]
        back = scale * (scaled - unit * (row_sum(scaled * unit) * (1.0 / D)))
        m.dm_all[0, whole_at(at), :] = back.astype(BF16)

    over_rows(shard, 16, norm_mlp)
    own_back = m.dm_all.at[0]
    dm_gather = gather(own_back, 1)
    dm_gather.start()
    dm_spread = Spread(wires, grid, team, own_back, m.dm_all)
    dm_spread.start()
    layer_return = Return(1, m.layer, m.layer_out)
    layer_return.park()
    dm_gather.half()
    m.stats[0:1, :] = jnp.sum(m.fold[0], axis=0, keepdims=True)
    for i in range(3):
        m.stats[3 + i : 4 + i, :] = jnp.sum(m.fold[i + 1], axis=0, keepdims=True)
    dm_gather.finish()
    mid_spread.side(groups)
    hid_spread = Spread(wires, grid, team, m.hid, m.hid_all)
    hid_spread.start()

    def narrow(i, carry):
        at = at_rows(i * STEP, STEP)
        d_inner = right_inner(m.dm_all[0], m.wd[at, :])
        gate = m.gate[:, at].astype(F32)
        upper = m.upper[:, at].astype(F32)
        m.gate[:, at], m.upper[:, at] = silu_back(gate, upper, jax.nn.sigmoid(gate), d_inner)
        return carry

    lax.fori_loop(0, hidden // STEP, narrow, 0)

    def make_d_mid(at):
        m.partial[:, at] = (
            right_inner(m.gate[...], m.wg[at, :]) + right_inner(m.upper[...], m.wu[at, :])
        ).astype(BF16)

    reduce.begin(make_d_mid)
    dm_spread.side(1)
    reduce.end()
    m.fold[0] = jnp.zeros_like(m.fold[0])

    def norm_d_mid(at):
        row = team.slot * shard + at.start + lax.broadcasted_iota(jnp.int32, (at.size, 1), 0)
        grad = jnp.where(row < length, m.grad_in[at, :].astype(F32), 0.0) + m.total[at, :]
        m.d_mid[at, :] = grad
        base = m.branch[at, :]
        scale = lax.rsqrt(row_sum(base * base) * (1.0 / D) + EPS)
        unit = base * scale
        m.fold[0] += folded(grad * unit)
        scaled = grad * m.a_gain[...]
        back = scale * (scaled - unit * (row_sum(scaled * unit) * (1.0 / D)))
        m.d_branch[whole_at(at), :] = back.astype(BF16)

    over_rows(shard, 16, norm_d_mid)
    d_gather = gather(m.d_branch, 2)
    d_gather.start()
    dm_spread.side(1)
    m.stats[1:2, :] = jnp.sum(m.fold[0], axis=0, keepdims=True)
    d_gather.half()
    d_gather.finish()
    dm_spread.side(groups)
    mid_spread.pair(groups)
    branch_spread = Spread(wires, grid, team, m.d_branch, m.branch_all)
    branch_spread.start()

    d_mix = m.partial.at[:, pl.ds(0, local)]
    d_mix[...] = right_inner(m.d_branch[...], m.wo[...]).astype(BF16)
    q_inner = jnp.zeros((rows, 1), F32)
    k_inner = jnp.zeros((rows, 1), F32)
    q_scale = m.scales[:, 0:1]
    k_scale = m.scales[:, 1:2]

    def unattend_head(head, carry):
        at = at_rows(head * HEAD, HEAD)
        _, d_v, d_q_hat, d_k_hat = head_back(
            m.queries[:, at],
            m.keys[:, at],
            m.values[:, at],
            d_mix[:, at],
            m.cosine[...],
            m.sine[...],
            length,
        )
        m.d_heads[:, at_rows(2 * local + head * HEAD, HEAD)] = d_v
        q_unit = m.q_raw[:, at] * q_scale
        k_unit = m.k_raw[:, at] * k_scale
        m.stats[2:3, at] = jnp.sum(d_q_hat * q_unit, axis=0, keepdims=True)
        m.stats[2:3, at_rows(local + head * HEAD, HEAD)] = jnp.sum(
            d_k_hat * k_unit, axis=0, keepdims=True
        )
        q_scaled = d_q_hat * m.q_gain[:, at]
        k_scaled = d_k_hat * m.k_gain[:, at]
        m.stage[0, :, at] = q_scaled
        m.stage[1, :, at] = k_scaled
        return carry[0] + row_sum(q_scaled * q_unit), carry[1] + row_sum(k_scaled * k_unit)

    q_inner, k_inner = lax.fori_loop(0, local // HEAD, unattend_head, (q_inner, k_inner))
    sums.start(q_inner, k_inner)
    q_inner, k_inner = sums.finish()
    for i, (raw, scale, inner) in enumerate(
        ((m.q_raw, q_scale, q_inner), (m.k_raw, k_scale, k_inner))
    ):
        factor = scale * scale * inner * (1.0 / D)
        m.d_heads[:, pl.ds(i * local, local)] = (
            scale * m.stage[i] - raw[...] * factor
        ).astype(BF16)
    m.stat_team[team.me] = m.stats[...]
    stat_at = wires.book(3 + count)
    stat_team = [
        wires.copy(m.stats, m.stat_team.at[team.me], (me, other), stat_at + i)
        for i, other in enumerate((team.sibling, team.across, team.far))
    ]
    for copy in stat_team:
        copy.start()

    layer_return.place()

    def make_input(at):
        m.partial[:, at] = (
            right_inner(m.d_heads[:, 0:local], m.qkv[0, at, :])
            + right_inner(m.d_heads[:, local : 2 * local], m.qkv[1, at, :])
            + right_inner(m.d_heads[:, 2 * local : 3 * local], m.qkv[2, at, :])
        ).astype(BF16)

    reduce.begin(make_input)

    mid_spread.drain()
    dm_spread.drain()
    for k in range(groups):
        m.mid_turned[:, pl.ds(k * rows, rows)] = jnp.transpose(
            m.mid_all[k, :, at_rows(grid.group * strip, strip)]
        )
    crossed = wires.book(3 * (hidden // STEP))
    crossing = (grid.group * lanes + (1 - grid.lane), team.me)

    def tile_of(lane):
        return at_rows((grid.group * lanes + lane) * tile, tile)

    def all_rows(field, columns):
        block = field[:, :, columns]
        return block.reshape(every, block.shape[2])

    def crossings(n):
        at = at_rows(n * STEP, STEP)
        spare = pl.ds(every, tile)
        return [
            wires.copy(m.wg.at[spare, at], m.x_gate.at[:, at], crossing, crossed + 3 * n),
            wires.copy(m.wu.at[spare, at], m.x_up.at[:, at], crossing, crossed + 3 * n + 1),
            wires.copy(m.wd.at[at, spare], m.x_down.at[at, :], crossing, crossed + 3 * n + 2),
        ]

    def again(n, carry):
        at = at_rows(n * STEP, STEP)

        def block_again(k, carry):
            gate = matmul(m.mid_all[k], m.wg[:, at])
            upper = matmul(m.mid_all[k], m.wu[:, at])
            d_inner = right_inner(m.dm_all[k], m.wd[at, :])
            sig, inner = silu_parts(gate, upper)
            kept = at_rows((k - 1) * rows, rows)
            m.keep[0, kept, :] = inner
            m.keep[1, kept, :], m.keep[2, kept, :] = silu_back(gate, upper, sig, d_inner)
            return carry

        lax.fori_loop(1, groups, block_again, 0)
        whole = pl.ds(rows, every - rows)
        m.wg[0:rows, at] = m.gate[:, at]
        m.wu[0:rows, at] = m.upper[:, at]
        m.wd[at, 0:rows] = jnp.transpose(m.inner[:, at])
        m.wg[whole, at] = m.keep[1]
        m.wu[whole, at] = m.keep[2]
        for k in range(1, groups):
            kept = pl.ds((k - 1) * rows, rows)
            m.wd[at, pl.ds(k * rows, rows)] = jnp.transpose(m.keep[0, kept, :])
        turned = m.mid_turned[at_rows((1 - grid.lane) * tile, tile), :]
        spare = pl.ds(every, tile)
        m.wg[spare, at] = matmul(turned, m.wg[0:every, at]).astype(BF16)
        m.wu[spare, at] = matmul(turned, m.wu[0:every, at]).astype(BF16)
        m.wd[at, spare] = matmul(m.wd[at, 0:every], all_rows(m.dm_all, tile_of(1 - grid.lane))).astype(BF16)
        for copy in crossings(n):
            copy.start()
        for place, event in events.items():
            pl.when(n == place)(event)
        return carry

    tiles = hidden // STEP
    stat_dp = [
        wires.copy(m.pack, m.stat_dp.at[me], (peer(step), team.me), stat_at + 2 + step)
        for step in range(1, count)
    ]
    grad_return = Return(0, m.closed, m.input_grad)
    out_gathers = [gather(m.layer_out, 3), gather(m.input_grad, 4)]

    def add_stats():
        for copy in stat_team:
            copy.wait()
        total = (m.stat_team[0] + m.stat_team[1]) + (m.stat_team[2] + m.stat_team[3])
        line = lax.broadcasted_iota(jnp.int32, total.shape, 0)
        total = jnp.where(line == 2, m.stats[...], total)
        m.pack[...] = jnp.zeros_like(m.pack)
        packed = m.pack.shape[1]
        for i in range(2):
            for j in range(pl.cdiv(width, packed)):
                piece = total[i : i + 1, j * packed : min((j + 1) * packed, width)]
                m.pack[3 * i + j : 3 * i + j + 1, 0 : piece.shape[1]] = piece
        m.pack[6:7, :] = total[2:3, 0:packed]
        m.pack[7:8, 0 : 2 * local - packed] = total[2:3, packed : 2 * local]
        for i in range(3):
            square = jnp.sum(total[3 + i : 4 + i, :], axis=1, keepdims=True)
            m.pack[7:8, 2 * local - packed + i * 128 : 2 * local - packed + (i + 1) * 128] = (
                jnp.broadcast_to(square, (1, 128))
            )
        m.stat_dp[me] = m.pack[...]
        for copy in stat_dp:
            copy.start()

    def close(at):
        row = team.slot * shard + at.start + lax.broadcasted_iota(jnp.int32, (at.size, 1), 0)
        m.closed[at, :] = jnp.where(row < length, m.total[at, :] + m.d_mid[at, :], 0.0).astype(BF16)

    def park():
        reduce.end()
        over_rows(shard, 16, close)
        grad_return.park()
        hid_spread.side(groups)

    def share():
        layer_return.wait()
        grad_return.wait()
        for one in out_gathers:
            one.start()

    events = {
        0: add_stats,
        1: park,
        tiles - 3: lambda: hid_spread.pair(groups),
        tiles - 2: lambda: branch_spread.side(groups),
    }
    lax.fori_loop(0, tiles, again, 0)
    hid_spread.drain()
    def put(source, target, index):
        return pltpu.make_async_copy(source, target, m.put.at[index])

    puts = []

    def store(value, target):
        slot = len(puts) % 2
        if len(puts) >= 2:
            puts[-2].wait()
        stage = m.stage.at[slot, pl.ds(0, value.shape[0]), pl.ds(0, value.shape[1])]
        stage[...] = value
        puts.append(put(stage, target, 2 + slot))
        puts[-1].start()

    late = []

    def bring(source, target):
        copy = pltpu.make_async_copy(source, target, m.late.at[len(late)])
        copy.start()
        late.append(copy)

    for k in range(1, groups):
        bring(m.hid_all.at[k], m.mid_all.at[k])
    turned_own = m.mid_turned.at[at_rows(grid.lane * tile, tile)]
    wide = m.stage.shape[2]
    high = rows

    def narrow_stage(slot):
        return m.stage.at[slot, :, pl.ds(0, tile)]

    def flush(copies, last, i, values):
        @pl.when(i > 0)
        def _():
            for copy in copies(i - 1):
                copy.wait()

        for copy, slot, value in zip(copies(i), last, values, strict=True):
            slot[...] = value
            copy.start()

    def wide_copies(i):
        at = at_rows(i * wide, wide)
        return [put(m.stage.at[0], m.g_own.at[:, at], 2), put(m.stage.at[1], m.u_own.at[:, at], 3)]

    def wide_part(i, carry):
        at = at_rows(i * wide, wide)
        flush(
            wide_copies,
            (m.stage.at[0], m.stage.at[1]),
            i,
            [matmul(turned_own[...], weight[0:every, at]) for weight in (m.wg, m.wu)],
        )
        return carry

    lax.fori_loop(0, hidden // wide, wide_part, 0)
    for copy in wide_copies(hidden // wide - 1):
        copy.wait()

    def high_at(i, slot):
        return at_rows((2 * i + slot) * high, high)

    def high_copies(i):
        return [put(narrow_stage(slot), m.d_own.at[high_at(i, slot), :], 2 + slot) for slot in range(2)]

    def high_part(i, carry):
        right = all_rows(m.dm_all, tile_of(grid.lane))
        flush(
            high_copies,
            (narrow_stage(0), narrow_stage(1)),
            i,
            [matmul(m.wd[high_at(i, slot), 0:every], right) for slot in range(2)],
        )
        return carry

    lax.fori_loop(0, hidden // high // 2, high_part, 0)
    for copy in high_copies(hidden // high // 2 - 1):
        copy.wait()

    for copy in late:
        copy.wait()
    for k in range(groups):
        source = m.mid_all.at[k] if k else m.hid
        m.mid_turned[:, pl.ds(k * rows, rows)] = jnp.transpose(
            source[:, at_rows(grid.group * strip, strip)]
        )
    wide_sums = RowSums(
        team, m.wide_mine, m.wide_came.at[0], m.wide_send.at[0], m.wide_recv.at[0]
    )
    spare_rows = every + tile

    def project_again(k, carry):
        block = at_rows(spare_rows + (k - 1) * rows, rows)
        lane = lax.broadcasted_iota(jnp.int32, (rows, 128), 1)
        found = jnp.zeros((rows, 128), F32)
        for i in range(2):
            raw = matmul(m.mid_all[k], m.qkv[i])
            m.wu[block, pl.ds(2 * local + i * local, local)] = raw.astype(BF16)
            found = jnp.where(lane == i, row_sum(raw * raw), found)
        m.wide_inner[at_rows((k - 1) * rows, rows), :] = found
        m.wu[block, pl.ds(local, local)] = matmul(m.mid_all[k], m.qkv[2]).astype(BF16)
        return carry

    lax.fori_loop(1, groups, project_again, 0)
    wide_sums.start(m.wide_inner[:, 0:1], m.wide_inner[:, 1:2])
    branch_spread.pair(groups)
    grad_return.place()
    branch_spread.drain()
    for k in range(1, groups):
        bring(m.branch_all.at[k], m.dm_all.at[k])
    for copy in late[groups - 1 :]:
        copy.wait()
    q_total, k_total = wide_sums.finish()
    lane = lax.broadcasted_iota(jnp.int32, (every - rows, 128), 1)
    m.wide_scales[...] = lax.rsqrt(jnp.where(lane == 0, q_total, k_total) * (1.0 / D) + EPS)
    m.wide_inner[...] = jnp.zeros_like(m.wide_inner)

    def attention_again(k, carry):
        back_length = m.lengths[
            m.order[lax.rem(grid.group - k + groups, groups) * lanes + grid.lane]
        ]
        block = at_rows(spare_rows + (k - 1) * rows, rows)
        inside = at_rows((k - 1) * rows, rows)
        q_scale = m.wide_scales[inside, 0:1]
        k_scale = m.wide_scales[inside, 1:2]
        d_mix[...] = right_inner(m.dm_all[k], m.wo[...]).astype(BF16)
        q_inner = jnp.zeros((rows, 1), F32)
        k_inner = jnp.zeros((rows, 1), F32)

        def head_again(head, carry):
            at = at_rows(head * HEAD, HEAD)
            q_unit = m.wu[block, at_rows(2 * local + head * HEAD, HEAD)].astype(F32) * q_scale
            k_unit = m.wu[block, at_rows(3 * local + head * HEAD, HEAD)].astype(F32) * k_scale
            mix, d_v, d_q_hat, d_k_hat = head_back(
                turn(q_unit * m.q_gain[:, at], m.cosine[...], m.sine[...]).astype(BF16),
                turn(k_unit * m.k_gain[:, at], m.cosine[...], m.sine[...]).astype(BF16),
                m.wu[block, at_rows(local + head * HEAD, HEAD)],
                d_mix[:, at],
                m.cosine[...],
                m.sine[...],
                back_length,
            )
            m.wu[block, at] = mix
            m.wg[block, at_rows(2 * local + head * HEAD, HEAD)] = d_v
            q_scaled = d_q_hat * m.q_gain[:, at]
            k_scaled = d_k_hat * m.k_gain[:, at]
            m.wg[block, at] = q_scaled.astype(BF16)
            m.wg[block, at_rows(local + head * HEAD, HEAD)] = k_scaled.astype(BF16)
            return carry[0] + row_sum(q_scaled * q_unit), carry[1] + row_sum(k_scaled * k_unit)

        q_inner, k_inner = lax.fori_loop(0, local // HEAD, head_again, (q_inner, k_inner))
        lane = lax.broadcasted_iota(jnp.int32, (rows, 128), 1)
        m.wide_inner[inside, :] = jnp.where(lane == 0, q_inner, jnp.where(lane == 1, k_inner, 0.0))
        return carry

    lax.fori_loop(1, groups, attention_again, 0)
    wide_sums = RowSums(
        team, m.wide_mine, m.wide_came.at[1], m.wide_send.at[1], m.wide_recv.at[1]
    )
    wide_sums.start(m.wide_inner[:, 0:1], m.wide_inner[:, 1:2])
    other, this = 1 - grid.lane, grid.lane
    others = pl.ds(spare_rows, every - rows)

    def lane_of(lane):
        return at_rows(grid.group * strip + lane * tile, tile)

    def o_part(lane):
        return left_inner(m.mix[...], m.d_branch[:, lane_of(lane)]) + left_inner(
            m.wu[others, 0:local],
            m.dm_all[1:groups, :, lane_of(lane)].reshape(every - rows, tile),
        )

    def heads_part(lane, at):
        turned = m.mid_turned.at[at_rows(lane * tile, tile)]
        return matmul(turned[:, 0:rows], m.d_heads[:, at]) + matmul(
            turned[:, rows:every], m.wg[others, at]
        )

    last = wires.book(4)
    finals = []
    spare = m.qkv.at[2, pl.ds(3 * tile, local), pl.ds(0, tile)]
    spare[...] = o_part(other).astype(BF16)
    finals.append(wires.copy(spare, m.x_o, crossing, last + 3))
    finals[-1].start()
    q_inner, k_inner = wide_sums.finish()
    lane = lax.broadcasted_iota(jnp.int32, (every - rows, 128), 1)
    m.wide_inner[...] = jnp.where(lane == 0, q_inner, k_inner)

    def close_heads(k, carry):
        block = at_rows(spare_rows + (k - 1) * rows, rows)
        inside = at_rows((k - 1) * rows, rows)
        for i in range(2):
            at = pl.ds(i * local, local)
            scale = m.wide_scales[inside, i : i + 1]
            factor = scale * scale * m.wide_inner[inside, i : i + 1] * (1.0 / D)
            raw = m.wu[block, pl.ds(2 * local + i * local, local)].astype(F32)
            m.wg[block, at] = (scale * m.wg[block, at].astype(F32) - raw * factor).astype(BF16)
        return carry

    lax.fori_loop(1, groups, close_heads, 0)
    for i, target in ((2, m.x_v), (0, m.x_q), (1, m.x_k)):
        spare = m.qkv.at[2, pl.ds(i * tile, tile)]
        spare[...] = heads_part(other, pl.ds(i * local, local)).astype(BF16)
        finals.append(wires.copy(spare, target, crossing, last + i))
        finals[-1].start()
    share()
    for i, target in enumerate((m.q_own, m.k_own, m.v_own)):
        store(heads_part(this, pl.ds(i * local, local)), target)
    output = o_part(this)
    for i in range(local // high):
        store(output[i * high : (i + 1) * high], m.o_own.at[pl.ds(i * high, high), :])
    for copy in puts[-2:]:
        copy.wait()

    def arrived(n, carry):
        for copy in crossings(n):
            copy.wait()
        return carry

    for one in out_gathers:
        one.half()
    for one in out_gathers:
        one.finish()
    for copy in stat_dp:
        copy.wait()
    m.stat_out[...] = sum([m.stat_dp[i] for i in range(1, count)], m.stat_dp[0])
    lax.fori_loop(0, tiles, arrived, 0)
    for copy in finals:
        copy.wait()


def whole_layer(grid, args):
    (hidden_in, upstream, lengths, order, q_weight, k_weight, v_weight, o_weight) = args[:8]
    (q_gain, k_gain, a_gain, g_weight, u_weight, d_weight, m_gain, cosine, sine) = args[8:]
    rows, width = hidden_in.shape
    local, hidden = q_weight.shape[1], g_weight.shape[1]
    count, groups = grid.count, grid.groups
    shard, strip, tile = rows // SLOTS, width // groups, width // count
    every = groups * rows
    deal = Deal(count, shard, width)
    chunk = (deal.rows, deal.columns)
    inputs = [
        ("lengths", SCALAR, lengths),
        ("order", SCALAR, order),
        ("hidden_in", ANY, hidden_in),
        ("upstream", ANY, upstream),
        ("q_weight", ANY, q_weight),
        ("k_weight", ANY, k_weight),
        ("v_weight", ANY, v_weight),
        ("o_weight", ANY, o_weight),
        ("g_weight", ANY, g_weight),
        ("u_weight", ANY, u_weight),
        ("d_weight", ANY, d_weight),
        ("q_gain", ON_CHIP, q_gain),
        ("k_gain", ON_CHIP, k_gain),
        ("a_gain", ON_CHIP, a_gain),
        ("m_gain", ON_CHIP, m_gain),
        ("cosine", ON_CHIP, cosine),
        ("sine", ON_CHIP, sine),
    ]
    outputs = [
        ("layer_out", (rows, width), BF16),
        ("input_grad", (rows, width), BF16),
        ("g_own", (tile, hidden), F32),
        ("u_own", (tile, hidden), F32),
        ("d_own", (hidden, tile), F32),
        ("q_own", (tile, local), F32),
        ("k_own", (tile, local), F32),
        ("v_own", (tile, local), F32),
        ("o_own", (local, tile), F32),
        ("x_gate", (tile, hidden), BF16),
        ("x_up", (tile, hidden), BF16),
        ("x_down", (hidden, tile), BF16),
        ("x_q", (tile, local), BF16),
        ("x_k", (tile, local), BF16),
        ("x_v", (tile, local), BF16),
        ("x_o", (local, tile), BF16),
        ("hid_all", (groups, rows, width), BF16),
        ("branch_all", (groups, rows, width), BF16),
        ("stat_out", (8, PACKED), F32),
    ]
    wires = 160
    scratch = [
        ("qkv", pltpu.VMEM((3, width, local), BF16)),
        ("wo", pltpu.VMEM((local, width), BF16)),
        ("wg", pltpu.VMEM((width, hidden), BF16)),
        ("wu", pltpu.VMEM((width, hidden), BF16)),
        ("wd", pltpu.VMEM((hidden, width), BF16)),
        ("hid", pltpu.VMEM((rows, width), BF16)),
        ("mid_all", pltpu.VMEM((groups, rows, width), BF16)),
        ("dm_all", pltpu.VMEM((groups, rows, width), BF16)),
        ("gate", pltpu.VMEM((rows, hidden), BF16)),
        ("upper", pltpu.VMEM((rows, hidden), BF16)),
        ("inner", pltpu.VMEM((rows, hidden), BF16)),
        ("q_raw", pltpu.VMEM((rows, local), F32)),
        ("k_raw", pltpu.VMEM((rows, local), F32)),
        ("queries", pltpu.VMEM((rows, local), BF16)),
        ("keys", pltpu.VMEM((rows, local), BF16)),
        ("values", pltpu.VMEM((rows, local), BF16)),
        ("scales", pltpu.VMEM((rows, 128), F32)),
        ("mix", pltpu.VMEM((rows, local), BF16)),
        ("d_branch", pltpu.VMEM((rows, width), BF16)),
        ("d_heads", pltpu.VMEM((rows, 3 * local), BF16)),
        ("mid_turned", pltpu.VMEM((strip, every), BF16)),
        ("keep", pltpu.VMEM((3, every - rows, STEP), BF16)),
        ("stage", pltpu.VMEM((2, rows, local), F32)),
        ("branch", pltpu.VMEM((shard, width), F32)),
        ("d_mid", pltpu.VMEM((shard, width), F32)),
        ("layer", pltpu.VMEM((shard, width), BF16)),
        ("closed", pltpu.VMEM((shard, width), BF16)),
        ("grad_in", pltpu.VMEM((shard, width), BF16)),
        ("parked", pltpu.VMEM((count,) + chunk, BF16)),
        ("parked_too", pltpu.VMEM((count,) + chunk, BF16)),
        ("back_leaving", pltpu.VMEM((count, 2) + chunk, BF16)),
        ("fold", pltpu.VMEM((4, 8, width), F32)),
        ("stats", pltpu.VMEM((8, width), F32)),
        ("stat_team", pltpu.VMEM((SLOTS, 8, width), F32)),
        ("pack", pltpu.VMEM((8, PACKED), F32)),
        ("stat_dp", pltpu.VMEM((count, 8, PACKED), F32)),
        ("partial", pltpu.VMEM((rows, width), BF16)),
        ("came", pltpu.VMEM((3, shard, width), BF16)),
        ("gone", pltpu.VMEM((shard, width), BF16)),
        ("total", pltpu.VMEM((shard, width), F32)),
        ("sum_mine", pltpu.VMEM((8, rows), F32)),
        ("sum_came", pltpu.VMEM((3, 8, rows), F32)),
        ("wide_mine", pltpu.VMEM((8, every - rows), F32)),
        ("wide_came", pltpu.VMEM((2, 3, 8, every - rows), F32)),
        ("wide_scales", pltpu.VMEM((every - rows, 128), F32)),
        ("wide_inner", pltpu.VMEM((every - rows, 128), F32)),
        ("wide_send", pltpu.SemaphoreType.DMA((2, 3))),
        ("wide_recv", pltpu.SemaphoreType.DMA((2, 3))),
        ("sum_send", pltpu.SemaphoreType.DMA((3,))),
        ("sum_recv", pltpu.SemaphoreType.DMA((3,))),
        ("reduce_send", pltpu.SemaphoreType.DMA((3, SPLIT))),
        ("reduce_recv", pltpu.SemaphoreType.DMA((3, SPLIT))),
        ("gather_send", pltpu.SemaphoreType.DMA((5, 3))),
        ("gather_recv", pltpu.SemaphoreType.DMA((5, 3))),
        ("wire_send", pltpu.SemaphoreType.DMA((wires,))),
        ("wire_recv", pltpu.SemaphoreType.DMA((wires,))),
        ("load", pltpu.SemaphoreType.DMA((9,))),
        ("put", pltpu.SemaphoreType.DMA((4,))),
        ("late", pltpu.SemaphoreType.DMA((2 * groups,))),
    ]
    names = [entry[0] for entry in inputs + outputs + scratch]
    results = pl.pallas_call(
        functools.partial(layer_kernel, names),
        out_shape=shaped(*[entry[1:] for entry in outputs]),
        in_specs=[entry[1] for entry in inputs],
        out_specs=(ANY,) * (len(outputs) - 1) + (ON_CHIP,),
        scratch_shapes=[entry[1] for entry in scratch],
        compiler_params=pltpu.CompilerParams(
            collective_id=4, has_side_effects=True, vmem_limit_bytes=63 * 2**20
        ),
        name="whole_layer",
    )(*[entry[2] for entry in inputs])
    return dict(zip([entry[0] for entry in outputs], results, strict=True))


def body(
    hidden_in,
    upstream_grad,
    seq_lengths,
    position_order,
    query_weight,
    key_weight,
    value_weight,
    output_weight,
    query_gain,
    key_gain,
    attn_gain,
    gate_weight,
    up_weight,
    down_weight,
    mlp_gain,
):
    count = lax.axis_size("dp")
    ways = lax.axis_size("tensor")
    myself = lax.axis_index("dp")
    part = lax.axis_index("tensor")
    grid = Grid(count)
    index = jnp.arange(count, dtype=jnp.int32)
    inverse = jnp.sum(
        index[None, :] * (position_order[None, :] == index[:, None]).astype(jnp.int32), axis=1
    )
    rows = hidden_in.shape[1]
    width = hidden_in.shape[2]
    shard = rows // ways
    if grid.lanes == 2 and 2 * query_weight.shape[1] + 3 * 128 <= 2 * PACKED and width <= 3 * PACKED and grid.groups * rows + width // count <= width:
        cosine, sine = rope_constants(rows, HEAD)
        found = whole_layer(
            grid,
            (
                hidden_in[0],
                upstream_grad[0],
                seq_lengths,
                position_order,
                query_weight,
                key_weight,
                value_weight,
                output_weight,
                query_gain[None],
                key_gain[None],
                attn_gain[None],
                gate_weight,
                up_weight,
                down_weight,
                mlp_gain[None],
                cosine,
                sine,
            ),
        )
        local = query_weight.shape[1]

        def joined(own, other):
            return found[own] + found[other].astype(F32)

        stats = found["stat_out"]
        gains = stats[6:8].reshape(-1)
        squares = gains[2 * local : 2 * local + 3 * 128 : 128]
        return (
            found["layer_out"][None],
            found["input_grad"][None],
            joined("q_own", "x_q"),
            joined("k_own", "x_k"),
            joined("v_own", "x_v"),
            joined("o_own", "x_o"),
            gains[:local],
            gains[local : 2 * local],
            stats[3:6].reshape(-1)[:width],
            joined("g_own", "x_gate"),
            joined("u_own", "x_up"),
            joined("d_own", "x_down"),
            stats[0:3].reshape(-1)[:width],
            jnp.sqrt(squares / (jnp.sum(seq_lengths).astype(F32) * D)),
        )

    piece = shard // count
    seq_here = jnp.sum(jnp.where(index == myself, position_order, 0))
    length = jnp.sum(jnp.where(index == seq_here, seq_lengths, 0))[None]
    slot = part % 2 * 2 + part // 2

    def exchange(pieces):
        return lax.all_to_all(pieces, "dp", split_axis=0, concat_axis=0, tiled=True)

    def my_rows(field):
        return lax.dynamic_slice_in_dim(field, slot * shard, shard, axis=0)

    first = exchange(my_rows(upstream_grad[0]).reshape(count, piece, width))
    second = exchange(jnp.take(first, position_order, axis=0))
    grad_in = second.reshape(shard, width)

    rows_low = hidden_in[0]
    my_low = my_rows(rows_low)
    local = query_weight.shape[1]
    strip = width // grid.groups
    tile = width // count

    def strip_of(field, group):
        return lax.dynamic_slice_in_dim(field, group * strip, strip, axis=1)

    def strips(field):
        found = [strip_of(field, grid.group)]
        for step in range(1, grid.groups):
            found.append(
                grid.shift_groups(
                    strip_of(field, (grid.group + step) % grid.groups), step
                )
            )
        return jnp.concatenate(found, axis=0)

    def tile_of(field, lane):
        return lax.dynamic_slice_in_dim(field, lane * tile, tile, axis=1)

    def reduced(product, field):
        sent = []
        for step in range(1, grid.lanes):
            other = product(tile_of(field, (grid.lane + step) % grid.lanes)).astype(BF16)
            sent.append(grid.shift_lanes(other, step))
        mine = product(tile_of(field, grid.lane))
        for other in sent:
            mine = mine + other.astype(F32)
        return mine

    hidden_strips = strips(rows_low)

    cosine, sine = rope_tables(rows, HEAD)
    cosine = jnp.concatenate([cosine, cosine], axis=1)
    sine = jnp.concatenate([-sine, sine], axis=1)
    gains = (query_gain[None], key_gain[None])
    q_raw, k_raw, queries, keys, values, scales, attn_mix, branch, mid_low = attend(
        length,
        rows_low,
        my_low,
        (query_weight, key_weight, value_weight, output_weight),
        gains,
        cosine,
        sine,
        attn_gain[None],
    )
    mix_all = jnp.concatenate([attn_mix] + grid.ring(attn_mix), axis=0)
    mid_others = shared_ring(grid, mid_low)

    gate = matmul(mid_low, gate_weight)
    upper = matmul(mid_low, up_weight)
    sig = jax.nn.sigmoid(gate)
    inner = (gate * sig * upper).astype(BF16)
    layer, d_mlp, mlp_gain_part, squares = settle(
        length,
        matmul(inner, down_weight).astype(BF16),
        my_low,
        branch,
        grad_in,
        attn_gain[None],
        mlp_gain[None],
    )
    d_mlp_others = shared_ring(grid, d_mlp)

    def inner_back(gate, upper, d_mlp):
        d_inner = right_inner(d_mlp, down_weight)
        sig = jax.nn.sigmoid(gate)
        d_gate = (d_inner * upper * sig * (1.0 + gate * (1.0 - sig))).astype(BF16)
        d_up = (d_inner * gate * sig).astype(BF16)
        return d_gate, d_up

    d_gate, d_up = inner_back(gate, upper, d_mlp)
    d_mid, attn_gain_part, d_branch, d_heads, query_gain_part, key_gain_part = unattend(
        length,
        (right_inner(d_gate, gate_weight) + right_inner(d_up, up_weight)).astype(BF16),
        branch,
        grad_in,
        attn_gain[None],
        output_weight,
        (q_raw, k_raw, queries, keys, values, scales),
        gains,
        cosine,
        sine,
    )
    d_branch_strips = strips(d_branch)
    d_heads_all = jnp.concatenate([d_heads] + grid.ring(d_heads), axis=0)
    layer_out, input_grad = close_layer(
        length,
        inverse,
        (
            right_inner(d_heads[:, :local], query_weight)
            + right_inner(d_heads[:, local : 2 * local], key_weight)
            + right_inner(d_heads[:, 2 * local :], value_weight)
        ).astype(BF16),
        d_mid,
        layer,
    )

    gate_o = matmul(mid_others, gate_weight)
    upper_o = matmul(mid_others, up_weight)
    inner_o = (jax.nn.silu(gate_o) * upper_o).astype(BF16)
    d_gate_o, d_up_o = inner_back(gate_o, upper_o, d_mlp_others)

    def strip_all(own, others):
        return jnp.concatenate([strip_of(own, grid.group), strip_of(others, grid.group)], axis=0)

    mid_strips = strip_all(mid_low, mid_others)
    d_mlp_strips = strip_all(d_mlp, d_mlp_others)
    d_gate_all = jnp.concatenate([d_gate, d_gate_o], axis=0)
    d_up_all = jnp.concatenate([d_up, d_up_o], axis=0)
    inner_all = jnp.concatenate([inner, inner_o], axis=0)
    gate_part = reduced(lambda tile: left_inner(tile, d_gate_all), mid_strips)
    up_part = reduced(lambda tile: left_inner(tile, d_up_all), mid_strips)
    down_part = reduced(lambda tile: left_inner(inner_all, tile), d_mlp_strips)
    output_part = reduced(lambda tile: left_inner(mix_all, tile), d_branch_strips)
    heads_part = reduced(lambda tile: left_inner(tile, d_heads_all), hidden_strips)
    query_part = heads_part[:, :local]
    key_part = heads_part[:, local : 2 * local]
    value_part = heads_part[:, 2 * local :]

    shared = jnp.concatenate(
        [jnp.sum(attn_gain_part, axis=0), jnp.sum(mlp_gain_part, axis=0), jnp.sum(squares, axis=(1, 2))]
    )
    shared = shared + sibling(shared)
    shared = shared + across(shared)
    sums = grid.total(jnp.concatenate([shared, query_gain_part[0], key_gain_part[0]]))
    attn_gain_grad = sums[:width]
    mlp_gain_grad = sums[width : 2 * width]
    squares = sums[2 * width : 2 * width + 3]
    query_gain_grad = sums[2 * width + 3 : 2 * width + 3 + local]
    key_gain_grad = sums[2 * width + 3 + local :]
    rms_values = jnp.sqrt(squares / (jnp.sum(seq_lengths).astype(F32) * D))

    return (
        layer_out[None],
        input_grad[None],
        query_part,
        key_part,
        value_part,
        output_part,
        query_gain_grad,
        key_gain_grad,
        attn_gain_grad,
        gate_part,
        up_part,
        down_part,
        mlp_gain_grad,
        rms_values,
    )


def solution(mesh):
    placed = (
        P("dp", None, None),
        P("dp", None, None),
        P(),
        P(),
        P(None, "tensor"),
        P(None, "tensor"),
        P(None, "tensor"),
        P("tensor", None),
        P("tensor"),
        P("tensor"),
        P(),
        P(None, "tensor"),
        P(None, "tensor"),
        P("tensor", None),
        P(),
    )
    return jax.shard_map(
        body,
        mesh=mesh,
        in_specs=placed,
        out_specs=(
            P("dp", None, None),
            P("dp", None, None),
            P("dp", "tensor"),
            P("dp", "tensor"),
            P("dp", "tensor"),
            P("tensor", "dp"),
            P("tensor"),
            P("tensor"),
            P(),
            P("dp", "tensor"),
            P("dp", "tensor"),
            P("tensor", "dp"),
            P(),
            P(),
        ),
        check_vma=False,
    )
```

```python
import functools
import math
import types

import jax
import jax.numpy as jnp
import numpy as np
from jax import lax
from jax.experimental import pallas as pl
from jax.experimental.pallas import tpu as pltpu
from jax.sharding import PartitionSpec as P

D = 2048
HEAD = 128
EPS = 1e-06
F32 = jnp.float32
BF16 = jnp.bfloat16


def matmul(left, right):
    return jnp.dot(left, right, preferred_element_type=F32)


def left_inner(left, right):
    return lax.dot_general(left, right, (((0,), (0,)), ((), ())), preferred_element_type=F32)


def right_inner(left, right):
    return lax.dot_general(left, right, (((1,), (1,)), ((), ())), preferred_element_type=F32)


def rope_tables(rows, width):
    places = jnp.arange(rows, dtype=F32)
    freq = jnp.power(F32(500000.0), -jnp.arange(width // 2, dtype=F32) * (2.0 / width))
    angle = places[:, None] * freq[None, :]
    return (jnp.cos(angle), jnp.sin(angle))


def rope_constants(rows, width):
    half = width // 2
    exponent = -np.arange(half, dtype=np.float32) * np.float32(2.0 / width)
    freq = np.power(np.float32(500000.0), exponent, dtype=np.float32)
    angle = (np.arange(rows, dtype=np.float32)[:, None] * freq[None, :]).astype(np.float64)
    cosine, sine = np.cos(angle), np.sin(angle)
    return (
        jnp.asarray(np.concatenate([cosine, cosine], axis=1), F32),
        jnp.asarray(np.concatenate([-sine, sine], axis=1), F32),
    )


class Grid:
    def __init__(self, count):
        self.count = count
        self.lanes = 2 ** ((count.bit_length() - 1) // 2)
        self.groups = count // self.lanes
        me = lax.axis_index("dp")
        self.group = me // self.lanes
        self.lane = me % self.lanes

    def shift_groups(self, field, step):
        pairs = [
            (g * self.lanes + a, ((g + step) % self.groups) * self.lanes + a)
            for g in range(self.groups)
            for a in range(self.lanes)
        ]
        return lax.ppermute(field, "dp", pairs)

    def shift_lanes(self, field, step):
        pairs = [
            (g * self.lanes + a, g * self.lanes + (a + step) % self.lanes)
            for g in range(self.groups)
            for a in range(self.lanes)
        ]
        return lax.ppermute(field, "dp", pairs)

    def ring(self, field):
        found = []
        for _ in range(self.groups - 1):
            field = self.shift_groups(field, 1)
            found.append(field)
        return found

    def total(self, field):
        step = 1
        while step < self.count:
            field = field + lax.ppermute(
                field, "dp", [(i, i ^ step) for i in range(self.count)]
            )
            step *= 2
        return field


def sibling(field):
    size = lax.axis_size("tensor")
    return lax.ppermute(field, "tensor", [(i, i ^ 1) for i in range(size)])


def across(field):
    size = lax.axis_size("tensor")
    return lax.ppermute(field, "tensor", [(i, (i + 2) % size) for i in range(size)])


def shared_ring(grid, rows_low):
    core = lax.axis_index("tensor") % 2
    half = rows_low.shape[0] // 2
    mine = lax.dynamic_slice_in_dim(rows_low, core * half, half, axis=0)
    pieces = []
    for piece in grid.ring(mine):
        pieces += [piece, sibling(piece)]
    return jnp.concatenate(pieces, axis=0)


SLOTS = 4
TILES = 4
AT = pl.DeviceIdType.MESH
VMEM_CAP = 56 * 2**20


class Team:
    def __init__(self):
        self.row = lax.axis_index("dp")
        self.me = lax.axis_index("tensor")
        self.side = self.me // 2
        self.core = self.me % 2
        self.slot = self.core * 2 + self.side
        self.sibling = self.side * 2 + (1 - self.core)
        self.across = (1 - self.side) * 2 + self.core
        self.far = (1 - self.side) * 2 + (1 - self.core)

    def meet(self, *others):
        barrier = pltpu.get_barrier_semaphore()
        for other in others:
            pl.semaphore_signal(barrier, inc=1, device_id=(self.row, other), device_id_type=AT)
        pl.semaphore_wait(barrier, len(others))

    def copy(self, source, target, send, recv, other):
        return pltpu.make_async_remote_copy(
            src_ref=source,
            dst_ref=target,
            send_sem=send,
            recv_sem=recv,
            device_id=(self.row, other),
            device_id_type=AT,
        )


def at_rows(start, size):
    return pl.ds(pl.multiple_of(start, size), size)


class Reduce:
    def scratch(rows, width):
        shard = rows // SLOTS
        return [
            pltpu.VMEM((rows, width), BF16),
            pltpu.VMEM((3, shard, width), BF16),
            pltpu.VMEM((shard, width), BF16),
            pltpu.VMEM((shard, width), F32),
            pltpu.SemaphoreType.DMA((3, TILES)),
            pltpu.SemaphoreType.DMA((3, TILES)),
        ]

    def __init__(self, team, partial, came, gone, total, send, recv):
        self.team, self.partial, self.came, self.gone, self.total = team, partial, came, gone, total
        self.shard, width = total.shape
        self.tiles = send.shape[1]
        self.tile = width // self.tiles
        self.send, self.recv = send, recv
        self.copies = {}

    def columns(self, tile):
        return pl.ds(tile * self.tile, self.tile)

    def block(self, core, side):
        return at_rows((core * 2 + side) * self.shard, self.shard)

    def launch(self, kind, tile, source, other):
        copy = self.team.copy(
            source,
            self.came.at[kind, :, self.columns(tile)],
            self.send.at[kind, tile],
            self.recv.at[kind, tile],
            other,
        )
        copy.start()
        self.copies[kind, tile] = copy

    def offer(self, tile):
        team, columns = self.team, self.columns(tile)
        for kind, side in ((0, 1 - team.side), (1, team.side)):
            self.launch(
                kind, tile, self.partial.at[self.block(1 - team.core, side), columns], team.sibling
            )

    def pass_on(self, tile):
        team, columns = self.team, self.columns(tile)
        self.copies[0, tile].wait_recv()
        mine = self.partial[self.block(team.core, 1 - team.side), columns].astype(F32)
        self.gone[:, columns] = (mine + self.came[0, :, columns].astype(F32)).astype(BF16)
        self.launch(2, tile, self.gone.at[:, columns], team.across)

    def finish(self, tile):
        team, columns = self.team, self.columns(tile)
        self.copies[1, tile].wait_recv()
        mine = self.partial[self.block(team.core, team.side), columns].astype(F32)
        mine = mine + self.came[1, :, columns].astype(F32)
        self.copies[2, tile].wait_recv()
        self.total[:, columns] = mine + self.came[2, :, columns].astype(F32)

    def settle(self):
        for copy in self.copies.values():
            copy.wait_send()

    def begin(self, make):
        self.copies = {}
        for tile in range(self.tiles):
            make(self.columns(tile))
            self.offer(tile)
            if tile:
                self.pass_on(tile - 1)
        self.pass_on(self.tiles - 1)

    def end(self):
        for tile in range(self.tiles):
            self.finish(tile)
        self.settle()

    def run(self, make):
        self.begin(make)
        self.end()


class Gather:
    scratch = [pltpu.SemaphoreType.DMA((3,)), pltpu.SemaphoreType.DMA((3,))]

    def __init__(self, team, whole, send, recv):
        self.team, self.whole = team, whole
        shard = whole.shape[0] // SLOTS
        mine = whole.at[at_rows(team.slot * shard, shard)]
        theirs = whole.at[at_rows((team.core * 2 + 1 - team.side) * shard, shard)]
        self.across = team.copy(mine, mine, send.at[0], recv.at[0], team.across)
        self.near = team.copy(mine, mine, send.at[1], recv.at[1], team.sibling)
        self.relay = team.copy(theirs, theirs, send.at[2], recv.at[2], team.sibling)

    def start(self):
        self.across.start()
        self.near.start()

    def half(self):
        self.across.wait_recv()
        self.relay.start()

    def finish(self):
        self.across.wait_send()
        self.near.wait()
        self.relay.wait()


class RowSums:
    def scratch(rows):
        return [
            pltpu.VMEM((8, rows), F32),
            pltpu.VMEM((3, 8, rows), F32),
            pltpu.SemaphoreType.DMA((3,)),
            pltpu.SemaphoreType.DMA((3,)),
        ]

    def __init__(self, team, mine, came, send, recv):
        self.team, self.mine, self.came = team, mine, came
        self.copies = [
            team.copy(mine, came.at[i], send.at[i], recv.at[i], other)
            for i, other in enumerate((team.sibling, team.across, team.far))
        ]

    def start(self, first, second):
        rows = first.shape[0]
        lane = lax.broadcasted_iota(jnp.int32, (rows, 128), 1)
        both = jnp.where(lane == 0, first, jnp.where(lane == 1, second, 0.0))
        self.mine[...] = jnp.transpose(both)[:8]
        for copy in self.copies:
            copy.start()

    def finish(self):
        for copy in self.copies:
            copy.wait()
        total = self.mine[...] + self.came[0] + (self.came[1] + self.came[2])
        rows = total.shape[1]
        wide = jnp.transpose(jnp.concatenate([total] * 16, axis=0))
        return wide[:, 0:1], wide[:, 1:2]


def turn(field, cosine, sine):
    return field * cosine + pltpu.roll(field, HEAD // 2, 1) * sine


def head_probs(queries, keys, length):
    rows = queries.shape[0]
    scores = right_inner(queries, keys) * (1.0 / math.sqrt(HEAD))
    row = lax.broadcasted_iota(jnp.int32, (rows, rows), 0)
    column = lax.broadcasted_iota(jnp.int32, (rows, rows), 1)
    masked = jnp.where((column <= row) & (column < length), scores, -1e30)
    expo = jnp.exp(masked - jnp.max(masked, axis=-1, keepdims=True))
    return expo / jnp.sum(expo, axis=-1, keepdims=True)


def row_sum(field):
    return jnp.sum(field, axis=-1, keepdims=True)


def over_rows(count, step, work):
    def one(i, carry):
        work(pl.ds(pl.multiple_of(i * step, step), step))
        return carry

    lax.fori_loop(0, count // step, one, 0)


def attend_kernel(
    length_ref,
    hidden,
    mine_hidden,
    q_weight,
    k_weight,
    v_weight,
    o_weight,
    q_gain,
    k_gain,
    cosine,
    sine,
    a_gain,
    q_raw,
    k_raw,
    queries,
    keys,
    values,
    scales,
    mix,
    branch,
    mid_low,
    weights,
    out_weight,
    load,
    *scratch,
):
    team = Team()
    sums = RowSums(team, *scratch[0:4])
    reduce = Reduce(team, *scratch[4:10])
    gather = Gather(team, mid_low, *scratch[10:12])
    loads = [
        pltpu.make_async_copy(source, weights.at[i], load.at[i])
        for i, source in enumerate((q_weight, k_weight, v_weight))
    ] + [pltpu.make_async_copy(o_weight, out_weight, load.at[3])]
    for one in loads:
        one.start()
    team.meet(team.sibling, team.across, team.far)
    rows, local = mix.shape
    width = mid_low.shape[1]
    length = length_ref[0]

    def project(i):
        loads[i].wait()
        return matmul(hidden[...], weights[i])

    q = project(0)
    q_raw[...] = q
    k = project(1)
    k_raw[...] = k
    sums.start(row_sum(q * q), row_sum(k * k))
    values[...] = project(2).astype(BF16)
    q_total, k_total = sums.finish()
    q_scale = lax.rsqrt(q_total * (1.0 / D) + EPS)
    k_scale = lax.rsqrt(k_total * (1.0 / D) + EPS)
    lane = lax.broadcasted_iota(jnp.int32, (rows, 128), 1)
    scales[...] = jnp.where(lane == 0, q_scale, k_scale)
    for head in range(local // HEAD):
        at = pl.ds(head * HEAD, HEAD)
        q = turn(q_raw[:, at] * q_scale * q_gain[:, at], cosine[...], sine[...]).astype(BF16)
        k = turn(k_raw[:, at] * k_scale * k_gain[:, at], cosine[...], sine[...]).astype(BF16)
        queries[:, at] = q
        keys[:, at] = k
        probs = head_probs(q, k, length).astype(BF16)
        mix[:, at] = matmul(probs, values[:, at]).astype(BF16)
    loads[3].wait()

    def make(at):
        reduce.partial[:, at] = matmul(mix[...], out_weight[:, at]).astype(BF16)

    reduce.run(make)
    shard = reduce.shard

    def norm(at):
        part = reduce.total[at, :]
        branch[at, :] = part
        unit = part * lax.rsqrt(row_sum(part * part) * (1.0 / D) + EPS)
        mid = mine_hidden[at, :].astype(F32) + a_gain[...] * unit
        whole_at = pl.ds(pl.multiple_of(team.slot * shard + at.start, at.size), at.size)
        mid_low[whole_at, :] = mid.astype(BF16)

    over_rows(shard, 16, norm)
    gather.start()
    gather.half()
    gather.finish()


ANY = pl.BlockSpec(memory_space=pl.ANY)
ON_CHIP = pl.BlockSpec(memory_space=pltpu.VMEM)
SCALAR = pl.BlockSpec(memory_space=pltpu.SMEM)


def shaped(*pairs):
    return tuple(jax.ShapeDtypeStruct(shape, kind) for shape, kind in pairs)


def attend(length, hidden, mine_hidden, weights, gains, cosine, sine, a_gain):
    rows, width = hidden.shape
    local = weights[0].shape[1]
    shard = rows // SLOTS
    return pl.pallas_call(
        attend_kernel,
        out_shape=shaped(
            ((rows, local), F32),
            ((rows, local), F32),
            ((rows, local), BF16),
            ((rows, local), BF16),
            ((rows, local), BF16),
            ((rows, 128), F32),
            ((rows, local), BF16),
            ((shard, width), F32),
            ((rows, width), BF16),
        ),
        in_specs=[SCALAR, ON_CHIP, ON_CHIP] + [ANY] * 4 + [ON_CHIP] * 5,
        out_specs=(ON_CHIP,) * 9,
        scratch_shapes=[
            pltpu.VMEM((3, width, local), BF16),
            pltpu.VMEM((local, width), BF16),
            pltpu.SemaphoreType.DMA((4,)),
        ]
        + RowSums.scratch(rows)
        + Reduce.scratch(rows, width)
        + Gather.scratch,
        compiler_params=pltpu.CompilerParams(
            collective_id=0, has_side_effects=True, vmem_limit_bytes=VMEM_CAP
        ),
        name="attend",
    )(length, hidden, mine_hidden, *weights, *gains, cosine, sine, a_gain)


def settle_kernel(
    length_ref,
    partial_in,
    mine_hidden,
    branch,
    grad_in,
    a_gain,
    m_gain,
    layer,
    d_mlp,
    m_gain_part,
    squares,
    *scratch,
):
    team = Team()
    reduce = Reduce(team, *scratch[0:6])
    gather = Gather(team, d_mlp, *scratch[6:8])
    team.meet(team.sibling, team.across)

    def make(at):
        reduce.partial[:, at] = partial_in[:, at]

    reduce.run(make)
    shard = reduce.shard
    length = length_ref[0]
    m_gain_part[...] = jnp.zeros_like(m_gain_part)
    squares[...] = jnp.zeros_like(squares)

    def folded(field):
        return sum([field[8 * i : 8 * i + 8] for i in range(field.shape[0] // 8)])

    def norm(at):
        part = reduce.total[at, :]
        scale = lax.rsqrt(row_sum(part * part) * (1.0 / D) + EPS)
        unit = part * scale
        base = branch[at, :]
        a_unit = base * lax.rsqrt(row_sum(base * base) * (1.0 / D) + EPS)
        attn_out = a_gain[...] * a_unit
        mlp_out = m_gain[...] * unit
        rows_f = mine_hidden[at, :].astype(F32)
        row = team.slot * shard + at.start + lax.broadcasted_iota(jnp.int32, (at.size, 1), 0)
        live = row < length
        layer[at, :] = jnp.where(live, rows_f + attn_out + mlp_out, 0.0).astype(BF16)
        grad = jnp.where(live, grad_in[at, :].astype(F32), 0.0)
        m_gain_part[...] += folded(grad * unit)
        for i, field in enumerate((rows_f, attn_out, mlp_out)):
            squares[i] += folded(jnp.where(live, field * field, 0.0))
        scaled = grad * m_gain[...]
        back = scale * (scaled - unit * (row_sum(scaled * unit) * (1.0 / D)))
        whole_at = pl.ds(pl.multiple_of(team.slot * shard + at.start, at.size), at.size)
        d_mlp[whole_at, :] = back.astype(BF16)

    over_rows(shard, 16, norm)
    gather.start()
    gather.half()
    gather.finish()


def settle(length, partial, mine_hidden, branch, grad_in, a_gain, m_gain):
    rows, width = partial.shape
    shard = rows // SLOTS
    return pl.pallas_call(
        settle_kernel,
        out_shape=shaped(
            ((shard, width), BF16),
            ((rows, width), BF16),
            ((8, width), F32),
            ((3, 8, width), F32),
        ),
        in_specs=[SCALAR] + [ON_CHIP] * 6,
        out_specs=(ON_CHIP,) * 4,
        scratch_shapes=Reduce.scratch(rows, width) + Gather.scratch,
        compiler_params=pltpu.CompilerParams(
            collective_id=1, has_side_effects=True, vmem_limit_bytes=VMEM_CAP
        ),
        name="settle",
    )(length, partial, mine_hidden, branch, grad_in, a_gain, m_gain)


def unattend_kernel(
    length_ref,
    partial_in,
    branch,
    grad_in,
    a_gain,
    o_weight,
    q_raw,
    k_raw,
    queries,
    keys,
    values,
    scales,
    q_gain,
    k_gain,
    cosine,
    sine,
    d_mid,
    a_gain_part,
    d_branch,
    d_heads,
    q_gain_part,
    k_gain_part,
    out_weight,
    d_mix,
    d_q,
    d_k,
    load,
    *scratch,
):
    team = Team()
    sums = RowSums(team, *scratch[0:4])
    reduce = Reduce(team, *scratch[4:10])
    gather = Gather(team, d_branch, *scratch[10:12])
    fetch = pltpu.make_async_copy(o_weight, out_weight, load.at[0])
    fetch.start()
    team.meet(team.sibling, team.across, team.far)
    rows, local = queries.shape

    def make(at):
        reduce.partial[:, at] = partial_in[:, at]

    reduce.run(make)
    shard = reduce.shard
    length = length_ref[0]
    a_gain_part[...] = jnp.zeros_like(a_gain_part)

    def norm(at):
        row = team.slot * shard + at.start + lax.broadcasted_iota(jnp.int32, (at.size, 1), 0)
        grad = jnp.where(row < length, grad_in[at, :].astype(F32), 0.0) + reduce.total[at, :]
        d_mid[at, :] = grad
        base = branch[at, :]
        scale = lax.rsqrt(row_sum(base * base) * (1.0 / D) + EPS)
        unit = base * scale
        product = grad * unit
        a_gain_part[...] += sum([product[8 * i : 8 * i + 8] for i in range(at.size // 8)])
        scaled = grad * a_gain[...]
        back = scale * (scaled - unit * (row_sum(scaled * unit) * (1.0 / D)))
        whole_at = pl.ds(pl.multiple_of(team.slot * shard + at.start, at.size), at.size)
        d_branch[whole_at, :] = back.astype(BF16)

    over_rows(shard, 16, norm)
    gather.start()
    gather.half()
    gather.finish()
    fetch.wait()
    d_mix[...] = right_inner(d_branch[...], out_weight[...]).astype(BF16)
    q_scale = scales[:, 0:1]
    k_scale = scales[:, 1:2]
    q_inner = jnp.zeros((rows, 1), F32)
    k_inner = jnp.zeros((rows, 1), F32)
    shrink = 1.0 / math.sqrt(HEAD)
    for head in range(local // HEAD):
        at = pl.ds(head * HEAD, HEAD)
        q, k, v, back = queries[:, at], keys[:, at], values[:, at], d_mix[:, at]
        probs = head_probs(q, k, length)
        d_probs = right_inner(back, v)
        d_scores = (probs * (d_probs - row_sum(probs * d_probs))).astype(BF16)
        d_heads[:, pl.ds(2 * local + head * HEAD, HEAD)] = left_inner(
            probs.astype(BF16), back
        ).astype(BF16)
        d_q_hat = turn(matmul(d_scores, k) * shrink, cosine[...], -sine[...])
        d_k_hat = turn(left_inner(d_scores, q) * shrink, cosine[...], -sine[...])
        q_unit = q_raw[:, at] * q_scale
        k_unit = k_raw[:, at] * k_scale
        q_gain_part[:, at] = jnp.sum(d_q_hat * q_unit, axis=0, keepdims=True)
        k_gain_part[:, at] = jnp.sum(d_k_hat * k_unit, axis=0, keepdims=True)
        q_scaled = d_q_hat * q_gain[:, at]
        k_scaled = d_k_hat * k_gain[:, at]
        d_q[:, at] = q_scaled
        d_k[:, at] = k_scaled
        q_inner += row_sum(q_scaled * q_unit)
        k_inner += row_sum(k_scaled * k_unit)
    sums.start(q_inner, k_inner)
    q_inner, k_inner = sums.finish()
    for i, (grad, raw, scale, inner) in enumerate(
        ((d_q, q_raw, q_scale, q_inner), (d_k, k_raw, k_scale, k_inner))
    ):
        factor = scale * scale * inner * (1.0 / D)
        d_heads[:, pl.ds(i * local, local)] = (scale * grad[...] - raw[...] * factor).astype(BF16)


def unattend(
    length, partial, branch, grad_in, a_gain, o_weight, kept, gains, cosine, sine
):
    rows, width = partial.shape
    local = o_weight.shape[0]
    shard = rows // SLOTS
    return pl.pallas_call(
        unattend_kernel,
        out_shape=shaped(
            ((shard, width), F32),
            ((8, width), F32),
            ((rows, width), BF16),
            ((rows, 3 * local), BF16),
            ((1, local), F32),
            ((1, local), F32),
        ),
        in_specs=[SCALAR] + [ON_CHIP] * 4 + [ANY] + [ON_CHIP] * 10,
        out_specs=(ON_CHIP,) * 6,
        scratch_shapes=[
            pltpu.VMEM((local, width), BF16),
            pltpu.VMEM((rows, local), BF16),
            pltpu.VMEM((rows, local), F32),
            pltpu.VMEM((rows, local), F32),
            pltpu.SemaphoreType.DMA((1,)),
        ]
        + RowSums.scratch(rows)
        + Reduce.scratch(rows, width)
        + Gather.scratch,
        compiler_params=pltpu.CompilerParams(
            collective_id=2, has_side_effects=True, vmem_limit_bytes=VMEM_CAP
        ),
        name="unattend",
    )(length, partial, branch, grad_in, a_gain, o_weight, *kept, *gains, cosine, sine)


class Deal:
    def __init__(self, count, shard, width):
        self.count = count
        self.columns = max(128, width // count)
        self.across = width // self.columns
        self.rows = shard * self.across // count

    def at(self, chunk, base=0):
        return (
            at_rows(base + (chunk // self.across) * self.rows, self.rows),
            at_rows((chunk % self.across) * self.columns, self.columns),
        )


def finish_kernel(
    length_ref,
    inverse,
    partial_in,
    d_mid,
    layer,
    layer_out,
    input_grad,
    closed,
    parked,
    leaving,
    deal_send,
    deal_recv,
    *scratch,
):
    team = Team()
    reduce = Reduce(team, *scratch[0:6])
    gathers = [
        Gather(team, whole, *scratch[6 + 2 * i : 8 + 2 * i])
        for i, whole in enumerate((layer_out, input_grad))
    ]
    count = lax.axis_size("dp")
    shard, width = d_mid.shape
    deal = Deal(count, shard, width)
    barrier = pltpu.get_barrier_semaphore()
    for step in range(1, count):
        pl.semaphore_signal(
            barrier, inc=1, device_id=(lax.rem(team.row + step, count), team.me), device_id_type=AT
        )
    for other in (team.sibling, team.across):
        pl.semaphore_signal(barrier, inc=1, device_id=(team.row, other), device_id_type=AT)
    pl.semaphore_wait(barrier, count + 1)

    def make(at):
        reduce.partial[:, at] = partial_in[:, at]

    reduce.run(make)
    length = length_ref[0]

    def close(at):
        row = team.slot * shard + at.start + lax.broadcasted_iota(jnp.int32, (at.size, 1), 0)
        closed[at, :] = jnp.where(row < length, reduce.total[at, :] + d_mid[at, :], 0.0).astype(BF16)

    over_rows(shard, 16, close)

    def send(phase, step, i, source, target):
        return pltpu.make_async_remote_copy(
            src_ref=source,
            dst_ref=target,
            send_sem=deal_send.at[phase, step, i],
            recv_sem=deal_recv.at[phase, step, i],
            device_id=(lax.rem(team.row + step, count), team.me),
            device_id_type=AT,
        )

    first = []
    for i, source in enumerate((layer, closed)):
        for step in range(1, count):
            other = lax.rem(team.row + step, count)
            copy = send(0, step, i, source.at[deal.at(other)], parked.at[team.row, i])
            copy.start()
            first.append(copy)
        parked[team.row, i] = source[deal.at(team.row)]
    for copy in first:
        copy.wait()
    mine = team.slot * shard
    second = []
    for i, target in enumerate((layer_out, input_grad)):
        for step in range(1, count):
            other = lax.rem(team.row + step, count)
            leaving[other, i] = parked[inverse[other], i]
            copy = send(1, step, i, leaving.at[other, i], target.at[deal.at(team.row, mine)])
            copy.start()
            second.append(copy)
        target[deal.at(team.row, mine)] = parked[inverse[team.row], i]
    for copy in second:
        copy.wait()
    for gather in gathers:
        gather.start()
    for gather in gathers:
        gather.half()
    for gather in gathers:
        gather.finish()


def close_layer(length, inverse, partial, d_mid, layer):
    rows, width = partial.shape
    shard = rows // SLOTS
    count = lax.axis_size("dp")
    deal = Deal(count, shard, width)
    chunk = (count, 2, deal.rows, deal.columns)
    return pl.pallas_call(
        finish_kernel,
        out_shape=shaped(((rows, width), BF16), ((rows, width), BF16)),
        in_specs=[SCALAR, SCALAR] + [ON_CHIP] * 3,
        out_specs=(ON_CHIP,) * 2,
        scratch_shapes=[
            pltpu.VMEM((shard, width), BF16),
            pltpu.VMEM(chunk, BF16),
            pltpu.VMEM(chunk, BF16),
            pltpu.SemaphoreType.DMA((2, count, 2)),
            pltpu.SemaphoreType.DMA((2, count, 2)),
        ]
        + Reduce.scratch(rows, width)
        + Gather.scratch * 2,
        compiler_params=pltpu.CompilerParams(
            collective_id=3, has_side_effects=True, vmem_limit_bytes=VMEM_CAP
        ),
        name="close_layer",
    )(length, inverse, partial, d_mid, layer)


SPLIT = 4
PACKED = 768
STEP = 256


class Wires:
    def __init__(self, send, recv):
        self.send, self.recv, self.used = send, recv, 0

    def book(self, number=1):
        self.used += number
        assert self.used <= self.send.shape[0]
        return self.used - number

    def copy(self, source, target, device, index):
        return pltpu.make_async_remote_copy(
            src_ref=source,
            dst_ref=target,
            send_sem=self.send.at[index],
            recv_sem=self.recv.at[index],
            device_id=device,
            device_id_type=AT,
        )


class Spread:
    def __init__(self, wires, grid, team, source, field):
        shard = source.shape[0] // SLOTS
        mine = at_rows(team.slot * shard, shard)
        half = at_rows(team.core * 2 * shard, 2 * shard)
        self.hops, self.sides, self.pairs = {}, {}, {}
        for step in range(1, grid.groups):
            group = lax.rem(grid.group + step, grid.groups)
            block = field.at[step]
            self.hops[step] = wires.copy(
                source.at[mine],
                block.at[mine],
                (group * grid.lanes + grid.lane, team.me),
                wires.book(),
            )
            self.sides[step] = wires.copy(
                block.at[mine], block.at[mine], (team.row, team.across), wires.book()
            )
            self.pairs[step] = wires.copy(
                block.at[half], block.at[half], (team.row, team.sibling), wires.book()
            )
        near = sorted(self.hops, key=lambda step: min(step, grid.groups - step))
        self.plan = {"hop": list(near), "side": list(near), "pair": list(near)}

    def start(self):
        for step in self.plan["hop"]:
            self.hops[step].start()

    def side(self, number=1):
        for step in self.plan["side"][:number]:
            self.hops[step].wait_recv()
            self.sides[step].start()
        del self.plan["side"][:number]

    def pair(self, number=1):
        for step in self.plan["pair"][:number]:
            self.sides[step].wait_recv()
            self.pairs[step].start()
        del self.plan["pair"][:number]

    def drain(self):
        self.side(len(self.hops))
        self.pair(len(self.hops))
        for step in self.hops:
            self.hops[step].wait_send()
            self.sides[step].wait_send()
            self.pairs[step].wait()


def silu_parts(gate, upper):
    sig = jax.nn.sigmoid(gate)
    return sig, (gate * sig * upper).astype(BF16)


def silu_back(gate, upper, sig, d_inner):
    d_gate = (d_inner * upper * sig * (1.0 + gate * (1.0 - sig))).astype(BF16)
    return d_gate, (d_inner * gate * sig).astype(BF16)


def head_back(q, k, v, back, cosine, sine, length):
    probs = head_probs(q, k, length)
    low = probs.astype(BF16)
    mix = matmul(low, v).astype(BF16)
    d_probs = right_inner(back, v)
    d_scores = (probs * (d_probs - row_sum(probs * d_probs))).astype(BF16)
    shrink = 1.0 / math.sqrt(HEAD)
    return (
        mix,
        left_inner(low, back).astype(BF16),
        turn(matmul(d_scores, k) * shrink, cosine, -sine),
        turn(left_inner(d_scores, q) * shrink, cosine, -sine),
    )


def folded(field):
    return sum([field[8 * i : 8 * i + 8] for i in range(field.shape[0] // 8)])


def layer_kernel(names, *refs):
    m = types.SimpleNamespace(**dict(zip(names, refs, strict=True)))
    team, grid = Team(), Grid(lax.axis_size("dp"))
    wires = Wires(m.wire_send, m.wire_recv)
    count, groups, lanes = grid.count, grid.groups, grid.lanes
    rows, width = m.hid.shape
    local, hidden = m.mix.shape[1], m.gate.shape[1]
    shard, strip, tile = rows // SLOTS, width // groups, width // count
    every = groups * rows
    me = team.row

    loads = {}

    def load(name, source, target):
        loads[name] = pltpu.make_async_copy(source, target, m.load.at[len(loads)])
        loads[name].start()

    load("hid", m.hidden_in, m.hid)
    load("q", m.q_weight, m.qkv.at[0])
    load("k", m.k_weight, m.qkv.at[1])
    load("v", m.v_weight, m.qkv.at[2])
    load("grad", m.upstream.at[at_rows(team.slot * shard, shard)], m.closed)
    load("o", m.o_weight, m.wo)
    load("g", m.g_weight, m.wg)
    load("u", m.u_weight, m.wu)
    load("d", m.d_weight, m.wd)

    def peer(step):
        return lax.rem(me + step, count)

    barrier = pltpu.get_barrier_semaphore()
    for step in range(1, count):
        pl.semaphore_signal(barrier, inc=1, device_id=(peer(step), team.me), device_id_type=AT)
    for other in (team.sibling, team.across, team.far):
        pl.semaphore_signal(barrier, inc=1, device_id=(me, other), device_id_type=AT)
    pl.semaphore_wait(barrier, count + 2)

    length = m.lengths[m.order[me]]

    def holder(sequence):
        found = jnp.int32(0)
        for place in range(count):
            found = jnp.where(m.order[place] == sequence, place, found)
        return found

    following = (lax.rem(grid.group + 1, groups) * lanes + grid.lane, team.me)
    sums = RowSums(team, m.sum_mine, m.sum_came, m.sum_send, m.sum_recv)
    deal = Deal(count, shard, width)

    class Return:
        def __init__(self, lot, source, target):
            self.lot, self.source = lot, source
            self.room = (m.parked, m.parked_too)[lot]
            start = wires.book(2 * count)
            self.parked = [
                wires.copy(
                    source.at[deal.at(peer(step))],
                    self.room.at[me],
                    (peer(step), team.me),
                    start + step,
                )
                for step in range(1, count)
            ]
            goal = target.at[deal.at(me, team.slot * shard)]
            self.placed = [
                wires.copy(
                    m.back_leaving.at[peer(step), lot],
                    goal,
                    (peer(step), team.me),
                    start + count + step,
                )
                for step in range(1, count)
            ]
            self.placed.append(
                pltpu.make_async_copy(m.back_leaving.at[me, lot], goal, m.put.at[lot])
            )
            self.holders = [holder(peer(step)) for step in range(count)]

        def park(self):
            for copy in self.parked:
                copy.start()
            self.room[me] = self.source[deal.at(me)]

        def place(self):
            for copy in self.parked:
                copy.wait()
            for step in range(count):
                m.back_leaving[peer(step), self.lot] = self.room[self.holders[step]]
            for copy in self.placed:
                copy.start()

        def wait(self):
            for copy in self.placed:
                copy.wait()

    loads["grad"].wait()
    dealt = wires.book(2 * count)
    first = []
    for step in range(1, count):
        copy = wires.copy(
            m.closed.at[deal.at(peer(step))],
            m.parked.at[me],
            (peer(step), team.me),
            dealt + step,
        )
        copy.start()
        first.append(copy)
    m.parked[me] = m.closed[deal.at(me)]

    loads["hid"].wait()

    loads["q"].wait()
    q = matmul(m.hid[...], m.qkv[0])
    m.q_raw[...] = q
    loads["k"].wait()
    k = matmul(m.hid[...], m.qkv[1])
    m.k_raw[...] = k
    sums.start(row_sum(q * q), row_sum(k * k))
    loads["v"].wait()
    m.values[...] = matmul(m.hid[...], m.qkv[2]).astype(BF16)
    q_total, k_total = sums.finish()
    q_scale = lax.rsqrt(q_total * (1.0 / D) + EPS)
    k_scale = lax.rsqrt(k_total * (1.0 / D) + EPS)
    lane = lax.broadcasted_iota(jnp.int32, (rows, 128), 1)
    m.scales[...] = jnp.where(lane == 0, q_scale, k_scale)

    def attend_head(head, carry):
        at = at_rows(head * HEAD, HEAD)
        q = turn(m.q_raw[:, at] * q_scale * m.q_gain[:, at], m.cosine[...], m.sine[...]).astype(BF16)
        k = turn(m.k_raw[:, at] * k_scale * m.k_gain[:, at], m.cosine[...], m.sine[...]).astype(BF16)
        m.queries[:, at] = q
        m.keys[:, at] = k
        probs = head_probs(q, k, length).astype(BF16)
        m.mix[:, at] = matmul(probs, m.values[:, at]).astype(BF16)
        return carry

    lax.fori_loop(0, local // HEAD, attend_head, 0)

    for copy in first:
        copy.wait()
    for step in range(1, count):
        m.back_leaving[peer(step), 0] = m.parked[m.order[peer(step)]]
    m.grad_in[deal.at(me)] = m.parked[m.order[me]]
    second = []
    for step in range(1, count):
        copy = wires.copy(
            m.back_leaving.at[peer(step), 0],
            m.grad_in.at[deal.at(me)],
            (peer(step), team.me),
            dealt + count + step,
        )
        copy.start()
        second.append(copy)

    reduce = Reduce(
        team, m.partial, m.came, m.gone, m.total, m.reduce_send, m.reduce_recv
    )

    def gather(whole, number):
        return Gather(team, whole, m.gather_send.at[number], m.gather_recv.at[number])

    loads["o"].wait()

    def make_branch(at):
        m.partial[:, at] = matmul(m.mix[...], m.wo[:, at]).astype(BF16)

    reduce.run(make_branch)
    own = m.mid_all.at[0]

    def whole_at(at):
        return pl.ds(pl.multiple_of(team.slot * shard + at.start, at.size), at.size)

    def norm_mid(at):
        part = m.total[at, :]
        m.branch[at, :] = part
        unit = part * lax.rsqrt(row_sum(part * part) * (1.0 / D) + EPS)
        mid = m.hid[whole_at(at), :].astype(F32) + m.a_gain[...] * unit
        m.mid_all[0, whole_at(at), :] = mid.astype(BF16)

    over_rows(shard, 16, norm_mid)
    mid_gather = gather(own, 0)
    mid_gather.start()
    mid_spread = Spread(wires, grid, team, own, m.mid_all)
    mid_spread.start()
    mid_gather.half()
    mid_gather.finish()
    loads["g"].wait()
    loads["u"].wait()

    def widen(i, carry):
        at = at_rows(i * STEP, STEP)
        gate = matmul(m.mid_all[0], m.wg[:, at])
        upper = matmul(m.mid_all[0], m.wu[:, at])
        m.gate[:, at] = gate.astype(BF16)
        m.upper[:, at] = upper.astype(BF16)
        m.inner[:, at] = silu_parts(gate, upper)[1]
        return carry

    lax.fori_loop(0, hidden // STEP, widen, 0)
    loads["d"].wait()

    def make_mlp(at):
        m.partial[:, at] = matmul(m.inner[...], m.wd[:, at]).astype(BF16)

    for copy in second:
        copy.wait()
    reduce.run(make_mlp)
    m.stats[...] = jnp.zeros_like(m.stats)
    m.fold[...] = jnp.zeros_like(m.fold)

    def norm_mlp(at):
        part = m.total[at, :]
        scale = lax.rsqrt(row_sum(part * part) * (1.0 / D) + EPS)
        unit = part * scale
        base = m.branch[at, :]
        a_unit = base * lax.rsqrt(row_sum(base * base) * (1.0 / D) + EPS)
        attn_out = m.a_gain[...] * a_unit
        mlp_out = m.m_gain[...] * unit
        rows_f = m.hid[whole_at(at), :].astype(F32)
        row = team.slot * shard + at.start + lax.broadcasted_iota(jnp.int32, (at.size, 1), 0)
        live = row < length
        m.layer[at, :] = jnp.where(live, rows_f + attn_out + mlp_out, 0.0).astype(BF16)
        grad = jnp.where(live, m.grad_in[at, :].astype(F32), 0.0)
        m.fold[0] += folded(grad * unit)
        for i, field in enumerate((rows_f, attn_out, mlp_out)):
            m.fold[i + 1] += folded(jnp.where(live, field * field, 0.0))
        scaled = grad * m.m_gain[...]
        back = scale * (scaled - unit * (row_sum(scaled * unit) * (1.0 / D)))
        m.dm_all[0, whole_at(at), :] = back.astype(BF16)

    over_rows(shard, 16, norm_mlp)
    own_back = m.dm_all.at[0]
    dm_gather = gather(own_back, 1)
    dm_gather.start()
    dm_spread = Spread(wires, grid, team, own_back, m.dm_all)
    dm_spread.start()
    layer_return = Return(1, m.layer, m.layer_out)
    layer_return.park()
    dm_gather.half()
    m.stats[0:1, :] = jnp.sum(m.fold[0], axis=0, keepdims=True)
    for i in range(3):
        m.stats[3 + i : 4 + i, :] = jnp.sum(m.fold[i + 1], axis=0, keepdims=True)
    dm_gather.finish()
    mid_spread.side(groups)
    hid_spread = Spread(wires, grid, team, m.hid, m.hid_all)
    hid_spread.start()

    def narrow(i, carry):
        at = at_rows(i * STEP, STEP)
        d_inner = right_inner(m.dm_all[0], m.wd[at, :])
        gate = m.gate[:, at].astype(F32)
        upper = m.upper[:, at].astype(F32)
        m.gate[:, at], m.upper[:, at] = silu_back(gate, upper, jax.nn.sigmoid(gate), d_inner)
        return carry

    lax.fori_loop(0, hidden // STEP, narrow, 0)

    def make_d_mid(at):
        m.partial[:, at] = (
            right_inner(m.gate[...], m.wg[at, :]) + right_inner(m.upper[...], m.wu[at, :])
        ).astype(BF16)

    reduce.begin(make_d_mid)
    dm_spread.side(1)
    reduce.end()
    m.fold[0] = jnp.zeros_like(m.fold[0])

    def norm_d_mid(at):
        row = team.slot * shard + at.start + lax.broadcasted_iota(jnp.int32, (at.size, 1), 0)
        grad = jnp.where(row < length, m.grad_in[at, :].astype(F32), 0.0) + m.total[at, :]
        m.d_mid[at, :] = grad
        base = m.branch[at, :]
        scale = lax.rsqrt(row_sum(base * base) * (1.0 / D) + EPS)
        unit = base * scale
        m.fold[0] += folded(grad * unit)
        scaled = grad * m.a_gain[...]
        back = scale * (scaled - unit * (row_sum(scaled * unit) * (1.0 / D)))
        m.d_branch[whole_at(at), :] = back.astype(BF16)

    over_rows(shard, 16, norm_d_mid)
    d_gather = gather(m.d_branch, 2)
    d_gather.start()
    dm_spread.side(1)
    m.stats[1:2, :] = jnp.sum(m.fold[0], axis=0, keepdims=True)
    d_gather.half()
    d_gather.finish()
    dm_spread.side(groups)
    mid_spread.pair(groups)
    branch_spread = Spread(wires, grid, team, m.d_branch, m.branch_all)
    branch_spread.start()

    d_mix = m.partial.at[:, pl.ds(0, local)]
    d_mix[...] = right_inner(m.d_branch[...], m.wo[...]).astype(BF16)
    q_inner = jnp.zeros((rows, 1), F32)
    k_inner = jnp.zeros((rows, 1), F32)
    q_scale = m.scales[:, 0:1]
    k_scale = m.scales[:, 1:2]

    def unattend_head(head, carry):
        at = at_rows(head * HEAD, HEAD)
        _, d_v, d_q_hat, d_k_hat = head_back(
            m.queries[:, at],
            m.keys[:, at],
            m.values[:, at],
            d_mix[:, at],
            m.cosine[...],
            m.sine[...],
            length,
        )
        m.d_heads[:, at_rows(2 * local + head * HEAD, HEAD)] = d_v
        q_unit = m.q_raw[:, at] * q_scale
        k_unit = m.k_raw[:, at] * k_scale
        m.stats[2:3, at] = jnp.sum(d_q_hat * q_unit, axis=0, keepdims=True)
        m.stats[2:3, at_rows(local + head * HEAD, HEAD)] = jnp.sum(
            d_k_hat * k_unit, axis=0, keepdims=True
        )
        q_scaled = d_q_hat * m.q_gain[:, at]
        k_scaled = d_k_hat * m.k_gain[:, at]
        m.stage[0, :, at] = q_scaled
        m.stage[1, :, at] = k_scaled
        return carry[0] + row_sum(q_scaled * q_unit), carry[1] + row_sum(k_scaled * k_unit)

    q_inner, k_inner = lax.fori_loop(0, local // HEAD, unattend_head, (q_inner, k_inner))
    sums.start(q_inner, k_inner)
    q_inner, k_inner = sums.finish()
    for i, (raw, scale, inner) in enumerate(
        ((m.q_raw, q_scale, q_inner), (m.k_raw, k_scale, k_inner))
    ):
        factor = scale * scale * inner * (1.0 / D)
        m.d_heads[:, pl.ds(i * local, local)] = (
            scale * m.stage[i] - raw[...] * factor
        ).astype(BF16)
    m.stat_team[team.me] = m.stats[...]
    stat_at = wires.book(3 + count)
    stat_team = [
        wires.copy(m.stats, m.stat_team.at[team.me], (me, other), stat_at + i)
        for i, other in enumerate((team.sibling, team.across, team.far))
    ]
    for copy in stat_team:
        copy.start()

    layer_return.place()

    def make_input(at):
        m.partial[:, at] = (
            right_inner(m.d_heads[:, 0:local], m.qkv[0, at, :])
            + right_inner(m.d_heads[:, local : 2 * local], m.qkv[1, at, :])
            + right_inner(m.d_heads[:, 2 * local : 3 * local], m.qkv[2, at, :])
        ).astype(BF16)

    mid_spread.drain()
    dm_spread.drain()
    for k in range(groups):
        m.mid_turned[:, pl.ds(k * rows, rows)] = jnp.transpose(
            m.mid_all[k, :, at_rows(grid.group * strip, strip)]
        )
    crossed = wires.book(3 * (hidden // STEP))
    crossing = (grid.group * lanes + (1 - grid.lane), team.me)

    def tile_of(lane):
        return at_rows((grid.group * lanes + lane) * tile, tile)

    def all_rows(field, columns):
        block = field[:, :, columns]
        return block.reshape(every, block.shape[2])

    def crossings(n):
        at = at_rows(n * STEP, STEP)
        spare = pl.ds(every, tile)
        return [
            wires.copy(m.wg.at[spare, at], m.x_gate.at[:, at], crossing, crossed + 3 * n),
            wires.copy(m.wu.at[spare, at], m.x_up.at[:, at], crossing, crossed + 3 * n + 1),
            wires.copy(m.wd.at[at, spare], m.x_down.at[at, :], crossing, crossed + 3 * n + 2),
        ]

    def again(n, carry):
        at = at_rows(n * STEP, STEP)

        def block_again(k, carry):
            gate = matmul(m.mid_all[k], m.wg[:, at])
            upper = matmul(m.mid_all[k], m.wu[:, at])
            d_inner = right_inner(m.dm_all[k], m.wd[at, :])
            sig, inner = silu_parts(gate, upper)
            kept = at_rows((k - 1) * rows, rows)
            m.keep[0, kept, :] = inner
            m.keep[1, kept, :], m.keep[2, kept, :] = silu_back(gate, upper, sig, d_inner)
            return carry

        lax.fori_loop(1, groups, block_again, 0)
        whole = pl.ds(rows, every - rows)
        m.wg[0:rows, at] = m.gate[:, at]
        m.wu[0:rows, at] = m.upper[:, at]
        m.wd[at, 0:rows] = jnp.transpose(m.inner[:, at])
        m.wg[whole, at] = m.keep[1]
        m.wu[whole, at] = m.keep[2]
        for k in range(1, groups):
            kept = pl.ds((k - 1) * rows, rows)
            m.wd[at, pl.ds(k * rows, rows)] = jnp.transpose(m.keep[0, kept, :])
        turned = m.mid_turned[at_rows((1 - grid.lane) * tile, tile), :]
        spare = pl.ds(every, tile)
        m.wg[spare, at] = matmul(turned, m.wg[0:every, at]).astype(BF16)
        m.wu[spare, at] = matmul(turned, m.wu[0:every, at]).astype(BF16)
        m.wd[at, spare] = matmul(m.wd[at, 0:every], all_rows(m.dm_all, tile_of(1 - grid.lane))).astype(BF16)
        for copy in crossings(n):
            copy.start()
        return carry

    def again_with_events(n, carry):
        again(n, carry)
        for place, event in events.items():
            pl.when(n == place)(event)
        return carry

    tiles = hidden // STEP
    stat_dp = [
        wires.copy(m.pack, m.stat_dp.at[me], (peer(step), team.me), stat_at + 2 + step)
        for step in range(1, count)
    ]
    grad_return = Return(0, m.closed, m.input_grad)
    out_gathers = [gather(m.layer_out, 3), gather(m.input_grad, 4)]

    def add_stats():
        for copy in stat_team:
            copy.wait()
        total = (m.stat_team[0] + m.stat_team[1]) + (m.stat_team[2] + m.stat_team[3])
        line = lax.broadcasted_iota(jnp.int32, total.shape, 0)
        total = jnp.where(line == 2, m.stats[...], total)
        m.pack[...] = jnp.zeros_like(m.pack)
        packed = m.pack.shape[1]
        for i in range(2):
            for j in range(pl.cdiv(width, packed)):
                piece = total[i : i + 1, j * packed : min((j + 1) * packed, width)]
                m.pack[3 * i + j : 3 * i + j + 1, 0 : piece.shape[1]] = piece
        m.pack[6:7, :] = total[2:3, 0:packed]
        m.pack[7:8, 0 : 2 * local - packed] = total[2:3, packed : 2 * local]
        for i in range(3):
            square = jnp.sum(total[3 + i : 4 + i, :], axis=1, keepdims=True)
            m.pack[7:8, 2 * local - packed + i * 128 : 2 * local - packed + (i + 1) * 128] = (
                jnp.broadcast_to(square, (1, 128))
            )
        m.stat_dp[me] = m.pack[...]
        for copy in stat_dp:
            copy.start()

    def close(at):
        row = team.slot * shard + at.start + lax.broadcasted_iota(jnp.int32, (at.size, 1), 0)
        m.closed[at, :] = jnp.where(row < length, m.total[at, :] + m.d_mid[at, :], 0.0).astype(BF16)

    def park():
        reduce.end()
        over_rows(shard, 16, close)
        grad_return.park()

    def share():
        layer_return.wait()
        grad_return.wait()
        for one in out_gathers:
            one.start()

    events = {
        2: park,
        tiles - 4: lambda: hid_spread.pair(groups),
        tiles - 3: lambda: branch_spread.side(groups),
    }
    lax.fori_loop(0, 1, again, 0)
    reduce.begin(make_input)
    hid_spread.side(groups)
    add_stats()
    lax.fori_loop(1, tiles, again_with_events, 0)
    hid_spread.drain()
    def put(source, target, index):
        return pltpu.make_async_copy(source, target, m.put.at[index])

    puts = []

    def store(value, target):
        slot = len(puts) % 2
        if len(puts) >= 2:
            puts[-2].wait()
        stage = m.stage.at[slot, pl.ds(0, value.shape[0]), pl.ds(0, value.shape[1])]
        stage[...] = value
        puts.append(put(stage, target, 2 + slot))
        puts[-1].start()

    late = []

    def bring(source, target):
        copy = pltpu.make_async_copy(source, target, m.late.at[len(late)])
        copy.start()
        late.append(copy)

    for k in range(1, groups):
        bring(m.hid_all.at[k], m.mid_all.at[k])
    for copy in late:
        copy.wait()
    for k in range(groups):
        source = m.mid_all.at[k] if k else m.hid
        for lane in range(lanes):
            m.gate[:, pl.ds(lane * every + k * rows, rows)] = jnp.transpose(
                source[:, at_rows(grid.group * strip + lane * tile, tile)]
            )
    wide_sums = RowSums(
        team, m.wide_mine, m.wide_came.at[0], m.wide_send.at[0], m.wide_recv.at[0]
    )
    spare_rows = every + tile

    def project_again(k, carry):
        block = at_rows(spare_rows + (k - 1) * rows, rows)
        lane = lax.broadcasted_iota(jnp.int32, (rows, 128), 1)
        found = jnp.zeros((rows, 128), F32)
        for i in range(2):
            raw = matmul(m.mid_all[k], m.qkv[i])
            m.wu[block, pl.ds(2 * local + i * local, local)] = raw.astype(BF16)
            found = jnp.where(lane == i, row_sum(raw * raw), found)
        m.wide_inner[at_rows((k - 1) * rows, rows), :] = found
        m.wu[block, pl.ds(local, local)] = matmul(m.mid_all[k], m.qkv[2]).astype(BF16)
        return carry

    lax.fori_loop(1, groups, project_again, 0)
    wide_sums.start(m.wide_inner[:, 0:1], m.wide_inner[:, 1:2])
    branch_spread.pair(groups)
    grad_return.place()
    branch_spread.drain()
    for k in range(1, groups):
        bring(m.branch_all.at[k], m.mid_all.at[k])
    for copy in late[groups - 1 :]:
        copy.wait()
    q_total, k_total = wide_sums.finish()
    lane = lax.broadcasted_iota(jnp.int32, (every - rows, 128), 1)
    m.wide_scales[...] = lax.rsqrt(jnp.where(lane == 0, q_total, k_total) * (1.0 / D) + EPS)
    m.wide_inner[...] = jnp.zeros_like(m.wide_inner)

    def attention_again(k, carry):
        back_length = m.lengths[
            m.order[lax.rem(grid.group - k + groups, groups) * lanes + grid.lane]
        ]
        block = at_rows(spare_rows + (k - 1) * rows, rows)
        inside = at_rows((k - 1) * rows, rows)
        q_scale = m.wide_scales[inside, 0:1]
        k_scale = m.wide_scales[inside, 1:2]
        d_mix[...] = right_inner(m.mid_all[k], m.wo[...]).astype(BF16)
        q_inner = jnp.zeros((rows, 1), F32)
        k_inner = jnp.zeros((rows, 1), F32)

        def head_again(head, carry):
            at = at_rows(head * HEAD, HEAD)
            q_unit = m.wu[block, at_rows(2 * local + head * HEAD, HEAD)].astype(F32) * q_scale
            k_unit = m.wu[block, at_rows(3 * local + head * HEAD, HEAD)].astype(F32) * k_scale
            mix, d_v, d_q_hat, d_k_hat = head_back(
                turn(q_unit * m.q_gain[:, at], m.cosine[...], m.sine[...]).astype(BF16),
                turn(k_unit * m.k_gain[:, at], m.cosine[...], m.sine[...]).astype(BF16),
                m.wu[block, at_rows(local + head * HEAD, HEAD)],
                d_mix[:, at],
                m.cosine[...],
                m.sine[...],
                back_length,
            )
            m.wu[block, at] = mix
            m.wg[block, at_rows(2 * local + head * HEAD, HEAD)] = d_v
            q_scaled = d_q_hat * m.q_gain[:, at]
            k_scaled = d_k_hat * m.k_gain[:, at]
            m.wg[block, at] = q_scaled.astype(BF16)
            m.wg[block, at_rows(local + head * HEAD, HEAD)] = k_scaled.astype(BF16)
            return carry[0] + row_sum(q_scaled * q_unit), carry[1] + row_sum(k_scaled * k_unit)

        q_inner, k_inner = lax.fori_loop(0, local // HEAD, head_again, (q_inner, k_inner))
        lane = lax.broadcasted_iota(jnp.int32, (rows, 128), 1)
        m.wide_inner[inside, :] = jnp.where(lane == 0, q_inner, jnp.where(lane == 1, k_inner, 0.0))
        return carry

    lax.fori_loop(1, groups, attention_again, 0)
    wide_sums = RowSums(
        team, m.wide_mine, m.wide_came.at[1], m.wide_send.at[1], m.wide_recv.at[1]
    )
    wide_sums.start(m.wide_inner[:, 0:1], m.wide_inner[:, 1:2])
    other, this = 1 - grid.lane, grid.lane
    others = pl.ds(spare_rows, every - rows)

    def lane_of(lane):
        return at_rows(grid.group * strip + lane * tile, tile)

    def o_part(lane):
        return left_inner(m.mix[...], m.d_branch[:, lane_of(lane)]) + left_inner(
            m.wu[others, 0:local],
            m.mid_all[1:groups, :, lane_of(lane)].reshape(every - rows, tile),
        )

    def heads_part(lane, at):
        first = at_rows(lane * every, rows)
        rest = pl.ds(pl.multiple_of(lane * every + rows, rows), every - rows)
        return matmul(m.gate[:, first], m.d_heads[:, at]) + matmul(
            m.gate[:, rest], m.wg[others, at]
        )

    last = wires.book(4)
    finals = []
    spare = m.qkv.at[2, pl.ds(3 * tile, local), pl.ds(0, tile)]
    spare[...] = o_part(other).astype(BF16)
    finals.append(wires.copy(spare, m.x_o, crossing, last + 3))
    finals[-1].start()
    q_inner, k_inner = wide_sums.finish()
    lane = lax.broadcasted_iota(jnp.int32, (every - rows, 128), 1)
    m.wide_inner[...] = jnp.where(lane == 0, q_inner, k_inner)

    def close_heads(k, carry):
        block = at_rows(spare_rows + (k - 1) * rows, rows)
        inside = at_rows((k - 1) * rows, rows)
        for i in range(2):
            at = pl.ds(i * local, local)
            scale = m.wide_scales[inside, i : i + 1]
            factor = scale * scale * m.wide_inner[inside, i : i + 1] * (1.0 / D)
            raw = m.wu[block, pl.ds(2 * local + i * local, local)].astype(F32)
            m.wg[block, at] = (scale * m.wg[block, at].astype(F32) - raw * factor).astype(BF16)
        return carry

    lax.fori_loop(1, groups, close_heads, 0)
    for i, target in ((2, m.x_v), (0, m.x_q), (1, m.x_k)):
        spare = m.qkv.at[2, pl.ds(i * tile, tile)]
        spare[...] = heads_part(other, pl.ds(i * local, local)).astype(BF16)
        finals.append(wires.copy(spare, target, crossing, last + i))
        finals[-1].start()
    share()
    turned_own = m.mid_turned.at[at_rows(grid.lane * tile, tile)]
    wide = m.stage.shape[2]
    high = rows

    def narrow_stage(slot):
        return m.stage.at[slot, :, pl.ds(0, tile)]

    def flush(copies, last, i, values):
        @pl.when(i > 0)
        def _():
            for copy in copies(i - 1):
                copy.wait()

        for copy, slot, value in zip(copies(i), last, values, strict=True):
            slot[...] = value
            copy.start()

    def wide_copies(i):
        at = at_rows(i * wide, wide)
        return [put(m.stage.at[0], m.g_own.at[:, at], 2), put(m.stage.at[1], m.u_own.at[:, at], 3)]

    def wide_part(i, carry):
        at = at_rows(i * wide, wide)
        flush(
            wide_copies,
            (m.stage.at[0], m.stage.at[1]),
            i,
            [matmul(turned_own[...], weight[0:every, at]) for weight in (m.wg, m.wu)],
        )
        return carry

    lax.fori_loop(0, hidden // wide, wide_part, 0)
    for copy in wide_copies(hidden // wide - 1):
        copy.wait()

    def high_at(i, slot):
        return at_rows((2 * i + slot) * high, high)

    def high_copies(i):
        return [put(narrow_stage(slot), m.d_own.at[high_at(i, slot), :], 2 + slot) for slot in range(2)]

    def high_part(i, carry):
        right = all_rows(m.dm_all, tile_of(grid.lane))
        flush(
            high_copies,
            (narrow_stage(0), narrow_stage(1)),
            i,
            [matmul(m.wd[high_at(i, slot), 0:every], right) for slot in range(2)],
        )
        return carry

    lax.fori_loop(0, hidden // high // 2, high_part, 0)
    for copy in high_copies(hidden // high // 2 - 1):
        copy.wait()
    for i, target in enumerate((m.q_own, m.k_own, m.v_own)):
        store(heads_part(this, pl.ds(i * local, local)), target)
    output = o_part(this)
    for i in range(local // high):
        store(output[i * high : (i + 1) * high], m.o_own.at[pl.ds(i * high, high), :])
    for copy in puts[-2:]:
        copy.wait()

    def arrived(n, carry):
        for copy in crossings(n):
            copy.wait()
        return carry

    for one in out_gathers:
        one.half()
    for one in out_gathers:
        one.finish()
    for copy in stat_dp:
        copy.wait()
    m.stat_out[...] = sum([m.stat_dp[i] for i in range(1, count)], m.stat_dp[0])
    lax.fori_loop(0, tiles, arrived, 0)
    for copy in finals:
        copy.wait()


def whole_layer(grid, args):
    (hidden_in, upstream, lengths, order, q_weight, k_weight, v_weight, o_weight) = args[:8]
    (q_gain, k_gain, a_gain, g_weight, u_weight, d_weight, m_gain, cosine, sine) = args[8:]
    rows, width = hidden_in.shape
    local, hidden = q_weight.shape[1], g_weight.shape[1]
    count, groups = grid.count, grid.groups
    shard, strip, tile = rows // SLOTS, width // groups, width // count
    every = groups * rows
    deal = Deal(count, shard, width)
    chunk = (deal.rows, deal.columns)
    inputs = [
        ("lengths", SCALAR, lengths),
        ("order", SCALAR, order),
        ("hidden_in", ANY, hidden_in),
        ("upstream", ANY, upstream),
        ("q_weight", ANY, q_weight),
        ("k_weight", ANY, k_weight),
        ("v_weight", ANY, v_weight),
        ("o_weight", ANY, o_weight),
        ("g_weight", ANY, g_weight),
        ("u_weight", ANY, u_weight),
        ("d_weight", ANY, d_weight),
        ("q_gain", ON_CHIP, q_gain),
        ("k_gain", ON_CHIP, k_gain),
        ("a_gain", ON_CHIP, a_gain),
        ("m_gain", ON_CHIP, m_gain),
        ("cosine", ON_CHIP, cosine),
        ("sine", ON_CHIP, sine),
    ]
    outputs = [
        ("layer_out", (rows, width), BF16),
        ("input_grad", (rows, width), BF16),
        ("g_own", (tile, hidden), F32),
        ("u_own", (tile, hidden), F32),
        ("d_own", (hidden, tile), F32),
        ("q_own", (tile, local), F32),
        ("k_own", (tile, local), F32),
        ("v_own", (tile, local), F32),
        ("o_own", (local, tile), F32),
        ("x_gate", (tile, hidden), BF16),
        ("x_up", (tile, hidden), BF16),
        ("x_down", (hidden, tile), BF16),
        ("x_q", (tile, local), BF16),
        ("x_k", (tile, local), BF16),
        ("x_v", (tile, local), BF16),
        ("x_o", (local, tile), BF16),
        ("hid_all", (groups, rows, width), BF16),
        ("branch_all", (groups, rows, width), BF16),
        ("stat_out", (8, PACKED), F32),
    ]
    wires = 160
    scratch = [
        ("qkv", pltpu.VMEM((3, width, local), BF16)),
        ("wo", pltpu.VMEM((local, width), BF16)),
        ("wg", pltpu.VMEM((width, hidden), BF16)),
        ("wu", pltpu.VMEM((width, hidden), BF16)),
        ("wd", pltpu.VMEM((hidden, width), BF16)),
        ("hid", pltpu.VMEM((rows, width), BF16)),
        ("mid_all", pltpu.VMEM((groups, rows, width), BF16)),
        ("dm_all", pltpu.VMEM((groups, rows, width), BF16)),
        ("gate", pltpu.VMEM((rows, hidden), BF16)),
        ("upper", pltpu.VMEM((rows, hidden), BF16)),
        ("inner", pltpu.VMEM((rows, hidden), BF16)),
        ("q_raw", pltpu.VMEM((rows, local), F32)),
        ("k_raw", pltpu.VMEM((rows, local), F32)),
        ("queries", pltpu.VMEM((rows, local), BF16)),
        ("keys", pltpu.VMEM((rows, local), BF16)),
        ("values", pltpu.VMEM((rows, local), BF16)),
        ("scales", pltpu.VMEM((rows, 128), F32)),
        ("mix", pltpu.VMEM((rows, local), BF16)),
        ("d_branch", pltpu.VMEM((rows, width), BF16)),
        ("d_heads", pltpu.VMEM((rows, 3 * local), BF16)),
        ("mid_turned", pltpu.VMEM((strip, every), BF16)),
        ("keep", pltpu.VMEM((3, every - rows, STEP), BF16)),
        ("stage", pltpu.VMEM((2, rows, local), F32)),
        ("branch", pltpu.VMEM((shard, width), F32)),
        ("d_mid", pltpu.VMEM((shard, width), F32)),
        ("layer", pltpu.VMEM((shard, width), BF16)),
        ("closed", pltpu.VMEM((shard, width), BF16)),
        ("grad_in", pltpu.VMEM((shard, width), BF16)),
        ("parked", pltpu.VMEM((count,) + chunk, BF16)),
        ("parked_too", pltpu.VMEM((count,) + chunk, BF16)),
        ("back_leaving", pltpu.VMEM((count, 2) + chunk, BF16)),
        ("fold", pltpu.VMEM((4, 8, width), F32)),
        ("stats", pltpu.VMEM((8, width), F32)),
        ("stat_team", pltpu.VMEM((SLOTS, 8, width), F32)),
        ("pack", pltpu.VMEM((8, PACKED), F32)),
        ("stat_dp", pltpu.VMEM((count, 8, PACKED), F32)),
        ("partial", pltpu.VMEM((rows, width), BF16)),
        ("came", pltpu.VMEM((3, shard, width), BF16)),
        ("gone", pltpu.VMEM((shard, width), BF16)),
        ("total", pltpu.VMEM((shard, width), F32)),
        ("sum_mine", pltpu.VMEM((8, rows), F32)),
        ("sum_came", pltpu.VMEM((3, 8, rows), F32)),
        ("wide_mine", pltpu.VMEM((8, every - rows), F32)),
        ("wide_came", pltpu.VMEM((2, 3, 8, every - rows), F32)),
        ("wide_scales", pltpu.VMEM((every - rows, 128), F32)),
        ("wide_inner", pltpu.VMEM((every - rows, 128), F32)),
        ("wide_send", pltpu.SemaphoreType.DMA((2, 3))),
        ("wide_recv", pltpu.SemaphoreType.DMA((2, 3))),
        ("sum_send", pltpu.SemaphoreType.DMA((3,))),
        ("sum_recv", pltpu.SemaphoreType.DMA((3,))),
        ("reduce_send", pltpu.SemaphoreType.DMA((3, SPLIT))),
        ("reduce_recv", pltpu.SemaphoreType.DMA((3, SPLIT))),
        ("gather_send", pltpu.SemaphoreType.DMA((5, 3))),
        ("gather_recv", pltpu.SemaphoreType.DMA((5, 3))),
        ("wire_send", pltpu.SemaphoreType.DMA((wires,))),
        ("wire_recv", pltpu.SemaphoreType.DMA((wires,))),
        ("load", pltpu.SemaphoreType.DMA((9,))),
        ("put", pltpu.SemaphoreType.DMA((4,))),
        ("late", pltpu.SemaphoreType.DMA((2 * groups,))),
    ]
    names = [entry[0] for entry in inputs + outputs + scratch]
    results = pl.pallas_call(
        functools.partial(layer_kernel, names),
        out_shape=shaped(*[entry[1:] for entry in outputs]),
        in_specs=[entry[1] for entry in inputs],
        out_specs=(ANY,) * (len(outputs) - 1) + (ON_CHIP,),
        scratch_shapes=[entry[1] for entry in scratch],
        compiler_params=pltpu.CompilerParams(
            collective_id=4, has_side_effects=True, vmem_limit_bytes=63 * 2**20
        ),
        name="whole_layer",
    )(*[entry[2] for entry in inputs])
    return dict(zip([entry[0] for entry in outputs], results, strict=True))


def body(
    hidden_in,
    upstream_grad,
    seq_lengths,
    position_order,
    query_weight,
    key_weight,
    value_weight,
    output_weight,
    query_gain,
    key_gain,
    attn_gain,
    gate_weight,
    up_weight,
    down_weight,
    mlp_gain,
):
    count = lax.axis_size("dp")
    ways = lax.axis_size("tensor")
    myself = lax.axis_index("dp")
    part = lax.axis_index("tensor")
    grid = Grid(count)
    index = jnp.arange(count, dtype=jnp.int32)
    inverse = jnp.sum(
        index[None, :] * (position_order[None, :] == index[:, None]).astype(jnp.int32), axis=1
    )
    rows = hidden_in.shape[1]
    width = hidden_in.shape[2]
    shard = rows // ways
    if grid.lanes == 2 and 2 * query_weight.shape[1] + 3 * 128 <= 2 * PACKED and width <= 3 * PACKED and width // count == rows and grid.groups * rows + width // count <= width:
        cosine, sine = rope_constants(rows, HEAD)
        found = whole_layer(
            grid,
            (
                hidden_in[0],
                upstream_grad[0],
                seq_lengths,
                position_order,
                query_weight,
                key_weight,
                value_weight,
                output_weight,
                query_gain[None],
                key_gain[None],
                attn_gain[None],
                gate_weight,
                up_weight,
                down_weight,
                mlp_gain[None],
                cosine,
                sine,
            ),
        )
        local = query_weight.shape[1]

        def joined(own, other):
            return found[own] + found[other].astype(F32)

        stats = found["stat_out"]
        gains = stats[6:8].reshape(-1)
        squares = gains[2 * local : 2 * local + 3 * 128 : 128]
        return (
            found["layer_out"][None],
            found["input_grad"][None],
            joined("q_own", "x_q"),
            joined("k_own", "x_k"),
            joined("v_own", "x_v"),
            joined("o_own", "x_o"),
            gains[:local],
            gains[local : 2 * local],
            stats[3:6].reshape(-1)[:width],
            joined("g_own", "x_gate"),
            joined("u_own", "x_up"),
            joined("d_own", "x_down"),
            stats[0:3].reshape(-1)[:width],
            jnp.sqrt(squares / (jnp.sum(seq_lengths).astype(F32) * D)),
        )

    piece = shard // count
    seq_here = jnp.sum(jnp.where(index == myself, position_order, 0))
    length = jnp.sum(jnp.where(index == seq_here, seq_lengths, 0))[None]
    slot = part % 2 * 2 + part // 2

    def exchange(pieces):
        return lax.all_to_all(pieces, "dp", split_axis=0, concat_axis=0, tiled=True)

    def my_rows(field):
        return lax.dynamic_slice_in_dim(field, slot * shard, shard, axis=0)

    first = exchange(my_rows(upstream_grad[0]).reshape(count, piece, width))
    second = exchange(jnp.take(first, position_order, axis=0))
    grad_in = second.reshape(shard, width)

    rows_low = hidden_in[0]
    my_low = my_rows(rows_low)
    local = query_weight.shape[1]
    strip = width // grid.groups
    tile = width // count

    def strip_of(field, group):
        return lax.dynamic_slice_in_dim(field, group * strip, strip, axis=1)

    def strips(field):
        found = [strip_of(field, grid.group)]
        for step in range(1, grid.groups):
            found.append(
                grid.shift_groups(
                    strip_of(field, (grid.group + step) % grid.groups), step
                )
            )
        return jnp.concatenate(found, axis=0)

    def tile_of(field, lane):
        return lax.dynamic_slice_in_dim(field, lane * tile, tile, axis=1)

    def reduced(product, field):
        sent = []
        for step in range(1, grid.lanes):
            other = product(tile_of(field, (grid.lane + step) % grid.lanes)).astype(BF16)
            sent.append(grid.shift_lanes(other, step))
        mine = product(tile_of(field, grid.lane))
        for other in sent:
            mine = mine + other.astype(F32)
        return mine

    hidden_strips = strips(rows_low)

    cosine, sine = rope_tables(rows, HEAD)
    cosine = jnp.concatenate([cosine, cosine], axis=1)
    sine = jnp.concatenate([-sine, sine], axis=1)
    gains = (query_gain[None], key_gain[None])
    q_raw, k_raw, queries, keys, values, scales, attn_mix, branch, mid_low = attend(
        length,
        rows_low,
        my_low,
        (query_weight, key_weight, value_weight, output_weight),
        gains,
        cosine,
        sine,
        attn_gain[None],
    )
    mix_all = jnp.concatenate([attn_mix] + grid.ring(attn_mix), axis=0)
    mid_others = shared_ring(grid, mid_low)

    gate = matmul(mid_low, gate_weight)
    upper = matmul(mid_low, up_weight)
    sig = jax.nn.sigmoid(gate)
    inner = (gate * sig * upper).astype(BF16)
    layer, d_mlp, mlp_gain_part, squares = settle(
        length,
        matmul(inner, down_weight).astype(BF16),
        my_low,
        branch,
        grad_in,
        attn_gain[None],
        mlp_gain[None],
    )
    d_mlp_others = shared_ring(grid, d_mlp)

    def inner_back(gate, upper, d_mlp):
        d_inner = right_inner(d_mlp, down_weight)
        sig = jax.nn.sigmoid(gate)
        d_gate = (d_inner * upper * sig * (1.0 + gate * (1.0 - sig))).astype(BF16)
        d_up = (d_inner * gate * sig).astype(BF16)
        return d_gate, d_up

    d_gate, d_up = inner_back(gate, upper, d_mlp)
    d_mid, attn_gain_part, d_branch, d_heads, query_gain_part, key_gain_part = unattend(
        length,
        (right_inner(d_gate, gate_weight) + right_inner(d_up, up_weight)).astype(BF16),
        branch,
        grad_in,
        attn_gain[None],
        output_weight,
        (q_raw, k_raw, queries, keys, values, scales),
        gains,
        cosine,
        sine,
    )
    d_branch_strips = strips(d_branch)
    d_heads_all = jnp.concatenate([d_heads] + grid.ring(d_heads), axis=0)
    layer_out, input_grad = close_layer(
        length,
        inverse,
        (
            right_inner(d_heads[:, :local], query_weight)
            + right_inner(d_heads[:, local : 2 * local], key_weight)
            + right_inner(d_heads[:, 2 * local :], value_weight)
        ).astype(BF16),
        d_mid,
        layer,
    )

    gate_o = matmul(mid_others, gate_weight)
    upper_o = matmul(mid_others, up_weight)
    inner_o = (jax.nn.silu(gate_o) * upper_o).astype(BF16)
    d_gate_o, d_up_o = inner_back(gate_o, upper_o, d_mlp_others)

    def strip_all(own, others):
        return jnp.concatenate([strip_of(own, grid.group), strip_of(others, grid.group)], axis=0)

    mid_strips = strip_all(mid_low, mid_others)
    d_mlp_strips = strip_all(d_mlp, d_mlp_others)
    d_gate_all = jnp.concatenate([d_gate, d_gate_o], axis=0)
    d_up_all = jnp.concatenate([d_up, d_up_o], axis=0)
    inner_all = jnp.concatenate([inner, inner_o], axis=0)
    gate_part = reduced(lambda tile: left_inner(tile, d_gate_all), mid_strips)
    up_part = reduced(lambda tile: left_inner(tile, d_up_all), mid_strips)
    down_part = reduced(lambda tile: left_inner(inner_all, tile), d_mlp_strips)
    output_part = reduced(lambda tile: left_inner(mix_all, tile), d_branch_strips)
    heads_part = reduced(lambda tile: left_inner(tile, d_heads_all), hidden_strips)
    query_part = heads_part[:, :local]
    key_part = heads_part[:, local : 2 * local]
    value_part = heads_part[:, 2 * local :]

    shared = jnp.concatenate(
        [jnp.sum(attn_gain_part, axis=0), jnp.sum(mlp_gain_part, axis=0), jnp.sum(squares, axis=(1, 2))]
    )
    shared = shared + sibling(shared)
    shared = shared + across(shared)
    sums = grid.total(jnp.concatenate([shared, query_gain_part[0], key_gain_part[0]]))
    attn_gain_grad = sums[:width]
    mlp_gain_grad = sums[width : 2 * width]
    squares = sums[2 * width : 2 * width + 3]
    query_gain_grad = sums[2 * width + 3 : 2 * width + 3 + local]
    key_gain_grad = sums[2 * width + 3 + local :]
    rms_values = jnp.sqrt(squares / (jnp.sum(seq_lengths).astype(F32) * D))

    return (
        layer_out[None],
        input_grad[None],
        query_part,
        key_part,
        value_part,
        output_part,
        query_gain_grad,
        key_gain_grad,
        attn_gain_grad,
        gate_part,
        up_part,
        down_part,
        mlp_gain_grad,
        rms_values,
    )


def solution(mesh):
    placed = (
        P("dp", None, None),
        P("dp", None, None),
        P(),
        P(),
        P(None, "tensor"),
        P(None, "tensor"),
        P(None, "tensor"),
        P("tensor", None),
        P("tensor"),
        P("tensor"),
        P(),
        P(None, "tensor"),
        P(None, "tensor"),
        P("tensor", None),
        P(),
    )
    return jax.shard_map(
        body,
        mesh=mesh,
        in_specs=placed,
        out_specs=(
            P("dp", None, None),
            P("dp", None, None),
            P("dp", "tensor"),
            P("dp", "tensor"),
            P("dp", "tensor"),
            P("tensor", "dp"),
            P("tensor"),
            P("tensor"),
            P(),
            P("dp", "tensor"),
            P("dp", "tensor"),
            P("tensor", "dp"),
            P(),
            P(),
        ),
        check_vma=False,
    )
```

```python
import functools
import math
import types

import jax
import jax.numpy as jnp
import numpy as np
from jax import lax
from jax.experimental import pallas as pl
from jax.experimental.pallas import tpu as pltpu
from jax.sharding import PartitionSpec as P

D = 2048
HEAD = 128
EPS = 1e-06
F32 = jnp.float32
BF16 = jnp.bfloat16


def matmul(left, right):
    return jnp.dot(left, right, preferred_element_type=F32)


def left_inner(left, right):
    return lax.dot_general(left, right, (((0,), (0,)), ((), ())), preferred_element_type=F32)


def right_inner(left, right):
    return lax.dot_general(left, right, (((1,), (1,)), ((), ())), preferred_element_type=F32)


def rope_tables(rows, width):
    places = jnp.arange(rows, dtype=F32)
    freq = jnp.power(F32(500000.0), -jnp.arange(width // 2, dtype=F32) * (2.0 / width))
    angle = places[:, None] * freq[None, :]
    return (jnp.cos(angle), jnp.sin(angle))


def rope_constants(rows, width):
    half = width // 2
    exponent = -np.arange(half, dtype=np.float32) * np.float32(2.0 / width)
    freq = np.power(np.float32(500000.0), exponent, dtype=np.float32)
    angle = (np.arange(rows, dtype=np.float32)[:, None] * freq[None, :]).astype(np.float64)
    cosine, sine = np.cos(angle), np.sin(angle)
    return (
        jnp.asarray(np.concatenate([cosine, cosine], axis=1), F32),
        jnp.asarray(np.concatenate([-sine, sine], axis=1), F32),
    )


class Grid:
    def __init__(self, count):
        self.count = count
        self.lanes = 2 ** ((count.bit_length() - 1) // 2)
        self.groups = count // self.lanes
        me = lax.axis_index("dp")
        self.group = me // self.lanes
        self.lane = me % self.lanes

    def shift_groups(self, field, step):
        pairs = [
            (g * self.lanes + a, ((g + step) % self.groups) * self.lanes + a)
            for g in range(self.groups)
            for a in range(self.lanes)
        ]
        return lax.ppermute(field, "dp", pairs)

    def shift_lanes(self, field, step):
        pairs = [
            (g * self.lanes + a, g * self.lanes + (a + step) % self.lanes)
            for g in range(self.groups)
            for a in range(self.lanes)
        ]
        return lax.ppermute(field, "dp", pairs)

    def ring(self, field):
        found = []
        for _ in range(self.groups - 1):
            field = self.shift_groups(field, 1)
            found.append(field)
        return found

    def total(self, field):
        step = 1
        while step < self.count:
            field = field + lax.ppermute(
                field, "dp", [(i, i ^ step) for i in range(self.count)]
            )
            step *= 2
        return field


def sibling(field):
    size = lax.axis_size("tensor")
    return lax.ppermute(field, "tensor", [(i, i ^ 1) for i in range(size)])


def across(field):
    size = lax.axis_size("tensor")
    return lax.ppermute(field, "tensor", [(i, (i + 2) % size) for i in range(size)])


def shared_ring(grid, rows_low):
    core = lax.axis_index("tensor") % 2
    half = rows_low.shape[0] // 2
    mine = lax.dynamic_slice_in_dim(rows_low, core * half, half, axis=0)
    pieces = []
    for piece in grid.ring(mine):
        pieces += [piece, sibling(piece)]
    return jnp.concatenate(pieces, axis=0)


SLOTS = 4
TILES = 4
AT = pl.DeviceIdType.MESH
VMEM_CAP = 56 * 2**20


class Team:
    def __init__(self):
        self.row = lax.axis_index("dp")
        self.me = lax.axis_index("tensor")
        self.side = self.me // 2
        self.core = self.me % 2
        self.slot = self.core * 2 + self.side
        self.sibling = self.side * 2 + (1 - self.core)
        self.across = (1 - self.side) * 2 + self.core
        self.far = (1 - self.side) * 2 + (1 - self.core)

    def meet(self, *others):
        barrier = pltpu.get_barrier_semaphore()
        for other in others:
            pl.semaphore_signal(barrier, inc=1, device_id=(self.row, other), device_id_type=AT)
        pl.semaphore_wait(barrier, len(others))

    def copy(self, source, target, send, recv, other):
        return pltpu.make_async_remote_copy(
            src_ref=source,
            dst_ref=target,
            send_sem=send,
            recv_sem=recv,
            device_id=(self.row, other),
            device_id_type=AT,
        )


def at_rows(start, size):
    return pl.ds(pl.multiple_of(start, size), size)


class Reduce:
    def scratch(rows, width):
        shard = rows // SLOTS
        return [
            pltpu.VMEM((rows, width), BF16),
            pltpu.VMEM((3, shard, width), BF16),
            pltpu.VMEM((shard, width), BF16),
            pltpu.VMEM((shard, width), F32),
            pltpu.SemaphoreType.DMA((3, TILES)),
            pltpu.SemaphoreType.DMA((3, TILES)),
        ]

    def __init__(self, team, partial, came, gone, total, send, recv):
        self.team, self.partial, self.came, self.gone, self.total = team, partial, came, gone, total
        self.shard, width = total.shape
        self.tiles = send.shape[1]
        self.tile = width // self.tiles
        self.send, self.recv = send, recv
        self.copies = {}

    def columns(self, tile):
        return pl.ds(tile * self.tile, self.tile)

    def block(self, core, side):
        return at_rows((core * 2 + side) * self.shard, self.shard)

    def launch(self, kind, tile, source, other):
        copy = self.team.copy(
            source,
            self.came.at[kind, :, self.columns(tile)],
            self.send.at[kind, tile],
            self.recv.at[kind, tile],
            other,
        )
        copy.start()
        self.copies[kind, tile] = copy

    def offer(self, tile):
        team, columns = self.team, self.columns(tile)
        for kind, side in ((0, 1 - team.side), (1, team.side)):
            self.launch(
                kind, tile, self.partial.at[self.block(1 - team.core, side), columns], team.sibling
            )

    def pass_on(self, tile):
        team, columns = self.team, self.columns(tile)
        self.copies[0, tile].wait_recv()
        mine = self.partial[self.block(team.core, 1 - team.side), columns].astype(F32)
        self.gone[:, columns] = (mine + self.came[0, :, columns].astype(F32)).astype(BF16)
        self.launch(2, tile, self.gone.at[:, columns], team.across)

    def finish(self, tile):
        team, columns = self.team, self.columns(tile)
        self.copies[1, tile].wait_recv()
        mine = self.partial[self.block(team.core, team.side), columns].astype(F32)
        mine = mine + self.came[1, :, columns].astype(F32)
        self.copies[2, tile].wait_recv()
        self.total[:, columns] = mine + self.came[2, :, columns].astype(F32)

    def settle(self):
        for copy in self.copies.values():
            copy.wait_send()

    def begin(self, make):
        self.copies = {}
        for tile in range(self.tiles):
            make(self.columns(tile))
            self.offer(tile)
            if tile:
                self.pass_on(tile - 1)
        self.pass_on(self.tiles - 1)

    def end(self):
        for tile in range(self.tiles):
            self.finish(tile)
        self.settle()

    def run(self, make):
        self.begin(make)
        self.end()


class Gather:
    scratch = [pltpu.SemaphoreType.DMA((3,)), pltpu.SemaphoreType.DMA((3,))]

    def __init__(self, team, whole, send, recv):
        self.team, self.whole = team, whole
        shard = whole.shape[0] // SLOTS
        mine = whole.at[at_rows(team.slot * shard, shard)]
        theirs = whole.at[at_rows((team.core * 2 + 1 - team.side) * shard, shard)]
        self.across = team.copy(mine, mine, send.at[0], recv.at[0], team.across)
        self.near = team.copy(mine, mine, send.at[1], recv.at[1], team.sibling)
        self.relay = team.copy(theirs, theirs, send.at[2], recv.at[2], team.sibling)

    def start(self):
        self.across.start()
        self.near.start()

    def half(self):
        self.across.wait_recv()
        self.relay.start()

    def finish(self):
        self.across.wait_send()
        self.near.wait()
        self.relay.wait()


class RowSums:
    def scratch(rows):
        return [
            pltpu.VMEM((8, rows), F32),
            pltpu.VMEM((3, 8, rows), F32),
            pltpu.SemaphoreType.DMA((3,)),
            pltpu.SemaphoreType.DMA((3,)),
        ]

    def __init__(self, team, mine, came, send, recv):
        self.team, self.mine, self.came = team, mine, came
        self.copies = [
            team.copy(mine, came.at[i], send.at[i], recv.at[i], other)
            for i, other in enumerate((team.sibling, team.across, team.far))
        ]

    def start(self, first, second):
        rows = first.shape[0]
        lane = lax.broadcasted_iota(jnp.int32, (rows, 128), 1)
        both = jnp.where(lane == 0, first, jnp.where(lane == 1, second, 0.0))
        self.mine[...] = jnp.transpose(both)[:8]
        for copy in self.copies:
            copy.start()

    def finish(self):
        for copy in self.copies:
            copy.wait()
        total = self.mine[...] + self.came[0] + (self.came[1] + self.came[2])
        rows = total.shape[1]
        wide = jnp.transpose(jnp.concatenate([total] * 16, axis=0))
        return wide[:, 0:1], wide[:, 1:2]


def turn(field, cosine, sine):
    return field * cosine + pltpu.roll(field, HEAD // 2, 1) * sine


def head_probs(queries, keys, length):
    rows = queries.shape[0]
    scores = right_inner(queries, keys) * (1.0 / math.sqrt(HEAD))
    row = lax.broadcasted_iota(jnp.int32, (rows, rows), 0)
    column = lax.broadcasted_iota(jnp.int32, (rows, rows), 1)
    masked = jnp.where((column <= row) & (column < length), scores, -1e30)
    expo = jnp.exp(masked - jnp.max(masked, axis=-1, keepdims=True))
    return expo / jnp.sum(expo, axis=-1, keepdims=True)


def row_sum(field):
    return jnp.sum(field, axis=-1, keepdims=True)


def over_rows(count, step, work):
    def one(i, carry):
        work(pl.ds(pl.multiple_of(i * step, step), step))
        return carry

    lax.fori_loop(0, count // step, one, 0)


def attend_kernel(
    length_ref,
    hidden,
    mine_hidden,
    q_weight,
    k_weight,
    v_weight,
    o_weight,
    q_gain,
    k_gain,
    cosine,
    sine,
    a_gain,
    q_raw,
    k_raw,
    queries,
    keys,
    values,
    scales,
    mix,
    branch,
    mid_low,
    weights,
    out_weight,
    load,
    *scratch,
):
    team = Team()
    sums = RowSums(team, *scratch[0:4])
    reduce = Reduce(team, *scratch[4:10])
    gather = Gather(team, mid_low, *scratch[10:12])
    loads = [
        pltpu.make_async_copy(source, weights.at[i], load.at[i])
        for i, source in enumerate((q_weight, k_weight, v_weight))
    ] + [pltpu.make_async_copy(o_weight, out_weight, load.at[3])]
    for one in loads:
        one.start()
    team.meet(team.sibling, team.across, team.far)
    rows, local = mix.shape
    width = mid_low.shape[1]
    length = length_ref[0]

    def project(i):
        loads[i].wait()
        return matmul(hidden[...], weights[i])

    q = project(0)
    q_raw[...] = q
    k = project(1)
    k_raw[...] = k
    sums.start(row_sum(q * q), row_sum(k * k))
    values[...] = project(2).astype(BF16)
    q_total, k_total = sums.finish()
    q_scale = lax.rsqrt(q_total * (1.0 / D) + EPS)
    k_scale = lax.rsqrt(k_total * (1.0 / D) + EPS)
    lane = lax.broadcasted_iota(jnp.int32, (rows, 128), 1)
    scales[...] = jnp.where(lane == 0, q_scale, k_scale)
    for head in range(local // HEAD):
        at = pl.ds(head * HEAD, HEAD)
        q = turn(q_raw[:, at] * q_scale * q_gain[:, at], cosine[...], sine[...]).astype(BF16)
        k = turn(k_raw[:, at] * k_scale * k_gain[:, at], cosine[...], sine[...]).astype(BF16)
        queries[:, at] = q
        keys[:, at] = k
        probs = head_probs(q, k, length).astype(BF16)
        mix[:, at] = matmul(probs, values[:, at]).astype(BF16)
    loads[3].wait()

    def make(at):
        reduce.partial[:, at] = matmul(mix[...], out_weight[:, at]).astype(BF16)

    reduce.run(make)
    shard = reduce.shard

    def norm(at):
        part = reduce.total[at, :]
        branch[at, :] = part
        unit = part * lax.rsqrt(row_sum(part * part) * (1.0 / D) + EPS)
        mid = mine_hidden[at, :].astype(F32) + a_gain[...] * unit
        whole_at = pl.ds(pl.multiple_of(team.slot * shard + at.start, at.size), at.size)
        mid_low[whole_at, :] = mid.astype(BF16)

    over_rows(shard, 16, norm)
    gather.start()
    gather.half()
    gather.finish()


ANY = pl.BlockSpec(memory_space=pl.ANY)
ON_CHIP = pl.BlockSpec(memory_space=pltpu.VMEM)
SCALAR = pl.BlockSpec(memory_space=pltpu.SMEM)


def shaped(*pairs):
    return tuple(jax.ShapeDtypeStruct(shape, kind) for shape, kind in pairs)


def attend(length, hidden, mine_hidden, weights, gains, cosine, sine, a_gain):
    rows, width = hidden.shape
    local = weights[0].shape[1]
    shard = rows // SLOTS
    return pl.pallas_call(
        attend_kernel,
        out_shape=shaped(
            ((rows, local), F32),
            ((rows, local), F32),
            ((rows, local), BF16),
            ((rows, local), BF16),
            ((rows, local), BF16),
            ((rows, 128), F32),
            ((rows, local), BF16),
            ((shard, width), F32),
            ((rows, width), BF16),
        ),
        in_specs=[SCALAR, ON_CHIP, ON_CHIP] + [ANY] * 4 + [ON_CHIP] * 5,
        out_specs=(ON_CHIP,) * 9,
        scratch_shapes=[
            pltpu.VMEM((3, width, local), BF16),
            pltpu.VMEM((local, width), BF16),
            pltpu.SemaphoreType.DMA((4,)),
        ]
        + RowSums.scratch(rows)
        + Reduce.scratch(rows, width)
        + Gather.scratch,
        compiler_params=pltpu.CompilerParams(
            collective_id=0, has_side_effects=True, vmem_limit_bytes=VMEM_CAP
        ),
        name="attend",
    )(length, hidden, mine_hidden, *weights, *gains, cosine, sine, a_gain)


def settle_kernel(
    length_ref,
    partial_in,
    mine_hidden,
    branch,
    grad_in,
    a_gain,
    m_gain,
    layer,
    d_mlp,
    m_gain_part,
    squares,
    *scratch,
):
    team = Team()
    reduce = Reduce(team, *scratch[0:6])
    gather = Gather(team, d_mlp, *scratch[6:8])
    team.meet(team.sibling, team.across)

    def make(at):
        reduce.partial[:, at] = partial_in[:, at]

    reduce.run(make)
    shard = reduce.shard
    length = length_ref[0]
    m_gain_part[...] = jnp.zeros_like(m_gain_part)
    squares[...] = jnp.zeros_like(squares)

    def folded(field):
        return sum([field[8 * i : 8 * i + 8] for i in range(field.shape[0] // 8)])

    def norm(at):
        part = reduce.total[at, :]
        scale = lax.rsqrt(row_sum(part * part) * (1.0 / D) + EPS)
        unit = part * scale
        base = branch[at, :]
        a_unit = base * lax.rsqrt(row_sum(base * base) * (1.0 / D) + EPS)
        attn_out = a_gain[...] * a_unit
        mlp_out = m_gain[...] * unit
        rows_f = mine_hidden[at, :].astype(F32)
        row = team.slot * shard + at.start + lax.broadcasted_iota(jnp.int32, (at.size, 1), 0)
        live = row < length
        layer[at, :] = jnp.where(live, rows_f + attn_out + mlp_out, 0.0).astype(BF16)
        grad = jnp.where(live, grad_in[at, :].astype(F32), 0.0)
        m_gain_part[...] += folded(grad * unit)
        for i, field in enumerate((rows_f, attn_out, mlp_out)):
            squares[i] += folded(jnp.where(live, field * field, 0.0))
        scaled = grad * m_gain[...]
        back = scale * (scaled - unit * (row_sum(scaled * unit) * (1.0 / D)))
        whole_at = pl.ds(pl.multiple_of(team.slot * shard + at.start, at.size), at.size)
        d_mlp[whole_at, :] = back.astype(BF16)

    over_rows(shard, 16, norm)
    gather.start()
    gather.half()
    gather.finish()


def settle(length, partial, mine_hidden, branch, grad_in, a_gain, m_gain):
    rows, width = partial.shape
    shard = rows // SLOTS
    return pl.pallas_call(
        settle_kernel,
        out_shape=shaped(
            ((shard, width), BF16),
            ((rows, width), BF16),
            ((8, width), F32),
            ((3, 8, width), F32),
        ),
        in_specs=[SCALAR] + [ON_CHIP] * 6,
        out_specs=(ON_CHIP,) * 4,
        scratch_shapes=Reduce.scratch(rows, width) + Gather.scratch,
        compiler_params=pltpu.CompilerParams(
            collective_id=1, has_side_effects=True, vmem_limit_bytes=VMEM_CAP
        ),
        name="settle",
    )(length, partial, mine_hidden, branch, grad_in, a_gain, m_gain)


def unattend_kernel(
    length_ref,
    partial_in,
    branch,
    grad_in,
    a_gain,
    o_weight,
    q_raw,
    k_raw,
    queries,
    keys,
    values,
    scales,
    q_gain,
    k_gain,
    cosine,
    sine,
    d_mid,
    a_gain_part,
    d_branch,
    d_heads,
    q_gain_part,
    k_gain_part,
    out_weight,
    d_mix,
    d_q,
    d_k,
    load,
    *scratch,
):
    team = Team()
    sums = RowSums(team, *scratch[0:4])
    reduce = Reduce(team, *scratch[4:10])
    gather = Gather(team, d_branch, *scratch[10:12])
    fetch = pltpu.make_async_copy(o_weight, out_weight, load.at[0])
    fetch.start()
    team.meet(team.sibling, team.across, team.far)
    rows, local = queries.shape

    def make(at):
        reduce.partial[:, at] = partial_in[:, at]

    reduce.run(make)
    shard = reduce.shard
    length = length_ref[0]
    a_gain_part[...] = jnp.zeros_like(a_gain_part)

    def norm(at):
        row = team.slot * shard + at.start + lax.broadcasted_iota(jnp.int32, (at.size, 1), 0)
        grad = jnp.where(row < length, grad_in[at, :].astype(F32), 0.0) + reduce.total[at, :]
        d_mid[at, :] = grad
        base = branch[at, :]
        scale = lax.rsqrt(row_sum(base * base) * (1.0 / D) + EPS)
        unit = base * scale
        product = grad * unit
        a_gain_part[...] += sum([product[8 * i : 8 * i + 8] for i in range(at.size // 8)])
        scaled = grad * a_gain[...]
        back = scale * (scaled - unit * (row_sum(scaled * unit) * (1.0 / D)))
        whole_at = pl.ds(pl.multiple_of(team.slot * shard + at.start, at.size), at.size)
        d_branch[whole_at, :] = back.astype(BF16)

    over_rows(shard, 16, norm)
    gather.start()
    gather.half()
    gather.finish()
    fetch.wait()
    d_mix[...] = right_inner(d_branch[...], out_weight[...]).astype(BF16)
    q_scale = scales[:, 0:1]
    k_scale = scales[:, 1:2]
    q_inner = jnp.zeros((rows, 1), F32)
    k_inner = jnp.zeros((rows, 1), F32)
    shrink = 1.0 / math.sqrt(HEAD)
    for head in range(local // HEAD):
        at = pl.ds(head * HEAD, HEAD)
        q, k, v, back = queries[:, at], keys[:, at], values[:, at], d_mix[:, at]
        probs = head_probs(q, k, length)
        d_probs = right_inner(back, v)
        d_scores = (probs * (d_probs - row_sum(probs * d_probs))).astype(BF16)
        d_heads[:, pl.ds(2 * local + head * HEAD, HEAD)] = left_inner(
            probs.astype(BF16), back
        ).astype(BF16)
        d_q_hat = turn(matmul(d_scores, k) * shrink, cosine[...], -sine[...])
        d_k_hat = turn(left_inner(d_scores, q) * shrink, cosine[...], -sine[...])
        q_unit = q_raw[:, at] * q_scale
        k_unit = k_raw[:, at] * k_scale
        q_gain_part[:, at] = jnp.sum(d_q_hat * q_unit, axis=0, keepdims=True)
        k_gain_part[:, at] = jnp.sum(d_k_hat * k_unit, axis=0, keepdims=True)
        q_scaled = d_q_hat * q_gain[:, at]
        k_scaled = d_k_hat * k_gain[:, at]
        d_q[:, at] = q_scaled
        d_k[:, at] = k_scaled
        q_inner += row_sum(q_scaled * q_unit)
        k_inner += row_sum(k_scaled * k_unit)
    sums.start(q_inner, k_inner)
    q_inner, k_inner = sums.finish()
    for i, (grad, raw, scale, inner) in enumerate(
        ((d_q, q_raw, q_scale, q_inner), (d_k, k_raw, k_scale, k_inner))
    ):
        factor = scale * scale * inner * (1.0 / D)
        d_heads[:, pl.ds(i * local, local)] = (scale * grad[...] - raw[...] * factor).astype(BF16)


def unattend(
    length, partial, branch, grad_in, a_gain, o_weight, kept, gains, cosine, sine
):
    rows, width = partial.shape
    local = o_weight.shape[0]
    shard = rows // SLOTS
    return pl.pallas_call(
        unattend_kernel,
        out_shape=shaped(
            ((shard, width), F32),
            ((8, width), F32),
            ((rows, width), BF16),
            ((rows, 3 * local), BF16),
            ((1, local), F32),
            ((1, local), F32),
        ),
        in_specs=[SCALAR] + [ON_CHIP] * 4 + [ANY] + [ON_CHIP] * 10,
        out_specs=(ON_CHIP,) * 6,
        scratch_shapes=[
            pltpu.VMEM((local, width), BF16),
            pltpu.VMEM((rows, local), BF16),
            pltpu.VMEM((rows, local), F32),
            pltpu.VMEM((rows, local), F32),
            pltpu.SemaphoreType.DMA((1,)),
        ]
        + RowSums.scratch(rows)
        + Reduce.scratch(rows, width)
        + Gather.scratch,
        compiler_params=pltpu.CompilerParams(
            collective_id=2, has_side_effects=True, vmem_limit_bytes=VMEM_CAP
        ),
        name="unattend",
    )(length, partial, branch, grad_in, a_gain, o_weight, *kept, *gains, cosine, sine)


class Deal:
    def __init__(self, count, shard, width):
        self.count = count
        self.columns = max(128, width // count)
        self.across = width // self.columns
        self.rows = shard * self.across // count

    def at(self, chunk, base=0):
        return (
            at_rows(base + (chunk // self.across) * self.rows, self.rows),
            at_rows((chunk % self.across) * self.columns, self.columns),
        )


def finish_kernel(
    length_ref,
    inverse,
    partial_in,
    d_mid,
    layer,
    layer_out,
    input_grad,
    closed,
    parked,
    leaving,
    deal_send,
    deal_recv,
    *scratch,
):
    team = Team()
    reduce = Reduce(team, *scratch[0:6])
    gathers = [
        Gather(team, whole, *scratch[6 + 2 * i : 8 + 2 * i])
        for i, whole in enumerate((layer_out, input_grad))
    ]
    count = lax.axis_size("dp")
    shard, width = d_mid.shape
    deal = Deal(count, shard, width)
    barrier = pltpu.get_barrier_semaphore()
    for step in range(1, count):
        pl.semaphore_signal(
            barrier, inc=1, device_id=(lax.rem(team.row + step, count), team.me), device_id_type=AT
        )
    for other in (team.sibling, team.across):
        pl.semaphore_signal(barrier, inc=1, device_id=(team.row, other), device_id_type=AT)
    pl.semaphore_wait(barrier, count + 1)

    def make(at):
        reduce.partial[:, at] = partial_in[:, at]

    reduce.run(make)
    length = length_ref[0]

    def close(at):
        row = team.slot * shard + at.start + lax.broadcasted_iota(jnp.int32, (at.size, 1), 0)
        closed[at, :] = jnp.where(row < length, reduce.total[at, :] + d_mid[at, :], 0.0).astype(BF16)

    over_rows(shard, 16, close)

    def send(phase, step, i, source, target):
        return pltpu.make_async_remote_copy(
            src_ref=source,
            dst_ref=target,
            send_sem=deal_send.at[phase, step, i],
            recv_sem=deal_recv.at[phase, step, i],
            device_id=(lax.rem(team.row + step, count), team.me),
            device_id_type=AT,
        )

    first = []
    for i, source in enumerate((layer, closed)):
        for step in range(1, count):
            other = lax.rem(team.row + step, count)
            copy = send(0, step, i, source.at[deal.at(other)], parked.at[team.row, i])
            copy.start()
            first.append(copy)
        parked[team.row, i] = source[deal.at(team.row)]
    for copy in first:
        copy.wait()
    mine = team.slot * shard
    second = []
    for i, target in enumerate((layer_out, input_grad)):
        for step in range(1, count):
            other = lax.rem(team.row + step, count)
            leaving[other, i] = parked[inverse[other], i]
            copy = send(1, step, i, leaving.at[other, i], target.at[deal.at(team.row, mine)])
            copy.start()
            second.append(copy)
        target[deal.at(team.row, mine)] = parked[inverse[team.row], i]
    for copy in second:
        copy.wait()
    for gather in gathers:
        gather.start()
    for gather in gathers:
        gather.half()
    for gather in gathers:
        gather.finish()


def close_layer(length, inverse, partial, d_mid, layer):
    rows, width = partial.shape
    shard = rows // SLOTS
    count = lax.axis_size("dp")
    deal = Deal(count, shard, width)
    chunk = (count, 2, deal.rows, deal.columns)
    return pl.pallas_call(
        finish_kernel,
        out_shape=shaped(((rows, width), BF16), ((rows, width), BF16)),
        in_specs=[SCALAR, SCALAR] + [ON_CHIP] * 3,
        out_specs=(ON_CHIP,) * 2,
        scratch_shapes=[
            pltpu.VMEM((shard, width), BF16),
            pltpu.VMEM(chunk, BF16),
            pltpu.VMEM(chunk, BF16),
            pltpu.SemaphoreType.DMA((2, count, 2)),
            pltpu.SemaphoreType.DMA((2, count, 2)),
        ]
        + Reduce.scratch(rows, width)
        + Gather.scratch * 2,
        compiler_params=pltpu.CompilerParams(
            collective_id=3, has_side_effects=True, vmem_limit_bytes=VMEM_CAP
        ),
        name="close_layer",
    )(length, inverse, partial, d_mid, layer)


SPLIT = 4
PACKED = 768
STEP = 256


class Wires:
    def __init__(self, send, recv):
        self.send, self.recv, self.used = send, recv, 0

    def book(self, number=1):
        self.used += number
        assert self.used <= self.send.shape[0]
        return self.used - number

    def copy(self, source, target, device, index):
        return pltpu.make_async_remote_copy(
            src_ref=source,
            dst_ref=target,
            send_sem=self.send.at[index],
            recv_sem=self.recv.at[index],
            device_id=device,
            device_id_type=AT,
        )


class Spread:
    def __init__(self, wires, grid, team, source, field):
        shard = source.shape[0] // SLOTS
        mine = at_rows(team.slot * shard, shard)
        half = at_rows(team.core * 2 * shard, 2 * shard)
        self.hops, self.sides, self.pairs = {}, {}, {}
        for step in range(1, grid.groups):
            group = lax.rem(grid.group + step, grid.groups)
            block = field.at[step]
            self.hops[step] = wires.copy(
                source.at[mine],
                block.at[mine],
                (group * grid.lanes + grid.lane, team.me),
                wires.book(),
            )
            self.sides[step] = wires.copy(
                block.at[mine], block.at[mine], (team.row, team.across), wires.book()
            )
            self.pairs[step] = wires.copy(
                block.at[half], block.at[half], (team.row, team.sibling), wires.book()
            )
        near = sorted(self.hops, key=lambda step: min(step, grid.groups - step))
        self.plan = {"hop": list(near), "side": list(near), "pair": list(near)}

    def start(self):
        for step in self.plan["hop"]:
            self.hops[step].start()

    def side(self, number=1):
        for step in self.plan["side"][:number]:
            self.hops[step].wait_recv()
            self.sides[step].start()
        del self.plan["side"][:number]

    def pair(self, number=1):
        for step in self.plan["pair"][:number]:
            self.sides[step].wait_recv()
            self.pairs[step].start()
        del self.plan["pair"][:number]

    def drain(self):
        self.side(len(self.hops))
        self.pair(len(self.hops))
        for step in self.hops:
            self.hops[step].wait_send()
            self.sides[step].wait_send()
            self.pairs[step].wait()


def silu_parts(gate, upper):
    sig = jax.nn.sigmoid(gate)
    return sig, (gate * sig * upper).astype(BF16)


def silu_back(gate, upper, sig, d_inner):
    d_gate = (d_inner * upper * sig * (1.0 + gate * (1.0 - sig))).astype(BF16)
    return d_gate, (d_inner * gate * sig).astype(BF16)


def head_back(q, k, v, back, cosine, sine, length):
    probs = head_probs(q, k, length)
    low = probs.astype(BF16)
    mix = matmul(low, v).astype(BF16)
    d_probs = right_inner(back, v)
    d_scores = (probs * (d_probs - row_sum(probs * d_probs))).astype(BF16)
    shrink = 1.0 / math.sqrt(HEAD)
    return (
        mix,
        left_inner(low, back).astype(BF16),
        turn(matmul(d_scores, k) * shrink, cosine, -sine),
        turn(left_inner(d_scores, q) * shrink, cosine, -sine),
    )


def folded(field):
    return sum([field[8 * i : 8 * i + 8] for i in range(field.shape[0] // 8)])


def layer_kernel(names, *refs):
    m = types.SimpleNamespace(**dict(zip(names, refs, strict=True)))
    team, grid = Team(), Grid(lax.axis_size("dp"))
    wires = Wires(m.wire_send, m.wire_recv)
    count, groups, lanes = grid.count, grid.groups, grid.lanes
    rows, width = m.hid.shape
    local, hidden = m.mix.shape[1], m.gate.shape[1]
    shard, strip, tile = rows // SLOTS, width // groups, width // count
    every = groups * rows
    me = team.row

    loads = {}

    def load(name, source, target):
        loads[name] = pltpu.make_async_copy(source, target, m.load.at[len(loads)])
        loads[name].start()

    load("hid", m.hidden_in, m.hid)
    load("q", m.q_weight, m.qkv.at[0])
    load("k", m.k_weight, m.qkv.at[1])
    load("v", m.v_weight, m.qkv.at[2])
    load("grad", m.upstream.at[at_rows(team.slot * shard, shard)], m.closed)
    load("o", m.o_weight, m.wo)
    load("g", m.g_weight, m.wg)
    load("u", m.u_weight, m.wu)
    load("d", m.d_weight, m.wd)

    def peer(step):
        return lax.rem(me + step, count)

    barrier = pltpu.get_barrier_semaphore()
    for step in range(1, count):
        pl.semaphore_signal(barrier, inc=1, device_id=(peer(step), team.me), device_id_type=AT)
    for other in (team.sibling, team.across, team.far):
        pl.semaphore_signal(barrier, inc=1, device_id=(me, other), device_id_type=AT)
    pl.semaphore_wait(barrier, count + 2)

    length = m.lengths[m.order[me]]

    def holder(sequence):
        found = jnp.int32(0)
        for place in range(count):
            found = jnp.where(m.order[place] == sequence, place, found)
        return found

    following = (lax.rem(grid.group + 1, groups) * lanes + grid.lane, team.me)
    sums = RowSums(team, m.sum_mine, m.sum_came, m.sum_send, m.sum_recv)
    deal = Deal(count, shard, width)

    class Return:
        def __init__(self, lot, source, target):
            self.lot, self.source = lot, source
            self.room = (m.parked, m.parked_too)[lot]
            start = wires.book(2 * count)
            self.parked = [
                wires.copy(
                    source.at[deal.at(peer(step))],
                    self.room.at[me],
                    (peer(step), team.me),
                    start + step,
                )
                for step in range(1, count)
            ]
            goal = target.at[deal.at(me, team.slot * shard)]
            self.placed = [
                wires.copy(
                    m.back_leaving.at[peer(step), lot],
                    goal,
                    (peer(step), team.me),
                    start + count + step,
                )
                for step in range(1, count)
            ]
            self.placed.append(
                pltpu.make_async_copy(m.back_leaving.at[me, lot], goal, m.put.at[lot])
            )
            self.holders = [holder(peer(step)) for step in range(count)]

        def park(self):
            for copy in self.parked:
                copy.start()
            self.room[me] = self.source[deal.at(me)]

        def place(self):
            for copy in self.parked:
                copy.wait()
            for step in range(count):
                m.back_leaving[peer(step), self.lot] = self.room[self.holders[step]]
            for copy in self.placed:
                copy.start()

        def wait(self):
            for copy in self.placed:
                copy.wait()

    loads["grad"].wait()
    dealt = wires.book(2 * count)
    first = []
    for step in range(1, count):
        copy = wires.copy(
            m.closed.at[deal.at(peer(step))],
            m.parked.at[me],
            (peer(step), team.me),
            dealt + step,
        )
        copy.start()
        first.append(copy)
    m.parked[me] = m.closed[deal.at(me)]

    loads["hid"].wait()

    loads["q"].wait()
    q = matmul(m.hid[...], m.qkv[0])
    m.q_raw[...] = q
    loads["k"].wait()
    k = matmul(m.hid[...], m.qkv[1])
    m.k_raw[...] = k
    sums.start(row_sum(q * q), row_sum(k * k))
    loads["v"].wait()
    m.values[...] = matmul(m.hid[...], m.qkv[2]).astype(BF16)
    q_total, k_total = sums.finish()
    q_scale = lax.rsqrt(q_total * (1.0 / D) + EPS)
    k_scale = lax.rsqrt(k_total * (1.0 / D) + EPS)
    lane = lax.broadcasted_iota(jnp.int32, (rows, 128), 1)
    m.scales[...] = jnp.where(lane == 0, q_scale, k_scale)

    def attend_head(head, carry):
        at = at_rows(head * HEAD, HEAD)
        q = turn(m.q_raw[:, at] * q_scale * m.q_gain[:, at], m.cosine[...], m.sine[...]).astype(BF16)
        k = turn(m.k_raw[:, at] * k_scale * m.k_gain[:, at], m.cosine[...], m.sine[...]).astype(BF16)
        m.queries[:, at] = q
        m.keys[:, at] = k
        probs = head_probs(q, k, length).astype(BF16)
        m.mix[:, at] = matmul(probs, m.values[:, at]).astype(BF16)
        return carry

    lax.fori_loop(0, local // HEAD, attend_head, 0)

    for copy in first:
        copy.wait()
    for step in range(1, count):
        m.back_leaving[peer(step), 0] = m.parked[m.order[peer(step)]]
    m.grad_in[deal.at(me)] = m.parked[m.order[me]]
    second = []
    for step in range(1, count):
        copy = wires.copy(
            m.back_leaving.at[peer(step), 0],
            m.grad_in.at[deal.at(me)],
            (peer(step), team.me),
            dealt + count + step,
        )
        copy.start()
        second.append(copy)

    reduce = Reduce(
        team, m.partial, m.came, m.gone, m.total, m.reduce_send, m.reduce_recv
    )

    def gather(whole, number):
        return Gather(team, whole, m.gather_send.at[number], m.gather_recv.at[number])

    loads["o"].wait()

    def make_branch(at):
        m.partial[:, at] = matmul(m.mix[...], m.wo[:, at]).astype(BF16)

    reduce.run(make_branch)
    own = m.mid_all.at[0]

    def whole_at(at):
        return pl.ds(pl.multiple_of(team.slot * shard + at.start, at.size), at.size)

    def norm_mid(at):
        part = m.total[at, :]
        m.branch[at, :] = part
        unit = part * lax.rsqrt(row_sum(part * part) * (1.0 / D) + EPS)
        mid = m.hid[whole_at(at), :].astype(F32) + m.a_gain[...] * unit
        m.mid_all[0, whole_at(at), :] = mid.astype(BF16)

    over_rows(shard, 16, norm_mid)
    mid_gather = gather(own, 0)
    mid_gather.start()
    mid_spread = Spread(wires, grid, team, own, m.mid_all)
    mid_spread.start()
    mid_gather.half()
    mid_gather.finish()
    loads["g"].wait()
    loads["u"].wait()

    def widen(i, carry):
        at = at_rows(i * STEP, STEP)
        gate = matmul(m.mid_all[0], m.wg[:, at])
        upper = matmul(m.mid_all[0], m.wu[:, at])
        m.gate[:, at] = gate.astype(BF16)
        m.upper[:, at] = upper.astype(BF16)
        m.inner[:, at] = silu_parts(gate, upper)[1]
        return carry

    lax.fori_loop(0, hidden // STEP, widen, 0)
    loads["d"].wait()

    def make_mlp(at):
        m.partial[:, at] = matmul(m.inner[...], m.wd[:, at]).astype(BF16)

    for copy in second:
        copy.wait()
    reduce.run(make_mlp)
    m.stats[...] = jnp.zeros_like(m.stats)
    m.fold[...] = jnp.zeros_like(m.fold)

    def norm_mlp(at):
        part = m.total[at, :]
        scale = lax.rsqrt(row_sum(part * part) * (1.0 / D) + EPS)
        unit = part * scale
        base = m.branch[at, :]
        a_unit = base * lax.rsqrt(row_sum(base * base) * (1.0 / D) + EPS)
        attn_out = m.a_gain[...] * a_unit
        mlp_out = m.m_gain[...] * unit
        rows_f = m.hid[whole_at(at), :].astype(F32)
        row = team.slot * shard + at.start + lax.broadcasted_iota(jnp.int32, (at.size, 1), 0)
        live = row < length
        m.layer[at, :] = jnp.where(live, rows_f + attn_out + mlp_out, 0.0).astype(BF16)
        grad = jnp.where(live, m.grad_in[at, :].astype(F32), 0.0)
        m.fold[0] += folded(grad * unit)
        for i, field in enumerate((rows_f, attn_out, mlp_out)):
            m.fold[i + 1] += folded(jnp.where(live, field * field, 0.0))
        scaled = grad * m.m_gain[...]
        back = scale * (scaled - unit * (row_sum(scaled * unit) * (1.0 / D)))
        m.dm_all[0, whole_at(at), :] = back.astype(BF16)

    over_rows(shard, 16, norm_mlp)
    own_back = m.dm_all.at[0]
    dm_gather = gather(own_back, 1)
    dm_gather.start()
    dm_spread = Spread(wires, grid, team, own_back, m.dm_all)
    dm_spread.start()
    layer_return = Return(1, m.layer, m.layer_out)
    layer_return.park()
    dm_gather.half()
    m.stats[0:1, :] = jnp.sum(m.fold[0], axis=0, keepdims=True)
    for i in range(3):
        m.stats[3 + i : 4 + i, :] = jnp.sum(m.fold[i + 1], axis=0, keepdims=True)
    dm_gather.finish()
    mid_spread.side(groups)
    hid_spread = Spread(wires, grid, team, m.hid, m.hid_all)
    hid_spread.start()

    def narrow(i, carry):
        at = at_rows(i * STEP, STEP)
        d_inner = right_inner(m.dm_all[0], m.wd[at, :])
        gate = m.gate[:, at].astype(F32)
        upper = m.upper[:, at].astype(F32)
        m.gate[:, at], m.upper[:, at] = silu_back(gate, upper, jax.nn.sigmoid(gate), d_inner)
        return carry

    lax.fori_loop(0, hidden // STEP, narrow, 0)

    def make_d_mid(at):
        m.partial[:, at] = (
            right_inner(m.gate[...], m.wg[at, :]) + right_inner(m.upper[...], m.wu[at, :])
        ).astype(BF16)

    reduce.begin(make_d_mid)
    dm_spread.side(1)
    reduce.end()
    m.fold[0] = jnp.zeros_like(m.fold[0])

    def norm_d_mid(at):
        row = team.slot * shard + at.start + lax.broadcasted_iota(jnp.int32, (at.size, 1), 0)
        grad = jnp.where(row < length, m.grad_in[at, :].astype(F32), 0.0) + m.total[at, :]
        m.d_mid[at, :] = grad
        base = m.branch[at, :]
        scale = lax.rsqrt(row_sum(base * base) * (1.0 / D) + EPS)
        unit = base * scale
        m.fold[0] += folded(grad * unit)
        scaled = grad * m.a_gain[...]
        back = scale * (scaled - unit * (row_sum(scaled * unit) * (1.0 / D)))
        m.d_branch[whole_at(at), :] = back.astype(BF16)

    over_rows(shard, 16, norm_d_mid)
    d_gather = gather(m.d_branch, 2)
    d_gather.start()
    dm_spread.side(1)
    m.stats[1:2, :] = jnp.sum(m.fold[0], axis=0, keepdims=True)
    d_gather.half()
    d_gather.finish()
    dm_spread.side(groups)
    mid_spread.pair(groups)
    branch_spread = Spread(wires, grid, team, m.d_branch, m.branch_all)
    branch_spread.start()

    d_mix = m.partial.at[:, pl.ds(0, local)]
    d_mix[...] = right_inner(m.d_branch[...], m.wo[...]).astype(BF16)
    q_inner = jnp.zeros((rows, 1), F32)
    k_inner = jnp.zeros((rows, 1), F32)
    q_scale = m.scales[:, 0:1]
    k_scale = m.scales[:, 1:2]

    def unattend_head(head, carry):
        at = at_rows(head * HEAD, HEAD)
        _, d_v, d_q_hat, d_k_hat = head_back(
            m.queries[:, at],
            m.keys[:, at],
            m.values[:, at],
            d_mix[:, at],
            m.cosine[...],
            m.sine[...],
            length,
        )
        m.d_heads[:, at_rows(2 * local + head * HEAD, HEAD)] = d_v
        q_unit = m.q_raw[:, at] * q_scale
        k_unit = m.k_raw[:, at] * k_scale
        m.stats[2:3, at] = jnp.sum(d_q_hat * q_unit, axis=0, keepdims=True)
        m.stats[2:3, at_rows(local + head * HEAD, HEAD)] = jnp.sum(
            d_k_hat * k_unit, axis=0, keepdims=True
        )
        q_scaled = d_q_hat * m.q_gain[:, at]
        k_scaled = d_k_hat * m.k_gain[:, at]
        m.stage[0, :, at] = q_scaled
        m.stage[1, :, at] = k_scaled
        return carry[0] + row_sum(q_scaled * q_unit), carry[1] + row_sum(k_scaled * k_unit)

    q_inner, k_inner = lax.fori_loop(0, local // HEAD, unattend_head, (q_inner, k_inner))
    sums.start(q_inner, k_inner)
    q_inner, k_inner = sums.finish()
    for i, (raw, scale, inner) in enumerate(
        ((m.q_raw, q_scale, q_inner), (m.k_raw, k_scale, k_inner))
    ):
        factor = scale * scale * inner * (1.0 / D)
        m.d_heads[:, pl.ds(i * local, local)] = (
            scale * m.stage[i] - raw[...] * factor
        ).astype(BF16)
    m.stat_team[team.me] = m.stats[...]
    stat_at = wires.book(3 + count)
    stat_team = [
        wires.copy(m.stats, m.stat_team.at[team.me], (me, other), stat_at + i)
        for i, other in enumerate((team.sibling, team.across, team.far))
    ]
    for copy in stat_team:
        copy.start()

    layer_return.place()

    def make_input(at):
        m.partial[:, at] = (
            right_inner(m.d_heads[:, 0:local], m.qkv[0, at, :])
            + right_inner(m.d_heads[:, local : 2 * local], m.qkv[1, at, :])
            + right_inner(m.d_heads[:, 2 * local : 3 * local], m.qkv[2, at, :])
        ).astype(BF16)

    mid_spread.drain()
    dm_spread.drain()
    for k in range(groups):
        m.mid_turned[:, pl.ds(k * rows, rows)] = jnp.transpose(
            m.mid_all[k, :, at_rows(grid.group * strip, strip)]
        )
    crossed = wires.book(3 * (hidden // STEP))
    crossing = (grid.group * lanes + (1 - grid.lane), team.me)

    def tile_of(lane):
        return at_rows((grid.group * lanes + lane) * tile, tile)

    def all_rows(field, columns):
        block = field[:, :, columns]
        return block.reshape(every, block.shape[2])

    def crossings(n):
        at = at_rows(n * STEP, STEP)
        spare = pl.ds(every, tile)
        return [
            wires.copy(m.wg.at[spare, at], m.x_gate.at[:, at], crossing, crossed + 3 * n),
            wires.copy(m.wu.at[spare, at], m.x_up.at[:, at], crossing, crossed + 3 * n + 1),
            wires.copy(m.wd.at[at, spare], m.x_down.at[at, :], crossing, crossed + 3 * n + 2),
        ]

    def again(n, carry):
        at = at_rows(n * STEP, STEP)

        def block_again(k, carry):
            gate = matmul(m.mid_all[k], m.wg[:, at])
            upper = matmul(m.mid_all[k], m.wu[:, at])
            d_inner = right_inner(m.dm_all[k], m.wd[at, :])
            sig, inner = silu_parts(gate, upper)
            kept = at_rows((k - 1) * rows, rows)
            m.keep[0, kept, :] = inner
            m.keep[1, kept, :], m.keep[2, kept, :] = silu_back(gate, upper, sig, d_inner)
            return carry

        lax.fori_loop(1, groups, block_again, 0)
        whole = pl.ds(rows, every - rows)
        m.wg[0:rows, at] = m.gate[:, at]
        m.wu[0:rows, at] = m.upper[:, at]
        m.wd[at, 0:rows] = jnp.transpose(m.inner[:, at])
        m.wg[whole, at] = m.keep[1]
        m.wu[whole, at] = m.keep[2]
        for k in range(1, groups):
            kept = pl.ds((k - 1) * rows, rows)
            m.wd[at, pl.ds(k * rows, rows)] = jnp.transpose(m.keep[0, kept, :])
        turned = m.mid_turned[at_rows((1 - grid.lane) * tile, tile), :]
        spare = pl.ds(every, tile)
        m.wg[spare, at] = matmul(turned, m.wg[0:every, at]).astype(BF16)
        m.wu[spare, at] = matmul(turned, m.wu[0:every, at]).astype(BF16)
        m.wd[at, spare] = matmul(m.wd[at, 0:every], all_rows(m.dm_all, tile_of(1 - grid.lane))).astype(BF16)
        for copy in crossings(n):
            copy.start()
        return carry

    def again_with_events(n, carry):
        again(n, carry)
        for place, event in events.items():
            pl.when(n == place)(event)
        return carry

    tiles = hidden // STEP
    stat_dp = [
        wires.copy(m.pack, m.stat_dp.at[me], (peer(step), team.me), stat_at + 2 + step)
        for step in range(1, count)
    ]
    grad_return = Return(0, m.closed, m.input_grad)
    out_gathers = [gather(m.layer_out, 3), gather(m.input_grad, 4)]

    def add_stats():
        for copy in stat_team:
            copy.wait()
        total = (m.stat_team[0] + m.stat_team[1]) + (m.stat_team[2] + m.stat_team[3])
        line = lax.broadcasted_iota(jnp.int32, total.shape, 0)
        total = jnp.where(line == 2, m.stats[...], total)
        m.pack[...] = jnp.zeros_like(m.pack)
        packed = m.pack.shape[1]
        for i in range(2):
            for j in range(pl.cdiv(width, packed)):
                piece = total[i : i + 1, j * packed : min((j + 1) * packed, width)]
                m.pack[3 * i + j : 3 * i + j + 1, 0 : piece.shape[1]] = piece
        m.pack[6:7, :] = total[2:3, 0:packed]
        m.pack[7:8, 0 : 2 * local - packed] = total[2:3, packed : 2 * local]
        for i in range(3):
            square = jnp.sum(total[3 + i : 4 + i, :], axis=1, keepdims=True)
            m.pack[7:8, 2 * local - packed + i * 128 : 2 * local - packed + (i + 1) * 128] = (
                jnp.broadcast_to(square, (1, 128))
            )
        m.stat_dp[me] = m.pack[...]
        for copy in stat_dp:
            copy.start()

    def close(at):
        row = team.slot * shard + at.start + lax.broadcasted_iota(jnp.int32, (at.size, 1), 0)
        m.closed[at, :] = jnp.where(row < length, m.total[at, :] + m.d_mid[at, :], 0.0).astype(BF16)

    def park():
        reduce.end()
        over_rows(shard, 16, close)
        grad_return.park()

    def share():
        layer_return.wait()
        grad_return.wait()
        for one in out_gathers:
            one.start()

    events = {
        2: park,
        tiles - 5: lambda: hid_spread.pair(2),
        tiles - 4: lambda: hid_spread.pair(groups),
        tiles - 3: lambda: branch_spread.side(2),
        tiles - 2: lambda: branch_spread.side(groups),
    }
    lax.fori_loop(0, 1, again, 0)
    reduce.begin(make_input)
    hid_spread.side(groups)
    add_stats()
    lax.fori_loop(1, tiles, again_with_events, 0)
    hid_spread.drain()
    def put(source, target, index):
        return pltpu.make_async_copy(source, target, m.put.at[index])

    puts = []

    def store(value, target):
        slot = len(puts) % 2
        if len(puts) >= 2:
            puts[-2].wait()
        stage = m.stage.at[slot, pl.ds(0, value.shape[0]), pl.ds(0, value.shape[1])]
        stage[...] = value
        puts.append(put(stage, target, 2 + slot))
        puts[-1].start()

    late = []

    def bring(source, target):
        copy = pltpu.make_async_copy(source, target, m.late.at[len(late)])
        copy.start()
        late.append(copy)

    for k in range(1, groups):
        bring(m.hid_all.at[k], m.mid_all.at[k])
    for copy in late:
        copy.wait()
    for k in range(groups):
        source = m.mid_all.at[k] if k else m.hid
        for lane in range(lanes):
            m.gate[:, pl.ds(lane * every + k * rows, rows)] = jnp.transpose(
                source[:, at_rows(grid.group * strip + lane * tile, tile)]
            )
    wide_sums = RowSums(
        team, m.wide_mine, m.wide_came.at[0], m.wide_send.at[0], m.wide_recv.at[0]
    )
    spare_rows = every + tile

    def project_again(k, carry):
        block = at_rows(spare_rows + (k - 1) * rows, rows)
        lane = lax.broadcasted_iota(jnp.int32, (rows, 128), 1)
        found = jnp.zeros((rows, 128), F32)
        for i in range(2):
            raw = matmul(m.mid_all[k], m.qkv[i])
            m.wu[block, pl.ds(2 * local + i * local, local)] = raw.astype(BF16)
            found = jnp.where(lane == i, row_sum(raw * raw), found)
        m.wide_inner[at_rows((k - 1) * rows, rows), :] = found
        m.wu[block, pl.ds(local, local)] = matmul(m.mid_all[k], m.qkv[2]).astype(BF16)
        return carry

    lax.fori_loop(1, groups, project_again, 0)
    wide_sums.start(m.wide_inner[:, 0:1], m.wide_inner[:, 1:2])
    branch_spread.pair(groups)
    grad_return.place()
    branch_spread.drain()
    for k in range(1, groups):
        bring(m.branch_all.at[k], m.mid_all.at[k])
    for copy in late[groups - 1 :]:
        copy.wait()
    q_total, k_total = wide_sums.finish()
    lane = lax.broadcasted_iota(jnp.int32, (every - rows, 128), 1)
    m.wide_scales[...] = lax.rsqrt(jnp.where(lane == 0, q_total, k_total) * (1.0 / D) + EPS)
    m.wide_inner[...] = jnp.zeros_like(m.wide_inner)

    def attention_again(k, carry):
        back_length = m.lengths[
            m.order[lax.rem(grid.group - k + groups, groups) * lanes + grid.lane]
        ]
        block = at_rows(spare_rows + (k - 1) * rows, rows)
        inside = at_rows((k - 1) * rows, rows)
        q_scale = m.wide_scales[inside, 0:1]
        k_scale = m.wide_scales[inside, 1:2]
        d_mix[...] = right_inner(m.mid_all[k], m.wo[...]).astype(BF16)
        q_inner = jnp.zeros((rows, 1), F32)
        k_inner = jnp.zeros((rows, 1), F32)

        def head_again(head, carry):
            at = at_rows(head * HEAD, HEAD)
            q_unit = m.wu[block, at_rows(2 * local + head * HEAD, HEAD)].astype(F32) * q_scale
            k_unit = m.wu[block, at_rows(3 * local + head * HEAD, HEAD)].astype(F32) * k_scale
            mix, d_v, d_q_hat, d_k_hat = head_back(
                turn(q_unit * m.q_gain[:, at], m.cosine[...], m.sine[...]).astype(BF16),
                turn(k_unit * m.k_gain[:, at], m.cosine[...], m.sine[...]).astype(BF16),
                m.wu[block, at_rows(local + head * HEAD, HEAD)],
                d_mix[:, at],
                m.cosine[...],
                m.sine[...],
                back_length,
            )
            m.wu[block, at] = mix
            m.wg[block, at_rows(2 * local + head * HEAD, HEAD)] = d_v
            q_scaled = d_q_hat * m.q_gain[:, at]
            k_scaled = d_k_hat * m.k_gain[:, at]
            m.wg[block, at] = q_scaled.astype(BF16)
            m.wg[block, at_rows(local + head * HEAD, HEAD)] = k_scaled.astype(BF16)
            return carry[0] + row_sum(q_scaled * q_unit), carry[1] + row_sum(k_scaled * k_unit)

        q_inner, k_inner = lax.fori_loop(0, local // HEAD, head_again, (q_inner, k_inner))
        lane = lax.broadcasted_iota(jnp.int32, (rows, 128), 1)
        m.wide_inner[inside, :] = jnp.where(lane == 0, q_inner, jnp.where(lane == 1, k_inner, 0.0))
        return carry

    lax.fori_loop(1, groups, attention_again, 0)
    wide_sums = RowSums(
        team, m.wide_mine, m.wide_came.at[1], m.wide_send.at[1], m.wide_recv.at[1]
    )
    wide_sums.start(m.wide_inner[:, 0:1], m.wide_inner[:, 1:2])
    other, this = 1 - grid.lane, grid.lane
    others = pl.ds(spare_rows, every - rows)

    def lane_of(lane):
        return at_rows(grid.group * strip + lane * tile, tile)

    def o_part(lane):
        return left_inner(m.mix[...], m.d_branch[:, lane_of(lane)]) + left_inner(
            m.wu[others, 0:local],
            m.mid_all[1:groups, :, lane_of(lane)].reshape(every - rows, tile),
        )

    def heads_part(lane, at):
        first = at_rows(lane * every, rows)
        rest = pl.ds(pl.multiple_of(lane * every + rows, rows), every - rows)
        return matmul(m.gate[:, first], m.d_heads[:, at]) + matmul(
            m.gate[:, rest], m.wg[others, at]
        )

    last = wires.book(4)
    finals = []
    spare = m.qkv.at[2, pl.ds(3 * tile, local), pl.ds(0, tile)]
    spare[...] = o_part(other).astype(BF16)
    finals.append(wires.copy(spare, m.x_o, crossing, last + 3))
    finals[-1].start()
    q_inner, k_inner = wide_sums.finish()
    lane = lax.broadcasted_iota(jnp.int32, (every - rows, 128), 1)
    m.wide_inner[...] = jnp.where(lane == 0, q_inner, k_inner)

    def close_heads(k, carry):
        block = at_rows(spare_rows + (k - 1) * rows, rows)
        inside = at_rows((k - 1) * rows, rows)
        for i in range(2):
            at = pl.ds(i * local, local)
            scale = m.wide_scales[inside, i : i + 1]
            factor = scale * scale * m.wide_inner[inside, i : i + 1] * (1.0 / D)
            raw = m.wu[block, pl.ds(2 * local + i * local, local)].astype(F32)
            m.wg[block, at] = (scale * m.wg[block, at].astype(F32) - raw * factor).astype(BF16)
        return carry

    lax.fori_loop(1, groups, close_heads, 0)
    for i, target in ((2, m.x_v), (0, m.x_q), (1, m.x_k)):
        spare = m.qkv.at[2, pl.ds(i * tile, tile)]
        spare[...] = heads_part(other, pl.ds(i * local, local)).astype(BF16)
        finals.append(wires.copy(spare, target, crossing, last + i))
        finals[-1].start()
    share()
    turned_own = m.mid_turned.at[at_rows(grid.lane * tile, tile)]
    wide = m.stage.shape[2]
    high = rows

    def narrow_stage(slot):
        return m.stage.at[slot, :, pl.ds(0, tile)]

    def flush(copies, last, i, values):
        @pl.when(i > 0)
        def _():
            for copy in copies(i - 1):
                copy.wait()

        for copy, slot, value in zip(copies(i), last, values, strict=True):
            slot[...] = value
            copy.start()

    def wide_copies(i):
        at = at_rows(i * wide, wide)
        return [put(m.stage.at[0], m.g_own.at[:, at], 2), put(m.stage.at[1], m.u_own.at[:, at], 3)]

    def wide_part(i, carry):
        at = at_rows(i * wide, wide)
        flush(
            wide_copies,
            (m.stage.at[0], m.stage.at[1]),
            i,
            [matmul(turned_own[...], weight[0:every, at]) for weight in (m.wg, m.wu)],
        )
        return carry

    lax.fori_loop(0, hidden // wide, wide_part, 0)
    for copy in wide_copies(hidden // wide - 1):
        copy.wait()

    def high_at(i, slot):
        return at_rows((2 * i + slot) * high, high)

    def high_copies(i):
        return [put(narrow_stage(slot), m.d_own.at[high_at(i, slot), :], 2 + slot) for slot in range(2)]

    def high_part(i, carry):
        right = all_rows(m.dm_all, tile_of(grid.lane))
        flush(
            high_copies,
            (narrow_stage(0), narrow_stage(1)),
            i,
            [matmul(m.wd[high_at(i, slot), 0:every], right) for slot in range(2)],
        )
        return carry

    lax.fori_loop(0, hidden // high // 2, high_part, 0)
    for copy in high_copies(hidden // high // 2 - 1):
        copy.wait()
    for i, target in enumerate((m.q_own, m.k_own, m.v_own)):
        store(heads_part(this, pl.ds(i * local, local)), target)
    output = o_part(this)
    for i in range(local // high):
        store(output[i * high : (i + 1) * high], m.o_own.at[pl.ds(i * high, high), :])
    for copy in puts[-2:]:
        copy.wait()

    def arrived(n, carry):
        for copy in crossings(n):
            copy.wait()
        return carry

    for one in out_gathers:
        one.half()
    for one in out_gathers:
        one.finish()
    for copy in stat_dp:
        copy.wait()
    m.stat_out[...] = sum([m.stat_dp[i] for i in range(1, count)], m.stat_dp[0])
    lax.fori_loop(0, tiles, arrived, 0)
    for copy in finals:
        copy.wait()


def whole_layer(grid, args):
    (hidden_in, upstream, lengths, order, q_weight, k_weight, v_weight, o_weight) = args[:8]
    (q_gain, k_gain, a_gain, g_weight, u_weight, d_weight, m_gain, cosine, sine) = args[8:]
    rows, width = hidden_in.shape
    local, hidden = q_weight.shape[1], g_weight.shape[1]
    count, groups = grid.count, grid.groups
    shard, strip, tile = rows // SLOTS, width // groups, width // count
    every = groups * rows
    deal = Deal(count, shard, width)
    chunk = (deal.rows, deal.columns)
    inputs = [
        ("lengths", SCALAR, lengths),
        ("order", SCALAR, order),
        ("hidden_in", ANY, hidden_in),
        ("upstream", ANY, upstream),
        ("q_weight", ANY, q_weight),
        ("k_weight", ANY, k_weight),
        ("v_weight", ANY, v_weight),
        ("o_weight", ANY, o_weight),
        ("g_weight", ANY, g_weight),
        ("u_weight", ANY, u_weight),
        ("d_weight", ANY, d_weight),
        ("q_gain", ON_CHIP, q_gain),
        ("k_gain", ON_CHIP, k_gain),
        ("a_gain", ON_CHIP, a_gain),
        ("m_gain", ON_CHIP, m_gain),
        ("cosine", ON_CHIP, cosine),
        ("sine", ON_CHIP, sine),
    ]
    outputs = [
        ("layer_out", (rows, width), BF16),
        ("input_grad", (rows, width), BF16),
        ("g_own", (tile, hidden), F32),
        ("u_own", (tile, hidden), F32),
        ("d_own", (hidden, tile), F32),
        ("q_own", (tile, local), F32),
        ("k_own", (tile, local), F32),
        ("v_own", (tile, local), F32),
        ("o_own", (local, tile), F32),
        ("x_gate", (tile, hidden), BF16),
        ("x_up", (tile, hidden), BF16),
        ("x_down", (hidden, tile), BF16),
        ("x_q", (tile, local), BF16),
        ("x_k", (tile, local), BF16),
        ("x_v", (tile, local), BF16),
        ("x_o", (local, tile), BF16),
        ("hid_all", (groups, rows, width), BF16),
        ("branch_all", (groups, rows, width), BF16),
        ("stat_out", (8, PACKED), F32),
    ]
    wires = 160
    scratch = [
        ("qkv", pltpu.VMEM((3, width, local), BF16)),
        ("wo", pltpu.VMEM((local, width), BF16)),
        ("wg", pltpu.VMEM((width, hidden), BF16)),
        ("wu", pltpu.VMEM((width, hidden), BF16)),
        ("wd", pltpu.VMEM((hidden, width), BF16)),
        ("hid", pltpu.VMEM((rows, width), BF16)),
        ("mid_all", pltpu.VMEM((groups, rows, width), BF16)),
        ("dm_all", pltpu.VMEM((groups, rows, width), BF16)),
        ("gate", pltpu.VMEM((rows, hidden), BF16)),
        ("upper", pltpu.VMEM((rows, hidden), BF16)),
        ("inner", pltpu.VMEM((rows, hidden), BF16)),
        ("q_raw", pltpu.VMEM((rows, local), F32)),
        ("k_raw", pltpu.VMEM((rows, local), F32)),
        ("queries", pltpu.VMEM((rows, local), BF16)),
        ("keys", pltpu.VMEM((rows, local), BF16)),
        ("values", pltpu.VMEM((rows, local), BF16)),
        ("scales", pltpu.VMEM((rows, 128), F32)),
        ("mix", pltpu.VMEM((rows, local), BF16)),
        ("d_branch", pltpu.VMEM((rows, width), BF16)),
        ("d_heads", pltpu.VMEM((rows, 3 * local), BF16)),
        ("mid_turned", pltpu.VMEM((strip, every), BF16)),
        ("keep", pltpu.VMEM((3, every - rows, STEP), BF16)),
        ("stage", pltpu.VMEM((2, rows, local), F32)),
        ("branch", pltpu.VMEM((shard, width), F32)),
        ("d_mid", pltpu.VMEM((shard, width), F32)),
        ("layer", pltpu.VMEM((shard, width), BF16)),
        ("closed", pltpu.VMEM((shard, width), BF16)),
        ("grad_in", pltpu.VMEM((shard, width), BF16)),
        ("parked", pltpu.VMEM((count,) + chunk, BF16)),
        ("parked_too", pltpu.VMEM((count,) + chunk, BF16)),
        ("back_leaving", pltpu.VMEM((count, 2) + chunk, BF16)),
        ("fold", pltpu.VMEM((4, 8, width), F32)),
        ("stats", pltpu.VMEM((8, width), F32)),
        ("stat_team", pltpu.VMEM((SLOTS, 8, width), F32)),
        ("pack", pltpu.VMEM((8, PACKED), F32)),
        ("stat_dp", pltpu.VMEM((count, 8, PACKED), F32)),
        ("partial", pltpu.VMEM((rows, width), BF16)),
        ("came", pltpu.VMEM((3, shard, width), BF16)),
        ("gone", pltpu.VMEM((shard, width), BF16)),
        ("total", pltpu.VMEM((shard, width), F32)),
        ("sum_mine", pltpu.VMEM((8, rows), F32)),
        ("sum_came", pltpu.VMEM((3, 8, rows), F32)),
        ("wide_mine", pltpu.VMEM((8, every - rows), F32)),
        ("wide_came", pltpu.VMEM((2, 3, 8, every - rows), F32)),
        ("wide_scales", pltpu.VMEM((every - rows, 128), F32)),
        ("wide_inner", pltpu.VMEM((every - rows, 128), F32)),
        ("wide_send", pltpu.SemaphoreType.DMA((2, 3))),
        ("wide_recv", pltpu.SemaphoreType.DMA((2, 3))),
        ("sum_send", pltpu.SemaphoreType.DMA((3,))),
        ("sum_recv", pltpu.SemaphoreType.DMA((3,))),
        ("reduce_send", pltpu.SemaphoreType.DMA((3, SPLIT))),
        ("reduce_recv", pltpu.SemaphoreType.DMA((3, SPLIT))),
        ("gather_send", pltpu.SemaphoreType.DMA((5, 3))),
        ("gather_recv", pltpu.SemaphoreType.DMA((5, 3))),
        ("wire_send", pltpu.SemaphoreType.DMA((wires,))),
        ("wire_recv", pltpu.SemaphoreType.DMA((wires,))),
        ("load", pltpu.SemaphoreType.DMA((9,))),
        ("put", pltpu.SemaphoreType.DMA((4,))),
        ("late", pltpu.SemaphoreType.DMA((2 * groups,))),
    ]
    names = [entry[0] for entry in inputs + outputs + scratch]
    results = pl.pallas_call(
        functools.partial(layer_kernel, names),
        out_shape=shaped(*[entry[1:] for entry in outputs]),
        in_specs=[entry[1] for entry in inputs],
        out_specs=(ANY,) * (len(outputs) - 1) + (ON_CHIP,),
        scratch_shapes=[entry[1] for entry in scratch],
        compiler_params=pltpu.CompilerParams(
            collective_id=4, has_side_effects=True, vmem_limit_bytes=63 * 2**20
        ),
        name="whole_layer",
    )(*[entry[2] for entry in inputs])
    return dict(zip([entry[0] for entry in outputs], results, strict=True))


def body(
    hidden_in,
    upstream_grad,
    seq_lengths,
    position_order,
    query_weight,
    key_weight,
    value_weight,
    output_weight,
    query_gain,
    key_gain,
    attn_gain,
    gate_weight,
    up_weight,
    down_weight,
    mlp_gain,
):
    count = lax.axis_size("dp")
    ways = lax.axis_size("tensor")
    myself = lax.axis_index("dp")
    part = lax.axis_index("tensor")
    grid = Grid(count)
    index = jnp.arange(count, dtype=jnp.int32)
    inverse = jnp.sum(
        index[None, :] * (position_order[None, :] == index[:, None]).astype(jnp.int32), axis=1
    )
    rows = hidden_in.shape[1]
    width = hidden_in.shape[2]
    shard = rows // ways
    if grid.lanes == 2 and 2 * query_weight.shape[1] + 3 * 128 <= 2 * PACKED and width <= 3 * PACKED and width // count == rows and grid.groups * rows + width // count <= width:
        cosine, sine = rope_constants(rows, HEAD)
        found = whole_layer(
            grid,
            (
                hidden_in[0],
                upstream_grad[0],
                seq_lengths,
                position_order,
                query_weight,
                key_weight,
                value_weight,
                output_weight,
                query_gain[None],
                key_gain[None],
                attn_gain[None],
                gate_weight,
                up_weight,
                down_weight,
                mlp_gain[None],
                cosine,
                sine,
            ),
        )
        local = query_weight.shape[1]

        def joined(own, other):
            return found[own] + found[other].astype(F32)

        stats = found["stat_out"]
        gains = stats[6:8].reshape(-1)
        squares = gains[2 * local : 2 * local + 3 * 128 : 128]
        return (
            found["layer_out"][None],
            found["input_grad"][None],
            joined("q_own", "x_q"),
            joined("k_own", "x_k"),
            joined("v_own", "x_v"),
            joined("o_own", "x_o"),
            gains[:local],
            gains[local : 2 * local],
            stats[3:6].reshape(-1)[:width],
            joined("g_own", "x_gate"),
            joined("u_own", "x_up"),
            joined("d_own", "x_down"),
            stats[0:3].reshape(-1)[:width],
            jnp.sqrt(squares / (jnp.sum(seq_lengths).astype(F32) * D)),
        )

    piece = shard // count
    seq_here = jnp.sum(jnp.where(index == myself, position_order, 0))
    length = jnp.sum(jnp.where(index == seq_here, seq_lengths, 0))[None]
    slot = part % 2 * 2 + part // 2

    def exchange(pieces):
        return lax.all_to_all(pieces, "dp", split_axis=0, concat_axis=0, tiled=True)

    def my_rows(field):
        return lax.dynamic_slice_in_dim(field, slot * shard, shard, axis=0)

    first = exchange(my_rows(upstream_grad[0]).reshape(count, piece, width))
    second = exchange(jnp.take(first, position_order, axis=0))
    grad_in = second.reshape(shard, width)

    rows_low = hidden_in[0]
    my_low = my_rows(rows_low)
    local = query_weight.shape[1]
    strip = width // grid.groups
    tile = width // count

    def strip_of(field, group):
        return lax.dynamic_slice_in_dim(field, group * strip, strip, axis=1)

    def strips(field):
        found = [strip_of(field, grid.group)]
        for step in range(1, grid.groups):
            found.append(
                grid.shift_groups(
                    strip_of(field, (grid.group + step) % grid.groups), step
                )
            )
        return jnp.concatenate(found, axis=0)

    def tile_of(field, lane):
        return lax.dynamic_slice_in_dim(field, lane * tile, tile, axis=1)

    def reduced(product, field):
        sent = []
        for step in range(1, grid.lanes):
            other = product(tile_of(field, (grid.lane + step) % grid.lanes)).astype(BF16)
            sent.append(grid.shift_lanes(other, step))
        mine = product(tile_of(field, grid.lane))
        for other in sent:
            mine = mine + other.astype(F32)
        return mine

    hidden_strips = strips(rows_low)

    cosine, sine = rope_tables(rows, HEAD)
    cosine = jnp.concatenate([cosine, cosine], axis=1)
    sine = jnp.concatenate([-sine, sine], axis=1)
    gains = (query_gain[None], key_gain[None])
    q_raw, k_raw, queries, keys, values, scales, attn_mix, branch, mid_low = attend(
        length,
        rows_low,
        my_low,
        (query_weight, key_weight, value_weight, output_weight),
        gains,
        cosine,
        sine,
        attn_gain[None],
    )
    mix_all = jnp.concatenate([attn_mix] + grid.ring(attn_mix), axis=0)
    mid_others = shared_ring(grid, mid_low)

    gate = matmul(mid_low, gate_weight)
    upper = matmul(mid_low, up_weight)
    sig = jax.nn.sigmoid(gate)
    inner = (gate * sig * upper).astype(BF16)
    layer, d_mlp, mlp_gain_part, squares = settle(
        length,
        matmul(inner, down_weight).astype(BF16),
        my_low,
        branch,
        grad_in,
        attn_gain[None],
        mlp_gain[None],
    )
    d_mlp_others = shared_ring(grid, d_mlp)

    def inner_back(gate, upper, d_mlp):
        d_inner = right_inner(d_mlp, down_weight)
        sig = jax.nn.sigmoid(gate)
        d_gate = (d_inner * upper * sig * (1.0 + gate * (1.0 - sig))).astype(BF16)
        d_up = (d_inner * gate * sig).astype(BF16)
        return d_gate, d_up

    d_gate, d_up = inner_back(gate, upper, d_mlp)
    d_mid, attn_gain_part, d_branch, d_heads, query_gain_part, key_gain_part = unattend(
        length,
        (right_inner(d_gate, gate_weight) + right_inner(d_up, up_weight)).astype(BF16),
        branch,
        grad_in,
        attn_gain[None],
        output_weight,
        (q_raw, k_raw, queries, keys, values, scales),
        gains,
        cosine,
        sine,
    )
    d_branch_strips = strips(d_branch)
    d_heads_all = jnp.concatenate([d_heads] + grid.ring(d_heads), axis=0)
    layer_out, input_grad = close_layer(
        length,
        inverse,
        (
            right_inner(d_heads[:, :local], query_weight)
            + right_inner(d_heads[:, local : 2 * local], key_weight)
            + right_inner(d_heads[:, 2 * local :], value_weight)
        ).astype(BF16),
        d_mid,
        layer,
    )

    gate_o = matmul(mid_others, gate_weight)
    upper_o = matmul(mid_others, up_weight)
    inner_o = (jax.nn.silu(gate_o) * upper_o).astype(BF16)
    d_gate_o, d_up_o = inner_back(gate_o, upper_o, d_mlp_others)

    def strip_all(own, others):
        return jnp.concatenate([strip_of(own, grid.group), strip_of(others, grid.group)], axis=0)

    mid_strips = strip_all(mid_low, mid_others)
    d_mlp_strips = strip_all(d_mlp, d_mlp_others)
    d_gate_all = jnp.concatenate([d_gate, d_gate_o], axis=0)
    d_up_all = jnp.concatenate([d_up, d_up_o], axis=0)
    inner_all = jnp.concatenate([inner, inner_o], axis=0)
    gate_part = reduced(lambda tile: left_inner(tile, d_gate_all), mid_strips)
    up_part = reduced(lambda tile: left_inner(tile, d_up_all), mid_strips)
    down_part = reduced(lambda tile: left_inner(inner_all, tile), d_mlp_strips)
    output_part = reduced(lambda tile: left_inner(mix_all, tile), d_branch_strips)
    heads_part = reduced(lambda tile: left_inner(tile, d_heads_all), hidden_strips)
    query_part = heads_part[:, :local]
    key_part = heads_part[:, local : 2 * local]
    value_part = heads_part[:, 2 * local :]

    shared = jnp.concatenate(
        [jnp.sum(attn_gain_part, axis=0), jnp.sum(mlp_gain_part, axis=0), jnp.sum(squares, axis=(1, 2))]
    )
    shared = shared + sibling(shared)
    shared = shared + across(shared)
    sums = grid.total(jnp.concatenate([shared, query_gain_part[0], key_gain_part[0]]))
    attn_gain_grad = sums[:width]
    mlp_gain_grad = sums[width : 2 * width]
    squares = sums[2 * width : 2 * width + 3]
    query_gain_grad = sums[2 * width + 3 : 2 * width + 3 + local]
    key_gain_grad = sums[2 * width + 3 + local :]
    rms_values = jnp.sqrt(squares / (jnp.sum(seq_lengths).astype(F32) * D))

    return (
        layer_out[None],
        input_grad[None],
        query_part,
        key_part,
        value_part,
        output_part,
        query_gain_grad,
        key_gain_grad,
        attn_gain_grad,
        gate_part,
        up_part,
        down_part,
        mlp_gain_grad,
        rms_values,
    )


def solution(mesh):
    placed = (
        P("dp", None, None),
        P("dp", None, None),
        P(),
        P(),
        P(None, "tensor"),
        P(None, "tensor"),
        P(None, "tensor"),
        P("tensor", None),
        P("tensor"),
        P("tensor"),
        P(),
        P(None, "tensor"),
        P(None, "tensor"),
        P("tensor", None),
        P(),
    )
    return jax.shard_map(
        body,
        mesh=mesh,
        in_specs=placed,
        out_specs=(
            P("dp", None, None),
            P("dp", None, None),
            P("dp", "tensor"),
            P("dp", "tensor"),
            P("dp", "tensor"),
            P("tensor", "dp"),
            P("tensor"),
            P("tensor"),
            P(),
            P("dp", "tensor"),
            P("dp", "tensor"),
            P("tensor", "dp"),
            P(),
            P(),
        ),
        check_vma=False,
    )
```
